32 devices in a mesh: dp: 8 (over z, x), mp: 4 (over y, core).
Axes of the slice: x: 2, y: 2, z: 4, core: 2. Of those that a mesh axis runs over, the one named last changes fastest.
Arguments:
- encoder_in: bfloat16 [7296, 768], P('dp'), may hold values from -6 to 6
- decoder_in: bfloat16 [1024, 768], P('dp'), may hold values from -6 to 6
- decoder_cotangent: float32 [1024, 768], P('dp'), may hold values from -6 to 6
- counts: int32 [8, 2], P('dp'), may hold values from 0 to 4, as said below
- prefix_len: int32 [32], P('dp'), may hold values from 1 to 32
- suffix_len: int32 [32], P('dp'), may hold values from 1 to 32
- project_in: float32 [3, 3, 768, 768], P(None, None, 'dp', 'mp'), may hold values from -0.21875 to 0.21875
- project_in_rows: float32 [3, 3, 768], replicated, may hold values from 6e-10 to 2.4e-09
- project_in_cols: float32 [3, 3, 768], replicated, may hold values from 6e-10 to 2.4e-09
- project_in_moment: float32 [3, 3, 768, 768], P(None, None, 'dp', 'mp'), may hold values from -3 to 3
- project_in_average: float32 [3, 3, 768, 768], P(None, None, 'dp', 'mp'), may hold values from -0.21875 to 0.21875
- project_out: float32 [3, 768, 768], P(None, 'mp', 'dp'), may hold values from -0.625 to 0.625
- project_out_rows: float32 [3, 768], replicated, may hold values from 6e-10 to 2.4e-09
- project_out_cols: float32 [3, 768], replicated, may hold values from 6e-10 to 2.4e-09
- project_out_moment: float32 [3, 768, 768], P(None, 'mp', 'dp'), may hold values from -3 to 3
- project_out_average: float32 [3, 768, 768], P(None, 'mp', 'dp'), may hold values from -0.625 to 0.625
- expand: float32 [2, 768, 3072], P(None, 'dp', 'mp'), may hold values from -0.21875 to 0.21875
- expand_rows: float32 [2, 768], replicated, may hold values from 5e-11 to 2e-10
- expand_cols: float32 [2, 3072], replicated, may hold values from 5e-11 to 2e-10
- expand_moment: float32 [2, 768, 3072], P(None, 'dp', 'mp'), may hold values from -3 to 3
- expand_average: float32 [2, 768, 3072], P(None, 'dp', 'mp'), may hold values from -0.21875 to 0.21875
- contract: float32 [2, 3072, 768], P(None, 'mp', 'dp'), may hold values from -0.109375 to 0.109375
- contract_rows: float32 [2, 3072], replicated, may hold values from 6e-10 to 2.4e-09
- contract_cols: float32 [2, 768], replicated, may hold values from 6e-10 to 2.4e-09
- contract_moment: float32 [2, 3072, 768], P(None, 'mp', 'dp'), may hold values from -3 to 3
- contract_average: float32 [2, 3072, 768], P(None, 'mp', 'dp'), may hold values from -0.109375 to 0.109375
- norm_gains: float32 [5, 768], P(None, 'dp'), may hold values from 0.35 to 1.95
- norm_gains_square: float32 [5, 768], P(None, 'dp'), may hold values from 6e-10 to 2.4e-09
- norm_gains_moment: float32 [5, 768], P(None, 'dp'), may hold values from -3 to 3
- norm_gains_average: float32 [5, 768], P(None, 'dp'), may hold values from 0.5 to 1.5
Outputs:
- decoder_out: float32 [1024, 768], P('dp')
- encoder_in_grad: float32 [7296, 768], P('dp')
- decoder_in_grad: float32 [1024, 768], P('dp')
- grad_norm: float32 [], replicated
- project_in_grad: float32 [3, 3, 768, 768], P(None, None, 'dp', 'mp')
- project_in_rows_new: float32 [3, 3, 768], replicated
- project_in_cols_new: float32 [3, 3, 768], replicated
- project_in_moment_new: float32 [3, 3, 768, 768], P(None, None, 'dp', 'mp')
- project_in_new: float32 [3, 3, 768, 768], P(None, None, 'dp', 'mp')
- project_in_average_new: float32 [3, 3, 768, 768], P(None, None, 'dp', 'mp')
- project_in_low: bfloat16 [3, 3, 768, 768], P(None, None, 'dp', 'mp')
- project_out_grad: float32 [3, 768, 768], P(None, 'mp', 'dp')
- project_out_rows_new: float32 [3, 768], replicated
- project_out_cols_new: float32 [3, 768], replicated
- project_out_moment_new: float32 [3, 768, 768], P(None, 'mp', 'dp')
- project_out_new: float32 [3, 768, 768], P(None, 'mp', 'dp')
- project_out_average_new: float32 [3, 768, 768], P(None, 'mp', 'dp')
- project_out_low: bfloat16 [3, 768, 768], P(None, 'mp', 'dp')
- expand_grad: float32 [2, 768, 3072], P(None, 'dp', 'mp')
- expand_rows_new: float32 [2, 768], replicated
- expand_cols_new: float32 [2, 3072], replicated
- expand_moment_new: float32 [2, 768, 3072], P(None, 'dp', 'mp')
- expand_new: float32 [2, 768, 3072], P(None, 'dp', 'mp')
- expand_average_new: float32 [2, 768, 3072], P(None, 'dp', 'mp')
- expand_low: bfloat16 [2, 768, 3072], P(None, 'dp', 'mp')
- contract_grad: float32 [2, 3072, 768], P(None, 'mp', 'dp')
- contract_rows_new: float32 [2, 3072], replicated
- contract_cols_new: float32 [2, 768], replicated
- contract_moment_new: float32 [2, 3072, 768], P(None, 'mp', 'dp')
- contract_new: float32 [2, 3072, 768], P(None, 'mp', 'dp')
- contract_average_new: float32 [2, 3072, 768], P(None, 'mp', 'dp')
- contract_low: bfloat16 [2, 3072, 768], P(None, 'mp', 'dp')
- norm_gains_grad: float32 [5, 768], P(None, 'dp')
- norm_gains_square_new: float32 [5, 768], P(None, 'dp')
- norm_gains_moment_new: float32 [5, 768], P(None, 'dp')
- norm_gains_new: float32 [5, 768], P(None, 'dp')
- norm_gains_average_new: float32 [5, 768], P(None, 'dp')
- norm_gains_low: bfloat16 [5, 768], P(None, 'dp')
The draws below stay inside these ranges and needn't reach their ends.
Inputs may be any that keep to these rules, and one draw needn't show every extreme that they name: Per group the image-text pairs take the first slots and the text-only pairs the next ones; the two counts of a group sum to at least half of 4, to at most 4, and to exactly 4 in at least one group.
All inputs are finite; a program needn't handle non-finite values.
Results may differ from the reference program's by a relative error of at most 0.0233.
Values may be sent and summed in bfloat16 or wider, within the bound.
No kernel may reach another device: no remote copies, remote signals or barrier semaphores. Data moves between devices by JAX's collectives and lax.ppermute only.
A program may use at most 128 MiB of HBM per device.

```python
import math
import jax
import jax.numpy as jnp
from jax import lax

D = 768
N_HEADS = 12
HEAD_DIM = 64
FF = 3072
PATCHES = 196
PREFIX = 32
SUFFIX = 32
PAIRS_DEV = 4
ENC_LEN = 228
GROUPS = 8
PAIRS = 32


def draw_counts(key, part):
    first, second, third = jax.random.split(jax.random.fold_in(key, 11), 3)
    lowest = (PAIRS_DEV + 1) // 2
    totals = jax.random.randint(first, (GROUPS,), lowest, PAIRS_DEV + 1)
    fullest = jax.random.randint(second, (), 0, GROUPS)
    totals = jnp.where(jnp.arange(GROUPS) == fullest, PAIRS_DEV, totals)
    images = jax.random.randint(third, (GROUPS,), 0, 1 << 20) % (totals + 1)
    return jnp.stack([images, totals - images], 1).astype(jnp.int32)


def draw_norm_gains(key, part):
    inner = jax.random.fold_in(key, 23)
    place = jnp.arange(D).astype(jnp.float32) / jnp.float32(D - 1)
    ramp = 0.5 + place
    noise = 1.0 + 0.1 * jnp.clip(jax.random.normal(inner, (5, D), jnp.float32), -3.0, 3.0)
    return (ramp[None, :] * noise).astype(jnp.float32)


def touch_ends(array, own_key, least, top_value):
    longest = array.shape.index(max(array.shape))
    spots = []
    for shift in (0, 1):
        where = [jax.random.randint(jax.random.fold_in(own_key, axis), (), 0, length) for axis, length in enumerate(array.shape)]
        where[longest] = (where[longest] + shift) % array.shape[longest]
        spots.append(tuple(where))
    return array.at[spots[0]].set(least).at[spots[1]].set(top_value)


def block_scale(rng, dims, pieces, least, top_value):
    def one(position, parts):
        draws = jax.random.uniform(jax.random.fold_in(jax.random.fold_in(rng, 6), position), (parts,), jnp.float32, least / len(pieces), top_value / len(pieces))
        return jnp.repeat(jnp.exp(draws), dims[position] // parts).reshape((-1,) + (1,) * (len(dims) - position - 1))

    factor_of = one(*pieces[0])
    for cut in pieces[1:]:
        factor_of = factor_of * one(*cut)
    return factor_of


def gaussian(rng, dims, width, limit, pieces=(), kind=jnp.bfloat16):
    result = jax.random.normal(rng, dims, jnp.float32) * width
    if len(pieces) > 0:
        result = block_scale(rng, dims, pieces, -0.22, 0.18) * result
    return jnp.clip(result, min=-limit, max=limit).astype(kind)


def setup_inputs(seed: int = 0) -> dict:
    arg_keys = jax.random.split(jax.random.key(seed), 31)
    return {
        "encoder_in": gaussian(arg_keys[0], (PAIRS * ENC_LEN, D), 1.0, 6.0, ((0, 8),)),
        "decoder_in": gaussian(arg_keys[1], (PAIRS * SUFFIX, D), 1.0, 6.0, ((0, 8),)),
        "decoder_cotangent": gaussian(arg_keys[2], (PAIRS * SUFFIX, D), 1.0, 6.0, ((0, 8),), jnp.float32),
        "counts": draw_counts(jax.random.fold_in(arg_keys[30], 71), 0),
        "prefix_len": touch_ends(jax.random.randint(arg_keys[4], (PAIRS,), 1, PREFIX + 1), jax.random.fold_in(arg_keys[4], 1), 1, PREFIX).astype(jnp.int32),
        "suffix_len": touch_ends(jax.random.randint(arg_keys[5], (PAIRS,), 1, SUFFIX + 1), jax.random.fold_in(arg_keys[5], 1), 1, SUFFIX).astype(jnp.int32),
        "project_in": gaussian(arg_keys[6], (3, 3, D, D), D ** -0.5, 0.21875, ((2, 8), (3, 4)), jnp.float32),
        "project_in_rows": jnp.clip(jnp.exp(jax.random.uniform(arg_keys[7], (3, 3, D), jnp.float32, math.log(5.999999941330714e-10), math.log(2.3999999765322855e-09))), 5.999999941330714e-10, 2.3999999765322855e-09),
        "project_in_cols": jnp.clip(jnp.exp(jax.random.uniform(arg_keys[8], (3, 3, D), jnp.float32, math.log(5.999999941330714e-10), math.log(2.3999999765322855e-09))), 5.999999941330714e-10, 2.3999999765322855e-09),
        "project_in_moment": gaussian(arg_keys[9], (3, 3, D, D), 0.5, 3.0, ((2, 8), (3, 4)), jnp.float32),
        "project_in_average": gaussian(arg_keys[10], (3, 3, D, D), D ** -0.5, 0.21875, ((2, 8), (3, 4)), jnp.float32),
        "project_out": gaussian(arg_keys[11], (3, D, D), (D // 8) ** -0.5, 0.625, ((1, 4), (2, 8)), jnp.float32),
        "project_out_rows": jnp.clip(jnp.exp(jax.random.uniform(arg_keys[12], (3, D), jnp.float32, math.log(5.999999941330714e-10), math.log(2.3999999765322855e-09))), 5.999999941330714e-10, 2.3999999765322855e-09),
        "project_out_cols": jnp.clip(jnp.exp(jax.random.uniform(arg_keys[13], (3, D), jnp.float32, math.log(5.999999941330714e-10), math.log(2.3999999765322855e-09))), 5.999999941330714e-10, 2.3999999765322855e-09),
        "project_out_moment": gaussian(arg_keys[14], (3, D, D), 0.5, 3.0, ((1, 4), (2, 8)), jnp.float32),
        "project_out_average": gaussian(arg_keys[15], (3, D, D), (D // 8) ** -0.5, 0.625, ((1, 4), (2, 8)), jnp.float32),
        "expand": gaussian(arg_keys[16], (2, D, FF), D ** -0.5, 0.21875, ((1, 8), (2, 4)), jnp.float32),
        "expand_rows": jnp.clip(jnp.exp(jax.random.uniform(arg_keys[17], (2, D), jnp.float32, math.log(5.00000006675716e-11), math.log(2.000000026702864e-10))), 5.00000006675716e-11, 2.000000026702864e-10),
        "expand_cols": jnp.clip(jnp.exp(jax.random.uniform(arg_keys[18], (2, FF), jnp.float32, math.log(5.00000006675716e-11), math.log(2.000000026702864e-10))), 5.00000006675716e-11, 2.000000026702864e-10),
        "expand_moment": gaussian(arg_keys[19], (2, D, FF), 0.5, 3.0, ((1, 8), (2, 4)), jnp.float32),
        "expand_average": gaussian(arg_keys[20], (2, D, FF), D ** -0.5, 0.21875, ((1, 8), (2, 4)), jnp.float32),
        "contract": gaussian(arg_keys[21], (2, FF, D), FF ** -0.5, 0.109375, ((1, 4), (2, 8)), jnp.float32),
        "contract_rows": jnp.clip(jnp.exp(jax.random.uniform(arg_keys[22], (2, FF), jnp.float32, math.log(5.999999941330714e-10), math.log(2.3999999765322855e-09))), 5.999999941330714e-10, 2.3999999765322855e-09),
        "contract_cols": jnp.clip(jnp.exp(jax.random.uniform(arg_keys[23], (2, D), jnp.float32, math.log(5.999999941330714e-10), math.log(2.3999999765322855e-09))), 5.999999941330714e-10, 2.3999999765322855e-09),
        "contract_moment": gaussian(arg_keys[24], (2, FF, D), 0.5, 3.0, ((1, 4), (2, 8)), jnp.float32),
        "contract_average": gaussian(arg_keys[25], (2, FF, D), FF ** -0.5, 0.109375, ((1, 4), (2, 8)), jnp.float32),
        "norm_gains": draw_norm_gains(jax.random.fold_in(arg_keys[30], 71), 0),
        "norm_gains_square": jnp.clip(jnp.exp(math.log(2.3999999765322855e-09) - 1.3862944 * jax.random.uniform(arg_keys[27], (5, D), jnp.float32) ** block_scale(arg_keys[27], (5, D), ((1, 8),), -0.2, 0.2)), 5.999999941330714e-10, 2.3999999765322855e-09),
        "norm_gains_moment": gaussian(arg_keys[28], (5, D), 0.5, 3.0, ((1, 8),), jnp.float32),
        "norm_gains_average": jnp.clip(1.0 + 0.1 * jax.random.normal(arg_keys[29], (5, D), jnp.float32), 0.5, 1.5),
    }


EPS_NORM = 1e-06
EPS_STAT = 1e-30
DECAY = 0.99
MOMENTUM = 0.9
AVERAGE = 0.6
RATE_MATRIX = 0.004
RATE_GAIN = 0.05
MASKED = -1000000000.0

@jax.custom_vjp
def low(v):
    return lax.optimization_barrier(v.astype(jnp.bfloat16)).astype(jnp.float32)

@jax.custom_vjp
def low_back(v):
    return v

def low_keep(v):
    return (low(v), None)

def low_pass(kept, grad):
    return (grad,)

def back_keep(v):
    return (v, None)

def back_low(kept, grad):
    return (low(grad),)
low.defvjp(low_keep, low_pass)
low_back.defvjp(back_keep, back_low)

def matmul(left, right):
    return jnp.dot(left, right, precision=lax.Precision.HIGHEST)

def rmsnorm(inputs, gain):
    return inputs * lax.rsqrt(lax.optimization_barrier(jnp.mean(inputs * inputs, -1, keepdims=True)) + EPS_NORM) * gain

def rounded(value):
    return low_back(low(value))

def attention(query_in, key_in, weights_in, weight_out, allowed, query_len, key_len):
    queries = rounded(matmul(query_in, weights_in[0])).reshape(PAIRS_DEV, query_len, N_HEADS, HEAD_DIM)
    keys_all = rounded(matmul(key_in, weights_in[1])).reshape(PAIRS_DEV, key_len, N_HEADS, HEAD_DIM)
    values_all = rounded(matmul(key_in, weights_in[2])).reshape(PAIRS_DEV, key_len, N_HEADS, HEAD_DIM)
    scores = jnp.einsum('pqhd,pkhd->phqk', queries, keys_all, precision=lax.Precision.HIGHEST) * HEAD_DIM ** (-0.5)
    scores = low_back(jnp.where(allowed, scores, MASKED))
    probs = low(jax.nn.softmax(scores, -1))
    mixed = jnp.einsum('phqk,pkhd->pqhd', probs, values_all, precision=lax.Precision.HIGHEST)
    mixed = rounded(mixed.reshape(PAIRS_DEV * query_len, D))
    return low_back(matmul(mixed, weight_out))

def feedforward(inputs, gain, weight_up, weight_down):
    hidden_in = low(rmsnorm(inputs, gain))
    upper = low_back(matmul(hidden_in, weight_up))
    active = low(jax.nn.gelu(upper, approximate=True))
    return low_back(matmul(active, weight_down))

def build_masks(count_row, prefix_row, suffix_row):
    slots = jnp.arange(PAIRS_DEV)
    images = slots < count_row[0]
    active = slots < count_row[0] + count_row[1]
    place = jnp.arange(ENC_LEN)
    key_ok = jnp.where(place[None, :] < PATCHES, images[:, None], place[None, :] - PATCHES < prefix_row[:, None])
    steps = jnp.arange(SUFFIX)
    causal = (steps[None, None, :] <= steps[None, :, None]) & (steps[None, None, :] < suffix_row[:, None, None])
    live = active[:, None] & (steps[None, :] < suffix_row[:, None])
    return (key_ok[:, None, None, :], causal[:, None], live.reshape(-1))

def forward(params, enc_x, dec_x, key_ok, causal):
    proj_in, proj_out, expand_w, contract_w, gains = params
    normed = low(rmsnorm(enc_x, gains[0]))
    enc_mid = enc_x + attention(normed, normed, proj_in[0], proj_out[0], key_ok, ENC_LEN, ENC_LEN)
    enc_end = enc_mid + feedforward(enc_mid, gains[1], expand_w[0], contract_w[0])
    memory = low(enc_end)
    normed = low(rmsnorm(dec_x, gains[2]))
    dec_one = dec_x + attention(normed, normed, proj_in[1], proj_out[1], causal, SUFFIX, SUFFIX)
    query_in = low(rmsnorm(dec_one, gains[3]))
    dec_two = dec_one + attention(query_in, memory, proj_in[2], proj_out[2], key_ok, SUFFIX, ENC_LEN)
    return dec_two + feedforward(dec_two, gains[4], expand_w[1], contract_w[1])

def update_matrix(gradient, weight, rows_old, cols_old, moment, average):
    square = gradient * gradient
    rows_new = DECAY * rows_old + (1.0 - DECAY) * (lax.optimization_barrier(jnp.mean(square, -1)) + EPS_STAT)
    cols_new = DECAY * cols_old + (1.0 - DECAY) * (lax.optimization_barrier(jnp.mean(square, -2)) + EPS_STAT)
    second = rows_new[..., :, None] * cols_new[..., None, :] / lax.optimization_barrier(jnp.mean(rows_new, -1))[..., None, None]
    stepped = gradient * lax.rsqrt(second)
    moment_new = MOMENTUM * moment + stepped
    weight_new = weight - RATE_MATRIX * (MOMENTUM * moment_new + stepped)
    average_new = AVERAGE * average + (1.0 - AVERAGE) * weight_new
    return (gradient, rows_new, cols_new, moment_new, weight_new, average_new, weight_new.astype(jnp.bfloat16))

def update_gains(gradient, weight, square_old, moment, average):
    square_new = DECAY * square_old + (1.0 - DECAY) * (gradient * gradient + EPS_STAT)
    stepped = gradient * lax.rsqrt(square_new)
    moment_new = MOMENTUM * moment + stepped
    weight_new = weight - RATE_GAIN * (MOMENTUM * moment_new + stepped)
    average_new = AVERAGE * average + (1.0 - AVERAGE) * weight_new
    return (gradient, square_new, moment_new, weight_new, average_new, weight_new.astype(jnp.bfloat16))

def reference(encoder_in, decoder_in, decoder_cotangent, counts, prefix_len, suffix_len, project_in, project_in_rows, project_in_cols, project_in_moment, project_in_average, project_out, project_out_rows, project_out_cols, project_out_moment, project_out_average, expand, expand_rows, expand_cols, expand_moment, expand_average, contract, contract_rows, contract_cols, contract_moment, contract_average, norm_gains, norm_gains_square, norm_gains_moment, norm_gains_average):
    masters = (project_in, project_out, expand, contract, norm_gains)
    params = tuple((item.astype(jnp.bfloat16).astype(jnp.float32) for item in masters))
    enc_rows = PAIRS_DEV * ENC_LEN
    dec_rows = PAIRS_DEV * SUFFIX
    inputs = (encoder_in.astype(jnp.float32).reshape(GROUPS, enc_rows, D), decoder_in.astype(jnp.float32).reshape(GROUPS, dec_rows, D), decoder_cotangent.reshape(GROUPS, dec_rows, D), counts, prefix_len.reshape(GROUPS, PAIRS_DEV), suffix_len.reshape(GROUPS, PAIRS_DEV))

    def one_group(totals, group):
        enc_x, dec_x, cotangent, count_row, prefix_row, suffix_row = group
        key_ok, causal, live = build_masks(count_row, prefix_row, suffix_row)

        def run(weights, enc_value, dec_value):
            return forward(weights, enc_value, dec_value, key_ok, causal)
        output, pullback = jax.vjp(run, params, enc_x, dec_x)
        weight_grads, enc_grad, dec_grad = pullback(jnp.where(live[:, None], cotangent, jnp.float32(0.0)))
        totals = tuple((a + b for a, b in zip(totals, weight_grads)))
        return (totals, (output, enc_grad, dec_grad))
    start = tuple((jnp.zeros_like(item) for item in params))
    totals, (outputs, enc_grads, dec_grads) = lax.scan(one_group, start, inputs)
    square = sum((jnp.sum(item * item) for item in totals))
    grad_norm = jnp.sqrt(square)
    factor = jnp.minimum(1.0, 1.0 / grad_norm)
    clipped = tuple((item * factor for item in totals))
    pin = update_matrix(clipped[0], project_in, project_in_rows, project_in_cols, project_in_moment, project_in_average)
    pout = update_matrix(clipped[1], project_out, project_out_rows, project_out_cols, project_out_moment, project_out_average)
    pexp = update_matrix(clipped[2], expand, expand_rows, expand_cols, expand_moment, expand_average)
    pcon = update_matrix(clipped[3], contract, contract_rows, contract_cols, contract_moment, contract_average)
    pgain = update_gains(clipped[4], norm_gains, norm_gains_square, norm_gains_moment, norm_gains_average)
    decoder_out = outputs.reshape(PAIRS * SUFFIX, D)
    encoder_in_grad = enc_grads.reshape(PAIRS * ENC_LEN, D)
    decoder_in_grad = dec_grads.reshape(PAIRS * SUFFIX, D)
    return (decoder_out, encoder_in_grad, decoder_in_grad, grad_norm, pin[0], pin[1], pin[2], pin[3], pin[4], pin[5], pin[6], pout[0], pout[1], pout[2], pout[3], pout[4], pout[5], pout[6], pexp[0], pexp[1], pexp[2], pexp[3], pexp[4], pexp[5], pexp[6], pcon[0], pcon[1], pcon[2], pcon[3], pcon[4], pcon[5], pcon[6], pgain[0], pgain[1], pgain[2], pgain[3], pgain[4], pgain[5])
```

```python
import functools

import jax
import jax.numpy as jnp
from jax import lax
from jax.sharding import PartitionSpec as P

D = 768
HEAD_DIM = 64
FF = 3072
PATCHES = 196
SUFFIX = 32
ENC_LEN = 228


EPS_NORM = 1e-06
EPS_STAT = 1e-30
DECAY = 0.99
MOMENTUM = 0.9
AVERAGE = 0.6
RATE_MATRIX = 0.004
RATE_GAIN = 0.05
MASKED = -1000000000.0


def rmsnorm(inputs, gain):
    return inputs * lax.rsqrt(jnp.mean(inputs * inputs, -1, keepdims=True) + EPS_NORM) * gain


def gelu_tanh(values):
    return jax.nn.gelu(values, approximate=True)


def attend(queries, keys_all, values_all, allowed):
    scores = jnp.einsum(
        "pqhd,pkhd->phqk", queries, keys_all, preferred_element_type=jnp.float32
    ) * HEAD_DIM ** (-0.5)
    scores = jnp.where(allowed, scores, MASKED)
    highest = jnp.max(scores, -1, keepdims=True)
    expons = jnp.exp(scores - highest)
    totals = jnp.sum(expons, -1, keepdims=True)
    probs = (expons / totals).astype(jnp.bfloat16)
    mixed = jnp.einsum(
        "phqk,pkhd->pqhd", probs, values_all, preferred_element_type=jnp.float32
    ).astype(jnp.bfloat16)
    return (mixed, highest + jnp.log(totals))


def attend_back(queries, keys_all, values_all, allowed, logsum, grad_mixed):
    scale = HEAD_DIM ** (-0.5)
    scores = (
        jnp.einsum("pqhd,pkhd->phqk", queries, keys_all, preferred_element_type=jnp.float32) * scale
    )
    scores = jnp.where(allowed, scores, MASKED)
    probs = jnp.exp(scores - logsum)
    grad_probs = jnp.einsum(
        "pqhd,pkhd->phqk", grad_mixed, values_all, preferred_element_type=jnp.float32
    )
    grad_scores = (probs * (grad_probs - jnp.sum(grad_probs * probs, -1, keepdims=True))).astype(
        jnp.bfloat16
    )
    grad_query = (
        jnp.einsum("phqk,pkhd->pqhd", grad_scores, keys_all, preferred_element_type=jnp.float32)
        * scale
    ).astype(jnp.bfloat16)
    grad_key = (
        jnp.einsum("phqk,pqhd->pkhd", grad_scores, queries, preferred_element_type=jnp.float32)
        * scale
    ).astype(jnp.bfloat16)
    grad_value = jnp.einsum(
        "phqk,pqhd->pkhd",
        probs.astype(jnp.bfloat16),
        grad_mixed,
        preferred_element_type=jnp.float32,
    ).astype(jnp.bfloat16)
    return (grad_query, grad_key, grad_value)


def update_matrix(
    gradient, weight, rows_old, cols_old, moment, average, row_sum, col_sum, row_index, col_index
):
    full_rows = rows_old.shape[-1]
    full_cols = cols_old.shape[-1]
    rows_new = DECAY * rows_old + (1.0 - DECAY) * (row_sum / full_cols + EPS_STAT)
    cols_new = DECAY * cols_old + (1.0 - DECAY) * (col_sum / full_rows + EPS_STAT)
    row_local = lax.dynamic_slice_in_dim(
        rows_new, row_index * gradient.shape[-2], gradient.shape[-2], rows_new.ndim - 1
    )
    col_local = lax.dynamic_slice_in_dim(
        cols_new, col_index * gradient.shape[-1], gradient.shape[-1], cols_new.ndim - 1
    )
    second = (
        row_local[..., :, None] * col_local[..., None, :] / jnp.mean(rows_new, -1)[..., None, None]
    )
    stepped = gradient * lax.rsqrt(second)
    moment_new = MOMENTUM * moment + stepped
    weight_new = weight - RATE_MATRIX * (MOMENTUM * moment_new + stepped)
    average_new = AVERAGE * average + (1.0 - AVERAGE) * weight_new
    return (
        gradient,
        rows_new,
        cols_new,
        moment_new,
        weight_new,
        average_new,
        weight_new.astype(jnp.bfloat16),
    )


def on_device(
    sizes,
    encoder_in,
    decoder_in,
    decoder_cotangent,
    counts,
    prefix_len,
    suffix_len,
    project_in,
    project_in_rows,
    project_in_cols,
    project_in_moment,
    project_in_average,
    project_out,
    project_out_rows,
    project_out_cols,
    project_out_moment,
    project_out_average,
    expand,
    expand_rows,
    expand_cols,
    expand_moment,
    expand_average,
    contract,
    contract_rows,
    contract_cols,
    contract_moment,
    contract_average,
    norm_gains,
    norm_gains_square,
    norm_gains_moment,
    norm_gains_average,
):

    dp_n, mp_n = sizes
    dp_index = lax.axis_index("dp")
    mp_index = lax.axis_index("mp")
    side = mp_index % 2
    pairs = prefix_len.shape[0]
    half = pairs // 2
    width = project_in.shape[-1]
    heads = width // HEAD_DIM
    hidden = expand.shape[-1]
    block = project_in.shape[-2]
    low = jnp.bfloat16
    f32 = jnp.float32

    def swap(value, axis, bit):
        count = dp_n if axis == "dp" else mp_n
        return lax.ppermute(value, axis, [(i, i ^ bit) for i in range(count)])

    def bits(count):
        return [1 << i for i in range(count.bit_length() - 1)]

    def gather(own):
        if dp_n > 8:
            return lax.all_gather(own, "dp", axis=1, tiled=True)
        rel = {0: own}
        for bit in reversed(bits(dp_n)):
            rel.update({place ^ bit: swap(piece, "dp", bit) for place, piece in list(rel.items())})
        full = jnp.zeros((own.shape[0], dp_n) + own.shape[1:], own.dtype)
        for place, piece in rel.items():
            full = lax.dynamic_update_slice(
                full, piece[:, None], (0, jnp.bitwise_xor(dp_index, place), 0, 0)
            )
        return full.reshape(own.shape[0], dp_n * own.shape[1], own.shape[2])

    def scatter(full):
        if dp_n > 8:
            return lax.psum_scatter(full, "dp", scatter_dimension=1, tiled=True)
        count = full.shape[0]
        keep = full
        for bit in bits(dp_n):
            mine = (dp_index // bit) % 2
            split = keep.reshape(count, -1, 2, block, full.shape[2])
            away = lax.dynamic_index_in_dim(split, 1 - mine, 2, False).astype(low)
            keep = lax.dynamic_index_in_dim(split, mine, 2, False) + swap(away, "dp", bit).astype(f32)
        return keep.reshape(count, block, full.shape[2])

    def total_dp(value):
        for bit in bits(dp_n):
            value = value + swap(value, "dp", bit)
        return value

    def reduce_own(partial):
        away = partial[half:].astype(low)
        mine = partial[:half] + swap(away, "mp", 1).astype(f32)
        for bit in bits(mp_n)[1:]:
            sent = mine.astype(low)
            mine = sent.astype(f32) + swap(sent, "mp", bit).astype(f32)
        return mine

    def both(own):
        return jnp.concatenate([own, swap(own, "mp", 1)], 0)

    def relative(value):
        split = value.reshape((half, 2) + value.shape[1:])
        return jnp.concatenate(
            [
                lax.dynamic_index_in_dim(split, side, 1, False),
                lax.dynamic_index_in_dim(split, 1 - side, 1, False),
            ],
            0,
        )

    def absolute(own):
        other = swap(own, "mp", 1)
        even = jnp.where(side == 0, own, other)
        odd = jnp.where(side == 0, other, own)
        return jnp.stack([even, odd], 1).reshape((pairs,) + own.shape[1:])

    gain_low = norm_gains.astype(low)
    gain_full = lax.dynamic_update_slice(
        jnp.zeros((5, D), low), gain_low, (0, dp_index * block)
    )
    gain_rows = total_dp(gain_full).astype(f32)

    def attention_block(layer):
        return jnp.concatenate(
            [project_in[layer, 0], project_in[layer, 1], project_in[layer, 2], project_out[layer].T], 1
        ).astype(low)[None]

    def feed_block(layer):
        return jnp.stack([expand[layer], contract[layer].T]).astype(low)

    own_blocks = [
        attention_block(0), feed_block(0), attention_block(1), attention_block(2), feed_block(1)
    ]
    enc_att, enc_feed, self_att, cross_att, dec_feed = [gather(item) for item in own_blocks]
    enc_att, self_att, cross_att = enc_att[0], self_att[0], cross_att[0]

    position = jnp.arange(pairs)
    own_place = 2 * jnp.arange(half) + side
    place_rel = jnp.concatenate([own_place, 2 * jnp.arange(half) + 1 - side])
    prefix_rel = relative(prefix_len)
    suffix_rel = relative(suffix_len)
    images = place_rel < counts[0, 0]
    active = place_rel < counts[0, 0] + counts[0, 1]
    place = jnp.arange(ENC_LEN)
    key_ok = jnp.where(
        place[None, :] < PATCHES, images[:, None], place[None, :] - PATCHES < prefix_rel[:, None]
    )[:, None, None, :]
    steps = jnp.arange(SUFFIX)
    causal = (
        (steps[None, None, :] <= steps[None, :, None])
        & (steps[None, None, :] < suffix_rel[:, None, None])
    )[:, None]
    live = active[:, None] & (steps[None, :] < suffix_rel[:, None])

    def mm(left, right):
        return jnp.einsum("ptd,dm->ptm", left, right, preferred_element_type=f32)

    def mm_t(left, right):
        return jnp.einsum("ptm,dm->ptd", left, right, preferred_element_type=f32)

    def outer(left, right):
        return jnp.einsum("ptd,ptm->dm", left, right, preferred_element_type=f32)

    def split_heads(flat):
        return flat.reshape(flat.shape[:2] + (heads, HEAD_DIM))

    def attn_forward(query_in, key_in, weight, allowed):
        queries = mm(query_in, weight[:, :width]).astype(low)
        keys_all = mm(key_in, weight[:, width : 2 * width]).astype(low)
        values_all = mm(key_in, weight[:, 2 * width : 3 * width]).astype(low)
        mixed, logsum = attend(
            split_heads(queries), split_heads(keys_all), split_heads(values_all), allowed
        )
        flat = mixed.reshape(queries.shape)
        partial = mm_t(flat, weight[:, 3 * width :])
        return partial, (queries, keys_all, values_all, flat, logsum)

    def attn_backward(query_in, key_in, weight, allowed, stored, grad_low):
        queries, keys_all, values_all, flat, logsum = stored
        grad_out = outer(grad_low, flat)
        grad_mixed = mm(grad_low, weight[:, 3 * width :]).astype(low)
        grad_query, grad_key, grad_value = attend_back(
            split_heads(queries),
            split_heads(keys_all),
            split_heads(values_all),
            allowed,
            logsum,
            split_heads(grad_mixed),
        )
        grad_query = grad_query.reshape(queries.shape)
        grad_key = grad_key.reshape(keys_all.shape)
        grad_value = grad_value.reshape(keys_all.shape)
        grads = jnp.concatenate(
            [outer(query_in, grad_query), outer(key_in, grad_key), outer(key_in, grad_value), grad_out], 1
        )
        back_query = mm_t(grad_query, weight[:, :width])
        back_key = mm_t(grad_key, weight[:, width : 2 * width]) + mm_t(
            grad_value, weight[:, 2 * width : 3 * width]
        )
        return grads[None], back_query, back_key

    def feed_forward(normed_low, weight):
        upper = mm(normed_low, weight[0])
        active_low = gelu_tanh(upper).astype(low)
        return mm_t(active_low, weight[1]), (upper, active_low)

    def feed_backward(normed_low, weight, stored, grad_low):
        upper, active_low = stored
        grad_down = outer(grad_low, active_low)
        grad_active = mm(grad_low, weight[1])
        pull = jax.vjp(gelu_tanh, upper)[1]
        grad_upper = pull(grad_active)[0].astype(low)
        grad_up = outer(normed_low, grad_upper)
        back = mm_t(grad_upper, weight[0])
        return jnp.stack([grad_up, grad_down]), back

    enc_rel = relative(encoder_in.reshape(pairs, ENC_LEN, D))
    dec_rel = relative(decoder_in.reshape(pairs, SUFFIX, D))
    cot_rel = relative(decoder_cotangent.reshape(pairs, SUFFIX, D))
    enc_x = enc_rel.astype(f32)
    dec_x = dec_rel.astype(f32)

    norm_enc = rmsnorm(enc_x, gain_rows[0]).astype(low)
    partial, kept_enc = attn_forward(norm_enc, norm_enc, enc_att, key_ok)
    norm_self = rmsnorm(dec_x, gain_rows[2]).astype(low)
    enc_mid = enc_x[:half] + reduce_own(partial)
    partial, kept_self = attn_forward(norm_self, norm_self, self_att, causal)
    dec_one = dec_x[:half] + reduce_own(partial)
    norm_mid = both(rmsnorm(enc_mid, gain_rows[1]).astype(low))
    partial, kept_feed = feed_forward(norm_mid, enc_feed)
    memory = both((enc_mid + reduce_own(partial)).astype(low))
    norm_cross = both(rmsnorm(dec_one, gain_rows[3]).astype(low))
    partial, kept_cross = attn_forward(norm_cross, memory, cross_att, key_ok)
    dec_two = dec_one + reduce_own(partial)
    norm_last = both(rmsnorm(dec_two, gain_rows[4]).astype(low))
    partial, kept_last = feed_forward(norm_last, dec_feed)
    out_own = dec_two + reduce_own(partial)
    decoder_out = absolute(out_own).reshape(pairs * SUFFIX, D)

    cot = jnp.where(live[:, :, None], cot_rel, f32(0.0))
    grads_dec, back = feed_backward(norm_last, dec_feed, kept_last, cot.astype(low))
    sum_dec = scatter(grads_dec)
    pull = jax.vjp(rmsnorm, dec_two, gain_rows[4])[1]
    grad_in, gain_four = pull(reduce_own(back))
    grad = cot[:half] + grad_in
    grads_cross, back_query, back_memory = attn_backward(
        norm_cross, memory, cross_att, key_ok, kept_cross, both(grad.astype(low))
    )
    sum_cross = scatter(grads_cross)
    grad_enc = reduce_own(back_memory)
    pull = jax.vjp(rmsnorm, dec_one, gain_rows[3])[1]
    grad_in, gain_three = pull(reduce_own(back_query))
    grad = grad + grad_in
    grads_self, back_query, back_key = attn_backward(
        norm_self, norm_self, self_att, causal, kept_self, both(grad.astype(low))
    )
    sum_self = scatter(grads_self)
    pull = jax.vjp(rmsnorm, dec_x[:half], gain_rows[2])[1]
    grad_in, gain_two = pull(reduce_own(back_query + back_key))
    decoder_in_grad = absolute(grad + grad_in).reshape(pairs * SUFFIX, D)

    grads_enc, back = feed_backward(norm_mid, enc_feed, kept_feed, both(grad_enc.astype(low)))
    sum_enc = scatter(grads_enc)
    pull = jax.vjp(rmsnorm, enc_mid, gain_rows[1])[1]
    grad_in, gain_one = pull(reduce_own(back))
    grad_enc = grad_enc + grad_in
    grads_att, back_query, back_key = attn_backward(
        norm_enc, norm_enc, enc_att, key_ok, kept_enc, both(grad_enc.astype(low))
    )
    sum_att = scatter(grads_att)
    pull = jax.vjp(rmsnorm, enc_x[:half], gain_rows[0])[1]
    grad_in, gain_zero = pull(reduce_own(back_query + back_key))
    encoder_in_grad = absolute(grad_enc + grad_in).reshape(pairs * ENC_LEN, D)

    gain_grad = jnp.stack([gain_zero, gain_one, gain_two, gain_three, gain_four])
    gain_grad = total_dp(gain_grad + swap(gain_grad, "mp", 1))
    grad_gain = lax.dynamic_slice(gain_grad, (0, dp_index * block), (5, block))

    att = jnp.concatenate([sum_att, sum_self, sum_cross], 0)
    grad_in = att[:, :, : 3 * width].reshape(3, block, 3, width).transpose(0, 2, 1, 3)
    grad_out = att[:, :, 3 * width :].transpose(0, 2, 1)
    grad_up = jnp.stack([sum_enc[0], sum_dec[0]])
    grad_down = jnp.stack([sum_enc[1], sum_dec[1]]).transpose(0, 2, 1)

    squares = [item * item for item in (grad_in, grad_out, grad_up, grad_down)]
    rows_part = [jnp.sum(item, -1) for item in squares]
    cols_part = [jnp.sum(item, -2) for item in squares]
    along_dp = [rows_part[0], cols_part[1], rows_part[2], cols_part[3]]
    along_mp = [cols_part[0], rows_part[1], cols_part[2], rows_part[3]]

    def spread_all(parts, axis, other):
        index, count = (dp_index, dp_n) if axis == "dp" else (mp_index, mp_n)
        flat = jnp.concatenate([item.reshape(-1) for item in parts])
        for bit in bits(mp_n if axis == "dp" else dp_n):
            flat = flat + swap(flat, other, bit)
        full = lax.dynamic_update_slice(
            jnp.zeros((count, flat.shape[0]), f32), flat[None], (index, 0)
        )
        for bit in bits(count):
            full = full + swap(full, axis, bit)
        result, start = [], 0
        for item in parts:
            size = item.size
            piece = full[:, start : start + size].reshape((count,) + item.shape)
            start += size
            piece = jnp.moveaxis(piece, 0, -2)
            result.append(piece.reshape(item.shape[:-1] + (count * item.shape[-1],)))
        return result

    row_in, col_out, row_up, col_down = spread_all(along_dp, "dp", "mp")
    col_in, row_out, col_up, row_down = spread_all(along_mp, "mp", "dp")
    total = (
        jnp.sum(row_in) + jnp.sum(row_out) + jnp.sum(row_up) + jnp.sum(row_down)
        + jnp.sum(gain_grad * gain_grad)
    )
    grad_norm = jnp.sqrt(total)
    factor = jnp.minimum(1.0, 1.0 / grad_norm)
    squared = factor * factor
    row_in, col_in, row_out, col_out = (
        row_in * squared,
        col_in * squared,
        row_out * squared,
        col_out * squared,
    )
    row_up, col_up, row_down, col_down = (
        row_up * squared,
        col_up * squared,
        row_down * squared,
        col_down * squared,
    )
    grad_in, grad_out, grad_up, grad_down = (
        grad_in * factor,
        grad_out * factor,
        grad_up * factor,
        grad_down * factor,
    )
    grad_gain = grad_gain * factor
    pin = update_matrix(
        grad_in,
        project_in,
        project_in_rows,
        project_in_cols,
        project_in_moment,
        project_in_average,
        row_in,
        col_in,
        dp_index,
        mp_index,
    )
    pout = update_matrix(
        grad_out,
        project_out,
        project_out_rows,
        project_out_cols,
        project_out_moment,
        project_out_average,
        row_out,
        col_out,
        mp_index,
        dp_index,
    )
    pexp = update_matrix(
        grad_up,
        expand,
        expand_rows,
        expand_cols,
        expand_moment,
        expand_average,
        row_up,
        col_up,
        dp_index,
        mp_index,
    )
    pcon = update_matrix(
        grad_down,
        contract,
        contract_rows,
        contract_cols,
        contract_moment,
        contract_average,
        row_down,
        col_down,
        mp_index,
        dp_index,
    )
    square_new = DECAY * norm_gains_square + (1.0 - DECAY) * (grad_gain * grad_gain + EPS_STAT)
    stepped = grad_gain * lax.rsqrt(square_new)
    moment_new = MOMENTUM * norm_gains_moment + stepped
    gains_new = norm_gains - RATE_GAIN * (MOMENTUM * moment_new + stepped)
    average_new = AVERAGE * norm_gains_average + (1.0 - AVERAGE) * gains_new
    return (
        decoder_out,
        encoder_in_grad,
        decoder_in_grad,
        grad_norm,
        pin[0],
        pin[1],
        pin[2],
        pin[3],
        pin[4],
        pin[5],
        pin[6],
        pout[0],
        pout[1],
        pout[2],
        pout[3],
        pout[4],
        pout[5],
        pout[6],
        pexp[0],
        pexp[1],
        pexp[2],
        pexp[3],
        pexp[4],
        pexp[5],
        pexp[6],
        pcon[0],
        pcon[1],
        pcon[2],
        pcon[3],
        pcon[4],
        pcon[5],
        pcon[6],
        grad_gain,
        square_new,
        moment_new,
        gains_new,
        average_new,
        gains_new.astype(jnp.bfloat16),
    )


def solution(mesh):
    placed = (
        P("dp", None),
        P("dp", None),
        P("dp", None),
        P("dp", None),
        P("dp"),
        P("dp"),
        P(None, None, "dp", "mp"),
        P(),
        P(),
        P(None, None, "dp", "mp"),
        P(None, None, "dp", "mp"),
        P(None, "mp", "dp"),
        P(),
        P(),
        P(None, "mp", "dp"),
        P(None, "mp", "dp"),
        P(None, "dp", "mp"),
        P(),
        P(),
        P(None, "dp", "mp"),
        P(None, "dp", "mp"),
        P(None, "mp", "dp"),
        P(),
        P(),
        P(None, "mp", "dp"),
        P(None, "mp", "dp"),
        P(None, "dp"),
        P(None, "dp"),
        P(None, "dp"),
        P(None, "dp"),
    )
    return jax.shard_map(
        functools.partial(on_device, (mesh.shape["dp"], mesh.shape["mp"])),
        mesh=mesh,
        in_specs=placed,
        out_specs=(
            P("dp", None),
            P("dp", None),
            P("dp", None),
            P(),
            P(None, None, "dp", "mp"),
            P(),
            P(),
            P(None, None, "dp", "mp"),
            P(None, None, "dp", "mp"),
            P(None, None, "dp", "mp"),
            P(None, None, "dp", "mp"),
            P(None, "mp", "dp"),
            P(),
            P(),
            P(None, "mp", "dp"),
            P(None, "mp", "dp"),
            P(None, "mp", "dp"),
            P(None, "mp", "dp"),
            P(None, "dp", "mp"),
            P(),
            P(),
            P(None, "dp", "mp"),
            P(None, "dp", "mp"),
            P(None, "dp", "mp"),
            P(None, "dp", "mp"),
            P(None, "mp", "dp"),
            P(),
            P(),
            P(None, "mp", "dp"),
            P(None, "mp", "dp"),
            P(None, "mp", "dp"),
            P(None, "mp", "dp"),
            P(None, "dp"),
            P(None, "dp"),
            P(None, "dp"),
            P(None, "dp"),
            P(None, "dp"),
            P(None, "dp"),
        ),
        check_vma=False,
    )
```

```python
import functools

import jax
import jax.numpy as jnp
from jax import lax
from jax.experimental import pallas as pl
from jax.experimental.pallas import tpu as pltpu
from jax.sharding import PartitionSpec as P

D = 768
HEAD_DIM = 64
FF = 3072
PATCHES = 196
SUFFIX = 32
ENC_LEN = 228


EPS_NORM = 1e-06
EPS_STAT = 1e-30
DECAY = 0.99
MOMENTUM = 0.9
AVERAGE = 0.6
RATE_MATRIX = 0.004
RATE_GAIN = 0.05
MASKED = -1000000000.0


LOW = jnp.bfloat16
F32 = jnp.float32
VMEM_LIMIT = 56 * 1024 * 1024


def dot(left, right, contract):
    return lax.dot_general(left, right, (contract, ((), ())), preferred_element_type=F32)


def mm(left, right):
    return dot(left, right, ((1,), (0,)))


def mm_t(left, right):
    return dot(left, right, ((1,), (1,)))


def t_mm(left, right):
    return dot(left, right, ((0,), (0,)))


def rms_scale(value):
    return lax.rsqrt(jnp.mean(value * value, -1, keepdims=True) + EPS_NORM)


def softmax(scores):
    expons = jnp.exp(scores - jnp.max(scores, -1, keepdims=True))
    return expons / jnp.sum(expons, -1, keepdims=True)


def gelu_parts(upper):
    inner = 0.7978845608028654 * (upper + 0.044715 * upper * upper * upper)
    bent = jnp.tanh(inner)
    value = 0.5 * upper * (1.0 + bent)
    slope = 0.5 * (1.0 + bent) + 0.5 * upper * (1.0 - bent * bent) * 0.7978845608028654 * (
        1.0 + 3.0 * 0.044715 * upper * upper
    )
    return value, slope


class Plan:
    def __init__(self, dp_n, block, width, hidden, pairs):
        self.dp_n, self.block, self.width, self.hidden, self.pairs = dp_n, block, width, hidden, pairs
        self.half = pairs // 2
        self.heads = width // HEAD_DIM
        self.direct = dp_n == 8

    def weight_specs(self, pieces):
        return [pl.BlockSpec(item.shape, lambda *_, n=item.ndim: (0,) * n) for item in pieces]

    def weight_scratch(self, pieces, count):
        return [pltpu.VMEM((count, D, D), LOW)]

    def assemble(self, meta, refs, scratch):
        if not self.direct:
            scratch[...] = refs[0][...]
            return
        for ref, places in zip(refs, ((0, 4, 2, 6), (1, 5, 3, 7))):
            for index, place in enumerate(places):
                row = pl.multiple_of(jnp.bitwise_xor(meta[0], place) * self.block, 32)
                scratch[:, pl.ds(row, self.block), :] = ref[index]

    def grad_shapes(self, count):
        if not self.direct:
            return [jax.ShapeDtypeStruct((count, D, D), F32)]
        shape = (count, self.dp_n // 2, self.block, D)
        return [jax.ShapeDtypeStruct(shape, LOW), jax.ShapeDtypeStruct(shape, F32)]

    def emit(self, meta, acc, refs):
        if not self.direct:
            refs[0][...] = acc[...]
            return
        mine = jnp.bitwise_and(meta[0], 1)
        for index in range(self.dp_n // 2):
            away = pl.multiple_of((2 * index + 1 - mine) * self.block, 32)
            here = pl.multiple_of((2 * index + mine) * self.block, 32)
            for count in range(acc.shape[0]):
                refs[0][count, index] = acc[count, pl.ds(away, self.block), :].astype(LOW)
                refs[1][count, index] = acc[count, pl.ds(here, self.block), :]


def whole(shape):
    return pl.BlockSpec(shape, lambda *_: (0,) * len(shape))


def own_spec(count, base, shape):
    return pl.BlockSpec(
        (1,) + shape, lambda p, _: (base + jnp.maximum(p - count, 0),) + (0,) * len(shape)
    )


def oth_spec(count, base, shape):
    return pl.BlockSpec(
        (1,) + shape, lambda p, _: (base + jnp.minimum(p, count - 1),) + (0,) * len(shape)
    )


def step_spec(shape):
    return pl.BlockSpec((1,) + shape, lambda p, _: (p,) + (0,) * len(shape))


def call(name, body, grid, meta, inputs, in_specs, outs, out_specs, scratch):
    return pl.pallas_call(
        body,
        name=name,
        out_shape=outs,
        grid_spec=pltpu.PrefetchScalarGridSpec(
            num_scalar_prefetch=1,
            grid=grid,
            in_specs=in_specs,
            out_specs=out_specs,
            scratch_shapes=scratch,
        ),
        compiler_params=pltpu.CompilerParams(
            dimension_semantics=("arbitrary",) * len(grid), vmem_limit_bytes=VMEM_LIMIT
        ),
    )(meta, *inputs)


def key_mask(meta, pairs, slot):
    place = lax.broadcasted_iota(jnp.int32, (1, ENC_LEN), 1)
    image, prefix = meta[1 + slot], meta[1 + pairs + slot]
    return (place < image * PATCHES) | ((place >= PATCHES) & (place < PATCHES + prefix))


def attend_heads(plan, queries, keys, values, allowed):
    mixed = []
    for head in range(plan.heads):
        cut = slice(head * HEAD_DIM, (head + 1) * HEAD_DIM)
        scores = jnp.where(allowed, mm_t(queries[:, cut], keys[:, cut]) * 0.125, MASKED)
        mixed.append(mm(softmax(scores).astype(LOW), values[:, cut]).astype(LOW))
    return jnp.concatenate(mixed, 1)


def attend_heads_back(plan, queries, keys, values, allowed, grad_mixed):
    grads = ([], [], [])
    for head in range(plan.heads):
        cut = slice(head * HEAD_DIM, (head + 1) * HEAD_DIM)
        query, key, value, grad = queries[:, cut], keys[:, cut], values[:, cut], grad_mixed[:, cut]
        probs = softmax(jnp.where(allowed, mm_t(query, key) * 0.125, MASKED))
        grad_probs = mm_t(grad, value)
        inner = jnp.sum(grad_probs * probs, -1, keepdims=True)
        grad_scores = (probs * (grad_probs - inner)).astype(LOW)
        grads[0].append((mm(grad_scores, key) * 0.125).astype(LOW))
        grads[1].append((t_mm(grad_scores, query) * 0.125).astype(LOW))
        grads[2].append(t_mm(probs.astype(LOW), grad).astype(LOW))
    return tuple(jnp.concatenate(item, 1) for item in grads)


def slot_of(plan, count, base, step):
    return jnp.where(step < count, plan.half + base + step, base + step - count)


def put(step, count, own, oth, value):
    @pl.when(step < count)
    def _():
        oth[0] = value

    @pl.when(step >= count)
    def _():
        own[0] = value


def encoder_attention(plan, meta, own, oth, gain, pieces, base, count):
    w3 = 3 * plan.width
    n = len(pieces)

    def body(meta, own_ref, oth_ref, gain_ref, *rest):
        refs, (own_out, oth_out, kept, weight) = rest[:n], rest[n:]
        step = pl.program_id(0)

        @pl.when(step == 0)
        def _():
            plan.assemble(meta, refs, weight)

        value = jnp.where(step < count, oth_ref[0], own_ref[0]).astype(F32)
        normed = (value * rms_scale(value) * gain_ref[...]).astype(LOW)
        joined = mm(normed, weight[0, :, :w3]).astype(LOW)
        allowed = key_mask(meta, plan.pairs, slot_of(plan, count, base, step))
        width = plan.width
        mixed = attend_heads(
            plan, joined[:, :width], joined[:, width : 2 * width], joined[:, 2 * width :], allowed
        )
        kept[0, :, :w3] = joined
        kept[0, :, w3:] = mixed
        put(step, count, own_out, oth_out, mm_t(mixed, weight[0, :, w3:]).astype(LOW))

    rows = (ENC_LEN, D)
    return call(
        "encoder_attention",
        body,
        (2 * count,),
        meta,
        (own, oth, gain, *pieces),
        [own_spec(count, base, rows), oth_spec(count, base, rows), whole((1, D)), *plan.weight_specs(pieces)],
        [jax.ShapeDtypeStruct((count,) + rows, LOW)] * 2
        + [jax.ShapeDtypeStruct((2 * count, ENC_LEN, w3 + plan.width), LOW)],
        [own_spec(count, 0, rows), oth_spec(count, 0, rows), step_spec((ENC_LEN, w3 + plan.width))],
        plan.weight_scratch(pieces, 1),
    )


def encoder_attention_back(plan, meta, own, oth, gain, pieces, kept, grad_own, grad_oth):
    count = plan.half
    width, w3 = plan.width, 3 * plan.width
    n = len(pieces)

    def body(meta, own_ref, oth_ref, gain_ref, kept_ref, grad_own_ref, grad_oth_ref, *rest):
        refs, (own_out, oth_out), grad_refs = rest[:n], rest[n : n + 2], rest[n + 2 : -2]
        weight, acc = rest[-2:]
        step = pl.program_id(0)

        @pl.when(step == 0)
        def _():
            plan.assemble(meta, refs, weight)
            acc[...] = jnp.zeros_like(acc)

        value = jnp.where(step < count, oth_ref[0], own_ref[0]).astype(F32)
        normed = (value * rms_scale(value) * gain_ref[...]).astype(LOW)
        grad = jnp.where(step < count, grad_oth_ref[0], grad_own_ref[0])
        allowed = key_mask(meta, plan.pairs, slot_of(plan, count, 0, step))
        grad_mixed = mm(grad, weight[0, :, w3:]).astype(LOW)
        acc[0, :, w3:] += t_mm(grad, kept_ref[0, :, w3:])
        joined = kept_ref[0, :, :w3]
        grads = attend_heads_back(
            plan, joined[:, :width], joined[:, width : 2 * width], joined[:, 2 * width :], allowed, grad_mixed
        )
        together = jnp.concatenate(grads, 1)
        acc[0, :, :w3] += t_mm(normed, together)
        put(step, count, own_out, oth_out, mm_t(together, weight[0, :, :w3]).astype(LOW))

        @pl.when(step == 2 * count - 1)
        def _():
            plan.emit(meta, acc, grad_refs)

    rows = (ENC_LEN, D)
    shapes = plan.grad_shapes(1)
    pair_specs = [own_spec(count, 0, rows), oth_spec(count, 0, rows)]
    return call(
        "encoder_attention_back",
        body,
        (2 * count,),
        meta,
        (own, oth, gain, kept, grad_own, grad_oth, *pieces),
        [*pair_specs, whole((1, D)), step_spec(kept.shape[1:]), *pair_specs, *plan.weight_specs(pieces)],
        [jax.ShapeDtypeStruct((count,) + rows, LOW)] * 2 + shapes,
        [*pair_specs, *[whole(item.shape) for item in shapes]],
        plan.weight_scratch(pieces, 1) + [pltpu.VMEM((1, D, D), F32)],
    )


def encoder_feed(plan, meta, own, oth, pieces, base, count):
    n = len(pieces)

    def body(meta, own_ref, oth_ref, *rest):
        refs, (own_out, oth_out, weight) = rest[:n], rest[n:]
        step = pl.program_id(0)

        @pl.when(step == 0)
        def _():
            plan.assemble(meta, refs, weight)

        normed = jnp.where(step < count, oth_ref[0], own_ref[0])
        active = gelu_parts(mm(normed, weight[0]))[0].astype(LOW)
        put(step, count, own_out, oth_out, mm_t(active, weight[1]).astype(LOW))

    rows = (ENC_LEN, D)
    return call(
        "encoder_feed",
        body,
        (2 * count,),
        meta,
        (own, oth, *pieces),
        [own_spec(count, base, rows), oth_spec(count, base, rows), *plan.weight_specs(pieces)],
        [jax.ShapeDtypeStruct((count,) + rows, LOW)] * 2,
        [own_spec(count, 0, rows), oth_spec(count, 0, rows)],
        plan.weight_scratch(pieces, 2),
    )


def encoder_feed_back(plan, meta, own, oth, grad_own, grad_oth, pieces):
    n = len(pieces)
    count = plan.half

    def body(meta, own_ref, oth_ref, grad_own_ref, grad_oth_ref, *rest):
        refs, (own_out, oth_out), grad_refs = rest[:n], rest[n : n + 2], rest[n + 2 : -2]
        weight, acc = rest[-2:]
        step = pl.program_id(0)

        @pl.when(step == 0)
        def _():
            plan.assemble(meta, refs, weight)
            acc[...] = jnp.zeros_like(acc)

        normed = jnp.where(step < count, oth_ref[0], own_ref[0])
        grad = jnp.where(step < count, grad_oth_ref[0], grad_own_ref[0])
        active, slope = gelu_parts(mm(normed, weight[0]))
        grad_upper = (slope * mm(grad, weight[1])).astype(LOW)
        put(step, count, own_out, oth_out, mm_t(grad_upper, weight[0]).astype(LOW))
        acc[0] += t_mm(normed, grad_upper)
        acc[1] += t_mm(grad, active.astype(LOW))

        @pl.when(step == 2 * count - 1)
        def _():
            plan.emit(meta, acc, grad_refs)

    rows = (ENC_LEN, D)
    shapes = plan.grad_shapes(2)
    pair_specs = [own_spec(count, 0, rows), oth_spec(count, 0, rows)]
    return call(
        "encoder_feed_back",
        body,
        (2 * count,),
        meta,
        (own, oth, grad_own, grad_oth, *pieces),
        [*pair_specs, *pair_specs, *plan.weight_specs(pieces)],
        [jax.ShapeDtypeStruct((count,) + rows, LOW)] * 2 + shapes,
        [*pair_specs, *[whole(item.shape) for item in shapes]],
        plan.weight_scratch(pieces, 2) + [pltpu.VMEM((2, D, D), F32)],
    )


def self_mask(plan, meta):
    rows = plan.pairs * SUFFIX
    query = lax.broadcasted_iota(jnp.int32, (rows, rows), 0)
    key = lax.broadcasted_iota(jnp.int32, (rows, rows), 1)
    pair = key // SUFFIX
    limit = jnp.zeros_like(key)
    for slot in range(plan.pairs):
        limit = jnp.where(pair == slot, meta[1 + 2 * plan.pairs + slot], limit)
    return (query // SUFFIX == pair) & (key <= query) & (key - pair * SUFFIX < limit)


def decoder_self(plan, meta, rows_in, gain, pieces):
    n = len(pieces)
    width, w3 = plan.width, 3 * plan.width
    rows = plan.pairs * SUFFIX
    mid = rows // 2

    def body(meta, in_ref, gain_ref, *rest):
        refs, (own_out, oth_out, kept, weight) = rest[:n], rest[n:]
        plan.assemble(meta, refs, weight)
        value = in_ref[...].astype(F32)
        normed = (value * rms_scale(value) * gain_ref[...]).astype(LOW)
        joined = mm(normed, weight[0, :, :w3]).astype(LOW)
        mixed = attend_heads(
            plan, joined[:, :width], joined[:, width : 2 * width], joined[:, 2 * width :], self_mask(plan, meta)
        )
        kept[:, :w3] = joined
        kept[:, w3:] = mixed
        partial = mm_t(mixed, weight[0, :, w3:]).astype(LOW)
        own_out[...] = partial[:mid]
        oth_out[...] = partial[mid:]

    return call(
        "decoder_self",
        body,
        (1,),
        meta,
        (rows_in, gain, *pieces),
        [whole((rows, D)), whole((1, D)), *plan.weight_specs(pieces)],
        [jax.ShapeDtypeStruct((mid, D), LOW)] * 2 + [jax.ShapeDtypeStruct((rows, 4 * width), LOW)],
        [whole((mid, D))] * 2 + [whole((rows, 4 * width))],
        plan.weight_scratch(pieces, 1),
    )


def decoder_self_back(plan, meta, rows_in, gain, pieces, kept, grad_own, grad_oth):
    n = len(pieces)
    width, w3 = plan.width, 3 * plan.width
    rows = plan.pairs * SUFFIX
    mid = rows // 2

    def body(meta, in_ref, gain_ref, kept_ref, grad_own_ref, grad_oth_ref, *rest):
        refs, (own_out, oth_out), grad_refs = rest[:n], rest[n : n + 2], rest[n + 2 : -2]
        weight, acc = rest[-2:]
        plan.assemble(meta, refs, weight)
        value = in_ref[...].astype(F32)
        normed = (value * rms_scale(value) * gain_ref[...]).astype(LOW)
        grad = jnp.concatenate([grad_own_ref[...], grad_oth_ref[...]], 0)
        grad_mixed = mm(grad, weight[0, :, w3:]).astype(LOW)
        acc[0, :, w3:] = t_mm(grad, kept_ref[:, w3:])
        joined = kept_ref[:, :w3]
        grads = attend_heads_back(
            plan,
            joined[:, :width],
            joined[:, width : 2 * width],
            joined[:, 2 * width :],
            self_mask(plan, meta),
            grad_mixed,
        )
        together = jnp.concatenate(grads, 1)
        acc[0, :, :w3] = t_mm(normed, together)
        partial = mm_t(together, weight[0, :, :w3]).astype(LOW)
        own_out[...] = partial[:mid]
        oth_out[...] = partial[mid:]
        plan.emit(meta, acc, grad_refs)

    shapes = plan.grad_shapes(1)
    return call(
        "decoder_self_back",
        body,
        (1,),
        meta,
        (rows_in, gain, kept, grad_own, grad_oth, *pieces),
        [whole((rows, D)), whole((1, D)), whole(kept.shape), whole((mid, D)), whole((mid, D)), *plan.weight_specs(pieces)],
        [jax.ShapeDtypeStruct((mid, D), LOW)] * 2 + shapes,
        [whole((mid, D))] * 2 + [whole(item.shape) for item in shapes],
        plan.weight_scratch(pieces, 1) + [pltpu.VMEM((1, D, D), F32)],
    )


def decoder_cross(plan, meta, own, oth, memory_own, memory_oth, pieces):
    n = len(pieces)
    count = plan.half
    width, w3 = plan.width, 3 * plan.width

    def body(meta, own_ref, oth_ref, memory_own_ref, memory_oth_ref, *rest):
        refs, (own_out, oth_out, kept_query, kept_key, weight) = rest[:n], rest[n:]
        step = pl.program_id(0)

        @pl.when(step == 0)
        def _():
            plan.assemble(meta, refs, weight)

        normed = jnp.where(step < count, oth_ref[0], own_ref[0])
        memory = jnp.where(step < count, memory_oth_ref[0], memory_own_ref[0])
        queries = mm(normed, weight[0, :, :width]).astype(LOW)
        both = mm(memory, weight[0, :, width:w3]).astype(LOW)
        allowed = key_mask(meta, plan.pairs, slot_of(plan, count, 0, step))
        mixed = attend_heads(plan, queries, both[:, :width], both[:, width:], allowed)
        kept_query[0, :, :width] = queries
        kept_query[0, :, width:] = mixed
        kept_key[0] = both
        put(step, count, own_out, oth_out, mm_t(mixed, weight[0, :, w3:]).astype(LOW))

    rows, long = (SUFFIX, D), (ENC_LEN, D)
    return call(
        "decoder_cross",
        body,
        (2 * count,),
        meta,
        (own, oth, memory_own, memory_oth, *pieces),
        [
            own_spec(count, 0, rows),
            oth_spec(count, 0, rows),
            own_spec(count, 0, long),
            oth_spec(count, 0, long),
            *plan.weight_specs(pieces),
        ],
        [jax.ShapeDtypeStruct((count,) + rows, LOW)] * 2
        + [
            jax.ShapeDtypeStruct((2 * count, SUFFIX, 2 * width), LOW),
            jax.ShapeDtypeStruct((2 * count, ENC_LEN, 2 * width), LOW),
        ],
        [
            own_spec(count, 0, rows),
            oth_spec(count, 0, rows),
            step_spec((SUFFIX, 2 * width)),
            step_spec((ENC_LEN, 2 * width)),
        ],
        plan.weight_scratch(pieces, 1),
    )


def decoder_cross_back(
    plan, meta, own, oth, memory_own, memory_oth, pieces, kept_query, kept_key, grad_own, grad_oth
):
    n = len(pieces)
    count = plan.half
    width, w3 = plan.width, 3 * plan.width

    def body(
        meta, own_ref, oth_ref, memory_own_ref, memory_oth_ref, query_ref, key_ref, grad_own_ref, grad_oth_ref, *rest
    ):
        refs, outs, grad_refs = rest[:n], rest[n : n + 4], rest[n + 4 : -2]
        weight, acc = rest[-2:]
        step = pl.program_id(0)

        @pl.when(step == 0)
        def _():
            plan.assemble(meta, refs, weight)
            acc[...] = jnp.zeros_like(acc)

        normed = jnp.where(step < count, oth_ref[0], own_ref[0])
        memory = jnp.where(step < count, memory_oth_ref[0], memory_own_ref[0])
        grad = jnp.where(step < count, grad_oth_ref[0], grad_own_ref[0])
        allowed = key_mask(meta, plan.pairs, slot_of(plan, count, 0, step))
        grad_mixed = mm(grad, weight[0, :, w3:]).astype(LOW)
        acc[0, :, w3:] += t_mm(grad, query_ref[0, :, width:])
        both = key_ref[0]
        grad_query, grad_key, grad_value = attend_heads_back(
            plan, query_ref[0, :, :width], both[:, :width], both[:, width:], allowed, grad_mixed
        )
        together = jnp.concatenate([grad_key, grad_value], 1)
        acc[0, :, :width] += t_mm(normed, grad_query)
        acc[0, :, width:w3] += t_mm(memory, together)
        put(step, count, outs[0], outs[1], mm_t(grad_query, weight[0, :, :width]).astype(LOW))
        put(step, count, outs[2], outs[3], mm_t(together, weight[0, :, width:w3]).astype(LOW))

        @pl.when(step == 2 * count - 1)
        def _():
            plan.emit(meta, acc, grad_refs)

    rows, long = (SUFFIX, D), (ENC_LEN, D)
    shapes = plan.grad_shapes(1)
    row_specs = [own_spec(count, 0, rows), oth_spec(count, 0, rows)]
    long_specs = [own_spec(count, 0, long), oth_spec(count, 0, long)]
    return call(
        "decoder_cross_back",
        body,
        (2 * count,),
        meta,
        (own, oth, memory_own, memory_oth, kept_query, kept_key, grad_own, grad_oth, *pieces),
        [
            *row_specs,
            *long_specs,
            step_spec(kept_query.shape[1:]),
            step_spec(kept_key.shape[1:]),
            *row_specs,
            *plan.weight_specs(pieces),
        ],
        [jax.ShapeDtypeStruct((count,) + rows, LOW)] * 2
        + [jax.ShapeDtypeStruct((count,) + long, LOW)] * 2
        + shapes,
        [*row_specs, *long_specs, *[whole(item.shape) for item in shapes]],
        plan.weight_scratch(pieces, 1) + [pltpu.VMEM((1, D, D), F32)],
    )


def decoder_feed(plan, meta, own, oth, grad_in, pieces):
    n = len(pieces)
    rows = plan.pairs * SUFFIX
    mid = rows // 2

    def body(meta, own_ref, oth_ref, grad_ref, *rest):
        refs, (own_out, oth_out), grad_refs = rest[:n], rest[n : n + 2], rest[n + 2 : -2]
        weight, acc = rest[-2:]
        plan.assemble(meta, refs, weight)
        normed = jnp.concatenate([own_ref[...], oth_ref[...]], 0)
        grad = grad_ref[...]
        active, slope = gelu_parts(mm(normed, weight[0]))
        active = active.astype(LOW)
        partial = mm_t(active, weight[1]).astype(LOW)
        grad_upper = (slope * mm(grad, weight[1])).astype(LOW)
        back = mm_t(grad_upper, weight[0]).astype(LOW)
        own_out[0] = partial[:mid]
        own_out[1] = back[:mid]
        oth_out[0] = partial[mid:]
        oth_out[1] = back[mid:]
        acc[0] = t_mm(normed, grad_upper)
        acc[1] = t_mm(grad, active)
        plan.emit(meta, acc, grad_refs)

    shapes = plan.grad_shapes(2)
    return call(
        "decoder_feed",
        body,
        (1,),
        meta,
        (own, oth, grad_in, *pieces),
        [whole((mid, D))] * 2 + [whole((rows, D)), *plan.weight_specs(pieces)],
        [jax.ShapeDtypeStruct((2, mid, D), LOW)] * 2 + shapes,
        [whole((2, mid, D))] * 2 + [whole(item.shape) for item in shapes],
        plan.weight_scratch(pieces, 2) + [pltpu.VMEM((2, D, D), F32)],
    )


def add_norm(meta, name, base, first, second, gain):
    def body(meta, base_ref, first_ref, second_ref, gain_ref, sum_ref, norm_ref):
        value = base_ref[...].astype(F32) + (first_ref[...].astype(F32) + second_ref[...].astype(F32))
        sum_ref[...] = value
        norm_ref[...] = (value * rms_scale(value) * gain_ref[...]).astype(LOW)

    shape = base.shape
    part = (1,) + shape[1:] if len(shape) == 3 else shape
    spec = (
        pl.BlockSpec(part, lambda p, _: (p, 0, 0)) if len(shape) == 3 else whole(shape)
    )
    return call(
        name,
        body,
        (shape[0] if len(shape) == 3 else 1,),
        meta,
        (base, first, second, gain),
        [spec, spec, spec, whole((1, D))],
        [jax.ShapeDtypeStruct(shape, F32), jax.ShapeDtypeStruct(shape, LOW)],
        [spec, spec],
        [],
    )


def norm_back(meta, name, inputs, gain, grad, first, second, want_low):
    def body(meta, in_ref, gain_ref, grad_ref, first_ref, second_ref, *outs):
        value = in_ref[...].astype(F32)
        scale = rms_scale(value)
        unit = value * scale
        back = first_ref[...].astype(F32) + second_ref[...].astype(F32)
        product = back * unit
        axes = tuple(range(value.ndim - 1))
        part = jnp.sum(product, axes)[None]
        weighted = product * gain_ref[...]
        total = grad_ref[...].astype(F32) + scale * (
            back * gain_ref[...] - unit * jnp.mean(weighted, -1, keepdims=True)
        )
        outs[0][...] = total
        if want_low:
            outs[1][...] = total.astype(LOW)
        step = pl.program_id(0)

        @pl.when(step == 0)
        def _():
            outs[-1][...] = part

        @pl.when(step > 0)
        def _():
            outs[-1][...] += part

    shape = inputs.shape
    part = (1,) + shape[1:] if len(shape) == 3 else shape
    spec = pl.BlockSpec(part, lambda p, _: (p, 0, 0)) if len(shape) == 3 else whole(shape)
    return call(
        name,
        body,
        (shape[0] if len(shape) == 3 else 1,),
        meta,
        (inputs, gain, grad, first, second),
        [spec, whole((1, D)), spec, spec, spec],
        [jax.ShapeDtypeStruct(shape, F32)]
        + [jax.ShapeDtypeStruct(shape, LOW)] * want_low
        + [jax.ShapeDtypeStruct((1, D), F32)],
        [spec] * (1 + want_low) + [whole((1, D))],
        [],
    )


def update_matrix(
    gradient, weight, rows_old, cols_old, moment, average, row_sum, col_sum, row_index, col_index
):
    full_rows = rows_old.shape[-1]
    full_cols = cols_old.shape[-1]
    rows_new = DECAY * rows_old + (1.0 - DECAY) * (row_sum / full_cols + EPS_STAT)
    cols_new = DECAY * cols_old + (1.0 - DECAY) * (col_sum / full_rows + EPS_STAT)
    row_local = lax.dynamic_slice_in_dim(
        rows_new, row_index * gradient.shape[-2], gradient.shape[-2], rows_new.ndim - 1
    )
    col_local = lax.dynamic_slice_in_dim(
        cols_new, col_index * gradient.shape[-1], gradient.shape[-1], cols_new.ndim - 1
    )
    second = (
        row_local[..., :, None] * col_local[..., None, :] / jnp.mean(rows_new, -1)[..., None, None]
    )
    stepped = gradient * lax.rsqrt(second)
    moment_new = MOMENTUM * moment + stepped
    weight_new = weight - RATE_MATRIX * (MOMENTUM * moment_new + stepped)
    average_new = AVERAGE * average + (1.0 - AVERAGE) * weight_new
    return (
        gradient,
        rows_new,
        cols_new,
        moment_new,
        weight_new,
        average_new,
        weight_new.astype(jnp.bfloat16),
    )


def on_device(
    sizes,
    encoder_in,
    decoder_in,
    decoder_cotangent,
    counts,
    prefix_len,
    suffix_len,
    project_in,
    project_in_rows,
    project_in_cols,
    project_in_moment,
    project_in_average,
    project_out,
    project_out_rows,
    project_out_cols,
    project_out_moment,
    project_out_average,
    expand,
    expand_rows,
    expand_cols,
    expand_moment,
    expand_average,
    contract,
    contract_rows,
    contract_cols,
    contract_moment,
    contract_average,
    norm_gains,
    norm_gains_square,
    norm_gains_moment,
    norm_gains_average,
):
    dp_n, mp_n = sizes
    dp_index = lax.axis_index("dp")
    mp_index = lax.axis_index("mp")
    side = mp_index % 2
    pairs = prefix_len.shape[0]
    half = pairs // 2
    width = project_in.shape[-1]
    block = project_in.shape[-2]
    plan = Plan(dp_n, block, width, expand.shape[-1], pairs)
    low, f32 = LOW, F32

    def swap(value, axis, bit):
        count = dp_n if axis == "dp" else mp_n
        return lax.ppermute(value, axis, [(i, i ^ bit) for i in range(count)])

    def bits(count):
        return [1 << i for i in range(count.bit_length() - 1)]

    def after(value, other):
        return lax.optimization_barrier((value, other))[0]

    def gather(own, gate):
        if gate is not None:
            own = after(own, gate)
        if not plan.direct:
            return [lax.all_gather(own, "dp", axis=1, tiled=True)], None
        two = jnp.stack([own, swap(own, "dp", 4)])
        more = swap(two, "dp", 2)
        four = jnp.concatenate([two, more], 0)
        return [four, swap(four, "dp", 1)], more

    def scatter(parts):
        if not plan.direct:
            return lax.psum_scatter(parts[0], "dp", scatter_dimension=1, tiled=True)
        away, keep = parts
        count = keep.shape[0]
        keep = keep + swap(away, "dp", 1).astype(f32)
        for bit in (2, 4):
            mine = (dp_index // bit) % 2
            split = keep.reshape(count, -1, 2, block, D)
            away = lax.dynamic_index_in_dim(split, 1 - mine, 2, False).astype(low)
            keep = lax.dynamic_index_in_dim(split, mine, 2, False) + swap(away, "dp", bit).astype(f32)
        return keep.reshape(count, block, D)

    def total_dp(value):
        for bit in bits(dp_n):
            value = value + swap(value, "dp", bit)
        return value

    def reduce_own(own, oth):
        sent = (own.astype(f32) + swap(oth, "mp", 1).astype(f32)).astype(low)
        for bit in bits(mp_n)[1:-1]:
            sent = (sent.astype(f32) + swap(sent, "mp", bit).astype(f32)).astype(low)
        return sent, swap(sent, "mp", bits(mp_n)[-1])

    def relative(value):
        split = value.reshape((half, 2) + value.shape[1:])
        return (
            lax.dynamic_index_in_dim(split, side, 1, False),
            lax.dynamic_index_in_dim(split, 1 - side, 1, False),
        )

    def absolute(own):
        other = swap(own, "mp", 1)
        even = jnp.where(side == 0, own, other)
        odd = jnp.where(side == 0, other, own)
        return jnp.stack([even, odd], 1).reshape((pairs,) + own.shape[1:])

    def core(value):
        return swap(value, "mp", 1)

    def attention_block(layer):
        return jnp.concatenate(
            [project_in[layer, 0], project_in[layer, 1], project_in[layer, 2], project_out[layer].T], 1
        ).astype(low)[None]

    def feed_block(layer):
        return jnp.stack([expand[layer], contract[layer].T]).astype(low)

    gain_full = lax.dynamic_update_slice(
        jnp.zeros((5, D), low), norm_gains.astype(low), (0, dp_index * block)
    )
    gain_rows = total_dp(gain_full).astype(f32)
    gains = [gain_rows[i : i + 1] for i in range(5)]

    enc_att, gate = gather(attention_block(0), None)
    enc_feed, gate = gather(feed_block(0), gate)
    self_att, gate = gather(attention_block(1), gate)
    cross_att, gate = gather(attention_block(2), gate)
    dec_feed, gate = gather(feed_block(1), gate)

    place_rel = jnp.concatenate([2 * jnp.arange(half) + side, 2 * jnp.arange(half) + 1 - side])
    prefix_rel = jnp.concatenate(relative(prefix_len))
    suffix_rel = jnp.concatenate(relative(suffix_len))
    images = place_rel < counts[0, 0]
    active = place_rel < counts[0, 0] + counts[0, 1]
    meta = jnp.concatenate(
        [dp_index[None].astype(jnp.int32), images.astype(jnp.int32), prefix_rel, suffix_rel]
    )
    steps = jnp.arange(SUFFIX)
    live = active[:, None] & (steps[None, :] < suffix_rel[:, None])

    mid = half * SUFFIX
    enc_own, enc_oth = relative(encoder_in.reshape(pairs, ENC_LEN, D))
    dec_rel = jnp.concatenate(relative(decoder_in.reshape(pairs, SUFFIX, D))).reshape(2 * mid, D)
    cot = jnp.concatenate(relative(decoder_cotangent.reshape(pairs, SUFFIX, D)))
    cot = jnp.where(live[:, :, None], cot, f32(0.0)).reshape(2 * mid, D)

    part = encoder_attention(plan, meta, enc_own, enc_oth, gains[0], enc_att, 0, half)
    kept_enc = part[2]
    sums = reduce_own(part[0], part[1])
    enc_mid, norm_mid = add_norm(meta, "add_norm_mid", enc_own, *sums, gains[1])
    norm_mid_oth = core(norm_mid)

    part = decoder_self(plan, meta, dec_rel, gains[2], self_att)
    kept_self = part[2]
    sums = reduce_own(part[0], part[1])
    dec_one, norm_cross = add_norm(meta, "add_norm_cross", dec_rel[:mid], *sums, gains[3])
    norm_cross_oth = core(norm_cross)

    part = encoder_feed(plan, meta, norm_mid, norm_mid_oth, enc_feed, 0, half)
    sums = reduce_own(part[0], part[1])
    memory = (enc_mid + (sums[0].astype(f32) + sums[1].astype(f32))).astype(low)
    memory_oth = core(memory)

    def triple(value):
        return value.reshape(half, SUFFIX, D)

    cross_in = (triple(norm_cross), triple(norm_cross_oth), memory, memory_oth, cross_att)
    part = decoder_cross(plan, meta, *cross_in)
    kept_cross = part[2:]
    sums = reduce_own(part[0], part[1])
    dec_two, norm_last = add_norm(
        meta, "add_norm_last", dec_one, sums[0].reshape(mid, D), sums[1].reshape(mid, D), gains[4]
    )
    part = decoder_feed(plan, meta, norm_last, core(norm_last), cot.astype(low), dec_feed)
    sum_dec = scatter(part[2:])
    sums = reduce_own(part[0], part[1])
    out_own = dec_two + (sums[0][0].astype(f32) + sums[1][0].astype(f32))
    decoder_out = absolute(triple(out_own)).reshape(2 * mid, D)
    grad, grad_low, gain_four = norm_back(
        meta, "norm_back_last", dec_two, gains[4], cot[:mid], sums[0][1], sums[1][1], True
    )
    part = decoder_cross_back(
        plan, meta, *cross_in, *kept_cross, triple(grad_low), triple(core(grad_low))
    )
    sum_cross = scatter(part[4:])
    sums_enc = reduce_own(part[2], part[3])
    sums = reduce_own(part[0], part[1])
    grad_enc = sums_enc[0].astype(f32) + sums_enc[1].astype(f32)
    enc_low = grad_enc.astype(low)
    grad, grad_low, gain_three = norm_back(
        meta, "norm_back_cross", dec_one, gains[3], grad, sums[0].reshape(mid, D), sums[1].reshape(mid, D), True
    )
    part = encoder_feed_back(plan, meta, norm_mid, norm_mid_oth, enc_low, core(enc_low), enc_feed)
    sum_enc = scatter(part[2:])
    sums = reduce_own(part[0], part[1])
    grad_enc, enc_low, gain_one = norm_back(
        meta, "norm_back_mid", enc_mid, gains[1], grad_enc, *sums, True
    )

    part = decoder_self_back(
        plan, meta, dec_rel, gains[2], self_att, kept_self, grad_low, core(grad_low)
    )
    sum_self = scatter(part[2:])
    sums = reduce_own(part[0], part[1])
    grad, gain_two = norm_back(meta, "norm_back_self", dec_rel[:mid], gains[2], grad, *sums, False)
    decoder_in_grad = absolute(triple(grad)).reshape(2 * mid, D)

    part = encoder_attention_back(
        plan, meta, enc_own, enc_oth, gains[0], enc_att, kept_enc, enc_low, core(enc_low)
    )
    sum_att = scatter(part[2:])
    sums = reduce_own(part[0], part[1])
    grad_enc, gain_zero = norm_back(meta, "norm_back_enc", enc_own, gains[0], grad_enc, *sums, False)
    encoder_in_grad = absolute(grad_enc).reshape(pairs * ENC_LEN, D)

    gain_grad = jnp.concatenate([gain_zero, gain_one, gain_two, gain_three, gain_four])
    gain_grad = total_dp(gain_grad + swap(gain_grad, "mp", 1))
    grad_gain = lax.dynamic_slice(gain_grad, (0, dp_index * block), (5, block))

    att = jnp.concatenate([sum_att, sum_self, sum_cross], 0)
    grad_in = att[:, :, : 3 * width].reshape(3, block, 3, width).transpose(0, 2, 1, 3)
    grad_out = att[:, :, 3 * width :].transpose(0, 2, 1)
    grad_up = jnp.stack([sum_enc[0], sum_dec[0]])
    grad_down = jnp.stack([sum_enc[1], sum_dec[1]]).transpose(0, 2, 1)

    squares = [item * item for item in (grad_in, grad_out, grad_up, grad_down)]
    rows_part = [jnp.sum(item, -1) for item in squares]
    cols_part = [jnp.sum(item, -2) for item in squares]
    along_dp = [rows_part[0], cols_part[1], rows_part[2], cols_part[3]]
    along_mp = [cols_part[0], rows_part[1], cols_part[2], rows_part[3]]

    def spread_all(parts, axis, other):
        index, count = (dp_index, dp_n) if axis == "dp" else (mp_index, mp_n)
        flat = jnp.concatenate([item.reshape(-1) for item in parts])
        for bit in bits(mp_n if axis == "dp" else dp_n):
            flat = flat + swap(flat, other, bit)
        full = lax.dynamic_update_slice(
            jnp.zeros((count, flat.shape[0]), f32), flat[None], (index, 0)
        )
        for bit in bits(count):
            full = full + swap(full, axis, bit)
        result, start = [], 0
        for item in parts:
            size = item.size
            piece = full[:, start : start + size].reshape((count,) + item.shape)
            start += size
            piece = jnp.moveaxis(piece, 0, -2)
            result.append(piece.reshape(item.shape[:-1] + (count * item.shape[-1],)))
        return result

    row_in, col_out, row_up, col_down = spread_all(along_dp, "dp", "mp")
    col_in, row_out, col_up, row_down = spread_all(along_mp, "mp", "dp")
    total = (
        jnp.sum(row_in) + jnp.sum(row_out) + jnp.sum(row_up) + jnp.sum(row_down)
        + jnp.sum(gain_grad * gain_grad)
    )
    grad_norm = jnp.sqrt(total)
    factor = jnp.minimum(1.0, 1.0 / grad_norm)
    squared = factor * factor
    row_in, col_in, row_out, col_out = (
        row_in * squared,
        col_in * squared,
        row_out * squared,
        col_out * squared,
    )
    row_up, col_up, row_down, col_down = (
        row_up * squared,
        col_up * squared,
        row_down * squared,
        col_down * squared,
    )
    grad_in, grad_out, grad_up, grad_down = (
        grad_in * factor,
        grad_out * factor,
        grad_up * factor,
        grad_down * factor,
    )
    grad_gain = grad_gain * factor
    pin = update_matrix(
        grad_in,
        project_in,
        project_in_rows,
        project_in_cols,
        project_in_moment,
        project_in_average,
        row_in,
        col_in,
        dp_index,
        mp_index,
    )
    pout = update_matrix(
        grad_out,
        project_out,
        project_out_rows,
        project_out_cols,
        project_out_moment,
        project_out_average,
        row_out,
        col_out,
        mp_index,
        dp_index,
    )
    pexp = update_matrix(
        grad_up,
        expand,
        expand_rows,
        expand_cols,
        expand_moment,
        expand_average,
        row_up,
        col_up,
        dp_index,
        mp_index,
    )
    pcon = update_matrix(
        grad_down,
        contract,
        contract_rows,
        contract_cols,
        contract_moment,
        contract_average,
        row_down,
        col_down,
        mp_index,
        dp_index,
    )
    square_new = DECAY * norm_gains_square + (1.0 - DECAY) * (grad_gain * grad_gain + EPS_STAT)
    stepped = grad_gain * lax.rsqrt(square_new)
    moment_new = MOMENTUM * norm_gains_moment + stepped
    gains_new = norm_gains - RATE_GAIN * (MOMENTUM * moment_new + stepped)
    average_new = AVERAGE * norm_gains_average + (1.0 - AVERAGE) * gains_new
    return (
        decoder_out,
        encoder_in_grad,
        decoder_in_grad,
        grad_norm,
        pin[0],
        pin[1],
        pin[2],
        pin[3],
        pin[4],
        pin[5],
        pin[6],
        pout[0],
        pout[1],
        pout[2],
        pout[3],
        pout[4],
        pout[5],
        pout[6],
        pexp[0],
        pexp[1],
        pexp[2],
        pexp[3],
        pexp[4],
        pexp[5],
        pexp[6],
        pcon[0],
        pcon[1],
        pcon[2],
        pcon[3],
        pcon[4],
        pcon[5],
        pcon[6],
        grad_gain,
        square_new,
        moment_new,
        gains_new,
        average_new,
        gains_new.astype(jnp.bfloat16),
    )


def solution(mesh):
    placed = (
        P("dp", None),
        P("dp", None),
        P("dp", None),
        P("dp", None),
        P("dp"),
        P("dp"),
        P(None, None, "dp", "mp"),
        P(),
        P(),
        P(None, None, "dp", "mp"),
        P(None, None, "dp", "mp"),
        P(None, "mp", "dp"),
        P(),
        P(),
        P(None, "mp", "dp"),
        P(None, "mp", "dp"),
        P(None, "dp", "mp"),
        P(),
        P(),
        P(None, "dp", "mp"),
        P(None, "dp", "mp"),
        P(None, "mp", "dp"),
        P(),
        P(),
        P(None, "mp", "dp"),
        P(None, "mp", "dp"),
        P(None, "dp"),
        P(None, "dp"),
        P(None, "dp"),
        P(None, "dp"),
    )
    return jax.shard_map(
        functools.partial(on_device, (mesh.shape["dp"], mesh.shape["mp"])),
        mesh=mesh,
        in_specs=placed,
        out_specs=(
            P("dp", None),
            P("dp", None),
            P("dp", None),
            P(),
            P(None, None, "dp", "mp"),
            P(),
            P(),
            P(None, None, "dp", "mp"),
            P(None, None, "dp", "mp"),
            P(None, None, "dp", "mp"),
            P(None, None, "dp", "mp"),
            P(None, "mp", "dp"),
            P(),
            P(),
            P(None, "mp", "dp"),
            P(None, "mp", "dp"),
            P(None, "mp", "dp"),
            P(None, "mp", "dp"),
            P(None, "dp", "mp"),
            P(),
            P(),
            P(None, "dp", "mp"),
            P(None, "dp", "mp"),
            P(None, "dp", "mp"),
            P(None, "dp", "mp"),
            P(None, "mp", "dp"),
            P(),
            P(),
            P(None, "mp", "dp"),
            P(None, "mp", "dp"),
            P(None, "mp", "dp"),
            P(None, "mp", "dp"),
            P(None, "dp"),
            P(None, "dp"),
            P(None, "dp"),
            P(None, "dp"),
            P(None, "dp"),
            P(None, "dp"),
        ),
        check_vma=False,
    )
```

```python
import functools

import jax
import jax.numpy as jnp
from jax import lax
from jax.experimental import pallas as pl
from jax.experimental.pallas import tpu as pltpu
from jax.sharding import PartitionSpec as P

D = 768
HEAD_DIM = 64
FF = 3072
PATCHES = 196
SUFFIX = 32
ENC_LEN = 228


EPS_NORM = 1e-06
EPS_STAT = 1e-30
DECAY = 0.99
MOMENTUM = 0.9
AVERAGE = 0.6
RATE_MATRIX = 0.004
RATE_GAIN = 0.05
MASKED = -1000000000.0


LOW = jnp.bfloat16
F32 = jnp.float32
VMEM_LIMIT = 56 * 1024 * 1024
LONG = (ENC_LEN + 7) // 8 * 8
EXACT = lax.Precision.HIGHEST


def dot(left, right, contract):
    return lax.dot_general(left, right, (contract, ((), ())), preferred_element_type=F32)


def mm(left, right):
    return dot(left, right, ((1,), (0,)))


def mm_t(left, right):
    return dot(left, right, ((1,), (1,)))


def t_mm(left, right):
    return dot(left, right, ((0,), (0,)))


def rms_scale(value):
    return lax.rsqrt(jnp.mean(value * value, -1, keepdims=True) + EPS_NORM)


def softmax(scores):
    expons = jnp.exp(scores - jnp.max(scores, -1, keepdims=True))
    return expons / jnp.sum(expons, -1, keepdims=True)


def gelu_parts(upper):
    inner = 0.7978845608028654 * (upper + 0.044715 * upper * upper * upper)
    bent = jnp.tanh(inner)
    value = 0.5 * upper * (1.0 + bent)
    slope = 0.5 * (1.0 + bent) + 0.5 * upper * (1.0 - bent * bent) * 0.7978845608028654 * (
        1.0 + 3.0 * 0.044715 * upper * upper
    )
    return value, slope


class Weight:
    def __init__(self, arrays, first=0, count=1):
        self.arrays, self.first, self.count = tuple(arrays), first, count


class Plan:
    def __init__(self, dp_n, block, width, hidden, pairs):
        self.dp_n, self.block, self.width, self.hidden, self.pairs = dp_n, block, width, hidden, pairs
        self.half = pairs // 2
        self.heads = width // HEAD_DIM
        self.direct = dp_n == 8

    def weight_specs(self, pieces):
        specs = []
        for item in pieces.arrays:
            lead = item.shape[:-3]
            shape = lead + (pieces.count,) + item.shape[-2:]
            at = (0,) * len(lead) + (pieces.first // pieces.count, 0, 0)
            specs.append(pl.BlockSpec(shape, lambda *_, at=at: at))
        return specs

    def weight_scratch(self, pieces, count):
        return [pltpu.VMEM((count, D, D), LOW)]

    def assemble(self, meta, pieces, refs, scratch):
        if not self.direct:
            scratch[...] = refs[0][...]
            return
        for ref, places in zip(refs, ((0, 4), (2, 6), (1, 5), (3, 7))):
            for index, place in enumerate(places):
                row = pl.multiple_of(jnp.bitwise_xor(meta[0], place) * self.block, 32)
                scratch[:, pl.ds(row, self.block), :] = ref[index, :, : self.block]

    def grad_shapes(self, count):
        if not self.direct:
            return [jax.ShapeDtypeStruct((count, D, D), F32)]
        shape = (self.dp_n // 2, count, self.block, D)
        return [jax.ShapeDtypeStruct(shape, LOW), jax.ShapeDtypeStruct(shape, F32)]

    def emit(self, meta, acc, refs):
        if not self.direct:
            refs[0][...] = acc[...]
            return
        for index in range(self.dp_n // 2):
            here = pl.multiple_of(jnp.bitwise_xor(meta[0], 2 * index) * self.block, 32)
            away = pl.multiple_of(jnp.bitwise_xor(meta[0], 2 * index + 1) * self.block, 32)
            for count in range(acc.shape[0]):
                refs[0][index, count] = acc[count, pl.ds(away, self.block), :].astype(LOW)
                refs[1][index, count] = acc[count, pl.ds(here, self.block), :]


def whole(shape):
    return pl.BlockSpec(shape, lambda *_: (0,) * len(shape))


def own_spec(count, base, shape):
    return pl.BlockSpec(
        (1,) + shape, lambda p, _: (base + jnp.maximum(p - count, 0),) + (0,) * len(shape)
    )


def oth_spec(count, base, shape):
    return pl.BlockSpec(
        (1,) + shape, lambda p, _: (base + jnp.minimum(p, count - 1),) + (0,) * len(shape)
    )


def step_spec(shape):
    return pl.BlockSpec((1,) + shape, lambda p, _: (p,) + (0,) * len(shape))


def call(name, body, grid, meta, inputs, in_specs, outs, out_specs, scratch):
    return pl.pallas_call(
        body,
        name=name,
        out_shape=outs,
        grid_spec=pltpu.PrefetchScalarGridSpec(
            num_scalar_prefetch=1,
            grid=grid,
            in_specs=in_specs,
            out_specs=out_specs,
            scratch_shapes=scratch,
        ),
        cost_estimate=pl.CostEstimate(flops=1, transcendentals=0, bytes_accessed=1),
        compiler_params=pltpu.CompilerParams(
            dimension_semantics=("arbitrary",) * len(grid), vmem_limit_bytes=VMEM_LIMIT
        ),
    )(meta, *inputs)


def key_mask(meta, pairs, slot):
    place = lax.broadcasted_iota(jnp.int32, (1, ENC_LEN), 1)
    image, prefix = meta[1 + slot], meta[1 + pairs + slot]
    return (place < image * PATCHES) | ((place >= PATCHES) & (place < PATCHES + prefix))


def attend_heads(plan, queries, keys, values, allowed):
    mixed = []
    for head in range(plan.heads):
        cut = slice(head * HEAD_DIM, (head + 1) * HEAD_DIM)
        scores = jnp.where(allowed, mm_t(queries[:, cut], keys[:, cut]) * 0.125, MASKED)
        mixed.append(mm(softmax(scores).astype(LOW), values[:, cut]).astype(LOW))
    return jnp.concatenate(mixed, 1)


def attend_heads_back(plan, queries, keys, values, allowed, grad_mixed):
    grads = ([], [], [])
    for head in range(plan.heads):
        cut = slice(head * HEAD_DIM, (head + 1) * HEAD_DIM)
        query, key, value, grad = queries[:, cut], keys[:, cut], values[:, cut], grad_mixed[:, cut]
        probs = softmax(jnp.where(allowed, mm_t(query, key) * 0.125, MASKED))
        grad_probs = mm_t(grad, value)
        inner = jnp.sum(grad_probs * probs, -1, keepdims=True)
        grad_scores = (probs * (grad_probs - inner)).astype(LOW)
        grads[0].append((mm(grad_scores, key) * 0.125).astype(LOW))
        grads[1].append((t_mm(grad_scores, query) * 0.125).astype(LOW))
        grads[2].append(t_mm(probs.astype(LOW), grad).astype(LOW))
    return tuple(jnp.concatenate(item, 1) for item in grads)


def slot_of(plan, count, base, step):
    return jnp.where(step < count, plan.half + base + step, base + step - count)


def pick(step, count, own, oth, rows):
    return jnp.where(step < count, oth[0, :rows], own[0, :rows])


def put(step, count, own, oth, value):
    @pl.when(step < count)
    def _():
        oth[0, : value.shape[0]] = value

    @pl.when(step >= count)
    def _():
        own[0, : value.shape[0]] = value


def encoder_attention(plan, meta, own, oth, gain, pieces, base, count):
    w3 = 3 * plan.width
    n = len(pieces.arrays)

    def body(meta, own_ref, oth_ref, gain_ref, *rest):
        refs, (own_out, oth_out, kept, weight) = rest[:n], rest[n:]
        step = pl.program_id(0)

        @pl.when(step == 0)
        def _():
            plan.assemble(meta, pieces, refs, weight)

        value = pick(step, count, own_ref, oth_ref, ENC_LEN).astype(F32)
        normed = (value * rms_scale(value) * gain_ref[...]).astype(LOW)
        joined = mm(normed, weight[0, :, :w3]).astype(LOW)
        allowed = key_mask(meta, plan.pairs, slot_of(plan, count, base, step))
        width = plan.width
        mixed = attend_heads(
            plan, joined[:, :width], joined[:, width : 2 * width], joined[:, 2 * width :], allowed
        )
        kept[0, :, :w3] = joined
        kept[0, :, w3:] = mixed
        put(step, count, own_out, oth_out, mm_t(mixed, weight[0, :, w3:]).astype(LOW))

    rows = (LONG, D)
    return call(
        "encoder_attention",
        body,
        (2 * count,),
        meta,
        (own, oth, gain, *pieces.arrays),
        [own_spec(count, base, rows), oth_spec(count, base, rows), whole((1, D)), *plan.weight_specs(pieces)],
        [jax.ShapeDtypeStruct((count,) + rows, LOW)] * 2
        + [jax.ShapeDtypeStruct((2 * count, ENC_LEN, w3 + plan.width), LOW)],
        [own_spec(count, 0, rows), oth_spec(count, 0, rows), step_spec((ENC_LEN, w3 + plan.width))],
        plan.weight_scratch(pieces, 1),
    )


def encoder_attention_back(plan, meta, own, oth, gain, pieces, kept, grad_own, grad_oth):
    count = plan.half
    width, w3 = plan.width, 3 * plan.width
    n = len(pieces.arrays)

    def body(meta, own_ref, oth_ref, gain_ref, kept_ref, grad_own_ref, grad_oth_ref, *rest):
        refs, (own_out, oth_out), grad_refs = rest[:n], rest[n : n + 2], rest[n + 2 : -2]
        weight, acc = rest[-2:]
        step = pl.program_id(0)

        @pl.when(step == 0)
        def _():
            plan.assemble(meta, pieces, refs, weight)
            acc[...] = jnp.zeros_like(acc)

        value = pick(step, count, own_ref, oth_ref, ENC_LEN).astype(F32)
        normed = (value * rms_scale(value) * gain_ref[...]).astype(LOW)
        grad = pick(step, count, grad_own_ref, grad_oth_ref, ENC_LEN)
        allowed = key_mask(meta, plan.pairs, slot_of(plan, count, 0, step))
        grad_mixed = mm(grad, weight[0, :, w3:]).astype(LOW)
        acc[0, :, w3:] += t_mm(grad, kept_ref[0, :, w3:])
        joined = kept_ref[0, :, :w3]
        grads = attend_heads_back(
            plan, joined[:, :width], joined[:, width : 2 * width], joined[:, 2 * width :], allowed, grad_mixed
        )
        together = jnp.concatenate(grads, 1)
        acc[0, :, :w3] += t_mm(normed, together)
        put(step, count, own_out, oth_out, mm_t(together, weight[0, :, :w3]).astype(LOW))

        @pl.when(step == 2 * count - 1)
        def _():
            plan.emit(meta, acc, grad_refs)

    rows = (LONG, D)
    shapes = plan.grad_shapes(1)
    pair_specs = [own_spec(count, 0, rows), oth_spec(count, 0, rows)]
    return call(
        "encoder_attention_back",
        body,
        (2 * count,),
        meta,
        (own, oth, gain, kept, grad_own, grad_oth, *pieces.arrays),
        [*pair_specs, whole((1, D)), step_spec(kept.shape[1:]), *pair_specs, *plan.weight_specs(pieces)],
        [jax.ShapeDtypeStruct((count,) + rows, LOW)] * 2 + shapes,
        [*pair_specs, *[whole(item.shape) for item in shapes]],
        plan.weight_scratch(pieces, 1) + [pltpu.VMEM((1, D, D), F32)],
    )


def encoder_feed(plan, meta, own, oth, pieces, base, count):
    n = len(pieces.arrays)

    def body(meta, own_ref, oth_ref, *rest):
        refs, (own_out, oth_out, weight) = rest[:n], rest[n:]
        step = pl.program_id(0)

        @pl.when(step == 0)
        def _():
            plan.assemble(meta, pieces, refs, weight)

        normed = pick(step, count, own_ref, oth_ref, ENC_LEN)
        active = gelu_parts(mm(normed, weight[0]))[0].astype(LOW)
        put(step, count, own_out, oth_out, mm_t(active, weight[1]).astype(LOW))

    rows = (LONG, D)
    return call(
        "encoder_feed",
        body,
        (2 * count,),
        meta,
        (own, oth, *pieces.arrays),
        [own_spec(count, base, rows), oth_spec(count, base, rows), *plan.weight_specs(pieces)],
        [jax.ShapeDtypeStruct((count,) + rows, LOW)] * 2,
        [own_spec(count, 0, rows), oth_spec(count, 0, rows)],
        plan.weight_scratch(pieces, 2),
    )


def encoder_feed_back(plan, meta, own, oth, grad_own, grad_oth, pieces):
    n = len(pieces.arrays)
    count = plan.half

    def body(meta, own_ref, oth_ref, grad_own_ref, grad_oth_ref, *rest):
        refs, (own_out, oth_out), grad_refs = rest[:n], rest[n : n + 2], rest[n + 2 : -2]
        weight, acc = rest[-2:]
        step = pl.program_id(0)

        @pl.when(step == 0)
        def _():
            plan.assemble(meta, pieces, refs, weight)
            acc[...] = jnp.zeros_like(acc)

        normed = pick(step, count, own_ref, oth_ref, ENC_LEN)
        grad = pick(step, count, grad_own_ref, grad_oth_ref, ENC_LEN)
        active, slope = gelu_parts(mm(normed, weight[0]))
        grad_upper = (slope * mm(grad, weight[1])).astype(LOW)
        put(step, count, own_out, oth_out, mm_t(grad_upper, weight[0]).astype(LOW))
        acc[0] += t_mm(normed, grad_upper)
        acc[1] += t_mm(grad, active.astype(LOW))

        @pl.when(step == 2 * count - 1)
        def _():
            plan.emit(meta, acc, grad_refs)

    rows = (LONG, D)
    shapes = plan.grad_shapes(2)
    pair_specs = [own_spec(count, 0, rows), oth_spec(count, 0, rows)]
    return call(
        "encoder_feed_back",
        body,
        (2 * count,),
        meta,
        (own, oth, grad_own, grad_oth, *pieces.arrays),
        [*pair_specs, *pair_specs, *plan.weight_specs(pieces)],
        [jax.ShapeDtypeStruct((count,) + rows, LOW)] * 2 + shapes,
        [*pair_specs, *[whole(item.shape) for item in shapes]],
        plan.weight_scratch(pieces, 2) + [pltpu.VMEM((2, D, D), F32)],
    )


def self_mask(plan, meta):
    rows = plan.pairs * SUFFIX
    query = lax.broadcasted_iota(jnp.int32, (rows, rows), 0)
    key = lax.broadcasted_iota(jnp.int32, (rows, rows), 1)
    pair = key // SUFFIX
    limit = jnp.zeros_like(key)
    for slot in range(plan.pairs):
        limit = jnp.where(pair == slot, meta[1 + 2 * plan.pairs + slot], limit)
    return (query // SUFFIX == pair) & (key <= query) & (key - pair * SUFFIX < limit)


def decoder_self(plan, meta, rows_in, gain, pieces):
    n = len(pieces.arrays)
    width, w3 = plan.width, 3 * plan.width
    rows = plan.pairs * SUFFIX
    mid = rows // 2

    def body(meta, in_ref, gain_ref, *rest):
        refs, (own_out, oth_out, kept, weight) = rest[:n], rest[n:]
        plan.assemble(meta, pieces, refs, weight)
        value = in_ref[...].astype(F32)
        normed = (value * rms_scale(value) * gain_ref[...]).astype(LOW)
        joined = mm(normed, weight[0, :, :w3]).astype(LOW)
        mixed = attend_heads(
            plan, joined[:, :width], joined[:, width : 2 * width], joined[:, 2 * width :], self_mask(plan, meta)
        )
        kept[:, :w3] = joined
        kept[:, w3:] = mixed
        partial = mm_t(mixed, weight[0, :, w3:]).astype(LOW)
        own_out[...] = partial[:mid]
        oth_out[...] = partial[mid:]

    return call(
        "decoder_self",
        body,
        (1,),
        meta,
        (rows_in, gain, *pieces.arrays),
        [whole((rows, D)), whole((1, D)), *plan.weight_specs(pieces)],
        [jax.ShapeDtypeStruct((mid, D), LOW)] * 2 + [jax.ShapeDtypeStruct((rows, 4 * width), LOW)],
        [whole((mid, D))] * 2 + [whole((rows, 4 * width))],
        plan.weight_scratch(pieces, 1),
    )


def decoder_self_back(plan, meta, rows_in, gain, pieces, kept, grad_own, grad_oth):
    n = len(pieces.arrays)
    width, w3 = plan.width, 3 * plan.width
    rows = plan.pairs * SUFFIX
    mid = rows // 2

    def body(meta, in_ref, gain_ref, kept_ref, grad_own_ref, grad_oth_ref, *rest):
        refs, (own_out, oth_out), grad_refs = rest[:n], rest[n : n + 2], rest[n + 2 : -2]
        weight, acc = rest[-2:]
        plan.assemble(meta, pieces, refs, weight)
        value = in_ref[...].astype(F32)
        normed = (value * rms_scale(value) * gain_ref[...]).astype(LOW)
        grad = jnp.concatenate([grad_own_ref[...], grad_oth_ref[...]], 0)
        grad_mixed = mm(grad, weight[0, :, w3:]).astype(LOW)
        acc[0, :, w3:] = t_mm(grad, kept_ref[:, w3:])
        joined = kept_ref[:, :w3]
        grads = attend_heads_back(
            plan,
            joined[:, :width],
            joined[:, width : 2 * width],
            joined[:, 2 * width :],
            self_mask(plan, meta),
            grad_mixed,
        )
        together = jnp.concatenate(grads, 1)
        acc[0, :, :w3] = t_mm(normed, together)
        partial = mm_t(together, weight[0, :, :w3]).astype(LOW)
        own_out[...] = partial[:mid]
        oth_out[...] = partial[mid:]
        plan.emit(meta, acc, grad_refs)

    shapes = plan.grad_shapes(1)
    return call(
        "decoder_self_back",
        body,
        (1,),
        meta,
        (rows_in, gain, kept, grad_own, grad_oth, *pieces.arrays),
        [whole((rows, D)), whole((1, D)), whole(kept.shape), whole((mid, D)), whole((mid, D)), *plan.weight_specs(pieces)],
        [jax.ShapeDtypeStruct((mid, D), LOW)] * 2 + shapes,
        [whole((mid, D))] * 2 + [whole(item.shape) for item in shapes],
        plan.weight_scratch(pieces, 1) + [pltpu.VMEM((1, D, D), F32)],
    )


def decoder_cross(plan, meta, own, oth, memory_own, memory_oth, pieces):
    n = len(pieces.arrays)
    count = plan.half
    width, w3 = plan.width, 3 * plan.width

    def body(meta, own_ref, oth_ref, memory_own_ref, memory_oth_ref, *rest):
        refs, (own_out, oth_out, kept_query, kept_key, weight) = rest[:n], rest[n:]
        step = pl.program_id(0)

        @pl.when(step == 0)
        def _():
            plan.assemble(meta, pieces, refs, weight)

        normed = pick(step, count, own_ref, oth_ref, SUFFIX)
        memory = pick(step, count, memory_own_ref, memory_oth_ref, ENC_LEN)
        queries = mm(normed, weight[0, :, :width]).astype(LOW)
        both = mm(memory, weight[0, :, width:w3]).astype(LOW)
        allowed = key_mask(meta, plan.pairs, slot_of(plan, count, 0, step))
        mixed = attend_heads(plan, queries, both[:, :width], both[:, width:], allowed)
        kept_query[0, :, :width] = queries
        kept_query[0, :, width:] = mixed
        kept_key[0] = both
        put(step, count, own_out, oth_out, mm_t(mixed, weight[0, :, w3:]).astype(LOW))

    rows, long = (SUFFIX, D), (LONG, D)
    return call(
        "decoder_cross",
        body,
        (2 * count,),
        meta,
        (own, oth, memory_own, memory_oth, *pieces.arrays),
        [
            own_spec(count, 0, rows),
            oth_spec(count, 0, rows),
            own_spec(count, 0, long),
            oth_spec(count, 0, long),
            *plan.weight_specs(pieces),
        ],
        [jax.ShapeDtypeStruct((count,) + rows, LOW)] * 2
        + [
            jax.ShapeDtypeStruct((2 * count, SUFFIX, 2 * width), LOW),
            jax.ShapeDtypeStruct((2 * count, ENC_LEN, 2 * width), LOW),
        ],
        [
            own_spec(count, 0, rows),
            oth_spec(count, 0, rows),
            step_spec((SUFFIX, 2 * width)),
            step_spec((ENC_LEN, 2 * width)),
        ],
        plan.weight_scratch(pieces, 1),
    )


def decoder_cross_back(
    plan, meta, own, oth, memory_own, memory_oth, pieces, kept_query, kept_key, grad_own, grad_oth
):
    n = len(pieces.arrays)
    count = plan.half
    width, w3 = plan.width, 3 * plan.width

    def body(
        meta, own_ref, oth_ref, memory_own_ref, memory_oth_ref, query_ref, key_ref, grad_own_ref, grad_oth_ref, *rest
    ):
        refs, outs, grad_refs = rest[:n], rest[n : n + 4], rest[n + 4 : -2]
        weight, acc = rest[-2:]
        step = pl.program_id(0)

        @pl.when(step == 0)
        def _():
            plan.assemble(meta, pieces, refs, weight)
            acc[...] = jnp.zeros_like(acc)

        normed = pick(step, count, own_ref, oth_ref, SUFFIX)
        memory = pick(step, count, memory_own_ref, memory_oth_ref, ENC_LEN)
        grad = pick(step, count, grad_own_ref, grad_oth_ref, SUFFIX)
        allowed = key_mask(meta, plan.pairs, slot_of(plan, count, 0, step))
        grad_mixed = mm(grad, weight[0, :, w3:]).astype(LOW)
        acc[0, :, w3:] += t_mm(grad, query_ref[0, :, width:])
        both = key_ref[0]
        grad_query, grad_key, grad_value = attend_heads_back(
            plan, query_ref[0, :, :width], both[:, :width], both[:, width:], allowed, grad_mixed
        )
        together = jnp.concatenate([grad_key, grad_value], 1)
        acc[0, :, :width] += t_mm(normed, grad_query)
        acc[0, :, width:w3] += t_mm(memory, together)
        put(step, count, outs[0], outs[1], mm_t(grad_query, weight[0, :, :width]).astype(LOW))
        put(step, count, outs[2], outs[3], mm_t(together, weight[0, :, width:w3]).astype(LOW))

        @pl.when(step == 2 * count - 1)
        def _():
            plan.emit(meta, acc, grad_refs)

    rows, long = (SUFFIX, D), (LONG, D)
    shapes = plan.grad_shapes(1)
    row_specs = [own_spec(count, 0, rows), oth_spec(count, 0, rows)]
    long_specs = [own_spec(count, 0, long), oth_spec(count, 0, long)]
    return call(
        "decoder_cross_back",
        body,
        (2 * count,),
        meta,
        (own, oth, memory_own, memory_oth, kept_query, kept_key, grad_own, grad_oth, *pieces.arrays),
        [
            *row_specs,
            *long_specs,
            step_spec(kept_query.shape[1:]),
            step_spec(kept_key.shape[1:]),
            *row_specs,
            *plan.weight_specs(pieces),
        ],
        [jax.ShapeDtypeStruct((count,) + rows, LOW)] * 2
        + [jax.ShapeDtypeStruct((count,) + long, LOW)] * 2
        + shapes,
        [*row_specs, *long_specs, *[whole(item.shape) for item in shapes]],
        plan.weight_scratch(pieces, 1) + [pltpu.VMEM((1, D, D), F32)],
    )


def decoder_feed(plan, meta, own, oth, grad_in, pieces):
    n = len(pieces.arrays)
    rows = plan.pairs * SUFFIX
    mid = rows // 2

    def body(meta, own_ref, oth_ref, grad_ref, *rest):
        refs, (own_out, oth_out), grad_refs = rest[:n], rest[n : n + 2], rest[n + 2 : -2]
        weight, acc = rest[-2:]
        plan.assemble(meta, pieces, refs, weight)
        normed = jnp.concatenate([own_ref[...], oth_ref[...]], 0)
        grad = grad_ref[...]
        active, slope = gelu_parts(mm(normed, weight[0]))
        active = active.astype(LOW)
        partial = mm_t(active, weight[1]).astype(LOW)
        grad_upper = (slope * mm(grad, weight[1])).astype(LOW)
        back = mm_t(grad_upper, weight[0]).astype(LOW)
        own_out[0] = partial[:mid]
        own_out[1] = back[:mid]
        oth_out[0] = partial[mid:]
        oth_out[1] = back[mid:]
        acc[0] = t_mm(normed, grad_upper)
        acc[1] = t_mm(grad, active)
        plan.emit(meta, acc, grad_refs)

    shapes = plan.grad_shapes(2)
    return call(
        "decoder_feed",
        body,
        (1,),
        meta,
        (own, oth, grad_in, *pieces.arrays),
        [whole((mid, D))] * 2 + [whole((rows, D)), *plan.weight_specs(pieces)],
        [jax.ShapeDtypeStruct((2, mid, D), LOW)] * 2 + shapes,
        [whole((2, mid, D))] * 2 + [whole(item.shape) for item in shapes],
        plan.weight_scratch(pieces, 2) + [pltpu.VMEM((2, D, D), F32)],
    )


def add_norm(meta, name, base, first, second, gain):
    def body(meta, base_ref, first_ref, second_ref, gain_ref, sum_ref, norm_ref):
        value = base_ref[...].astype(F32) + (first_ref[...].astype(F32) + second_ref[...].astype(F32))
        sum_ref[...] = value
        norm_ref[...] = (value * rms_scale(value) * gain_ref[...]).astype(LOW)

    shape = base.shape
    part = (1,) + shape[1:] if len(shape) == 3 else shape
    spec = (
        pl.BlockSpec(part, lambda p, _: (p, 0, 0)) if len(shape) == 3 else whole(shape)
    )
    return call(
        name,
        body,
        (shape[0] if len(shape) == 3 else 1,),
        meta,
        (base, first, second, gain),
        [spec, spec, spec, whole((1, D))],
        [jax.ShapeDtypeStruct(shape, F32), jax.ShapeDtypeStruct(shape, LOW)],
        [spec, spec],
        [],
    )


def norm_back(meta, name, inputs, gain, grad, first, second, want_low):
    def body(meta, in_ref, gain_ref, grad_ref, first_ref, second_ref, *outs):
        value = in_ref[...].astype(F32)
        scale = rms_scale(value)
        unit = value * scale
        back = first_ref[...].astype(F32) + second_ref[...].astype(F32)
        product = back * unit
        real = product[0, :ENC_LEN] if value.ndim == 3 else product
        part = jnp.sum(real, 0, keepdims=True)
        weighted = product * gain_ref[...]
        total = grad_ref[...].astype(F32) + scale * (
            back * gain_ref[...] - unit * jnp.mean(weighted, -1, keepdims=True)
        )
        outs[0][...] = total
        if want_low:
            outs[1][...] = total.astype(LOW)
        step = pl.program_id(0)

        @pl.when(step == 0)
        def _():
            outs[-1][...] = part

        @pl.when(step > 0)
        def _():
            outs[-1][...] += part

    shape = inputs.shape
    part = (1,) + shape[1:] if len(shape) == 3 else shape
    spec = pl.BlockSpec(part, lambda p, _: (p, 0, 0)) if len(shape) == 3 else whole(shape)
    return call(
        name,
        body,
        (shape[0] if len(shape) == 3 else 1,),
        meta,
        (inputs, gain, grad, first, second),
        [spec, whole((1, D)), spec, spec, spec],
        [jax.ShapeDtypeStruct(shape, F32)]
        + [jax.ShapeDtypeStruct(shape, LOW)] * want_low
        + [jax.ShapeDtypeStruct((1, D), F32)],
        [spec] * (1 + want_low) + [whole((1, D))],
        [],
    )


def fold(plan, meta, keeps, mores, split):
    n = len(keeps)
    counts = [item.shape[1] for item in keeps]
    total = sum(counts)
    tail = keeps[0].shape[2:]
    blocks = keeps[0].shape[0]

    def body(meta, *rest):
        keep_refs, more_refs, outs = rest[:n], rest[n : 2 * n], rest[2 * n :]
        for index in range(blocks):
            start = 0
            out, at = split(index)
            for keep_ref, more_ref, count in zip(keep_refs, more_refs, counts):
                value = keep_ref[index] + more_ref[index].astype(F32)
                outs[out][at, start : start + count] = value.astype(outs[out].dtype)
                start += count

    places = [split(index) for index in range(blocks)]
    outs = [
        jax.ShapeDtypeStruct((sum(place[0] == out for place in places), total) + tail, LOW if out else F32)
        for out in range(1 + max(place[0] for place in places))
    ]
    return call(
        "fold",
        body,
        (1,),
        meta,
        (*keeps, *mores),
        [whole(item.shape) for item in (*keeps, *mores)],
        outs,
        [whole(item.shape) for item in outs],
        [],
    )


def halves(index):
    return index % 2, index // 2


def apart(index):
    return index, 0


def one_hot(rows, offset):
    row = lax.broadcasted_iota(jnp.int32, (rows, D), 0)
    lane = lax.broadcasted_iota(jnp.int32, (rows, D), 1)
    return (lane == row + offset).astype(F32)


def collect(plan, meta, pieces, attention):
    count = pieces[0].shape[-3]
    n = len(pieces)
    shape = pieces[0].shape[-3:]
    groups = D // plan.width

    def body(meta, *rest):
        refs, (out, tile_out) = rest[:n], rest[n:]
        dp_at, mp_at = meta[0], meta[1 + 3 * plan.pairs]
        group = lax.broadcasted_iota(jnp.int32, (8, D), 1) // plan.width
        row = lax.broadcasted_iota(jnp.int32, (8, D), 0)
        place = one_hot(plan.block, dp_at * plan.block)
        for index in range(count):
            value = refs[0][0, index]
            for ref in refs[1:]:
                value = value + ref[0, index].astype(F32)
            out[index] = value
            square = value * value
            lanes = jnp.broadcast_to(jnp.sum(square, 0, keepdims=True), (8, D))
            if attention:
                mask = (group == row).astype(F32)
            else:
                mask = (row == 0).astype(F32)
            sums = lax.dot_general(
                mask, square, (((1,), (1,)), ((), ())), precision=EXACT, preferred_element_type=F32
            )
            tile = lax.dot_general(
                sums, place, (((1,), (0,)), ((), ())), precision=EXACT, preferred_element_type=F32
            )
            if attention:
                spread = jnp.zeros_like(tile)
                for part in range(groups):
                    shift = lax.rem(mp_at * plan.width + (D - part * plan.width), D)
                    moved = pltpu.roll(jnp.where(group == part, lanes, 0.0), shift, 1)
                    spread = jnp.where(row == 4 + part, moved, spread)
            else:
                spread = jnp.where(row == 4 + mp_at, lanes, 0.0)
            tile_out[index] = jnp.where(row < 4, tile, spread)

    return call(
        "collect",
        body,
        (1,),
        meta,
        tuple(pieces),
        [whole(item.shape) for item in pieces],
        [jax.ShapeDtypeStruct(shape, F32), jax.ShapeDtypeStruct((count, 8, D), F32)],
        [whole(shape), whole((count, 8, D))],
        [],
    )


def finish(plan, meta, early, late, statistics, gain_state):
    counts = [item.shape for item in statistics]

    def body(meta, early_ref, late_ref, *rest):
        olds, gains = rest[:8], rest[8:12]
        norm_out, news, rates, gain_outs = rest[12], rest[13:21], rest[21], rest[22:]
        tiles = [late_ref[2], early_ref[1], early_ref[0]]
        feeds = [(late_ref[0], late_ref[1]), (early_ref[2], early_ref[3])]
        gain_sum = 0.5 * late_ref[3]
        total = jnp.sum(gain_sum * gain_sum)
        for tile in tiles:
            total = total + jnp.sum(tile[:4])
        for up, down in feeds:
            total = total + jnp.sum(up[:1]) + jnp.sum(down[:1])
        totals = jnp.full((8, D), total, F32)
        norm = jnp.sqrt(totals)
        factor = jnp.minimum(1.0, 1.0 / norm)
        squared = (factor * factor)[:1]
        norm_out[...] = norm[:, :128]
        rates[...] = factor[:, :128]

        def renew(old, sums, number):
            return DECAY * old + (1.0 - DECAY) * (sums * squared / number + EPS_STAT)

        for layer, tile in enumerate(tiles):
            for part in range(3):
                news[0][layer, part : part + 1] = renew(olds[0][layer, part : part + 1], tile[part : part + 1], D)
                news[1][layer, part : part + 1] = renew(
                    olds[1][layer, part : part + 1], tile[4 + part : 5 + part], D
                )
            news[2][layer : layer + 1] = renew(olds[2][layer : layer + 1], tile[7:8], D)
            news[3][layer : layer + 1] = renew(olds[3][layer : layer + 1], tile[3:4], D)
        for layer, (up, down) in enumerate(feeds):
            news[4][layer : layer + 1] = renew(olds[4][layer : layer + 1], up[:1], FF)
            news[7][layer : layer + 1] = renew(olds[7][layer : layer + 1], down[:1], FF)
            for part in range(FF // D):
                cut = slice(part * D, (part + 1) * D)
                news[5][layer : layer + 1, cut] = renew(
                    olds[5][layer : layer + 1, cut], up[4 + part : 5 + part], D
                )
                news[6][layer : layer + 1, cut] = renew(
                    olds[6][layer : layer + 1, cut], down[4 + part : 5 + part], D
                )
        shift = lax.rem(D - meta[0] * plan.block, D)
        grad = (pltpu.roll(gain_sum, shift, 1) * factor)[:5, : plan.block]
        master, square, moment, average = [item[...] for item in gains]
        square_new = DECAY * square + (1.0 - DECAY) * (grad * grad + EPS_STAT)
        stepped = grad * lax.rsqrt(square_new)
        moment_new = MOMENTUM * moment + stepped
        master_new = master - RATE_GAIN * (MOMENTUM * moment_new + stepped)
        values = (
            grad,
            square_new,
            moment_new,
            master_new,
            AVERAGE * average + (1.0 - AVERAGE) * master_new,
            master_new,
        )
        for out, value in zip(gain_outs, values):
            out[...] = value.astype(out.dtype)

    small = gain_state[0].shape
    outs = (
        [jax.ShapeDtypeStruct((8, 128), F32)]
        + [jax.ShapeDtypeStruct(shape, F32) for shape in counts]
        + [jax.ShapeDtypeStruct((8, 128), F32)]
        + [jax.ShapeDtypeStruct(small, F32)] * 5
        + [jax.ShapeDtypeStruct(small, LOW)]
    )
    inputs = (early, late, *statistics, *gain_state)
    return call(
        "finish",
        body,
        (1,),
        meta,
        inputs,
        [whole(item.shape) for item in inputs],
        outs,
        [whole(item.shape) for item in outs],
        [],
    )


def step_values(grad, scale, master, moment, average):
    stepped = grad * scale
    moment_new = MOMENTUM * moment + stepped
    master_new = master - RATE_MATRIX * (MOMENTUM * moment_new + stepped)
    return grad, moment_new, master_new, AVERAGE * average + (1.0 - AVERAGE) * master_new


def exact(left, right, contract):
    return lax.dot_general(left, right, (contract, ((), ())), precision=EXACT, preferred_element_type=F32)


def update_attention(plan, meta, rates, grads, rows_in, cols_in, rows_out, cols_out, state_in, state_out):
    width, block = plan.width, plan.block

    def body(meta, rates_ref, grad_a, grad_b, rin, cin, rout, cout, *rest):
        ins, outs = rest[:6], rest[6:]
        layer = pl.program_id(0)
        dp_at, mp_at = meta[0], meta[1 + 3 * plan.pairs]
        grad = jnp.where(layer == 0, grad_a[0], jnp.where(layer == 1, grad_b[1], grad_b[0]))
        grad = grad * rates_ref[:1, :1]
        local = one_hot(block, dp_at * block)
        means = jnp.mean(rin[0], -1, keepdims=True)
        row_scale = lax.rsqrt(exact(local, rin[0] / means, ((1,), (1,))))
        shift = lax.rem(D - mp_at * width, D)
        col_scale = lax.rsqrt(pltpu.roll(jnp.concatenate([cin[0]] * 3, 0)[:8], shift, 1)[:3, :width])
        for part in range(3):
            values = step_values(
                grad[:, part * width : (part + 1) * width],
                row_scale[:, part : part + 1] * col_scale[part : part + 1],
                ins[0][0, part],
                ins[1][0, part],
                ins[2][0, part],
            )
            for out, value in zip(outs[:4], values):
                out[0, part] = value
            outs[4][0, part] = values[2].astype(LOW)
        turned = jnp.transpose(grad[:, 3 * width :])
        row, col = rout[pl.ds(layer, 1), :], cout[pl.ds(layer, 1), :]
        mean = jnp.mean(row, -1, keepdims=True)
        row_scale = lax.rsqrt(
            exact(one_hot(width, mp_at * width), jnp.broadcast_to(row / mean, (8, D)), ((1,), (1,)))
        )[:, :1]
        shift = lax.rem(D - dp_at * block, D)
        col_scale = lax.rsqrt(pltpu.roll(jnp.broadcast_to(col, (8, D)), shift, 1)[:1, :block])
        values = step_values(turned, row_scale * col_scale, ins[3][0], ins[4][0], ins[5][0])
        for out, value in zip(outs[5:9], values):
            out[0] = value
        outs[9][0] = values[2].astype(LOW)

    def spec(shape):
        return pl.BlockSpec((1,) + shape, lambda p, _: (p,) + (0,) * len(shape))

    shape_in, shape_out = (3, block, width), (width, block)
    outs = (
        [jax.ShapeDtypeStruct((3,) + shape_in, F32)] * 4
        + [jax.ShapeDtypeStruct((3,) + shape_in, LOW)]
        + [jax.ShapeDtypeStruct((3,) + shape_out, F32)] * 4
        + [jax.ShapeDtypeStruct((3,) + shape_out, LOW)]
    )
    return call(
        "update_attention",
        body,
        (3,),
        meta,
        (rates, *grads, rows_in, cols_in, rows_out, cols_out, *state_in, *state_out),
        [whole((8, 128)), whole((1, block, D)), whole((2, block, D))]
        + [spec((3, D)), spec((3, D)), whole((3, D)), whole((3, D))]
        + [spec(shape_in)] * 3
        + [spec(shape_out)] * 3,
        outs,
        [spec(shape_in)] * 5 + [spec(shape_out)] * 5,
        [],
    )


def update_feed(plan, meta, rates, grads, rows_up, cols_up, rows_down, cols_down, state_up, state_down):
    hidden, block = plan.hidden, plan.block

    def body(meta, rates_ref, grad_a, grad_b, rup, cup, rdown, cdown, *rest):
        ins, outs = rest[:6], rest[6:]
        layer = pl.program_id(0)
        local = one_hot(block, meta[0] * block)
        lanes = pl.ds(pl.multiple_of(meta[1 + 3 * plan.pairs] * hidden, 128), hidden)
        one = pl.ds(layer, 1)
        mean_up = jnp.mean(rup[one, :], -1, keepdims=True)
        mean_down = jnp.mean(rdown[one, :], -1, keepdims=True)
        along = (rup[one, :] / mean_up, cdown[one, :])
        across = (cup[one, lanes], rdown[one, lanes] / mean_down)
        for part in range(2):
            grad = jnp.where(layer == 0, grad_a[part], grad_b[part]) * rates_ref[:1, :1]
            row_scale = lax.rsqrt(exact(local, jnp.broadcast_to(along[part], (8, D)), ((1,), (1,))))[:, :1]
            values = step_values(
                grad,
                row_scale * lax.rsqrt(across[part]),
                ins[3 * part][0],
                ins[3 * part + 1][0],
                ins[3 * part + 2][0],
            )
            for out, value in zip(outs[5 * part : 5 * part + 4], values):
                out[0] = value
            outs[5 * part + 4][0] = values[2].astype(LOW)

    state = pl.BlockSpec((1, block, hidden), lambda p, _: (p, 0, 0))
    outs = ([jax.ShapeDtypeStruct((2, block, hidden), F32)] * 4 + [jax.ShapeDtypeStruct((2, block, hidden), LOW)]) * 2
    values = call(
        "update_feed",
        body,
        (2,),
        meta,
        (
            rates,
            *grads,
            rows_up,
            cols_up,
            rows_down,
            cols_down,
            *state_up,
            *[item.transpose(0, 2, 1) for item in state_down],
        ),
        [whole((8, 128)), *[whole((2, block, D))] * 2]
        + [whole((2, D)), whole((2, FF)), whole((2, FF)), whole((2, D))]
        + [state] * 6,
        outs,
        [state] * 10,
        [],
    )
    return [*values[:5], *[item.transpose(0, 2, 1) for item in values[5:]]]


def on_device(
    sizes,
    encoder_in,
    decoder_in,
    decoder_cotangent,
    counts,
    prefix_len,
    suffix_len,
    project_in,
    project_in_rows,
    project_in_cols,
    project_in_moment,
    project_in_average,
    project_out,
    project_out_rows,
    project_out_cols,
    project_out_moment,
    project_out_average,
    expand,
    expand_rows,
    expand_cols,
    expand_moment,
    expand_average,
    contract,
    contract_rows,
    contract_cols,
    contract_moment,
    contract_average,
    norm_gains,
    norm_gains_square,
    norm_gains_moment,
    norm_gains_average,
):
    dp_n, mp_n = sizes
    dp_index = lax.axis_index("dp")
    mp_index = lax.axis_index("mp")
    side = mp_index % 2
    pairs = prefix_len.shape[0]
    half = pairs // 2
    width = project_in.shape[-1]
    block = project_in.shape[-2]
    plan = Plan(dp_n, block, width, expand.shape[-1], pairs)
    low, f32 = LOW, F32

    def swap(value, axis, bit):
        count = dp_n if axis == "dp" else mp_n
        return lax.ppermute(value, axis, [(i, i ^ bit) for i in range(count)])

    def bits(count):
        return [1 << i for i in range(count.bit_length() - 1)]

    hold = lax.optimization_barrier

    def widen(own, four):
        two = jnp.stack([own, four])
        return two, swap(two, "dp", 2), swap(two, "dp", 1)

    def scatter(parts, attention):
        summed = lax.psum_scatter(parts[0], "dp", scatter_dimension=1, tiled=True)
        return collect(plan, meta, [summed[None]], attention)

    def total_dp(value):
        for bit in bits(dp_n):
            value = value + swap(value, "dp", bit)
        return value

    def total_all(value):
        for bit in bits(mp_n):
            value = value + swap(value, "mp", bit)
        return total_dp(value)

    def reduce_own(own, oth):
        sent = (own.astype(f32) + swap(oth, "mp", 1).astype(f32)).astype(low)
        for bit in bits(mp_n)[1:-1]:
            sent = (sent.astype(f32) + swap(sent, "mp", bit).astype(f32)).astype(low)
        return sent, swap(sent, "mp", bits(mp_n)[-1])

    def relative(value):
        split = value.reshape((half, 2) + value.shape[1:])
        return (
            lax.dynamic_index_in_dim(split, side, 1, False),
            lax.dynamic_index_in_dim(split, 1 - side, 1, False),
        )

    def absolute(own):
        other = swap(own, "mp", 1)
        even = jnp.where(side == 0, own, other)
        odd = jnp.where(side == 0, other, own)
        return jnp.stack([even, odd], 1).reshape((pairs,) + own.shape[1:])

    def core(value):
        return swap(value, "mp", 1)

    def attention_block(layer):
        return jnp.concatenate(
            [project_in[layer, 0], project_in[layer, 1], project_in[layer, 2], project_out[layer].T], 1
        ).astype(low)[None]

    def feed_block(layer):
        return jnp.stack([expand[layer], contract[layer].T]).astype(low)

    direct = plan.direct
    own_a = attention_block(0)
    own_b = feed_block(0)
    own_c = jnp.concatenate([attention_block(1), attention_block(2)], 0)
    own_d = feed_block(1)
    gain_full = lax.dynamic_update_slice(
        jnp.zeros((8, D), low), norm_gains.astype(low), (0, dp_index * block)
    )
    if direct:
        own_a = jnp.concatenate([own_a, gain_full[None]], 1)
        four, own_b = hold((swap(own_a, "dp", 4), own_b))
        two, far, side_one = widen(own_a, four)
        four_b = swap(own_b, "dp", 4)
        far, side_one = hold((far, side_one))
        arrays = (two, far, side_one, swap(far, "dp", 1))
        gain_rows = sum(jnp.sum(item[:, 0, block:].astype(f32), 0) for item in arrays)
    else:
        arrays = [lax.all_gather(own_a, "dp", axis=1, tiled=True)]
        gain_rows = total_dp(gain_full).astype(f32)
    gains = [gain_rows[i : i + 1] for i in range(5)]

    place_rel = jnp.concatenate([2 * jnp.arange(half) + side, 2 * jnp.arange(half) + 1 - side])
    prefix_rel = jnp.concatenate(relative(prefix_len))
    suffix_rel = jnp.concatenate(relative(suffix_len))
    images = place_rel < counts[0, 0]
    active = place_rel < counts[0, 0] + counts[0, 1]
    meta = jnp.concatenate(
        [
            dp_index[None].astype(jnp.int32),
            images.astype(jnp.int32),
            prefix_rel,
            suffix_rel,
            mp_index[None].astype(jnp.int32),
        ]
    )
    steps = jnp.arange(SUFFIX)
    live = active[:, None] & (steps[None, :] < suffix_rel[:, None])

    mid = half * SUFFIX
    enc_own, enc_oth = relative(
        jnp.pad(encoder_in.reshape(pairs, ENC_LEN, D), ((0, 0), (0, LONG - ENC_LEN), (0, 0)))
    )
    dec_rel = jnp.concatenate(relative(decoder_in.reshape(pairs, SUFFIX, D))).reshape(2 * mid, D)
    cot = jnp.concatenate(relative(decoder_cotangent.reshape(pairs, SUFFIX, D)))
    cot = jnp.where(live[:, :, None], cot, f32(0.0)).reshape(2 * mid, D)
    cot_low = cot.astype(low)

    def triple(value):
        return value.reshape(half, SUFFIX, D)

    if direct:
        *arrays, four_b, own_c = hold((*arrays, four_b, own_c))
        two, far, side_one = widen(own_b, four_b)
        four_c = swap(own_c, "dp", 4)
    enc_att = Weight(arrays)
    own, oth, kept_enc = encoder_attention(plan, meta, enc_own, enc_oth, gains[0], enc_att, 0, half)
    if direct:
        own, oth, dec_rel, cot, cot_low = hold((own, oth, dec_rel, cot, cot_low))
    sums = reduce_own(own, oth)
    if direct:
        far, side_one, _ = hold((far, side_one, sums[0]))
        arrays = (two, far, side_one, swap(far, "dp", 1))
    else:
        arrays = [lax.all_gather(own_b, "dp", axis=1, tiled=True)]
    enc_feed = Weight(arrays, 0, 2)
    enc_mid, norm_mid = add_norm(meta, "add_norm_mid", enc_own, *sums, gains[1])
    norm_mid_oth = core(norm_mid)

    if direct:
        norm_mid_oth, four_c, own_d = hold((norm_mid_oth, four_c, own_d))
        two, far, side_one = widen(own_c, four_c)
        four_d = swap(own_d, "dp", 4)
    own, oth = encoder_feed(plan, meta, norm_mid, norm_mid_oth, enc_feed, 0, half)
    sums = reduce_own(own, oth)
    if direct:
        far, side_one, _ = hold((far, side_one, sums[0]))
        arrays = (two, far, side_one, swap(far, "dp", 1))
    else:
        arrays = [lax.all_gather(own_c, "dp", axis=1, tiled=True)]
    if direct:
        *arrays, four_d = hold((*arrays, four_d))
        two, far, side_one = widen(own_d, four_d)
    self_att, cross_att = Weight(arrays, 0), Weight(arrays, 1)

    own, oth, kept_self = decoder_self(plan, meta, dec_rel, gains[2], self_att)
    sums_self = reduce_own(own, oth)
    memory = (enc_mid + (sums[0].astype(f32) + sums[1].astype(f32))).astype(low)
    memory_oth = core(memory)
    dec_one, norm_cross = add_norm(meta, "add_norm_cross", dec_rel[:mid], *sums_self, gains[3])
    norm_cross_oth = core(norm_cross)

    if direct:
        norm_cross_oth, far, side_one = hold((norm_cross_oth, far, side_one))
        arrays = (two, far, side_one, swap(far, "dp", 1))
    cross_in = (triple(norm_cross), triple(norm_cross_oth), memory, memory_oth, cross_att)
    own, oth, *kept_cross = decoder_cross(plan, meta, *cross_in)
    sums = reduce_own(own, oth)
    if not direct:
        arrays = [lax.all_gather(own_d, "dp", axis=1, tiled=True)]
    dec_feed = Weight(arrays, 0, 2)
    dec_two, norm_last = add_norm(
        meta, "add_norm_last", dec_one, sums[0].reshape(mid, D), sums[1].reshape(mid, D), gains[4]
    )

    own, oth, *grads_dec = decoder_feed(plan, meta, norm_last, core(norm_last), cot_low, dec_feed)
    if direct:
        more_dec = swap(grads_dec[0], "dp", 1)
    sums = reduce_own(own, oth)
    out_own = dec_two + (sums[0][0].astype(f32) + sums[1][0].astype(f32))
    grad, grad_low, gain_four = norm_back(
        meta, "norm_back_last", dec_two, gains[4], cot[:mid], sums[0][1], sums[1][1], True
    )

    own, oth, own_long, oth_long, *grads_cross = decoder_cross_back(
        plan, meta, *cross_in, *kept_cross, triple(grad_low), triple(core(grad_low))
    )
    if direct:
        own, oth, own_long, oth_long, more_dec = hold((own, oth, own_long, oth_long, more_dec))
        more_cross = swap(grads_cross[0], "dp", 1)
    sums = reduce_own(own, oth)
    if direct:
        own_long, oth_long, _ = hold((own_long, oth_long, sums[0]))
    sums_enc = reduce_own(own_long, oth_long)
    grad, grad_low, gain_three = norm_back(
        meta, "norm_back_cross", dec_one, gains[3], grad, sums[0].reshape(mid, D), sums[1].reshape(mid, D), True
    )
    grad_low_oth = core(grad_low)
    if direct:
        keep, more_dec, _, grad_low_oth = hold((grads_dec[1], more_dec, sums_enc[0], grad_low_oth))
        keep_dec, away_dec = fold(plan, meta, [keep], [more_dec], halves)

    own_self, oth_self, *grads_self = decoder_self_back(
        plan, meta, dec_rel, gains[2], self_att, kept_self, grad_low, grad_low_oth
    )
    decoder_out = absolute(triple(out_own)).reshape(2 * mid, D)
    if direct:
        *sums_enc, own_self, oth_self, away_dec = hold((*sums_enc, own_self, oth_self, away_dec))
    sums_self = reduce_own(own_self, oth_self)
    grad_enc = sums_enc[0].astype(f32) + sums_enc[1].astype(f32)
    enc_low = grad_enc.astype(low)
    enc_low_oth = core(enc_low)

    if direct:
        enc_low_oth, decoder_out, away_dec, more_cross, away_self = hold(
            (enc_low_oth, decoder_out, away_dec, more_cross, grads_self[0])
        )
        more_self = swap(away_self, "dp", 1)
        more_dec = swap(away_dec, "dp", 2)
    own, oth, *grads_enc = encoder_feed_back(plan, meta, norm_mid, norm_mid_oth, enc_low, enc_low_oth, enc_feed)
    if direct:
        own, oth, more_self, more_dec, *sums_self = hold((own, oth, more_self, more_dec, *sums_self))
        more_enc = swap(grads_enc[0], "dp", 1)
    sums = reduce_own(own, oth)
    if direct:
        keep_cross, keep_self, more_cross, more_self, keep_dec, more_dec, *sums_self, _ = hold(
            (grads_cross[1], grads_self[1], more_cross, more_self, keep_dec, more_dec, *sums_self, sums[0])
        )
        keep_dec, away_dec = fold(plan, meta, [keep_dec], [more_dec], halves)
        more_dec = swap(away_dec, "dp", 4)
        keep_mid, away_mid = fold(plan, meta, [keep_cross, keep_self], [more_cross, more_self], halves)
        more_mid = swap(away_mid, "dp", 2)
    grad, gain_two = norm_back(meta, "norm_back_self", dec_rel[:mid], gains[2], grad, *sums_self, False)
    decoder_in_grad = absolute(triple(grad)).reshape(2 * mid, D)
    if direct:
        *sums, away_mid, away_dec, decoder_in_grad = hold((*sums, away_mid, away_dec, decoder_in_grad))
    grad_enc, enc_low, gain_one = norm_back(
        meta, "norm_back_mid", enc_mid, gains[1], grad_enc, *sums, True
    )
    enc_low_oth = core(enc_low)

    if direct:
        keep_enc, away_enc = fold(plan, meta, [grads_enc[1]], [more_enc], halves)
        enc_low_oth, decoder_in_grad, away_enc, more_dec = hold((enc_low_oth, decoder_in_grad, away_enc, more_dec))
        more_enc = swap(away_enc, "dp", 2)
    own, oth, *grads_att = encoder_attention_back(
        plan, meta, enc_own, enc_oth, gains[0], enc_att, kept_enc, enc_low, enc_low_oth
    )
    if direct:
        more_att = swap(grads_att[0], "dp", 1)
        own, oth, more_mid = hold((own, oth, more_mid))
    sums = reduce_own(own, oth)
    if direct:
        keep_mid, more_mid, keep_enc, keep_dec, _ = hold((keep_mid, more_mid, keep_enc, keep_dec, sums[0]))
        keep_mid, away_mid = fold(plan, meta, [keep_mid], [more_mid], halves)
        more_mid = swap(away_mid, "dp", 4)
        keep_enc, away_enc = fold(plan, meta, [keep_enc], [more_enc], halves)
        more_enc = swap(away_enc, "dp", 4)
        sum_dec = collect(plan, meta, [keep_dec, more_dec], False)
        mine, *others = fold(plan, meta, [grads_att[1]], [more_att], apart)
        mine, *others, more_mid, _ = hold((mine, *others, more_mid, sum_dec[1]))
        pieces_att = [mine] + [swap(item, "dp", 2 * (i + 1)) for i, item in enumerate(others)]
        sum_mid = collect(plan, meta, [keep_mid, more_mid], True)
    else:
        sum_dec = scatter(grads_dec, False)
        sum_mid = [
            jnp.concatenate(item) for item in zip(scatter(grads_cross, True), scatter(grads_self, True))
        ]
    early = total_all(jnp.concatenate([sum_mid[1], sum_dec[1]]))
    grad_enc, gain_zero = norm_back(meta, "norm_back_enc", enc_own, gains[0], grad_enc, *sums, False)
    if direct:
        sum_enc = collect(plan, meta, [keep_enc, more_enc], False)
        sum_att = collect(plan, meta, pieces_att, True)
    else:
        sum_enc = scatter(grads_enc, False)
        sum_att = scatter(grads_att, True)
    encoder_in_grad = absolute(grad_enc)[:, :ENC_LEN].reshape(pairs * ENC_LEN, D)
    gain_tile = jnp.concatenate(
        [gain_zero, gain_one, gain_two, gain_three, gain_four, jnp.zeros((3, D), f32)]
    )[None]
    late = total_all(jnp.concatenate([sum_enc[1], sum_att[1], gain_tile]))
    done = finish(
        plan,
        meta,
        early,
        late,
        (
            project_in_rows,
            project_in_cols,
            project_out_rows,
            project_out_cols,
            expand_rows,
            expand_cols,
            contract_rows,
            contract_cols,
        ),
        (norm_gains, norm_gains_square, norm_gains_moment, norm_gains_average),
    )
    grad_norm, news, rates, pgain = done[0][0, 0], done[1:9], done[9], done[10:]
    att = update_attention(
        plan,
        meta,
        rates,
        (sum_att[0], sum_mid[0]),
        *news[:4],
        (project_in, project_in_moment, project_in_average),
        (project_out, project_out_moment, project_out_average),
    )
    feed = update_feed(
        plan,
        meta,
        rates,
        (sum_enc[0], sum_dec[0]),
        *news[4:],
        (expand, expand_moment, expand_average),
        (contract, contract_moment, contract_average),
    )
    return (
        decoder_out,
        encoder_in_grad,
        decoder_in_grad,
        grad_norm,
        att[0],
        news[0],
        news[1],
        *att[1:5],
        att[5],
        news[2],
        news[3],
        *att[6:10],
        feed[0],
        news[4],
        news[5],
        *feed[1:5],
        feed[5],
        news[6],
        news[7],
        *feed[6:10],
        *pgain,
    )


def solution(mesh):
    placed = (
        P("dp", None),
        P("dp", None),
        P("dp", None),
        P("dp", None),
        P("dp"),
        P("dp"),
        P(None, None, "dp", "mp"),
        P(),
        P(),
        P(None, None, "dp", "mp"),
        P(None, None, "dp", "mp"),
        P(None, "mp", "dp"),
        P(),
        P(),
        P(None, "mp", "dp"),
        P(None, "mp", "dp"),
        P(None, "dp", "mp"),
        P(),
        P(),
        P(None, "dp", "mp"),
        P(None, "dp", "mp"),
        P(None, "mp", "dp"),
        P(),
        P(),
        P(None, "mp", "dp"),
        P(None, "mp", "dp"),
        P(None, "dp"),
        P(None, "dp"),
        P(None, "dp"),
        P(None, "dp"),
    )
    return jax.shard_map(
        functools.partial(on_device, (mesh.shape["dp"], mesh.shape["mp"])),
        mesh=mesh,
        in_specs=placed,
        out_specs=(
            P("dp", None),
            P("dp", None),
            P("dp", None),
            P(),
            P(None, None, "dp", "mp"),
            P(),
            P(),
            P(None, None, "dp", "mp"),
            P(None, None, "dp", "mp"),
            P(None, None, "dp", "mp"),
            P(None, None, "dp", "mp"),
            P(None, "mp", "dp"),
            P(),
            P(),
            P(None, "mp", "dp"),
            P(None, "mp", "dp"),
            P(None, "mp", "dp"),
            P(None, "mp", "dp"),
            P(None, "dp", "mp"),
            P(),
            P(),
            P(None, "dp", "mp"),
            P(None, "dp", "mp"),
            P(None, "dp", "mp"),
            P(None, "dp", "mp"),
            P(None, "mp", "dp"),
            P(),
            P(),
            P(None, "mp", "dp"),
            P(None, "mp", "dp"),
            P(None, "mp", "dp"),
            P(None, "mp", "dp"),
            P(None, "dp"),
            P(None, "dp"),
            P(None, "dp"),
            P(None, "dp"),
            P(None, "dp"),
            P(None, "dp"),
        ),
        check_vma=False,
    )
```

```python
import functools

import jax
import jax.numpy as jnp
from jax import lax
from jax.experimental import pallas as pl
from jax.experimental.pallas import tpu as pltpu
from jax.sharding import PartitionSpec as P

D = 768
HEAD_DIM = 64
FF = 3072
PATCHES = 196
SUFFIX = 32
ENC_LEN = 228


EPS_NORM = 1e-06
EPS_STAT = 1e-30
DECAY = 0.99
MOMENTUM = 0.9
AVERAGE = 0.6
RATE_MATRIX = 0.004
RATE_GAIN = 0.05
MASKED = -1000000000.0


LOW = jnp.bfloat16
F32 = jnp.float32
VMEM_LIMIT = 56 * 1024 * 1024
LONG = (ENC_LEN + 7) // 8 * 8
EXACT = lax.Precision.HIGHEST


def dot(left, right, contract):
    return lax.dot_general(left, right, (contract, ((), ())), preferred_element_type=F32)


def mm(left, right):
    return dot(left, right, ((1,), (0,)))


def mm_t(left, right):
    return dot(left, right, ((1,), (1,)))


def t_mm(left, right):
    return dot(left, right, ((0,), (0,)))


def rms_scale(value):
    return lax.rsqrt(jnp.mean(value * value, -1, keepdims=True) + EPS_NORM)


def softmax(scores):
    expons = jnp.exp(scores - jnp.max(scores, -1, keepdims=True))
    return expons / jnp.sum(expons, -1, keepdims=True)


def gelu_parts(upper):
    inner = 0.7978845608028654 * (upper + 0.044715 * upper * upper * upper)
    bent = jnp.tanh(inner)
    value = 0.5 * upper * (1.0 + bent)
    slope = 0.5 * (1.0 + bent) + 0.5 * upper * (1.0 - bent * bent) * 0.7978845608028654 * (
        1.0 + 3.0 * 0.044715 * upper * upper
    )
    return value, slope


class Plan:
    def __init__(self, dp_n, block, width, hidden, pairs):
        self.dp_n, self.block, self.width, self.hidden, self.pairs = dp_n, block, width, hidden, pairs
        self.half = pairs // 2
        self.heads = width // HEAD_DIM
        self.direct = dp_n == 8

    def weight_specs(self, pieces):
        return [whole(item.shape) for item in flat(pieces)]

    def weight_scratch(self, pieces):
        return [pltpu.VMEM((len(pieces), D, D), LOW)]

    def assemble(self, meta, pieces, refs, scratch):
        refs = iter(refs)
        for count in range(len(pieces)):
            if not self.direct:
                scratch[count] = next(refs)[...]
                continue
            _, height, start = pieces[count]
            for places in ((0, 4), (2, 6), (1, 5), (3, 7)):
                ref = next(refs)
                for index, place in enumerate(places):
                    row = pl.multiple_of(jnp.bitwise_xor(meta[0], place) * self.block, 32)
                    first = start + index * height
                    scratch[count, pl.ds(row, self.block), :] = ref[first : first + self.block]

    def grad_shapes(self, count):
        if not self.direct:
            return [jax.ShapeDtypeStruct((count, D, D), F32)]
        shape = (self.dp_n // 2, count, self.block, D)
        return [jax.ShapeDtypeStruct(shape, LOW), jax.ShapeDtypeStruct(shape, F32)]

    def emit(self, meta, acc, refs):
        if not self.direct:
            refs[0][...] = acc[...]
            return
        for index in range(self.dp_n // 2):
            here = pl.multiple_of(jnp.bitwise_xor(meta[0], 2 * index) * self.block, 32)
            away = pl.multiple_of(jnp.bitwise_xor(meta[0], 2 * index + 1) * self.block, 32)
            for count in range(acc.shape[0]):
                refs[0][index, count] = acc[count, pl.ds(away, self.block), :].astype(LOW)
                refs[1][index, count] = acc[count, pl.ds(here, self.block), :]


def flat(pieces):
    return [item for arrays, _, _ in pieces for item in arrays]


def whole(shape):
    return pl.BlockSpec(shape, lambda *_: (0,) * len(shape))


def own_spec(count, base, shape):
    return pl.BlockSpec(
        (1,) + shape, lambda p, _: (base + jnp.maximum(p - count, 0),) + (0,) * len(shape)
    )


def oth_spec(count, base, shape):
    return pl.BlockSpec(
        (1,) + shape, lambda p, _: (base + jnp.minimum(p, count - 1),) + (0,) * len(shape)
    )


def step_spec(shape):
    return pl.BlockSpec((1,) + shape, lambda p, _: (p,) + (0,) * len(shape))


def call(name, body, grid, meta, inputs, in_specs, outs, out_specs, scratch):
    return pl.pallas_call(
        body,
        name=name,
        out_shape=outs,
        grid_spec=pltpu.PrefetchScalarGridSpec(
            num_scalar_prefetch=1,
            grid=grid,
            in_specs=in_specs,
            out_specs=out_specs,
            scratch_shapes=scratch,
        ),
        cost_estimate=pl.CostEstimate(flops=1, transcendentals=0, bytes_accessed=1),
        compiler_params=pltpu.CompilerParams(
            dimension_semantics=("arbitrary",) * len(grid), vmem_limit_bytes=VMEM_LIMIT
        ),
    )(meta, *inputs)


def key_mask(meta, pairs, slot):
    place = lax.broadcasted_iota(jnp.int32, (1, ENC_LEN), 1)
    image, prefix = meta[1 + slot], meta[1 + pairs + slot]
    return (place < image * PATCHES) | ((place >= PATCHES) & (place < PATCHES + prefix))


def attend_heads(plan, queries, keys, values, allowed):
    mixed = []
    for head in range(plan.heads):
        cut = slice(head * HEAD_DIM, (head + 1) * HEAD_DIM)
        scores = jnp.where(allowed, mm_t(queries[:, cut], keys[:, cut]) * 0.125, MASKED)
        mixed.append(mm(softmax(scores).astype(LOW), values[:, cut]).astype(LOW))
    return jnp.concatenate(mixed, 1)


def attend_heads_back(plan, queries, keys, values, allowed, grad_mixed):
    grads = ([], [], [])
    for head in range(plan.heads):
        cut = slice(head * HEAD_DIM, (head + 1) * HEAD_DIM)
        query, key, value, grad = queries[:, cut], keys[:, cut], values[:, cut], grad_mixed[:, cut]
        probs = softmax(jnp.where(allowed, mm_t(query, key) * 0.125, MASKED))
        grad_probs = mm_t(grad, value)
        inner = jnp.sum(grad_probs * probs, -1, keepdims=True)
        grad_scores = (probs * (grad_probs - inner)).astype(LOW)
        grads[0].append((mm(grad_scores, key) * 0.125).astype(LOW))
        grads[1].append((t_mm(grad_scores, query) * 0.125).astype(LOW))
        grads[2].append(t_mm(probs.astype(LOW), grad).astype(LOW))
    return tuple(jnp.concatenate(item, 1) for item in grads)


def slot_of(plan, count, base, step):
    return jnp.where(step < count, plan.half + base + step, base + step - count)


def pick(step, count, own, oth, rows):
    return jnp.where(step < count, oth[0, :rows], own[0, :rows])


def put(step, count, own, oth, value):
    @pl.when(step < count)
    def _():
        oth[0, : value.shape[0]] = value

    @pl.when(step >= count)
    def _():
        own[0, : value.shape[0]] = value


def encoder_attention(plan, meta, own, oth, gain, pieces, base, count):
    w3 = 3 * plan.width
    n = len(flat(pieces))

    def body(meta, own_ref, oth_ref, gain_ref, *rest):
        refs, (own_out, oth_out, kept, weight) = rest[:n], rest[n:]
        step = pl.program_id(0)

        @pl.when(step == 0)
        def _():
            plan.assemble(meta, pieces, refs, weight)

        value = pick(step, count, own_ref, oth_ref, ENC_LEN).astype(F32)
        normed = (value * rms_scale(value) * gain_ref[...]).astype(LOW)
        joined = mm(normed, weight[0, :, :w3]).astype(LOW)
        allowed = key_mask(meta, plan.pairs, slot_of(plan, count, base, step))
        width = plan.width
        mixed = attend_heads(
            plan, joined[:, :width], joined[:, width : 2 * width], joined[:, 2 * width :], allowed
        )
        kept[0, :, :w3] = joined
        kept[0, :, w3:] = mixed
        put(step, count, own_out, oth_out, mm_t(mixed, weight[0, :, w3:]).astype(LOW))

    rows = (LONG, D)
    return call(
        "encoder_attention",
        body,
        (2 * count,),
        meta,
        (own, oth, gain, *flat(pieces)),
        [own_spec(count, base, rows), oth_spec(count, base, rows), whole((1, D)), *plan.weight_specs(pieces)],
        [jax.ShapeDtypeStruct((count,) + rows, LOW)] * 2
        + [jax.ShapeDtypeStruct((2 * count, ENC_LEN, w3 + plan.width), LOW)],
        [own_spec(count, 0, rows), oth_spec(count, 0, rows), step_spec((ENC_LEN, w3 + plan.width))],
        plan.weight_scratch(pieces),
    )


def encoder_attention_back(plan, meta, own, oth, gain, pieces, kept, grad_own, grad_oth):
    count = plan.half
    width, w3 = plan.width, 3 * plan.width
    n = len(flat(pieces))

    def body(meta, own_ref, oth_ref, gain_ref, kept_ref, grad_own_ref, grad_oth_ref, *rest):
        refs, (own_out, oth_out), grad_refs = rest[:n], rest[n : n + 2], rest[n + 2 : -2]
        weight, acc = rest[-2:]
        step = pl.program_id(0)

        @pl.when(step == 0)
        def _():
            plan.assemble(meta, pieces, refs, weight)
            acc[...] = jnp.zeros_like(acc)

        value = pick(step, count, own_ref, oth_ref, ENC_LEN).astype(F32)
        normed = (value * rms_scale(value) * gain_ref[...]).astype(LOW)
        grad = pick(step, count, grad_own_ref, grad_oth_ref, ENC_LEN)
        allowed = key_mask(meta, plan.pairs, slot_of(plan, count, 0, step))
        grad_mixed = mm(grad, weight[0, :, w3:]).astype(LOW)
        acc[0, :, w3:] += t_mm(grad, kept_ref[0, :, w3:])
        joined = kept_ref[0, :, :w3]
        grads = attend_heads_back(
            plan, joined[:, :width], joined[:, width : 2 * width], joined[:, 2 * width :], allowed, grad_mixed
        )
        together = jnp.concatenate(grads, 1)
        acc[0, :, :w3] += t_mm(normed, together)
        put(step, count, own_out, oth_out, mm_t(together, weight[0, :, :w3]).astype(LOW))

        @pl.when(step == 2 * count - 1)
        def _():
            plan.emit(meta, acc, grad_refs)

    rows = (LONG, D)
    shapes = plan.grad_shapes(1)
    pair_specs = [own_spec(count, 0, rows), oth_spec(count, 0, rows)]
    return call(
        "encoder_attention_back",
        body,
        (2 * count,),
        meta,
        (own, oth, gain, kept, grad_own, grad_oth, *flat(pieces)),
        [*pair_specs, whole((1, D)), step_spec(kept.shape[1:]), *pair_specs, *plan.weight_specs(pieces)],
        [jax.ShapeDtypeStruct((count,) + rows, LOW)] * 2 + shapes,
        [*pair_specs, *[whole(item.shape) for item in shapes]],
        plan.weight_scratch(pieces) + [pltpu.VMEM((1, D, D), F32)],
    )


def encoder_feed(plan, meta, own, oth, pieces, base, count):
    n = len(flat(pieces))

    def body(meta, own_ref, oth_ref, *rest):
        refs, (own_out, oth_out, weight) = rest[:n], rest[n:]
        step = pl.program_id(0)

        @pl.when(step == 0)
        def _():
            plan.assemble(meta, pieces, refs, weight)

        normed = pick(step, count, own_ref, oth_ref, ENC_LEN)
        active = gelu_parts(mm(normed, weight[0]))[0].astype(LOW)
        put(step, count, own_out, oth_out, mm_t(active, weight[1]).astype(LOW))

    rows = (LONG, D)
    return call(
        "encoder_feed",
        body,
        (2 * count,),
        meta,
        (own, oth, *flat(pieces)),
        [own_spec(count, base, rows), oth_spec(count, base, rows), *plan.weight_specs(pieces)],
        [jax.ShapeDtypeStruct((count,) + rows, LOW)] * 2,
        [own_spec(count, 0, rows), oth_spec(count, 0, rows)],
        plan.weight_scratch(pieces),
    )


def encoder_feed_back(plan, meta, own, oth, grad_own, grad_oth, pieces):
    n = len(flat(pieces))
    count = plan.half

    def body(meta, own_ref, oth_ref, grad_own_ref, grad_oth_ref, *rest):
        refs, (own_out, oth_out), grad_refs = rest[:n], rest[n : n + 2], rest[n + 2 : -2]
        weight, acc = rest[-2:]
        step = pl.program_id(0)

        @pl.when(step == 0)
        def _():
            plan.assemble(meta, pieces, refs, weight)
            acc[...] = jnp.zeros_like(acc)

        normed = pick(step, count, own_ref, oth_ref, ENC_LEN)
        grad = pick(step, count, grad_own_ref, grad_oth_ref, ENC_LEN)
        active, slope = gelu_parts(mm(normed, weight[0]))
        grad_upper = (slope * mm(grad, weight[1])).astype(LOW)
        put(step, count, own_out, oth_out, mm_t(grad_upper, weight[0]).astype(LOW))
        acc[0] += t_mm(normed, grad_upper)
        acc[1] += t_mm(grad, active.astype(LOW))

        @pl.when(step == 2 * count - 1)
        def _():
            for index in range(2):
                size = len(grad_refs) // 2
                plan.emit(meta, acc.at[pl.ds(index, 1)], grad_refs[index * size : (index + 1) * size])

    rows = (LONG, D)
    shapes = plan.grad_shapes(1) * 2
    pair_specs = [own_spec(count, 0, rows), oth_spec(count, 0, rows)]
    return call(
        "encoder_feed_back",
        body,
        (2 * count,),
        meta,
        (own, oth, grad_own, grad_oth, *flat(pieces)),
        [*pair_specs, *pair_specs, *plan.weight_specs(pieces)],
        [jax.ShapeDtypeStruct((count,) + rows, LOW)] * 2 + shapes,
        [*pair_specs, *[whole(item.shape) for item in shapes]],
        plan.weight_scratch(pieces) + [pltpu.VMEM((2, D, D), F32)],
    )


def self_mask(plan, meta):
    rows = plan.pairs * SUFFIX
    query = lax.broadcasted_iota(jnp.int32, (rows, rows), 0)
    key = lax.broadcasted_iota(jnp.int32, (rows, rows), 1)
    pair = key // SUFFIX
    limit = jnp.zeros_like(key)
    for slot in range(plan.pairs):
        limit = jnp.where(pair == slot, meta[1 + 2 * plan.pairs + slot], limit)
    return (query // SUFFIX == pair) & (key <= query) & (key - pair * SUFFIX < limit)


def decoder_self(plan, meta, rows_in, gain, pieces):
    n = len(flat(pieces))
    width, w3 = plan.width, 3 * plan.width
    rows = plan.pairs * SUFFIX
    mid = rows // 2

    def body(meta, in_ref, gain_ref, *rest):
        refs, (own_out, oth_out, kept, weight) = rest[:n], rest[n:]
        plan.assemble(meta, pieces, refs, weight)
        value = in_ref[...].astype(F32)
        normed = (value * rms_scale(value) * gain_ref[...]).astype(LOW)
        joined = mm(normed, weight[0, :, :w3]).astype(LOW)
        mixed = attend_heads(
            plan, joined[:, :width], joined[:, width : 2 * width], joined[:, 2 * width :], self_mask(plan, meta)
        )
        kept[:, :w3] = joined
        kept[:, w3:] = mixed
        partial = mm_t(mixed, weight[0, :, w3:]).astype(LOW)
        own_out[...] = partial[:mid]
        oth_out[...] = partial[mid:]

    return call(
        "decoder_self",
        body,
        (1,),
        meta,
        (rows_in, gain, *flat(pieces)),
        [whole((rows, D)), whole((1, D)), *plan.weight_specs(pieces)],
        [jax.ShapeDtypeStruct((mid, D), LOW)] * 2 + [jax.ShapeDtypeStruct((rows, 4 * width), LOW)],
        [whole((mid, D))] * 2 + [whole((rows, 4 * width))],
        plan.weight_scratch(pieces),
    )


def decoder_self_back(plan, meta, rows_in, gain, pieces, kept, grad_own, grad_oth):
    n = len(flat(pieces))
    width, w3 = plan.width, 3 * plan.width
    rows = plan.pairs * SUFFIX
    mid = rows // 2

    def body(meta, in_ref, gain_ref, kept_ref, grad_own_ref, grad_oth_ref, *rest):
        refs, (own_out, oth_out), grad_refs = rest[:n], rest[n : n + 2], rest[n + 2 : -2]
        weight, acc = rest[-2:]
        plan.assemble(meta, pieces, refs, weight)
        value = in_ref[...].astype(F32)
        normed = (value * rms_scale(value) * gain_ref[...]).astype(LOW)
        grad = jnp.concatenate([grad_own_ref[...], grad_oth_ref[...]], 0)
        grad_mixed = mm(grad, weight[0, :, w3:]).astype(LOW)
        acc[0, :, w3:] = t_mm(grad, kept_ref[:, w3:])
        joined = kept_ref[:, :w3]
        grads = attend_heads_back(
            plan,
            joined[:, :width],
            joined[:, width : 2 * width],
            joined[:, 2 * width :],
            self_mask(plan, meta),
            grad_mixed,
        )
        together = jnp.concatenate(grads, 1)
        acc[0, :, :w3] = t_mm(normed, together)
        partial = mm_t(together, weight[0, :, :w3]).astype(LOW)
        own_out[...] = partial[:mid]
        oth_out[...] = partial[mid:]
        plan.emit(meta, acc, grad_refs)

    shapes = plan.grad_shapes(1)
    return call(
        "decoder_self_back",
        body,
        (1,),
        meta,
        (rows_in, gain, kept, grad_own, grad_oth, *flat(pieces)),
        [whole((rows, D)), whole((1, D)), whole(kept.shape), whole((mid, D)), whole((mid, D)), *plan.weight_specs(pieces)],
        [jax.ShapeDtypeStruct((mid, D), LOW)] * 2 + shapes,
        [whole((mid, D))] * 2 + [whole(item.shape) for item in shapes],
        plan.weight_scratch(pieces) + [pltpu.VMEM((1, D, D), F32)],
    )


def decoder_cross(plan, meta, own, oth, memory_own, memory_oth, pieces):
    n = len(flat(pieces))
    count = plan.half
    width, w3 = plan.width, 3 * plan.width

    def body(meta, own_ref, oth_ref, memory_own_ref, memory_oth_ref, *rest):
        refs, (own_out, oth_out, kept_query, kept_key, weight) = rest[:n], rest[n:]
        step = pl.program_id(0)

        @pl.when(step == 0)
        def _():
            plan.assemble(meta, pieces, refs, weight)

        normed = pick(step, count, own_ref, oth_ref, SUFFIX)
        memory = pick(step, count, memory_own_ref, memory_oth_ref, ENC_LEN)
        queries = mm(normed, weight[0, :, :width]).astype(LOW)
        both = mm(memory, weight[0, :, width:w3]).astype(LOW)
        allowed = key_mask(meta, plan.pairs, slot_of(plan, count, 0, step))
        mixed = attend_heads(plan, queries, both[:, :width], both[:, width:], allowed)
        kept_query[0, :, :width] = queries
        kept_query[0, :, width:] = mixed
        kept_key[0] = both
        put(step, count, own_out, oth_out, mm_t(mixed, weight[0, :, w3:]).astype(LOW))

    rows, long = (SUFFIX, D), (LONG, D)
    return call(
        "decoder_cross",
        body,
        (2 * count,),
        meta,
        (own, oth, memory_own, memory_oth, *flat(pieces)),
        [
            own_spec(count, 0, rows),
            oth_spec(count, 0, rows),
            own_spec(count, 0, long),
            oth_spec(count, 0, long),
            *plan.weight_specs(pieces),
        ],
        [jax.ShapeDtypeStruct((count,) + rows, LOW)] * 2
        + [
            jax.ShapeDtypeStruct((2 * count, SUFFIX, 2 * width), LOW),
            jax.ShapeDtypeStruct((2 * count, ENC_LEN, 2 * width), LOW),
        ],
        [
            own_spec(count, 0, rows),
            oth_spec(count, 0, rows),
            step_spec((SUFFIX, 2 * width)),
            step_spec((ENC_LEN, 2 * width)),
        ],
        plan.weight_scratch(pieces),
    )


def decoder_cross_back(
    plan, meta, own, oth, memory_own, memory_oth, pieces, kept_query, kept_key, grad_own, grad_oth
):
    n = len(flat(pieces))
    count = plan.half
    width, w3 = plan.width, 3 * plan.width

    def body(
        meta, own_ref, oth_ref, memory_own_ref, memory_oth_ref, query_ref, key_ref, grad_own_ref, grad_oth_ref, *rest
    ):
        refs, outs, grad_refs = rest[:n], rest[n : n + 4], rest[n + 4 : -2]
        weight, acc = rest[-2:]
        step = pl.program_id(0)

        @pl.when(step == 0)
        def _():
            plan.assemble(meta, pieces, refs, weight)
            acc[...] = jnp.zeros_like(acc)

        normed = pick(step, count, own_ref, oth_ref, SUFFIX)
        memory = pick(step, count, memory_own_ref, memory_oth_ref, ENC_LEN)
        grad = pick(step, count, grad_own_ref, grad_oth_ref, SUFFIX)
        allowed = key_mask(meta, plan.pairs, slot_of(plan, count, 0, step))
        grad_mixed = mm(grad, weight[0, :, w3:]).astype(LOW)
        acc[0, :, w3:] += t_mm(grad, query_ref[0, :, width:])
        both = key_ref[0]
        grad_query, grad_key, grad_value = attend_heads_back(
            plan, query_ref[0, :, :width], both[:, :width], both[:, width:], allowed, grad_mixed
        )
        together = jnp.concatenate([grad_key, grad_value], 1)
        acc[0, :, :width] += t_mm(normed, grad_query)
        acc[0, :, width:w3] += t_mm(memory, together)
        put(step, count, outs[0], outs[1], mm_t(grad_query, weight[0, :, :width]).astype(LOW))
        put(step, count, outs[2], outs[3], mm_t(together, weight[0, :, width:w3]).astype(LOW))

        @pl.when(step == 2 * count - 1)
        def _():
            plan.emit(meta, acc, grad_refs)

    rows, long = (SUFFIX, D), (LONG, D)
    shapes = plan.grad_shapes(1)
    row_specs = [own_spec(count, 0, rows), oth_spec(count, 0, rows)]
    long_specs = [own_spec(count, 0, long), oth_spec(count, 0, long)]
    return call(
        "decoder_cross_back",
        body,
        (2 * count,),
        meta,
        (own, oth, memory_own, memory_oth, kept_query, kept_key, grad_own, grad_oth, *flat(pieces)),
        [
            *row_specs,
            *long_specs,
            step_spec(kept_query.shape[1:]),
            step_spec(kept_key.shape[1:]),
            *row_specs,
            *plan.weight_specs(pieces),
        ],
        [jax.ShapeDtypeStruct((count,) + rows, LOW)] * 2
        + [jax.ShapeDtypeStruct((count,) + long, LOW)] * 2
        + shapes,
        [*row_specs, *long_specs, *[whole(item.shape) for item in shapes]],
        plan.weight_scratch(pieces) + [pltpu.VMEM((1, D, D), F32)],
    )


def decoder_feed(plan, meta, own, oth, grad_in, pieces):
    n = len(flat(pieces))
    rows = plan.pairs * SUFFIX
    mid = rows // 2

    def body(meta, own_ref, oth_ref, grad_ref, *rest):
        refs, (own_out, oth_out), grad_refs = rest[:n], rest[n : n + 2], rest[n + 2 : -2]
        weight, acc = rest[-2:]
        plan.assemble(meta, pieces, refs, weight)
        normed = jnp.concatenate([own_ref[...], oth_ref[...]], 0)
        grad = grad_ref[...]
        active, slope = gelu_parts(mm(normed, weight[0]))
        active = active.astype(LOW)
        partial = mm_t(active, weight[1]).astype(LOW)
        grad_upper = (slope * mm(grad, weight[1])).astype(LOW)
        back = mm_t(grad_upper, weight[0]).astype(LOW)
        own_out[0] = partial[:mid]
        own_out[1] = back[:mid]
        oth_out[0] = partial[mid:]
        oth_out[1] = back[mid:]
        acc[0] = t_mm(normed, grad_upper)
        acc[1] = t_mm(grad, active)
        plan.emit(meta, acc, grad_refs)

    shapes = plan.grad_shapes(2)
    return call(
        "decoder_feed",
        body,
        (1,),
        meta,
        (own, oth, grad_in, *flat(pieces)),
        [whole((mid, D))] * 2 + [whole((rows, D)), *plan.weight_specs(pieces)],
        [jax.ShapeDtypeStruct((2, mid, D), LOW)] * 2 + shapes,
        [whole((2, mid, D))] * 2 + [whole(item.shape) for item in shapes],
        plan.weight_scratch(pieces) + [pltpu.VMEM((2, D, D), F32)],
    )


def add_norm(meta, name, base, first, second, gain):
    def body(meta, base_ref, first_ref, second_ref, gain_ref, sum_ref, norm_ref):
        value = base_ref[...].astype(F32) + (first_ref[...].astype(F32) + second_ref[...].astype(F32))
        sum_ref[...] = value
        norm_ref[...] = (value * rms_scale(value) * gain_ref[...]).astype(LOW)

    shape = base.shape
    part = (1,) + shape[1:] if len(shape) == 3 else shape
    spec = (
        pl.BlockSpec(part, lambda p, _: (p, 0, 0)) if len(shape) == 3 else whole(shape)
    )
    return call(
        name,
        body,
        (shape[0] if len(shape) == 3 else 1,),
        meta,
        (base, first, second, gain),
        [spec, spec, spec, whole((1, D))],
        [jax.ShapeDtypeStruct(shape, F32), jax.ShapeDtypeStruct(shape, LOW)],
        [spec, spec],
        [],
    )


def norm_back(meta, name, inputs, gain, grad, first, second, want_low):
    def body(meta, in_ref, gain_ref, grad_ref, first_ref, second_ref, *outs):
        value = in_ref[...].astype(F32)
        scale = rms_scale(value)
        unit = value * scale
        back = first_ref[...].astype(F32) + second_ref[...].astype(F32)
        product = back * unit
        real = product[0, :ENC_LEN] if value.ndim == 3 else product
        part = jnp.sum(real, 0, keepdims=True)
        weighted = product * gain_ref[...]
        total = grad_ref[...].astype(F32) + scale * (
            back * gain_ref[...] - unit * jnp.mean(weighted, -1, keepdims=True)
        )
        outs[0][...] = total
        if want_low:
            outs[1][...] = total.astype(LOW)
        step = pl.program_id(0)

        @pl.when(step == 0)
        def _():
            outs[-1][...] = part

        @pl.when(step > 0)
        def _():
            outs[-1][...] += part

    shape = inputs.shape
    part = (1,) + shape[1:] if len(shape) == 3 else shape
    spec = pl.BlockSpec(part, lambda p, _: (p, 0, 0)) if len(shape) == 3 else whole(shape)
    return call(
        name,
        body,
        (shape[0] if len(shape) == 3 else 1,),
        meta,
        (inputs, gain, grad, first, second),
        [spec, whole((1, D)), spec, spec, spec],
        [jax.ShapeDtypeStruct(shape, F32)]
        + [jax.ShapeDtypeStruct(shape, LOW)] * want_low
        + [jax.ShapeDtypeStruct((1, D), F32)],
        [spec] * (1 + want_low) + [whole((1, D))],
        [],
    )


def fold(plan, meta, keeps, mores, split):
    n = len(keeps)
    counts = [item.shape[1] for item in keeps]
    total = sum(counts)
    tail = keeps[0].shape[2:]
    blocks = keeps[0].shape[0]

    def body(meta, *rest):
        keep_refs, more_refs, outs = rest[:n], rest[n : 2 * n], rest[2 * n :]
        for index in range(blocks):
            start = 0
            out, at = split(index)
            for keep_ref, more_ref, count in zip(keep_refs, more_refs, counts):
                value = keep_ref[index] + more_ref[index].astype(F32)
                outs[out][at, start : start + count] = value.astype(outs[out].dtype)
                start += count

    places = [split(index) for index in range(blocks)]
    outs = [
        jax.ShapeDtypeStruct((sum(place[0] == out for place in places), total) + tail, LOW if out else F32)
        for out in range(1 + max(place[0] for place in places))
    ]
    return call(
        "fold",
        body,
        (1,),
        meta,
        (*keeps, *mores),
        [whole(item.shape) for item in (*keeps, *mores)],
        outs,
        [whole(item.shape) for item in outs],
        [],
    )


def halves(index):
    return index % 2, index // 2


def apart(index):
    return index, 0


def one_hot(rows, offset):
    row = lax.broadcasted_iota(jnp.int32, (rows, D), 0)
    lane = lax.broadcasted_iota(jnp.int32, (rows, D), 1)
    return (lane == row + offset).astype(F32)


def collect(plan, meta, pieces, attention):
    count = pieces[0].shape[-3]
    n = len(pieces)
    shape = pieces[0].shape[-3:]
    groups = D // plan.width

    def body(meta, *rest):
        refs, (out, tile_out) = rest[:n], rest[n:]
        dp_at, mp_at = meta[0], meta[1 + 3 * plan.pairs]
        group = lax.broadcasted_iota(jnp.int32, (8, D), 1) // plan.width
        row = lax.broadcasted_iota(jnp.int32, (8, D), 0)
        place = one_hot(plan.block, dp_at * plan.block)
        def one(index, _):
            heads = (jnp.zeros((8, D), jnp.int32) + index) < attention
            value = refs[0][0, index]
            for ref in refs[1:]:
                value = value + ref[0, index].astype(F32)
            out[index] = value
            square = value * value
            lanes = jnp.broadcast_to(jnp.sum(square, 0, keepdims=True), (8, D))
            mask = jnp.where(heads, (group == row).astype(F32), (row == 0).astype(F32))
            sums = lax.dot_general(
                mask, square, (((1,), (1,)), ((), ())), precision=EXACT, preferred_element_type=F32
            )
            tile = lax.dot_general(
                sums, place, (((1,), (0,)), ((), ())), precision=EXACT, preferred_element_type=F32
            )
            spread = jnp.zeros_like(tile)
            for part in range(groups):
                shift = lax.rem(mp_at * plan.width + (D - part * plan.width), D)
                moved = pltpu.roll(jnp.where(group == part, lanes, 0.0), shift, 1)
                spread = jnp.where(row == 4 + part, moved, spread)
            spread = jnp.where(heads, spread, jnp.where(row == 4 + mp_at, lanes, 0.0))
            tile_out[index] = jnp.where(row < 4, tile, spread)
            return 0

        lax.fori_loop(0, count, one, 0)

    return call(
        "collect",
        body,
        (1,),
        meta,
        tuple(pieces),
        [whole(item.shape) for item in pieces],
        [jax.ShapeDtypeStruct(shape, F32), jax.ShapeDtypeStruct((count, 8, D), F32)],
        [whole(shape), whole((count, 8, D))],
        [],
    )


def finish(plan, meta, sums, statistics, gain_state):
    counts = [item.shape for item in statistics]

    def body(meta, sum_ref, *rest):
        olds, gains = rest[:8], rest[8:12]
        norm_out, news, rates, gain_outs = rest[12], rest[13:21], rest[21], rest[22:]
        tiles = [sum_ref[6], sum_ref[1], sum_ref[0]]
        feeds = [(sum_ref[2], sum_ref[3]), (sum_ref[4], sum_ref[5])]
        gain_sum = 0.5 * sum_ref[7]
        total = jnp.sum(gain_sum * gain_sum)
        for tile in tiles:
            total = total + jnp.sum(tile[:4])
        for up, down in feeds:
            total = total + jnp.sum(up[:1]) + jnp.sum(down[:1])
        totals = jnp.full((8, D), total, F32)
        norm = jnp.sqrt(totals)
        factor = jnp.minimum(1.0, 1.0 / norm)
        squared = (factor * factor)[:1]
        norm_out[...] = norm[:, :128]
        rates[...] = factor[:, :128]

        def renew(old, sums, number):
            return DECAY * old + (1.0 - DECAY) * (sums * squared / number + EPS_STAT)

        for layer, tile in enumerate(tiles):
            for part in range(3):
                news[0][layer, part : part + 1] = renew(olds[0][layer, part : part + 1], tile[part : part + 1], D)
                news[1][layer, part : part + 1] = renew(
                    olds[1][layer, part : part + 1], tile[4 + part : 5 + part], D
                )
            news[2][layer : layer + 1] = renew(olds[2][layer : layer + 1], tile[7:8], D)
            news[3][layer : layer + 1] = renew(olds[3][layer : layer + 1], tile[3:4], D)
        for layer, (up, down) in enumerate(feeds):
            news[4][layer : layer + 1] = renew(olds[4][layer : layer + 1], up[:1], FF)
            news[7][layer : layer + 1] = renew(olds[7][layer : layer + 1], down[:1], FF)
            for part in range(FF // D):
                cut = slice(part * D, (part + 1) * D)
                news[5][layer : layer + 1, cut] = renew(
                    olds[5][layer : layer + 1, cut], up[4 + part : 5 + part], D
                )
                news[6][layer : layer + 1, cut] = renew(
                    olds[6][layer : layer + 1, cut], down[4 + part : 5 + part], D
                )
        shift = lax.rem(D - meta[0] * plan.block, D)
        grad = (pltpu.roll(gain_sum, shift, 1) * factor)[:5, : plan.block]
        master, square, moment, average = [item[...] for item in gains]
        square_new = DECAY * square + (1.0 - DECAY) * (grad * grad + EPS_STAT)
        stepped = grad * lax.rsqrt(square_new)
        moment_new = MOMENTUM * moment + stepped
        master_new = master - RATE_GAIN * (MOMENTUM * moment_new + stepped)
        values = (
            grad,
            square_new,
            moment_new,
            master_new,
            AVERAGE * average + (1.0 - AVERAGE) * master_new,
            master_new,
        )
        for out, value in zip(gain_outs, values):
            out[...] = value.astype(out.dtype)

    small = gain_state[0].shape
    outs = (
        [jax.ShapeDtypeStruct((8, 128), F32)]
        + [jax.ShapeDtypeStruct(shape, F32) for shape in counts]
        + [jax.ShapeDtypeStruct((8, 128), F32)]
        + [jax.ShapeDtypeStruct(small, F32)] * 5
        + [jax.ShapeDtypeStruct(small, LOW)]
    )
    inputs = (sums, *statistics, *gain_state)
    return call(
        "finish",
        body,
        (1,),
        meta,
        inputs,
        [whole(item.shape) for item in inputs],
        outs,
        [whole(item.shape) for item in outs],
        [],
    )


def step_values(grad, scale, master, moment, average):
    stepped = grad * scale
    moment_new = MOMENTUM * moment + stepped
    master_new = master - RATE_MATRIX * (MOMENTUM * moment_new + stepped)
    return grad, moment_new, master_new, AVERAGE * average + (1.0 - AVERAGE) * master_new


def columns(rows, offset, size):
    filled = jnp.concatenate([rows] * (8 // rows.shape[0] + 1), 0)[:8]
    wide = (size + 127) // 128 * 128
    return jnp.transpose(pltpu.roll(filled, lax.rem(D - offset, D), 1)[:, :wide])[:size]


def update_attention(plan, meta, rates, grads, rows_in, cols_in, rows_out, cols_out, state_in, state_out):
    width, block = plan.width, plan.block

    def body(meta, rates_ref, grad_a, grad_b, rin, cin, rout, cout, *rest):
        ins, outs = rest[:6], rest[6:]
        layer = pl.program_id(0)
        dp_at, mp_at = meta[0], meta[1 + 3 * plan.pairs]
        grad = jnp.where(layer == 0, grad_a[0], jnp.where(layer == 1, grad_b[1], grad_b[0]))
        grad = grad * rates_ref[:1, :1]
        means = jnp.mean(rin[0], -1, keepdims=True)
        row_scale = lax.rsqrt(columns(rin[0] / means, dp_at * block, block))
        shift = lax.rem(D - mp_at * width, D)
        col_scale = lax.rsqrt(pltpu.roll(jnp.concatenate([cin[0]] * 3, 0)[:8], shift, 1)[:3, :width])
        for part in range(3):
            values = step_values(
                grad[:, part * width : (part + 1) * width],
                row_scale[:, part : part + 1] * col_scale[part : part + 1],
                ins[0][0, part],
                ins[1][0, part],
                ins[2][0, part],
            )
            for out, value in zip(outs[:4], values):
                out[0, part] = value
            outs[4][0, part] = values[2].astype(LOW)
        turned = jnp.transpose(grad[:, 3 * width :])
        row, col = rout[pl.ds(layer, 1), :], cout[pl.ds(layer, 1), :]
        mean = jnp.mean(row, -1, keepdims=True)
        row_scale = lax.rsqrt(columns(row / mean, mp_at * width, width))[:, :1]
        shift = lax.rem(D - dp_at * block, D)
        col_scale = lax.rsqrt(pltpu.roll(jnp.broadcast_to(col, (8, D)), shift, 1)[:1, :block])
        values = step_values(turned, row_scale * col_scale, ins[3][0], ins[4][0], ins[5][0])
        for out, value in zip(outs[5:9], values):
            out[0] = value
        outs[9][0] = values[2].astype(LOW)

    def spec(shape):
        return pl.BlockSpec((1,) + shape, lambda p, _: (p,) + (0,) * len(shape))

    shape_in, shape_out = (3, block, width), (width, block)
    outs = (
        [jax.ShapeDtypeStruct((3,) + shape_in, F32)] * 4
        + [jax.ShapeDtypeStruct((3,) + shape_in, LOW)]
        + [jax.ShapeDtypeStruct((3,) + shape_out, F32)] * 4
        + [jax.ShapeDtypeStruct((3,) + shape_out, LOW)]
    )
    return call(
        "update_attention",
        body,
        (3,),
        meta,
        (rates, *grads, rows_in, cols_in, rows_out, cols_out, *state_in, *state_out),
        [whole((8, 128)), whole((1, block, D)), whole((2, block, D))]
        + [spec((3, D)), spec((3, D)), whole((3, D)), whole((3, D))]
        + [spec(shape_in)] * 3
        + [spec(shape_out)] * 3,
        outs,
        [spec(shape_in)] * 5 + [spec(shape_out)] * 5,
        [],
    )


def update_feed(plan, meta, rates, grads, rows_up, cols_up, rows_down, cols_down, state_up, state_down):
    hidden, block = plan.hidden, plan.block

    def body(meta, rates_ref, grad_a, grad_b, rup, cup, rdown, cdown, *rest):
        ins, outs = rest[:6], rest[6:]
        layer = pl.program_id(0)
        lanes = pl.ds(pl.multiple_of(meta[1 + 3 * plan.pairs] * hidden, 128), hidden)
        one = pl.ds(layer, 1)
        mean_up = jnp.mean(rup[one, :], -1, keepdims=True)
        mean_down = jnp.mean(rdown[one, :], -1, keepdims=True)
        along = (rup[one, :] / mean_up, cdown[one, :])
        across = (cup[one, lanes], rdown[one, lanes] / mean_down)
        for part in range(2):
            grad = jnp.where(layer == 0, grad_a[part], grad_b[part]) * rates_ref[:1, :1]
            row_scale = lax.rsqrt(columns(along[part], meta[0] * block, block))[:, :1]
            values = step_values(
                grad,
                row_scale * lax.rsqrt(across[part]),
                ins[3 * part][0],
                ins[3 * part + 1][0],
                ins[3 * part + 2][0],
            )
            for out, value in zip(outs[5 * part : 5 * part + 4], values):
                out[0] = value
            outs[5 * part + 4][0] = values[2].astype(LOW)

    state = pl.BlockSpec((1, block, hidden), lambda p, _: (p, 0, 0))
    outs = ([jax.ShapeDtypeStruct((2, block, hidden), F32)] * 4 + [jax.ShapeDtypeStruct((2, block, hidden), LOW)]) * 2
    values = call(
        "update_feed",
        body,
        (2,),
        meta,
        (
            rates,
            *grads,
            rows_up,
            cols_up,
            rows_down,
            cols_down,
            *state_up,
            *[item.transpose(0, 2, 1) for item in state_down],
        ),
        [whole((8, 128)), *[whole((2, block, D))] * 2]
        + [whole((2, D)), whole((2, FF)), whole((2, FF)), whole((2, D))]
        + [state] * 6,
        outs,
        [state] * 10,
        [],
    )
    return [*values[:5], *[item.transpose(0, 2, 1) for item in values[5:]]]


def on_device(
    sizes,
    encoder_in,
    decoder_in,
    decoder_cotangent,
    counts,
    prefix_len,
    suffix_len,
    project_in,
    project_in_rows,
    project_in_cols,
    project_in_moment,
    project_in_average,
    project_out,
    project_out_rows,
    project_out_cols,
    project_out_moment,
    project_out_average,
    expand,
    expand_rows,
    expand_cols,
    expand_moment,
    expand_average,
    contract,
    contract_rows,
    contract_cols,
    contract_moment,
    contract_average,
    norm_gains,
    norm_gains_square,
    norm_gains_moment,
    norm_gains_average,
):
    dp_n, mp_n = sizes
    dp_index = lax.axis_index("dp")
    mp_index = lax.axis_index("mp")
    side = mp_index % 2
    pairs = prefix_len.shape[0]
    half = pairs // 2
    width = project_in.shape[-1]
    block = project_in.shape[-2]
    plan = Plan(dp_n, block, width, expand.shape[-1], pairs)
    low, f32 = LOW, F32

    def swap(value, axis, bit):
        count = dp_n if axis == "dp" else mp_n
        return lax.ppermute(value, axis, [(i, i ^ bit) for i in range(count)])

    def bits(count):
        return [1 << i for i in range(count.bit_length() - 1)]

    hold = lax.optimization_barrier

    class Gather:
        def __init__(self, blocks):
            self.items, self.sent, self.own = [{} for _ in blocks], [], list(blocks)

        def step(self, chain, *sends, later=()):
            names = [(item, name) for item, name in self.sent if (name, item) not in later]
            late = [(item, name) for item, name in self.sent if (name, item) in later]
            chain, values, self.own = hold(
                (list(chain), [self.items[item][name] for item, name in names], self.own)
            )
            for (item, name), value in zip(names, values):
                self.items[item][name] = value
            self.sent = late
            for name, item in sends:
                if name == "fours":
                    four = swap(jnp.concatenate([self.own[at] for at in item]), "dp", 4)
                    for place, at in enumerate(item):
                        self.items[at]["four"] = four[place * block : (place + 1) * block]
                        self.sent.append((at, "four"))
                    continue
                parts = self.items[item]
                if name == "four":
                    parts[name] = swap(self.own[item], "dp", 4)
                    self.sent.append((item, name))
                    continue
                if "two" not in parts:
                    parts["two"] = jnp.concatenate([self.own[item], parts["four"]])
                if name == "far":
                    parts[name] = swap(parts["two"], "dp", 2)
                else:
                    parts[name] = swap(parts["two" if name == "near" else "far"], "dp", 1)
                self.sent.append((item, name))
            return chain

        def take(self, item, index=0):
            parts = self.items[item]
            height = self.own[item].shape[0]
            return [parts[name] for name in ("two", "far", "near", "last")], height, index * block

    class Plain:
        def __init__(self, blocks):
            self.own = list(blocks)

        def step(self, chain, *sends, later=()):
            return chain

        def take(self, item, index=0):
            own = self.own[item][index * block : (index + 1) * block]
            return [lax.all_gather(own, "dp", axis=0, tiled=True)], D, 0

    def scatter(parts, attention):
        summed = lax.psum_scatter(parts[0], "dp", scatter_dimension=1, tiled=True)
        return collect(plan, meta, [summed[None]], attention)

    def total(value, axes):
        for axis, count in axes:
            for bit in bits(count):
                sent = value.astype(low)
                value = sent.astype(value.dtype) + swap(sent, axis, bit).astype(value.dtype)
        return value

    def total_dp(value):
        return total(value, [("dp", dp_n)])

    def total_all(value):
        return total(value, [("mp", mp_n), ("dp", dp_n)])

    def reduce_own(own, oth, first=()):
        sent = (own.astype(f32) + swap(oth, "mp", 1).astype(f32)).astype(low)
        for bit in bits(mp_n)[1:-1]:
            sent = (sent.astype(f32) + swap(sent, "mp", bit).astype(f32)).astype(low)
        sent, first = hold((sent, first))
        return sent, swap(sent, "mp", bits(mp_n)[-1])

    def relative(value):
        split = value.reshape((half, 2) + value.shape[1:])
        return (
            lax.dynamic_index_in_dim(split, side, 1, False),
            lax.dynamic_index_in_dim(split, 1 - side, 1, False),
        )

    def absolute(own):
        other = swap(own, "mp", 1)
        even = jnp.where(side == 0, own, other)
        odd = jnp.where(side == 0, other, own)
        return jnp.stack([even, odd], 1).reshape((pairs,) + own.shape[1:])

    def core(value):
        return swap(value, "mp", 1)

    def attention_block(layer):
        return jnp.concatenate(
            [project_in[layer, 0], project_in[layer, 1], project_in[layer, 2], project_out[layer].T], 1
        ).astype(low)

    def feed_block(layer):
        return [expand[layer].astype(low), contract[layer].T.astype(low)]

    direct = plan.direct
    gain_full = lax.dynamic_update_slice(
        jnp.zeros((8, D), low), norm_gains.astype(low), (0, dp_index * block)
    )
    blocks = [
        attention_block(0),
        *feed_block(0),
        attention_block(1),
        attention_block(2),
        jnp.concatenate(feed_block(1)),
    ]
    if direct:
        blocks[0] = jnp.concatenate([blocks[0], gain_full], 0)
    gather = (Gather if direct else Plain)(blocks)
    gather.step((), ("four", 0))
    gather.step((), ("far", 0), ("near", 0), ("four", 1))
    gather.step((), ("last", 0), later=(("four", 1),))
    enc_att = [gather.take(0)]
    if direct:
        height = block + 8
        gain_rows = sum(
            item[at : at + 8].astype(f32) for item in enc_att[0][0] for at in (block, height + block)
        )
    else:
        gain_rows = total_dp(gain_full).astype(f32)
    gains = [gain_rows[i : i + 1] for i in range(5)]

    place_rel = jnp.concatenate([2 * jnp.arange(half) + side, 2 * jnp.arange(half) + 1 - side])
    prefix_rel = jnp.concatenate(relative(prefix_len))
    suffix_rel = jnp.concatenate(relative(suffix_len))
    images = place_rel < counts[0, 0]
    active = place_rel < counts[0, 0] + counts[0, 1]
    meta = jnp.concatenate(
        [
            dp_index[None].astype(jnp.int32),
            images.astype(jnp.int32),
            prefix_rel,
            suffix_rel,
            mp_index[None].astype(jnp.int32),
        ]
    )
    steps = jnp.arange(SUFFIX)
    live = active[:, None] & (steps[None, :] < suffix_rel[:, None])

    mid = half * SUFFIX
    enc_own, enc_oth = relative(
        jnp.pad(encoder_in.reshape(pairs, ENC_LEN, D), ((0, 0), (0, LONG - ENC_LEN), (0, 0)))
    )
    dec_rel = jnp.concatenate(relative(decoder_in.reshape(pairs, SUFFIX, D))).reshape(2 * mid, D)
    cot = jnp.concatenate(relative(decoder_cotangent.reshape(pairs, SUFFIX, D)))
    cot = jnp.where(live[:, :, None], cot, f32(0.0)).reshape(2 * mid, D)
    cot_low = cot.astype(low)

    def triple(value):
        return value.reshape(half, SUFFIX, D)

    (enc_oth,) = gather.step((enc_oth,), ("far", 1), ("near", 1), ("four", 2), later=(("last", 0),))
    own, oth, kept_enc = encoder_attention(plan, meta, enc_own, enc_oth, gains[0], enc_att, 0, half)
    own, oth, dec_rel, cot, cot_low = gather.step(
        (own, oth, dec_rel, cot, cot_low), ("last", 1), ("near", 2), ("far", 2), ("fours", (3, 4))
    )
    sums = gather.step(reduce_own(own, oth), ("last", 2))
    enc_feed = [gather.take(1), gather.take(2)]
    enc_mid, norm_mid = add_norm(meta, "add_norm_mid", enc_own, *sums, gains[1])
    norm_mid_oth = core(norm_mid)

    (norm_mid_oth,) = gather.step(
        (norm_mid_oth,), ("far", 3), ("near", 3), ("four", 5), later=(("last", 2),)
    )
    own, oth = encoder_feed(plan, meta, norm_mid, norm_mid_oth, enc_feed, 0, half)
    own, oth = gather.step((own, oth), ("last", 3), ("far", 4), ("near", 4), later=(("four", 5),))
    sums = reduce_own(own, oth)
    (dec_rel,) = gather.step((dec_rel,), ("last", 4), later=(("last", 3),))

    self_att = [gather.take(3)]
    own, oth, kept_self = decoder_self(plan, meta, dec_rel, gains[2], self_att)
    sums = gather.step(sums)
    sums_self = reduce_own(own, oth, sums)
    gather.step((sums_self[0],), ("far", 5), ("near", 5))
    cross_att = [gather.take(4)]
    memory = (enc_mid + (sums[0].astype(f32) + sums[1].astype(f32))).astype(low)
    dec_one, norm_cross = add_norm(meta, "add_norm_cross", dec_rel[:mid], *sums_self, gains[3])
    memory, norm_cross = gather.step((memory, norm_cross), ("last", 5))
    memory_oth = core(memory)
    norm_cross_oth = core(norm_cross)

    cross_in = (triple(norm_cross), triple(norm_cross_oth), memory, memory_oth, cross_att)
    own, oth, *kept_cross = decoder_cross(plan, meta, *cross_in)
    sums = reduce_own(own, oth)
    dec_two, norm_last = add_norm(
        meta, "add_norm_last", dec_one, sums[0].reshape(mid, D), sums[1].reshape(mid, D), gains[4]
    )
    dec_feed = [gather.take(5), gather.take(5, 1)]

    own, oth, *grads_dec = decoder_feed(plan, meta, norm_last, core(norm_last), cot_low, dec_feed)
    if direct:
        more_dec = swap(grads_dec[0], "dp", 1)
    sums = reduce_own(own, oth)
    out_own = dec_two + (sums[0][0].astype(f32) + sums[1][0].astype(f32))
    grad, grad_low, gain_four = norm_back(
        meta, "norm_back_last", dec_two, gains[4], cot[:mid], sums[0][1], sums[1][1], True
    )

    own, oth, own_long, oth_long, *grads_cross = decoder_cross_back(
        plan, meta, *cross_in, *kept_cross, triple(grad_low), triple(core(grad_low))
    )
    if direct:
        own, oth, own_long, oth_long, more_dec = hold((own, oth, own_long, oth_long, more_dec))
        more_cross = swap(grads_cross[0], "dp", 1)
    sums = reduce_own(own, oth)
    sums_enc = reduce_own(own_long, oth_long, sums)
    if direct:
        keep, more_dec, _ = hold((grads_dec[1], more_dec, sums[0]))
        keep_dec, away_dec = fold(plan, meta, [keep], [more_dec], halves)
        *sums, away_dec = hold((*sums, away_dec))
        more_dec = swap(away_dec, "dp", 2)
    grad, grad_low, gain_three = norm_back(
        meta, "norm_back_cross", dec_one, gains[3], grad, sums[0].reshape(mid, D), sums[1].reshape(mid, D), True
    )
    grad_low_oth = core(grad_low)

    own_self, oth_self, *grads_self = decoder_self_back(
        plan, meta, dec_rel, gains[2], self_att, kept_self, grad_low, grad_low_oth
    )
    decoder_out = absolute(triple(out_own)).reshape(2 * mid, D)
    if direct:
        own_self, oth_self, decoder_out = hold((own_self, oth_self, decoder_out))
    sums_self = reduce_own(own_self, oth_self)
    if direct:
        *sums_enc, _, decoder_out, more_cross, more_dec = hold(
            (*sums_enc, sums_self[0], decoder_out, more_cross, more_dec)
        )
    grad_enc = sums_enc[0].astype(f32) + sums_enc[1].astype(f32)
    enc_low = grad_enc.astype(low)
    enc_low_oth = core(enc_low)

    if direct:
        keep_dec, away_dec = fold(plan, meta, [keep_dec], [more_dec], halves)
        enc_low_oth, away_self, away_dec = hold((enc_low_oth, grads_self[0], away_dec))
        more_self = swap(away_self, "dp", 1)
        more_dec = swap(away_dec, "dp", 4)
    own, oth, *grads_enc = encoder_feed_back(plan, meta, norm_mid, norm_mid_oth, enc_low, enc_low_oth, enc_feed)
    if direct:
        own, oth, more_self, more_dec, *sums_self = hold((own, oth, more_self, more_dec, *sums_self))
        more_up, more_down = [swap(item, "dp", 1) for item in grads_enc[::2]]
    sums = reduce_own(own, oth)
    if direct:
        keep_cross, keep_self, more_cross, more_self, _ = hold(
            (grads_cross[1], grads_self[1], more_cross, more_self, sums[0])
        )
        keep_mid, away_mid = fold(plan, meta, [keep_cross, keep_self], [more_cross, more_self], halves)
        more_mid = swap(away_mid, "dp", 2)
        sums_self, _ = hold((sums_self, away_mid))
    grad, gain_two = norm_back(meta, "norm_back_self", dec_rel[:mid], gains[2], grad, *sums_self, False)
    decoder_in_grad = absolute(triple(grad)).reshape(2 * mid, D)
    if direct:
        sum_dec = collect(plan, meta, [keep_dec, more_dec], 0)
        *sums, sum_dec, decoder_in_grad, more_up = hold((*sums, sum_dec, decoder_in_grad, more_up))
    grad_enc, enc_low, gain_one = norm_back(
        meta, "norm_back_mid", enc_mid, gains[1], grad_enc, *sums, True
    )
    if direct:
        enc_low, more_down, more_mid = hold((enc_low, more_down, more_mid))
    enc_low_oth = core(enc_low)

    if direct:
        keep_mid, away_mid = fold(plan, meta, [keep_mid], [more_mid], halves)
        keep_enc, away_enc = fold(plan, meta, grads_enc[1::2], [more_up, more_down], halves)
        enc_low_oth, away_enc, away_mid = hold((enc_low_oth, away_enc, away_mid))
        more_mid = swap(away_mid, "dp", 4)
        more_enc = swap(away_enc, "dp", 2)
    own, oth, *grads_att = encoder_attention_back(
        plan, meta, enc_own, enc_oth, gains[0], enc_att, kept_enc, enc_low, enc_low_oth
    )
    if direct:
        more_att = swap(grads_att[0], "dp", 1)
        own, oth, more_enc, more_mid = hold((own, oth, more_enc, more_mid))
        keep_enc, away_enc = fold(plan, meta, [keep_enc], [more_enc], halves)
        more_enc = swap(away_enc, "dp", 4)
    sums = reduce_own(own, oth)
    if direct:
        keep_att, more_att, _, _ = hold((grads_att[1], more_att, away_enc, sums[0]))
        mine, *others = fold(plan, meta, [keep_att], [more_att], apart)
        others, more_enc, sums = hold((others, more_enc, sums))
        pieces_att = [mine] + [swap(item, "dp", 2 * (i + 1)) for i, item in enumerate(others)]
        sum_mid = collect(plan, meta, [keep_mid, more_mid], 2)
        sum_enc = collect(plan, meta, [keep_enc, more_enc], 0)
        tiles = [sum_mid[1], sum_enc[1], sum_dec[1]]
    else:
        sum_dec = scatter(grads_dec, 0)
        sum_mid = [jnp.concatenate(item) for item in zip(scatter(grads_cross, 1), scatter(grads_self, 1))]
        sum_enc = scatter([jnp.concatenate(grads_enc)], 0)
        tiles = [sum_mid[1], sum_enc[1], sum_dec[1]]
    grad_enc, gain_zero = norm_back(meta, "norm_back_enc", enc_own, gains[0], grad_enc, *sums, False)
    if direct:
        *pieces_att, _, _ = hold((*pieces_att, sum_enc[1], gain_zero))
    sum_att = collect(plan, meta, pieces_att, 1) if direct else scatter(grads_att, 1)
    encoder_in_grad = absolute(grad_enc)[:, :ENC_LEN].reshape(pairs * ENC_LEN, D)
    gain_tile = jnp.concatenate(
        [gain_zero, gain_one, gain_two, gain_three, gain_four, jnp.zeros((3, D), f32)]
    )[None]
    tiles = total_all(jnp.concatenate([*tiles, sum_att[1], gain_tile]))
    done = finish(
        plan,
        meta,
        tiles,
        (
            project_in_rows,
            project_in_cols,
            project_out_rows,
            project_out_cols,
            expand_rows,
            expand_cols,
            contract_rows,
            contract_cols,
        ),
        (norm_gains, norm_gains_square, norm_gains_moment, norm_gains_average),
    )
    grad_norm, news, rates, pgain = done[0][0, 0], done[1:9], done[9], done[10:]
    att = update_attention(
        plan,
        meta,
        rates,
        (sum_att[0], sum_mid[0]),
        *news[:4],
        (project_in, project_in_moment, project_in_average),
        (project_out, project_out_moment, project_out_average),
    )
    feed = update_feed(
        plan,
        meta,
        rates,
        (sum_enc[0], sum_dec[0]),
        *news[4:],
        (expand, expand_moment, expand_average),
        (contract, contract_moment, contract_average),
    )
    return (
        decoder_out,
        encoder_in_grad,
        decoder_in_grad,
        grad_norm,
        att[0],
        news[0],
        news[1],
        *att[1:5],
        att[5],
        news[2],
        news[3],
        *att[6:10],
        feed[0],
        news[4],
        news[5],
        *feed[1:5],
        feed[5],
        news[6],
        news[7],
        *feed[6:10],
        *pgain,
    )


def solution(mesh):
    placed = (
        P("dp", None),
        P("dp", None),
        P("dp", None),
        P("dp", None),
        P("dp"),
        P("dp"),
        P(None, None, "dp", "mp"),
        P(),
        P(),
        P(None, None, "dp", "mp"),
        P(None, None, "dp", "mp"),
        P(None, "mp", "dp"),
        P(),
        P(),
        P(None, "mp", "dp"),
        P(None, "mp", "dp"),
        P(None, "dp", "mp"),
        P(),
        P(),
        P(None, "dp", "mp"),
        P(None, "dp", "mp"),
        P(None, "mp", "dp"),
        P(),
        P(),
        P(None, "mp", "dp"),
        P(None, "mp", "dp"),
        P(None, "dp"),
        P(None, "dp"),
        P(None, "dp"),
        P(None, "dp"),
    )
    return jax.shard_map(
        functools.partial(on_device, (mesh.shape["dp"], mesh.shape["mp"])),
        mesh=mesh,
        in_specs=placed,
        out_specs=(
            P("dp", None),
            P("dp", None),
            P("dp", None),
            P(),
            P(None, None, "dp", "mp"),
            P(),
            P(),
            P(None, None, "dp", "mp"),
            P(None, None, "dp", "mp"),
            P(None, None, "dp", "mp"),
            P(None, None, "dp", "mp"),
            P(None, "mp", "dp"),
            P(),
            P(),
            P(None, "mp", "dp"),
            P(None, "mp", "dp"),
            P(None, "mp", "dp"),
            P(None, "mp", "dp"),
            P(None, "dp", "mp"),
            P(),
            P(),
            P(None, "dp", "mp"),
            P(None, "dp", "mp"),
            P(None, "dp", "mp"),
            P(None, "dp", "mp"),
            P(None, "mp", "dp"),
            P(),
            P(),
            P(None, "mp", "dp"),
            P(None, "mp", "dp"),
            P(None, "mp", "dp"),
            P(None, "mp", "dp"),
            P(None, "dp"),
            P(None, "dp"),
            P(None, "dp"),
            P(None, "dp"),
            P(None, "dp"),
            P(None, "dp"),
        ),
        check_vma=False,
    )
```

```python
import functools

import jax
import jax.numpy as jnp
from jax import lax
from jax.experimental import pallas as pl
from jax.experimental.pallas import tpu as pltpu
from jax.sharding import PartitionSpec as P

D = 768
HEAD_DIM = 64
FF = 3072
PATCHES = 196
SUFFIX = 32
ENC_LEN = 228


EPS_NORM = 1e-06
EPS_STAT = 1e-30
DECAY = 0.99
MOMENTUM = 0.9
AVERAGE = 0.6
RATE_MATRIX = 0.004
RATE_GAIN = 0.05
MASKED = -1000000000.0


LOW = jnp.bfloat16
F32 = jnp.float32
VMEM_LIMIT = 56 * 1024 * 1024
LONG = (ENC_LEN + 7) // 8 * 8
EXACT = lax.Precision.HIGHEST


def dot(left, right, contract):
    return lax.dot_general(left, right, (contract, ((), ())), preferred_element_type=F32)


def mm(left, right):
    return dot(left, right, ((1,), (0,)))


def mm_t(left, right):
    return dot(left, right, ((1,), (1,)))


def t_mm(left, right):
    return dot(left, right, ((0,), (0,)))


def rms_scale(value):
    return lax.rsqrt(jnp.mean(value * value, -1, keepdims=True) + EPS_NORM)


def softmax(scores):
    expons = jnp.exp(scores - jnp.max(scores, -1, keepdims=True))
    return expons / jnp.sum(expons, -1, keepdims=True)


def gelu_parts(upper):
    inner = 0.7978845608028654 * (upper + 0.044715 * upper * upper * upper)
    bent = jnp.tanh(inner)
    value = 0.5 * upper * (1.0 + bent)
    slope = 0.5 * (1.0 + bent) + 0.5 * upper * (1.0 - bent * bent) * 0.7978845608028654 * (
        1.0 + 3.0 * 0.044715 * upper * upper
    )
    return value, slope


class Plan:
    def __init__(self, dp_n, block, width, hidden, pairs):
        self.dp_n, self.block, self.width, self.hidden, self.pairs = dp_n, block, width, hidden, pairs
        self.half = pairs // 2
        self.heads = width // HEAD_DIM
        self.direct = dp_n == 8

    def weight_specs(self, pieces):
        return [whole(item.shape) for item in flat(pieces)]

    def weight_scratch(self, pieces):
        return [pltpu.VMEM((len(pieces), D, D), LOW)]

    def assemble(self, meta, pieces, refs, scratch):
        refs = iter(refs)
        for count in range(len(pieces)):
            if not self.direct:
                scratch[count] = next(refs)[...]
                continue
            _, height, start = pieces[count]
            for places in ((0, 4), (2, 6), (1, 5), (3, 7)):
                ref = next(refs)
                for index, place in enumerate(places):
                    row = pl.multiple_of(jnp.bitwise_xor(meta[0], place) * self.block, 32)
                    first = start + index * height
                    scratch[count, pl.ds(row, self.block), :] = ref[first : first + self.block]

    def grad_shapes(self, count):
        if not self.direct:
            return [jax.ShapeDtypeStruct((count, D, D), F32)]
        shape = (self.dp_n // 2, count, self.block, D)
        return [jax.ShapeDtypeStruct(shape, LOW), jax.ShapeDtypeStruct(shape, F32)]

    def emit(self, meta, acc, refs):
        if not self.direct:
            refs[0][...] = acc[...]
            return
        for index in range(self.dp_n // 2):
            here = pl.multiple_of(jnp.bitwise_xor(meta[0], 2 * index) * self.block, 32)
            away = pl.multiple_of(jnp.bitwise_xor(meta[0], 2 * index + 1) * self.block, 32)
            for count in range(acc.shape[0]):
                refs[0][index, count] = acc[count, pl.ds(away, self.block), :].astype(LOW)
                refs[1][index, count] = acc[count, pl.ds(here, self.block), :]


def flat(pieces):
    return [item for arrays, _, _ in pieces for item in arrays]


def whole(shape):
    return pl.BlockSpec(shape, lambda *_: (0,) * len(shape))


def own_spec(count, base, shape):
    return pl.BlockSpec(
        (1,) + shape, lambda p, _: (base + jnp.maximum(p - count, 0),) + (0,) * len(shape)
    )


def oth_spec(count, base, shape):
    return pl.BlockSpec(
        (1,) + shape, lambda p, _: (base + jnp.minimum(p, count - 1),) + (0,) * len(shape)
    )


def step_spec(shape):
    return pl.BlockSpec((1,) + shape, lambda p, _: (p,) + (0,) * len(shape))


def call(name, body, grid, meta, inputs, in_specs, outs, out_specs, scratch):
    return pl.pallas_call(
        body,
        name=name,
        out_shape=outs,
        grid_spec=pltpu.PrefetchScalarGridSpec(
            num_scalar_prefetch=1,
            grid=grid,
            in_specs=in_specs,
            out_specs=out_specs,
            scratch_shapes=scratch,
        ),
        cost_estimate=pl.CostEstimate(flops=1, transcendentals=0, bytes_accessed=1),
        compiler_params=pltpu.CompilerParams(
            dimension_semantics=("arbitrary",) * len(grid), vmem_limit_bytes=VMEM_LIMIT
        ),
    )(meta, *inputs)


def key_mask(meta, pairs, slot):
    place = lax.broadcasted_iota(jnp.int32, (1, ENC_LEN), 1)
    image, prefix = meta[1 + slot], meta[1 + pairs + slot]
    return (place < image * PATCHES) | ((place >= PATCHES) & (place < PATCHES + prefix))


def attend_heads(plan, queries, keys, values, allowed):
    mixed = []
    for head in range(plan.heads):
        cut = slice(head * HEAD_DIM, (head + 1) * HEAD_DIM)
        scores = jnp.where(allowed, mm_t(queries[:, cut], keys[:, cut]) * 0.125, MASKED)
        mixed.append(mm(softmax(scores).astype(LOW), values[:, cut]).astype(LOW))
    return jnp.concatenate(mixed, 1)


def attend_heads_back(plan, queries, keys, values, allowed, grad_mixed):
    grads = ([], [], [])
    for head in range(plan.heads):
        cut = slice(head * HEAD_DIM, (head + 1) * HEAD_DIM)
        query, key, value, grad = queries[:, cut], keys[:, cut], values[:, cut], grad_mixed[:, cut]
        probs = softmax(jnp.where(allowed, mm_t(query, key) * 0.125, MASKED))
        grad_probs = mm_t(grad, value)
        inner = jnp.sum(grad_probs * probs, -1, keepdims=True)
        grad_scores = (probs * (grad_probs - inner)).astype(LOW)
        grads[0].append((mm(grad_scores, key) * 0.125).astype(LOW))
        grads[1].append((t_mm(grad_scores, query) * 0.125).astype(LOW))
        grads[2].append(t_mm(probs.astype(LOW), grad).astype(LOW))
    return tuple(jnp.concatenate(item, 1) for item in grads)


def slot_of(plan, count, base, step):
    return jnp.where(step < count, plan.half + base + step, base + step - count)


def pick(step, count, own, oth, rows):
    return jnp.where(step < count, oth[0, :rows], own[0, :rows])


def put(step, count, own, oth, value):
    @pl.when(step < count)
    def _():
        oth[0, : value.shape[0]] = value

    @pl.when(step >= count)
    def _():
        own[0, : value.shape[0]] = value


def encoder_attention(plan, meta, own, oth, gain, pieces, base, count):
    w3 = 3 * plan.width
    n = len(flat(pieces))

    def body(meta, own_ref, oth_ref, gain_ref, *rest):
        refs, (own_out, oth_out, kept, weight) = rest[:n], rest[n:]
        step = pl.program_id(0)

        @pl.when(step == 0)
        def _():
            plan.assemble(meta, pieces, refs, weight)

        value = pick(step, count, own_ref, oth_ref, ENC_LEN).astype(F32)
        normed = (value * rms_scale(value) * gain_ref[...]).astype(LOW)
        joined = mm(normed, weight[0, :, :w3]).astype(LOW)
        allowed = key_mask(meta, plan.pairs, slot_of(plan, count, base, step))
        width = plan.width
        mixed = attend_heads(
            plan, joined[:, :width], joined[:, width : 2 * width], joined[:, 2 * width :], allowed
        )
        kept[0, :, :w3] = joined
        kept[0, :, w3:] = mixed
        put(step, count, own_out, oth_out, mm_t(mixed, weight[0, :, w3:]).astype(LOW))

    rows = (LONG, D)
    return call(
        "encoder_attention",
        body,
        (2 * count,),
        meta,
        (own, oth, gain, *flat(pieces)),
        [own_spec(count, base, rows), oth_spec(count, base, rows), whole((1, D)), *plan.weight_specs(pieces)],
        [jax.ShapeDtypeStruct((count,) + rows, LOW)] * 2
        + [jax.ShapeDtypeStruct((2 * count, ENC_LEN, w3 + plan.width), LOW)],
        [own_spec(count, 0, rows), oth_spec(count, 0, rows), step_spec((ENC_LEN, w3 + plan.width))],
        plan.weight_scratch(pieces),
    )


def encoder_attention_back(plan, meta, own, oth, gain, pieces, kept, grad_own, grad_oth):
    count = plan.half
    width, w3 = plan.width, 3 * plan.width
    n = len(flat(pieces))

    def body(meta, own_ref, oth_ref, gain_ref, kept_ref, grad_own_ref, grad_oth_ref, *rest):
        refs, (own_out, oth_out), grad_refs = rest[:n], rest[n : n + 2], rest[n + 2 : -2]
        weight, acc = rest[-2:]
        step = pl.program_id(0)

        @pl.when(step == 0)
        def _():
            plan.assemble(meta, pieces, refs, weight)
            acc[...] = jnp.zeros_like(acc)

        value = pick(step, count, own_ref, oth_ref, ENC_LEN).astype(F32)
        normed = (value * rms_scale(value) * gain_ref[...]).astype(LOW)
        grad = pick(step, count, grad_own_ref, grad_oth_ref, ENC_LEN)
        allowed = key_mask(meta, plan.pairs, slot_of(plan, count, 0, step))
        grad_mixed = mm(grad, weight[0, :, w3:]).astype(LOW)
        acc[0, :, w3:] += t_mm(grad, kept_ref[0, :, w3:])
        joined = kept_ref[0, :, :w3]
        grads = attend_heads_back(
            plan, joined[:, :width], joined[:, width : 2 * width], joined[:, 2 * width :], allowed, grad_mixed
        )
        together = jnp.concatenate(grads, 1)
        acc[0, :, :w3] += t_mm(normed, together)
        put(step, count, own_out, oth_out, mm_t(together, weight[0, :, :w3]).astype(LOW))

        @pl.when(step == 2 * count - 1)
        def _():
            plan.emit(meta, acc, grad_refs)

    rows = (LONG, D)
    shapes = plan.grad_shapes(1)
    pair_specs = [own_spec(count, 0, rows), oth_spec(count, 0, rows)]
    return call(
        "encoder_attention_back",
        body,
        (2 * count,),
        meta,
        (own, oth, gain, kept, grad_own, grad_oth, *flat(pieces)),
        [*pair_specs, whole((1, D)), step_spec(kept.shape[1:]), *pair_specs, *plan.weight_specs(pieces)],
        [jax.ShapeDtypeStruct((count,) + rows, LOW)] * 2 + shapes,
        [*pair_specs, *[whole(item.shape) for item in shapes]],
        plan.weight_scratch(pieces) + [pltpu.VMEM((1, D, D), F32)],
    )


def encoder_feed(plan, meta, own, oth, pieces, base, count):
    n = len(flat(pieces))

    def body(meta, own_ref, oth_ref, *rest):
        refs, (own_out, oth_out, weight) = rest[:n], rest[n:]
        step = pl.program_id(0)

        @pl.when(step == 0)
        def _():
            plan.assemble(meta, pieces, refs, weight)

        normed = pick(step, count, own_ref, oth_ref, ENC_LEN)
        active = gelu_parts(mm(normed, weight[0]))[0].astype(LOW)
        put(step, count, own_out, oth_out, mm_t(active, weight[1]).astype(LOW))

    rows = (LONG, D)
    return call(
        "encoder_feed",
        body,
        (2 * count,),
        meta,
        (own, oth, *flat(pieces)),
        [own_spec(count, base, rows), oth_spec(count, base, rows), *plan.weight_specs(pieces)],
        [jax.ShapeDtypeStruct((count,) + rows, LOW)] * 2,
        [own_spec(count, 0, rows), oth_spec(count, 0, rows)],
        plan.weight_scratch(pieces),
    )


def encoder_feed_back(plan, meta, own, oth, grad_own, grad_oth, pieces):
    n = len(flat(pieces))
    count = plan.half

    def body(meta, own_ref, oth_ref, grad_own_ref, grad_oth_ref, *rest):
        refs, (own_out, oth_out), grad_refs = rest[:n], rest[n : n + 2], rest[n + 2 : -2]
        weight, acc = rest[-2:]
        step = pl.program_id(0)

        @pl.when(step == 0)
        def _():
            plan.assemble(meta, pieces, refs, weight)
            acc[...] = jnp.zeros_like(acc)

        normed = pick(step, count, own_ref, oth_ref, ENC_LEN)
        grad = pick(step, count, grad_own_ref, grad_oth_ref, ENC_LEN)
        active, slope = gelu_parts(mm(normed, weight[0]))
        grad_upper = (slope * mm(grad, weight[1])).astype(LOW)
        put(step, count, own_out, oth_out, mm_t(grad_upper, weight[0]).astype(LOW))
        acc[0] += t_mm(normed, grad_upper)
        acc[1] += t_mm(grad, active.astype(LOW))

        @pl.when(step == 2 * count - 1)
        def _():
            for index in range(2):
                size = len(grad_refs) // 2
                plan.emit(meta, acc.at[pl.ds(index, 1)], grad_refs[index * size : (index + 1) * size])

    rows = (LONG, D)
    shapes = plan.grad_shapes(1) * 2
    pair_specs = [own_spec(count, 0, rows), oth_spec(count, 0, rows)]
    return call(
        "encoder_feed_back",
        body,
        (2 * count,),
        meta,
        (own, oth, grad_own, grad_oth, *flat(pieces)),
        [*pair_specs, *pair_specs, *plan.weight_specs(pieces)],
        [jax.ShapeDtypeStruct((count,) + rows, LOW)] * 2 + shapes,
        [*pair_specs, *[whole(item.shape) for item in shapes]],
        plan.weight_scratch(pieces) + [pltpu.VMEM((2, D, D), F32)],
    )


def self_mask(plan, meta):
    rows = plan.pairs * SUFFIX
    query = lax.broadcasted_iota(jnp.int32, (rows, rows), 0)
    key = lax.broadcasted_iota(jnp.int32, (rows, rows), 1)
    pair = key // SUFFIX
    limit = jnp.zeros_like(key)
    for slot in range(plan.pairs):
        limit = jnp.where(pair == slot, meta[1 + 2 * plan.pairs + slot], limit)
    return (query // SUFFIX == pair) & (key <= query) & (key - pair * SUFFIX < limit)


def decoder_self(plan, meta, rows_in, gain, pieces):
    n = len(flat(pieces))
    width, w3 = plan.width, 3 * plan.width
    rows = plan.pairs * SUFFIX
    mid = rows // 2

    def body(meta, in_ref, gain_ref, *rest):
        refs, (own_out, oth_out, kept, weight) = rest[:n], rest[n:]
        plan.assemble(meta, pieces, refs, weight)
        value = in_ref[...].astype(F32)
        normed = (value * rms_scale(value) * gain_ref[...]).astype(LOW)
        joined = mm(normed, weight[0, :, :w3]).astype(LOW)
        mixed = attend_heads(
            plan, joined[:, :width], joined[:, width : 2 * width], joined[:, 2 * width :], self_mask(plan, meta)
        )
        kept[:, :w3] = joined
        kept[:, w3:] = mixed
        partial = mm_t(mixed, weight[0, :, w3:]).astype(LOW)
        own_out[...] = partial[:mid]
        oth_out[...] = partial[mid:]

    return call(
        "decoder_self",
        body,
        (1,),
        meta,
        (rows_in, gain, *flat(pieces)),
        [whole((rows, D)), whole((1, D)), *plan.weight_specs(pieces)],
        [jax.ShapeDtypeStruct((mid, D), LOW)] * 2 + [jax.ShapeDtypeStruct((rows, 4 * width), LOW)],
        [whole((mid, D))] * 2 + [whole((rows, 4 * width))],
        plan.weight_scratch(pieces),
    )


def decoder_self_back(plan, meta, rows_in, gain, pieces, kept, grad_own, grad_oth):
    n = len(flat(pieces))
    width, w3 = plan.width, 3 * plan.width
    rows = plan.pairs * SUFFIX
    mid = rows // 2

    def body(meta, in_ref, gain_ref, kept_ref, grad_own_ref, grad_oth_ref, *rest):
        refs, (own_out, oth_out), grad_refs = rest[:n], rest[n : n + 2], rest[n + 2 : -2]
        weight, acc = rest[-2:]
        plan.assemble(meta, pieces, refs, weight)
        value = in_ref[...].astype(F32)
        normed = (value * rms_scale(value) * gain_ref[...]).astype(LOW)
        grad = jnp.concatenate([grad_own_ref[...], grad_oth_ref[...]], 0)
        grad_mixed = mm(grad, weight[0, :, w3:]).astype(LOW)
        acc[0, :, w3:] = t_mm(grad, kept_ref[:, w3:])
        joined = kept_ref[:, :w3]
        grads = attend_heads_back(
            plan,
            joined[:, :width],
            joined[:, width : 2 * width],
            joined[:, 2 * width :],
            self_mask(plan, meta),
            grad_mixed,
        )
        together = jnp.concatenate(grads, 1)
        acc[0, :, :w3] = t_mm(normed, together)
        partial = mm_t(together, weight[0, :, :w3]).astype(LOW)
        own_out[...] = partial[:mid]
        oth_out[...] = partial[mid:]
        plan.emit(meta, acc, grad_refs)

    shapes = plan.grad_shapes(1)
    return call(
        "decoder_self_back",
        body,
        (1,),
        meta,
        (rows_in, gain, kept, grad_own, grad_oth, *flat(pieces)),
        [whole((rows, D)), whole((1, D)), whole(kept.shape), whole((mid, D)), whole((mid, D)), *plan.weight_specs(pieces)],
        [jax.ShapeDtypeStruct((mid, D), LOW)] * 2 + shapes,
        [whole((mid, D))] * 2 + [whole(item.shape) for item in shapes],
        plan.weight_scratch(pieces) + [pltpu.VMEM((1, D, D), F32)],
    )


def decoder_cross(plan, meta, own, oth, memory_own, memory_oth, pieces):
    n = len(flat(pieces))
    count = plan.half
    width, w3 = plan.width, 3 * plan.width

    def body(meta, own_ref, oth_ref, memory_own_ref, memory_oth_ref, *rest):
        refs, (own_out, oth_out, kept_query, kept_key, weight) = rest[:n], rest[n:]
        step = pl.program_id(0)

        @pl.when(step == 0)
        def _():
            plan.assemble(meta, pieces, refs, weight)

        normed = pick(step, count, own_ref, oth_ref, SUFFIX)
        memory = pick(step, count, memory_own_ref, memory_oth_ref, ENC_LEN)
        queries = mm(normed, weight[0, :, :width]).astype(LOW)
        both = mm(memory, weight[0, :, width:w3]).astype(LOW)
        allowed = key_mask(meta, plan.pairs, slot_of(plan, count, 0, step))
        mixed = attend_heads(plan, queries, both[:, :width], both[:, width:], allowed)
        kept_query[0, :, :width] = queries
        kept_query[0, :, width:] = mixed
        kept_key[0] = both
        put(step, count, own_out, oth_out, mm_t(mixed, weight[0, :, w3:]).astype(LOW))

    rows, long = (SUFFIX, D), (LONG, D)
    return call(
        "decoder_cross",
        body,
        (2 * count,),
        meta,
        (own, oth, memory_own, memory_oth, *flat(pieces)),
        [
            own_spec(count, 0, rows),
            oth_spec(count, 0, rows),
            own_spec(count, 0, long),
            oth_spec(count, 0, long),
            *plan.weight_specs(pieces),
        ],
        [jax.ShapeDtypeStruct((count,) + rows, LOW)] * 2
        + [
            jax.ShapeDtypeStruct((2 * count, SUFFIX, 2 * width), LOW),
            jax.ShapeDtypeStruct((2 * count, ENC_LEN, 2 * width), LOW),
        ],
        [
            own_spec(count, 0, rows),
            oth_spec(count, 0, rows),
            step_spec((SUFFIX, 2 * width)),
            step_spec((ENC_LEN, 2 * width)),
        ],
        plan.weight_scratch(pieces),
    )


def decoder_cross_back(
    plan, meta, own, oth, memory_own, memory_oth, pieces, kept_query, kept_key, grad_own, grad_oth
):
    n = len(flat(pieces))
    count = plan.half
    width, w3 = plan.width, 3 * plan.width
    rows = plan.pairs * SUFFIX
    mid = rows // 2

    def body(
        meta, own_ref, oth_ref, memory_own_ref, memory_oth_ref, query_ref, key_ref, grad_own_ref, grad_oth_ref, *rest
    ):
        refs, outs, grad_refs = rest[:n], rest[n : n + 4], rest[n + 4 : -4]
        weight, acc, grad_mixed, grad_query = rest[-4:]
        step = pl.program_id(0)

        @pl.when(step == 0)
        def _():
            plan.assemble(meta, pieces, refs, weight)
            grad = jnp.concatenate([grad_oth_ref[...], grad_own_ref[...]], 0).reshape(rows, D)
            grad_mixed[...] = mm(grad, weight[0, :, w3:]).astype(LOW)
            acc[0, :, w3:] = t_mm(grad, query_ref[:, :, width:].reshape(rows, width))
            acc[0, :, width:w3] = jnp.zeros((D, w3 - width), F32)

        memory = pick(step, count, memory_own_ref, memory_oth_ref, ENC_LEN)
        allowed = key_mask(meta, plan.pairs, slot_of(plan, count, 0, step))
        both = key_ref[0]
        here = pl.ds(pl.multiple_of(step * SUFFIX, SUFFIX), SUFFIX)
        query, grad_key, grad_value = attend_heads_back(
            plan, query_ref[step, :, :width], both[:, :width], both[:, width:], allowed, grad_mixed[here, :]
        )
        grad_query[here, :] = query
        together = jnp.concatenate([grad_key, grad_value], 1)
        acc[0, :, width:w3] += t_mm(memory, together)
        put(step, count, outs[2], outs[3], mm_t(together, weight[0, :, width:w3]).astype(LOW))

        @pl.when(step == 2 * count - 1)
        def _():
            normed = jnp.concatenate([oth_ref[...], own_ref[...]], 0).reshape(rows, D)
            queries = grad_query[...]
            acc[0, :, :width] = t_mm(normed, queries)
            back = mm_t(queries, weight[0, :, :width]).astype(LOW)
            outs[1][...] = back[:mid].reshape(count, SUFFIX, D)
            outs[0][...] = back[mid:].reshape(count, SUFFIX, D)
            plan.emit(meta, acc, grad_refs)

    part, long = (count, SUFFIX, D), (LONG, D)
    shapes = plan.grad_shapes(1)
    long_specs = [own_spec(count, 0, long), oth_spec(count, 0, long)]
    return call(
        "decoder_cross_back",
        body,
        (2 * count,),
        meta,
        (own, oth, memory_own, memory_oth, kept_query, kept_key, grad_own, grad_oth, *flat(pieces)),
        [
            whole(part),
            whole(part),
            *long_specs,
            whole(kept_query.shape),
            step_spec(kept_key.shape[1:]),
            whole(part),
            whole(part),
            *plan.weight_specs(pieces),
        ],
        [jax.ShapeDtypeStruct(part, LOW)] * 2
        + [jax.ShapeDtypeStruct((count,) + long, LOW)] * 2
        + shapes,
        [whole(part), whole(part), *long_specs, *[whole(item.shape) for item in shapes]],
        plan.weight_scratch(pieces)
        + [pltpu.VMEM((1, D, D), F32)]
        + [pltpu.VMEM((rows, width), LOW), pltpu.VMEM((rows, width), LOW)],
    )


def decoder_feed(plan, meta, own, oth, grad_in, pieces):
    n = len(flat(pieces))
    rows = plan.pairs * SUFFIX
    mid = rows // 2

    def body(meta, own_ref, oth_ref, grad_ref, *rest):
        refs, (own_out, oth_out), grad_refs = rest[:n], rest[n : n + 2], rest[n + 2 : -2]
        weight, acc = rest[-2:]
        plan.assemble(meta, pieces, refs, weight)
        normed = jnp.concatenate([own_ref[...], oth_ref[...]], 0)
        grad = grad_ref[...]
        active, slope = gelu_parts(mm(normed, weight[0]))
        active = active.astype(LOW)
        partial = mm_t(active, weight[1]).astype(LOW)
        grad_upper = (slope * mm(grad, weight[1])).astype(LOW)
        back = mm_t(grad_upper, weight[0]).astype(LOW)
        own_out[0] = partial[:mid]
        own_out[1] = back[:mid]
        oth_out[0] = partial[mid:]
        oth_out[1] = back[mid:]
        acc[0] = t_mm(normed, grad_upper)
        acc[1] = t_mm(grad, active)
        plan.emit(meta, acc, grad_refs)

    shapes = plan.grad_shapes(2)
    return call(
        "decoder_feed",
        body,
        (1,),
        meta,
        (own, oth, grad_in, *flat(pieces)),
        [whole((mid, D))] * 2 + [whole((rows, D)), *plan.weight_specs(pieces)],
        [jax.ShapeDtypeStruct((2, mid, D), LOW)] * 2 + shapes,
        [whole((2, mid, D))] * 2 + [whole(item.shape) for item in shapes],
        plan.weight_scratch(pieces) + [pltpu.VMEM((2, D, D), F32)],
    )


def add_norm(meta, name, base, first, second, gain):
    def body(meta, base_ref, first_ref, second_ref, gain_ref, sum_ref, norm_ref):
        value = base_ref[...].astype(F32) + (first_ref[...].astype(F32) + second_ref[...].astype(F32))
        sum_ref[...] = value
        norm_ref[...] = (value * rms_scale(value) * gain_ref[...]).astype(LOW)

    shape = base.shape
    part = (1,) + shape[1:] if len(shape) == 3 else shape
    spec = (
        pl.BlockSpec(part, lambda p, _: (p, 0, 0)) if len(shape) == 3 else whole(shape)
    )
    return call(
        name,
        body,
        (shape[0] if len(shape) == 3 else 1,),
        meta,
        (base, first, second, gain),
        [spec, spec, spec, whole((1, D))],
        [jax.ShapeDtypeStruct(shape, F32), jax.ShapeDtypeStruct(shape, LOW)],
        [spec, spec],
        [],
    )


def norm_back(meta, name, inputs, gain, grad, first, second, want_low):
    def body(meta, in_ref, gain_ref, grad_ref, first_ref, second_ref, *outs):
        value = in_ref[...].astype(F32)
        scale = rms_scale(value)
        unit = value * scale
        back = first_ref[...].astype(F32) + second_ref[...].astype(F32)
        product = back * unit
        real = product[0, :ENC_LEN] if value.ndim == 3 else product
        part = jnp.sum(real, 0, keepdims=True)
        weighted = product * gain_ref[...]
        total = grad_ref[...].astype(F32) + scale * (
            back * gain_ref[...] - unit * jnp.mean(weighted, -1, keepdims=True)
        )
        outs[0][...] = total
        if want_low:
            outs[1][...] = total.astype(LOW)
        step = pl.program_id(0)

        @pl.when(step == 0)
        def _():
            outs[-1][...] = part

        @pl.when(step > 0)
        def _():
            outs[-1][...] += part

    shape = inputs.shape
    part = (1,) + shape[1:] if len(shape) == 3 else shape
    spec = pl.BlockSpec(part, lambda p, _: (p, 0, 0)) if len(shape) == 3 else whole(shape)
    return call(
        name,
        body,
        (shape[0] if len(shape) == 3 else 1,),
        meta,
        (inputs, gain, grad, first, second),
        [spec, whole((1, D)), spec, spec, spec],
        [jax.ShapeDtypeStruct(shape, F32)]
        + [jax.ShapeDtypeStruct(shape, LOW)] * want_low
        + [jax.ShapeDtypeStruct((1, D), F32)],
        [spec] * (1 + want_low) + [whole((1, D))],
        [],
    )


def fold(plan, meta, keeps, mores, split):
    n = len(keeps)
    counts = [item.shape[1] for item in keeps]
    total = sum(counts)
    tail = keeps[0].shape[2:]
    blocks = keeps[0].shape[0]

    def body(meta, *rest):
        keep_refs, more_refs, outs = rest[:n], rest[n : 2 * n], rest[2 * n :]
        for index in range(blocks):
            start = 0
            out, at = split(index)
            for keep_ref, more_ref, count in zip(keep_refs, more_refs, counts):
                value = keep_ref[index] + more_ref[index].astype(F32)
                outs[out][at, start : start + count] = value.astype(outs[out].dtype)
                start += count

    places = [split(index) for index in range(blocks)]
    outs = [
        jax.ShapeDtypeStruct((sum(place[0] == out for place in places), total) + tail, LOW if out else F32)
        for out in range(1 + max(place[0] for place in places))
    ]
    return call(
        "fold",
        body,
        (1,),
        meta,
        (*keeps, *mores),
        [whole(item.shape) for item in (*keeps, *mores)],
        outs,
        [whole(item.shape) for item in outs],
        [],
    )


def halves(index):
    return index % 2, index // 2


def apart(index):
    return index, 0


def pack_first(plan, meta, project_in, project_out, gains):
    width, block = plan.width, plan.block

    def body(meta, in_ref, out_ref, gain_ref, packed):
        parts = [in_ref[0, index] for index in range(3)] + [jnp.transpose(out_ref[0])]
        packed[:block] = jnp.concatenate(parts, 1).astype(LOW)
        rows = jnp.concatenate([gain_ref[...], jnp.zeros((3, block), F32)], 0)
        wide = jnp.concatenate([rows, jnp.zeros((8, D - block), F32)], 1)
        packed[block:] = pltpu.roll(wide, meta[0] * block, 1).astype(LOW)

    shape = (block + 8, D)
    return call(
        "pack_first",
        body,
        (1,),
        meta,
        (project_in, project_out, gains),
        [
            pl.BlockSpec((1,) + project_in.shape[1:], lambda *_: (0, 0, 0, 0)),
            pl.BlockSpec((1,) + project_out.shape[1:], lambda *_: (0, 0, 0)),
            whole(gains.shape),
        ],
        [jax.ShapeDtypeStruct(shape, LOW)],
        [whole(shape)],
        [],
    )[0]


def one_hot(rows, offset):
    row = lax.broadcasted_iota(jnp.int32, (rows, D), 0)
    lane = lax.broadcasted_iota(jnp.int32, (rows, D), 1)
    return (lane == row + offset).astype(F32)


def collect(plan, meta, pieces, attention):
    count = pieces[0].shape[-3]
    n = len(pieces)
    shape = pieces[0].shape[-3:]
    groups = D // plan.width

    def body(meta, *rest):
        refs, (out, tile_out) = rest[:n], rest[n:]
        dp_at, mp_at = meta[0], meta[1 + 3 * plan.pairs]
        group = lax.broadcasted_iota(jnp.int32, (8, D), 1) // plan.width
        row = lax.broadcasted_iota(jnp.int32, (8, D), 0)
        place = one_hot(plan.block, dp_at * plan.block)
        def one(index, _):
            heads = (jnp.zeros((8, D), jnp.int32) + index) < attention
            value = refs[0][0, index]
            for ref in refs[1:]:
                value = value + ref[0, index].astype(F32)
            out[index] = value
            square = value * value
            lanes = jnp.broadcast_to(jnp.sum(square, 0, keepdims=True), (8, D))
            mask = jnp.where(heads, (group == row).astype(F32), (row == 0).astype(F32))
            sums = lax.dot_general(
                mask, square, (((1,), (1,)), ((), ())), precision=EXACT, preferred_element_type=F32
            )
            tile = lax.dot_general(
                sums, place, (((1,), (0,)), ((), ())), precision=EXACT, preferred_element_type=F32
            )
            spread = jnp.zeros_like(tile)
            for part in range(groups):
                shift = lax.rem(mp_at * plan.width + (D - part * plan.width), D)
                moved = pltpu.roll(jnp.where(group == part, lanes, 0.0), shift, 1)
                spread = jnp.where(row == 4 + part, moved, spread)
            spread = jnp.where(heads, spread, jnp.where(row == 4 + mp_at, lanes, 0.0))
            tile_out[index] = jnp.where(row < 4, tile, spread)
            return 0

        lax.fori_loop(0, count, one, 0)

    return call(
        "collect",
        body,
        (1,),
        meta,
        tuple(pieces),
        [whole(item.shape) for item in pieces],
        [jax.ShapeDtypeStruct(shape, F32), jax.ShapeDtypeStruct((count, 8, D), F32)],
        [whole(shape), whole((count, 8, D))],
        [],
    )


def finish(plan, meta, sums, statistics, gain_state):
    counts = [item.shape for item in statistics]

    def body(meta, sum_ref, *rest):
        olds, gains = rest[:8], rest[8:12]
        norm_out, news, rates, gain_outs = rest[12], rest[13:21], rest[21], rest[22:]
        tiles = [sum_ref[6], sum_ref[1], sum_ref[0]]
        feeds = [(sum_ref[2], sum_ref[3]), (sum_ref[4], sum_ref[5])]
        gain_sum = 0.5 * sum_ref[7]
        total = jnp.sum(gain_sum * gain_sum)
        for tile in tiles:
            total = total + jnp.sum(tile[:4])
        for up, down in feeds:
            total = total + jnp.sum(up[:1]) + jnp.sum(down[:1])
        totals = jnp.full((8, D), total, F32)
        norm = jnp.sqrt(totals)
        factor = jnp.minimum(1.0, 1.0 / norm)
        squared = (factor * factor)[:1]
        norm_out[...] = norm[:, :128]
        rates[...] = factor[:, :128]

        def renew(old, sums, number):
            return DECAY * old + (1.0 - DECAY) * (sums * squared / number + EPS_STAT)

        for layer, tile in enumerate(tiles):
            for part in range(3):
                news[0][layer, part : part + 1] = renew(olds[0][layer, part : part + 1], tile[part : part + 1], D)
                news[1][layer, part : part + 1] = renew(
                    olds[1][layer, part : part + 1], tile[4 + part : 5 + part], D
                )
            news[2][layer : layer + 1] = renew(olds[2][layer : layer + 1], tile[7:8], D)
            news[3][layer : layer + 1] = renew(olds[3][layer : layer + 1], tile[3:4], D)
        for layer, (up, down) in enumerate(feeds):
            news[4][layer : layer + 1] = renew(olds[4][layer : layer + 1], up[:1], FF)
            news[7][layer : layer + 1] = renew(olds[7][layer : layer + 1], down[:1], FF)
            for part in range(FF // D):
                cut = slice(part * D, (part + 1) * D)
                news[5][layer : layer + 1, cut] = renew(
                    olds[5][layer : layer + 1, cut], up[4 + part : 5 + part], D
                )
                news[6][layer : layer + 1, cut] = renew(
                    olds[6][layer : layer + 1, cut], down[4 + part : 5 + part], D
                )
        shift = lax.rem(D - meta[0] * plan.block, D)
        grad = (pltpu.roll(gain_sum, shift, 1) * factor)[:5, : plan.block]
        master, square, moment, average = [item[...] for item in gains]
        square_new = DECAY * square + (1.0 - DECAY) * (grad * grad + EPS_STAT)
        stepped = grad * lax.rsqrt(square_new)
        moment_new = MOMENTUM * moment + stepped
        master_new = master - RATE_GAIN * (MOMENTUM * moment_new + stepped)
        values = (
            grad,
            square_new,
            moment_new,
            master_new,
            AVERAGE * average + (1.0 - AVERAGE) * master_new,
            master_new,
        )
        for out, value in zip(gain_outs, values):
            out[...] = value.astype(out.dtype)

    small = gain_state[0].shape
    outs = (
        [jax.ShapeDtypeStruct((8, 128), F32)]
        + [jax.ShapeDtypeStruct(shape, F32) for shape in counts]
        + [jax.ShapeDtypeStruct((8, 128), F32)]
        + [jax.ShapeDtypeStruct(small, F32)] * 5
        + [jax.ShapeDtypeStruct(small, LOW)]
    )
    inputs = (sums, *statistics, *gain_state)
    return call(
        "finish",
        body,
        (1,),
        meta,
        inputs,
        [whole(item.shape) for item in inputs],
        outs,
        [whole(item.shape) for item in outs],
        [],
    )


def step_values(grad, scale, master, moment, average):
    stepped = grad * scale
    moment_new = MOMENTUM * moment + stepped
    master_new = master - RATE_MATRIX * (MOMENTUM * moment_new + stepped)
    return grad, moment_new, master_new, AVERAGE * average + (1.0 - AVERAGE) * master_new


def columns(rows, offset, size):
    filled = jnp.concatenate([rows] * (8 // rows.shape[0] + 1), 0)[:8]
    wide = (size + 127) // 128 * 128
    return jnp.transpose(pltpu.roll(filled, lax.rem(D - offset, D), 1)[:, :wide])[:size]


def update_attention(plan, meta, rates, grads, rows_in, cols_in, rows_out, cols_out, state_in, state_out):
    width, block = plan.width, plan.block

    def body(meta, rates_ref, grad_a, grad_b, rin, cin, rout, cout, *rest):
        ins, outs = rest[:6], rest[6:]
        layer = pl.program_id(0)
        dp_at, mp_at = meta[0], meta[1 + 3 * plan.pairs]
        grad = jnp.where(layer == 0, grad_a[0], jnp.where(layer == 1, grad_b[1], grad_b[0]))
        grad = grad * rates_ref[:1, :1]
        means = jnp.mean(rin[0], -1, keepdims=True)
        row_scale = lax.rsqrt(columns(rin[0] / means, dp_at * block, block))
        shift = lax.rem(D - mp_at * width, D)
        col_scale = lax.rsqrt(pltpu.roll(jnp.concatenate([cin[0]] * 3, 0)[:8], shift, 1)[:3, :width])
        for part in range(3):
            values = step_values(
                grad[:, part * width : (part + 1) * width],
                row_scale[:, part : part + 1] * col_scale[part : part + 1],
                ins[0][0, part],
                ins[1][0, part],
                ins[2][0, part],
            )
            for out, value in zip(outs[:4], values):
                out[0, part] = value
            outs[4][0, part] = values[2].astype(LOW)
        turned = jnp.transpose(grad[:, 3 * width :])
        row, col = rout[pl.ds(layer, 1), :], cout[pl.ds(layer, 1), :]
        mean = jnp.mean(row, -1, keepdims=True)
        row_scale = lax.rsqrt(columns(row / mean, mp_at * width, width))[:, :1]
        shift = lax.rem(D - dp_at * block, D)
        col_scale = lax.rsqrt(pltpu.roll(jnp.broadcast_to(col, (8, D)), shift, 1)[:1, :block])
        values = step_values(turned, row_scale * col_scale, ins[3][0], ins[4][0], ins[5][0])
        for out, value in zip(outs[5:9], values):
            out[0] = value
        outs[9][0] = values[2].astype(LOW)

    def spec(shape):
        return pl.BlockSpec((1,) + shape, lambda p, _: (p,) + (0,) * len(shape))

    shape_in, shape_out = (3, block, width), (width, block)
    outs = (
        [jax.ShapeDtypeStruct((3,) + shape_in, F32)] * 4
        + [jax.ShapeDtypeStruct((3,) + shape_in, LOW)]
        + [jax.ShapeDtypeStruct((3,) + shape_out, F32)] * 4
        + [jax.ShapeDtypeStruct((3,) + shape_out, LOW)]
    )
    return call(
        "update_attention",
        body,
        (3,),
        meta,
        (rates, *grads, rows_in, cols_in, rows_out, cols_out, *state_in, *state_out),
        [whole((8, 128)), whole((1, block, D)), whole((2, block, D))]
        + [spec((3, D)), spec((3, D)), whole((3, D)), whole((3, D))]
        + [spec(shape_in)] * 3
        + [spec(shape_out)] * 3,
        outs,
        [spec(shape_in)] * 5 + [spec(shape_out)] * 5,
        [],
    )


def update_feed(plan, meta, rates, grads, rows_up, cols_up, rows_down, cols_down, state_up, state_down):
    hidden, block = plan.hidden, plan.block

    def body(meta, rates_ref, grad_a, grad_b, rup, cup, rdown, cdown, *rest):
        ins, outs = rest[:6], rest[6:]
        layer = pl.program_id(0)
        lanes = pl.ds(pl.multiple_of(meta[1 + 3 * plan.pairs] * hidden, 128), hidden)
        one = pl.ds(layer, 1)
        mean_up = jnp.mean(rup[one, :], -1, keepdims=True)
        mean_down = jnp.mean(rdown[one, :], -1, keepdims=True)
        along = (rup[one, :] / mean_up, cdown[one, :])
        across = (cup[one, lanes], rdown[one, lanes] / mean_down)
        for part in range(2):
            grad = jnp.where(layer == 0, grad_a[part], grad_b[part]) * rates_ref[:1, :1]
            row_scale = lax.rsqrt(columns(along[part], meta[0] * block, block))[:, :1]
            values = step_values(
                grad,
                row_scale * lax.rsqrt(across[part]),
                ins[3 * part][0],
                ins[3 * part + 1][0],
                ins[3 * part + 2][0],
            )
            for out, value in zip(outs[5 * part : 5 * part + 4], values):
                out[0] = value
            outs[5 * part + 4][0] = values[2].astype(LOW)

    state = pl.BlockSpec((1, block, hidden), lambda p, _: (p, 0, 0))
    outs = ([jax.ShapeDtypeStruct((2, block, hidden), F32)] * 4 + [jax.ShapeDtypeStruct((2, block, hidden), LOW)]) * 2
    values = call(
        "update_feed",
        body,
        (2,),
        meta,
        (
            rates,
            *grads,
            rows_up,
            cols_up,
            rows_down,
            cols_down,
            *state_up,
            *[item.transpose(0, 2, 1) for item in state_down],
        ),
        [whole((8, 128)), *[whole((2, block, D))] * 2]
        + [whole((2, D)), whole((2, FF)), whole((2, FF)), whole((2, D))]
        + [state] * 6,
        outs,
        [state] * 10,
        [],
    )
    return [*values[:5], *[item.transpose(0, 2, 1) for item in values[5:]]]


def on_device(
    sizes,
    encoder_in,
    decoder_in,
    decoder_cotangent,
    counts,
    prefix_len,
    suffix_len,
    project_in,
    project_in_rows,
    project_in_cols,
    project_in_moment,
    project_in_average,
    project_out,
    project_out_rows,
    project_out_cols,
    project_out_moment,
    project_out_average,
    expand,
    expand_rows,
    expand_cols,
    expand_moment,
    expand_average,
    contract,
    contract_rows,
    contract_cols,
    contract_moment,
    contract_average,
    norm_gains,
    norm_gains_square,
    norm_gains_moment,
    norm_gains_average,
):
    dp_n, mp_n = sizes
    dp_index = lax.axis_index("dp")
    mp_index = lax.axis_index("mp")
    side = mp_index % 2
    pairs = prefix_len.shape[0]
    half = pairs // 2
    width = project_in.shape[-1]
    block = project_in.shape[-2]
    plan = Plan(dp_n, block, width, expand.shape[-1], pairs)
    low, f32 = LOW, F32

    def swap(value, axis, bit):
        count = dp_n if axis == "dp" else mp_n
        return lax.ppermute(value, axis, [(i, i ^ bit) for i in range(count)])

    def bits(count):
        return [1 << i for i in range(count.bit_length() - 1)]

    hold = lax.optimization_barrier

    class Gather:
        def __init__(self, blocks):
            self.items, self.sent, self.own = [{} for _ in blocks], [], list(blocks)

        def step(self, chain, *sends, later=()):
            names = [(item, name) for item, name in self.sent if (name, item) not in later]
            late = [(item, name) for item, name in self.sent if (name, item) in later]
            values = [self.items[item][name] for item, name in names]
            if names:
                chain, values, self.own = hold((list(chain), values, self.own))
            for (item, name), value in zip(names, values):
                self.items[item][name] = value
            self.sent = late
            for name, item in sends:
                if name == "fours":
                    four = swap(jnp.concatenate([self.own[at] for at in item]), "dp", 4)
                    for place, at in enumerate(item):
                        self.items[at]["four"] = four[place * block : (place + 1) * block]
                        self.sent.append((at, "four"))
                    continue
                parts = self.items[item]
                if name == "four":
                    parts[name] = swap(self.own[item], "dp", 4)
                    self.sent.append((item, name))
                    continue
                if "two" not in parts:
                    parts["two"] = jnp.concatenate([self.own[item], parts["four"]])
                if name == "far":
                    parts[name] = swap(parts["two"], "dp", 2)
                else:
                    parts[name] = swap(parts["two" if name == "near" else "far"], "dp", 1)
                self.sent.append((item, name))
            return chain

        def take(self, item, index=0):
            parts = self.items[item]
            height = self.own[item].shape[0]
            return [parts[name] for name in ("two", "far", "near", "last")], height, index * block

    class Plain:
        def __init__(self, blocks):
            self.own = list(blocks)

        def step(self, chain, *sends, later=()):
            return chain

        def take(self, item, index=0):
            own = self.own[item][index * block : (index + 1) * block]
            return [lax.all_gather(own, "dp", axis=0, tiled=True)], D, 0

    def scatter(parts, attention):
        summed = lax.psum_scatter(parts[0], "dp", scatter_dimension=1, tiled=True)
        return collect(plan, meta, [summed[None]], attention)

    def total(value, axes):
        for axis, count in axes:
            for bit in bits(count):
                sent = value.astype(low)
                value = sent.astype(value.dtype) + swap(sent, axis, bit).astype(value.dtype)
        return value

    def total_dp(value):
        return total(value, [("dp", dp_n)])

    def total_all(value):
        return total(value, [("mp", mp_n), ("dp", dp_n)])

    def reduce_own(own, oth, first=()):
        sent = (own.astype(f32) + swap(oth, "mp", 1).astype(f32)).astype(low)
        for bit in bits(mp_n)[1:-1]:
            sent = (sent.astype(f32) + swap(sent, "mp", bit).astype(f32)).astype(low)
        sent, first = hold((sent, first))
        return sent, swap(sent, "mp", bits(mp_n)[-1])

    def relative(value):
        split = value.reshape((half, 2) + value.shape[1:])
        return (
            lax.dynamic_index_in_dim(split, side, 1, False),
            lax.dynamic_index_in_dim(split, 1 - side, 1, False),
        )

    def absolute(own):
        other = swap(own, "mp", 1)
        even = jnp.where(side == 0, own, other)
        odd = jnp.where(side == 0, other, own)
        return jnp.stack([even, odd], 1).reshape((pairs,) + own.shape[1:])

    def core(value):
        return swap(value, "mp", 1)

    def attention_block(layer):
        return jnp.concatenate(
            [project_in[layer, 0], project_in[layer, 1], project_in[layer, 2], project_out[layer].T], 1
        ).astype(low)

    def feed_block(layer):
        return [expand[layer].astype(low), contract[layer].T.astype(low)]

    direct = plan.direct
    place = dp_index[None].astype(jnp.int32)
    if direct:
        first = pack_first(plan, place, project_in, project_out, norm_gains)
    else:
        first = attention_block(0)
    blocks = [
        first,
        *feed_block(0),
        attention_block(1),
        attention_block(2),
        jnp.concatenate(feed_block(1)),
    ]
    gather = (Gather if direct else Plain)(blocks)
    gather.step((), ("four", 0))
    gather.step((), ("far", 0), ("near", 0), ("four", 1))
    gather.step((), ("last", 0), later=(("four", 1),))
    enc_att = [gather.take(0)]
    if direct:
        height = block + 8
        gain_rows = sum(
            item[at : at + 8].astype(f32) for item in enc_att[0][0] for at in (block, height + block)
        )
    else:
        gain_full = lax.dynamic_update_slice(
            jnp.zeros((8, D), low), norm_gains.astype(low), (0, dp_index * block)
        )
        gain_rows = total_dp(gain_full).astype(f32)
    gains = [gain_rows[i : i + 1] for i in range(5)]

    place_rel = jnp.concatenate([2 * jnp.arange(half) + side, 2 * jnp.arange(half) + 1 - side])
    prefix_rel = jnp.concatenate(relative(prefix_len))
    suffix_rel = jnp.concatenate(relative(suffix_len))
    images = place_rel < counts[0, 0]
    active = place_rel < counts[0, 0] + counts[0, 1]
    meta = jnp.concatenate(
        [
            dp_index[None].astype(jnp.int32),
            images.astype(jnp.int32),
            prefix_rel,
            suffix_rel,
            mp_index[None].astype(jnp.int32),
        ]
    )
    steps = jnp.arange(SUFFIX)
    live = active[:, None] & (steps[None, :] < suffix_rel[:, None])

    mid = half * SUFFIX
    enc_own, enc_oth = relative(
        jnp.pad(encoder_in.reshape(pairs, ENC_LEN, D), ((0, 0), (0, LONG - ENC_LEN), (0, 0)))
    )
    dec_rel = jnp.concatenate(relative(decoder_in.reshape(pairs, SUFFIX, D))).reshape(2 * mid, D)
    cot = jnp.concatenate(relative(decoder_cotangent.reshape(pairs, SUFFIX, D)))
    cot = jnp.where(live[:, :, None], cot, f32(0.0)).reshape(2 * mid, D)
    cot_low = cot.astype(low)

    def triple(value):
        return value.reshape(half, SUFFIX, D)

    (enc_oth,) = gather.step((enc_oth,), ("far", 1), ("near", 1), ("four", 2), later=(("last", 0),))
    own, oth, kept_enc = encoder_attention(plan, meta, enc_own, enc_oth, gains[0], enc_att, 0, half)
    own, oth, dec_rel, cot, cot_low = gather.step(
        (own, oth, dec_rel, cot, cot_low), ("last", 1), ("near", 2), ("far", 2), ("fours", (3, 4))
    )
    sums = gather.step(reduce_own(own, oth), ("last", 2))
    enc_feed = [gather.take(1), gather.take(2)]
    enc_mid, norm_mid = add_norm(meta, "add_norm_mid", enc_own, *sums, gains[1])
    norm_mid_oth = core(norm_mid)

    (norm_mid_oth,) = gather.step(
        (norm_mid_oth,), ("far", 3), ("near", 3), ("four", 5), later=(("last", 2),)
    )
    own, oth = encoder_feed(plan, meta, norm_mid, norm_mid_oth, enc_feed, 0, half)
    own, oth = gather.step((own, oth), ("last", 3), ("far", 4), ("near", 4), later=(("four", 5),))
    sums = reduce_own(own, oth)
    (dec_rel,) = gather.step((dec_rel,), ("last", 4), later=(("last", 3),))

    self_att = [gather.take(3)]
    own, oth, kept_self = decoder_self(plan, meta, dec_rel, gains[2], self_att)
    sums = gather.step(sums)
    sums_self = reduce_own(own, oth, sums)
    gather.step((sums_self[0],), ("far", 5), ("near", 5))
    cross_att = [gather.take(4)]
    memory = (enc_mid + (sums[0].astype(f32) + sums[1].astype(f32))).astype(low)
    dec_one, norm_cross = add_norm(meta, "add_norm_cross", dec_rel[:mid], *sums_self, gains[3])
    memory, norm_cross = gather.step((memory, norm_cross), ("last", 5))
    memory_oth = core(memory)
    norm_cross_oth = core(norm_cross)

    cross_in = (triple(norm_cross), triple(norm_cross_oth), memory, memory_oth, cross_att)
    own, oth, *kept_cross = decoder_cross(plan, meta, *cross_in)
    sums = reduce_own(own, oth)
    dec_two, norm_last = add_norm(
        meta, "add_norm_last", dec_one, sums[0].reshape(mid, D), sums[1].reshape(mid, D), gains[4]
    )
    dec_feed = [gather.take(5), gather.take(5, 1)]

    own, oth, *grads_dec = decoder_feed(plan, meta, norm_last, core(norm_last), cot_low, dec_feed)
    if direct:
        more_dec = swap(grads_dec[0], "dp", 1)
    sums = reduce_own(own, oth)
    out_own = dec_two + (sums[0][0].astype(f32) + sums[1][0].astype(f32))
    grad, grad_low, gain_four = norm_back(
        meta, "norm_back_last", dec_two, gains[4], cot[:mid], sums[0][1], sums[1][1], True
    )

    own, oth, own_long, oth_long, *grads_cross = decoder_cross_back(
        plan, meta, *cross_in, *kept_cross, triple(grad_low), triple(core(grad_low))
    )
    if direct:
        own, oth, own_long, oth_long, more_dec = hold((own, oth, own_long, oth_long, more_dec))
        more_cross = swap(grads_cross[0], "dp", 1)
    sums = reduce_own(own, oth)
    sums_enc = reduce_own(own_long, oth_long, sums)
    if direct:
        keep, more_dec, _ = hold((grads_dec[1], more_dec, sums[0]))
        keep_dec, away_dec = fold(plan, meta, [keep], [more_dec], halves)
        *sums, away_dec = hold((*sums, away_dec))
        more_dec = swap(away_dec, "dp", 2)
    grad, grad_low, gain_three = norm_back(
        meta, "norm_back_cross", dec_one, gains[3], grad, sums[0].reshape(mid, D), sums[1].reshape(mid, D), True
    )
    grad_low_oth = core(grad_low)

    own_self, oth_self, *grads_self = decoder_self_back(
        plan, meta, dec_rel, gains[2], self_att, kept_self, grad_low, grad_low_oth
    )
    decoder_out = absolute(triple(out_own)).reshape(2 * mid, D)
    if direct:
        own_self, oth_self, decoder_out = hold((own_self, oth_self, decoder_out))
    sums_self = reduce_own(own_self, oth_self)
    if direct:
        *sums_enc, _, decoder_out, more_cross, more_dec = hold(
            (*sums_enc, sums_self[0], decoder_out, more_cross, more_dec)
        )
    grad_enc = sums_enc[0].astype(f32) + sums_enc[1].astype(f32)
    enc_low = grad_enc.astype(low)
    enc_low_oth = core(enc_low)

    if direct:
        keep_dec, away_dec = fold(plan, meta, [keep_dec], [more_dec], halves)
        enc_low_oth, away_self, away_dec = hold((enc_low_oth, grads_self[0], away_dec))
        more_self = swap(away_self, "dp", 1)
        more_dec = swap(away_dec, "dp", 4)
    own, oth, *grads_enc = encoder_feed_back(plan, meta, norm_mid, norm_mid_oth, enc_low, enc_low_oth, enc_feed)
    if direct:
        own, oth, more_self, more_dec, *sums_self = hold((own, oth, more_self, more_dec, *sums_self))
        more_up, more_down = [swap(item, "dp", 1) for item in grads_enc[::2]]
    sums = reduce_own(own, oth)
    if direct:
        keep_cross, keep_self, more_cross, more_self, _ = hold(
            (grads_cross[1], grads_self[1], more_cross, more_self, sums[0])
        )
        keep_mid, away_mid = fold(plan, meta, [keep_cross, keep_self], [more_cross, more_self], halves)
        more_mid = swap(away_mid, "dp", 2)
        sums_self, _ = hold((sums_self, away_mid))
    grad, gain_two = norm_back(meta, "norm_back_self", dec_rel[:mid], gains[2], grad, *sums_self, False)
    decoder_in_grad = absolute(triple(grad)).reshape(2 * mid, D)
    if direct:
        sum_dec = collect(plan, meta, [keep_dec, more_dec], 0)
        *sums, sum_dec, decoder_in_grad, more_up = hold((*sums, sum_dec, decoder_in_grad, more_up))
    grad_enc, enc_low, gain_one = norm_back(
        meta, "norm_back_mid", enc_mid, gains[1], grad_enc, *sums, True
    )
    if direct:
        enc_low, more_down, more_mid = hold((enc_low, more_down, more_mid))
    enc_low_oth = core(enc_low)

    if direct:
        keep_mid, away_mid = fold(plan, meta, [keep_mid], [more_mid], halves)
        keep_enc, away_enc = fold(plan, meta, grads_enc[1::2], [more_up, more_down], halves)
        enc_low_oth, away_enc, away_mid = hold((enc_low_oth, away_enc, away_mid))
        more_mid = swap(away_mid, "dp", 4)
        more_enc = swap(away_enc, "dp", 2)
    own, oth, *grads_att = encoder_attention_back(
        plan, meta, enc_own, enc_oth, gains[0], enc_att, kept_enc, enc_low, enc_low_oth
    )
    if direct:
        more_att = swap(grads_att[0], "dp", 1)
        own, oth, more_enc, more_mid = hold((own, oth, more_enc, more_mid))
        keep_enc, away_enc = fold(plan, meta, [keep_enc], [more_enc], halves)
        more_enc = swap(away_enc, "dp", 4)
    sums = reduce_own(own, oth)
    if direct:
        keep_att, more_att, _, _ = hold((grads_att[1], more_att, away_enc, sums[0]))
        mine, *others = fold(plan, meta, [keep_att], [more_att], apart)
        others, more_enc, sums = hold((others, more_enc, sums))
        pieces_att = [mine] + [swap(item, "dp", 2 * (i + 1)) for i, item in enumerate(others)]
        sum_mid = collect(plan, meta, [keep_mid, more_mid], 2)
        sum_enc = collect(plan, meta, [keep_enc, more_enc], 0)
        tiles = [sum_mid[1], sum_enc[1], sum_dec[1]]
    else:
        sum_dec = scatter(grads_dec, 0)
        sum_mid = [jnp.concatenate(item) for item in zip(scatter(grads_cross, 1), scatter(grads_self, 1))]
        sum_enc = scatter([jnp.concatenate(grads_enc)], 0)
        tiles = [sum_mid[1], sum_enc[1], sum_dec[1]]
    grad_enc, gain_zero = norm_back(meta, "norm_back_enc", enc_own, gains[0], grad_enc, *sums, False)
    if direct:
        *pieces_att, _, _ = hold((*pieces_att, sum_enc[1], gain_zero))
    sum_att = collect(plan, meta, pieces_att, 1) if direct else scatter(grads_att, 1)
    encoder_in_grad = absolute(grad_enc)[:, :ENC_LEN].reshape(pairs * ENC_LEN, D)
    gain_tile = jnp.concatenate(
        [gain_zero, gain_one, gain_two, gain_three, gain_four, jnp.zeros((3, D), f32)]
    )[None]
    tiles = total_all(jnp.concatenate([*tiles, sum_att[1], gain_tile]))
    done = finish(
        plan,
        meta,
        tiles,
        (
            project_in_rows,
            project_in_cols,
            project_out_rows,
            project_out_cols,
            expand_rows,
            expand_cols,
            contract_rows,
            contract_cols,
        ),
        (norm_gains, norm_gains_square, norm_gains_moment, norm_gains_average),
    )
    grad_norm, news, rates, pgain = done[0][0, 0], done[1:9], done[9], done[10:]
    att = update_attention(
        plan,
        meta,
        rates,
        (sum_att[0], sum_mid[0]),
        *news[:4],
        (project_in, project_in_moment, project_in_average),
        (project_out, project_out_moment, project_out_average),
    )
    feed = update_feed(
        plan,
        meta,
        rates,
        (sum_enc[0], sum_dec[0]),
        *news[4:],
        (expand, expand_moment, expand_average),
        (contract, contract_moment, contract_average),
    )
    return (
        decoder_out,
        encoder_in_grad,
        decoder_in_grad,
        grad_norm,
        att[0],
        news[0],
        news[1],
        *att[1:5],
        att[5],
        news[2],
        news[3],
        *att[6:10],
        feed[0],
        news[4],
        news[5],
        *feed[1:5],
        feed[5],
        news[6],
        news[7],
        *feed[6:10],
        *pgain,
    )


def solution(mesh):
    placed = (
        P("dp", None),
        P("dp", None),
        P("dp", None),
        P("dp", None),
        P("dp"),
        P("dp"),
        P(None, None, "dp", "mp"),
        P(),
        P(),
        P(None, None, "dp", "mp"),
        P(None, None, "dp", "mp"),
        P(None, "mp", "dp"),
        P(),
        P(),
        P(None, "mp", "dp"),
        P(None, "mp", "dp"),
        P(None, "dp", "mp"),
        P(),
        P(),
        P(None, "dp", "mp"),
        P(None, "dp", "mp"),
        P(None, "mp", "dp"),
        P(),
        P(),
        P(None, "mp", "dp"),
        P(None, "mp", "dp"),
        P(None, "dp"),
        P(None, "dp"),
        P(None, "dp"),
        P(None, "dp"),
    )
    return jax.shard_map(
        functools.partial(on_device, (mesh.shape["dp"], mesh.shape["mp"])),
        mesh=mesh,
        in_specs=placed,
        out_specs=(
            P("dp", None),
            P("dp", None),
            P("dp", None),
            P(),
            P(None, None, "dp", "mp"),
            P(),
            P(),
            P(None, None, "dp", "mp"),
            P(None, None, "dp", "mp"),
            P(None, None, "dp", "mp"),
            P(None, None, "dp", "mp"),
            P(None, "mp", "dp"),
            P(),
            P(),
            P(None, "mp", "dp"),
            P(None, "mp", "dp"),
            P(None, "mp", "dp"),
            P(None, "mp", "dp"),
            P(None, "dp", "mp"),
            P(),
            P(),
            P(None, "dp", "mp"),
            P(None, "dp", "mp"),
            P(None, "dp", "mp"),
            P(None, "dp", "mp"),
            P(None, "mp", "dp"),
            P(),
            P(),
            P(None, "mp", "dp"),
            P(None, "mp", "dp"),
            P(None, "mp", "dp"),
            P(None, "mp", "dp"),
            P(None, "dp"),
            P(None, "dp"),
            P(None, "dp"),
            P(None, "dp"),
            P(None, "dp"),
            P(None, "dp"),
        ),
        check_vma=False,
    )
```

```python
import functools

import jax
import jax.numpy as jnp
from jax import lax
from jax.experimental import pallas as pl
from jax.experimental.pallas import tpu as pltpu
from jax.sharding import PartitionSpec as P

D = 768
HEAD_DIM = 64
FF = 3072
PATCHES = 196
SUFFIX = 32
ENC_LEN = 228


EPS_NORM = 1e-06
EPS_STAT = 1e-30
DECAY = 0.99
MOMENTUM = 0.9
AVERAGE = 0.6
RATE_MATRIX = 0.004
RATE_GAIN = 0.05
MASKED = -1000000000.0


LOW = jnp.bfloat16
F32 = jnp.float32
VMEM_LIMIT = 56 * 1024 * 1024
LONG = (ENC_LEN + 7) // 8 * 8
EXACT = lax.Precision.HIGHEST


def dot(left, right, contract):
    return lax.dot_general(left, right, (contract, ((), ())), preferred_element_type=F32)


def mm(left, right):
    return dot(left, right, ((1,), (0,)))


def mm_t(left, right):
    return dot(left, right, ((1,), (1,)))


def t_mm(left, right):
    return dot(left, right, ((0,), (0,)))


def rms_scale(value):
    return lax.rsqrt(jnp.mean(value * value, -1, keepdims=True) + EPS_NORM)


def softmax(scores):
    expons = jnp.exp(scores - jnp.max(scores, -1, keepdims=True))
    return expons / jnp.sum(expons, -1, keepdims=True)


def gelu_parts(upper):
    inner = 0.7978845608028654 * (upper + 0.044715 * upper * upper * upper)
    bent = jnp.tanh(inner)
    value = 0.5 * upper * (1.0 + bent)
    slope = 0.5 * (1.0 + bent) + 0.5 * upper * (1.0 - bent * bent) * 0.7978845608028654 * (
        1.0 + 3.0 * 0.044715 * upper * upper
    )
    return value, slope


class Plan:
    def __init__(self, dp_n, block, width, hidden, pairs):
        self.dp_n, self.block, self.width, self.hidden, self.pairs = dp_n, block, width, hidden, pairs
        self.half = pairs // 2
        self.heads = width // HEAD_DIM
        self.direct = dp_n == 8

    def weight_specs(self, pieces):
        return [whole(item.shape) for item in flat(pieces)]

    def weight_scratch(self, pieces):
        return [pltpu.VMEM((len(pieces), D, D), LOW)]

    def assemble(self, meta, pieces, refs, scratch):
        refs = iter(refs)
        for count in range(len(pieces)):
            if not self.direct:
                scratch[count] = next(refs)[...]
                continue
            _, height, start = pieces[count]
            for places in ((0, 4), (2, 6), (1, 5), (3, 7)):
                ref = next(refs)
                for index, place in enumerate(places):
                    row = pl.multiple_of(jnp.bitwise_xor(meta[0], place) * self.block, 32)
                    first = start + index * height
                    scratch[count, pl.ds(row, self.block), :] = ref[first : first + self.block]

    def grad_shapes(self, count):
        if not self.direct:
            return [jax.ShapeDtypeStruct((count, D, D), F32)]
        shape = (self.dp_n // 2, count, self.block, D)
        return [jax.ShapeDtypeStruct(shape, LOW), jax.ShapeDtypeStruct(shape, F32)]

    def emit(self, meta, acc, refs):
        if not self.direct:
            refs[0][...] = acc[...]
            return
        for index in range(self.dp_n // 2):
            here = pl.multiple_of(jnp.bitwise_xor(meta[0], 2 * index) * self.block, 32)
            away = pl.multiple_of(jnp.bitwise_xor(meta[0], 2 * index + 1) * self.block, 32)
            for count in range(acc.shape[0]):
                refs[0][index, count] = acc[count, pl.ds(away, self.block), :].astype(LOW)
                refs[1][index, count] = acc[count, pl.ds(here, self.block), :]


def flat(pieces):
    return [item for arrays, _, _ in pieces for item in arrays]


def whole(shape):
    return pl.BlockSpec(shape, lambda *_: (0,) * len(shape))


def own_spec(count, base, shape):
    return pl.BlockSpec(
        (1,) + shape, lambda p, _: (base + jnp.maximum(p - count, 0),) + (0,) * len(shape)
    )


def oth_spec(count, base, shape):
    return pl.BlockSpec(
        (1,) + shape, lambda p, _: (base + jnp.minimum(p, count - 1),) + (0,) * len(shape)
    )


def step_spec(shape):
    return pl.BlockSpec((1,) + shape, lambda p, _: (p,) + (0,) * len(shape))


def call(name, body, grid, meta, inputs, in_specs, outs, out_specs, scratch):
    return pl.pallas_call(
        body,
        name=name,
        out_shape=outs,
        grid_spec=pltpu.PrefetchScalarGridSpec(
            num_scalar_prefetch=1,
            grid=grid,
            in_specs=in_specs,
            out_specs=out_specs,
            scratch_shapes=scratch,
        ),
        cost_estimate=pl.CostEstimate(flops=1, transcendentals=0, bytes_accessed=1),
        compiler_params=pltpu.CompilerParams(
            dimension_semantics=("arbitrary",) * len(grid), vmem_limit_bytes=VMEM_LIMIT
        ),
    )(meta, *inputs)


def key_mask(meta, pairs, slot):
    place = lax.broadcasted_iota(jnp.int32, (1, ENC_LEN), 1)
    image, prefix = meta[1 + slot], meta[1 + pairs + slot]
    return (place < image * PATCHES) | ((place >= PATCHES) & (place < PATCHES + prefix))


def attend_heads(plan, queries, keys, values, allowed):
    mixed = []
    for head in range(plan.heads):
        cut = slice(head * HEAD_DIM, (head + 1) * HEAD_DIM)
        scores = jnp.where(allowed, mm_t(queries[:, cut], keys[:, cut]) * 0.125, MASKED)
        mixed.append(mm(softmax(scores).astype(LOW), values[:, cut]).astype(LOW))
    return jnp.concatenate(mixed, 1)


def attend_heads_back(plan, queries, keys, values, allowed, grad_mixed):
    grads = ([], [], [])
    for head in range(plan.heads):
        cut = slice(head * HEAD_DIM, (head + 1) * HEAD_DIM)
        query, key, value, grad = queries[:, cut], keys[:, cut], values[:, cut], grad_mixed[:, cut]
        probs = softmax(jnp.where(allowed, mm_t(query, key) * 0.125, MASKED))
        grad_probs = mm_t(grad, value)
        inner = jnp.sum(grad_probs * probs, -1, keepdims=True)
        grad_scores = (probs * (grad_probs - inner)).astype(LOW)
        grads[0].append((mm(grad_scores, key) * 0.125).astype(LOW))
        grads[1].append((t_mm(grad_scores, query) * 0.125).astype(LOW))
        grads[2].append(t_mm(probs.astype(LOW), grad).astype(LOW))
    return tuple(jnp.concatenate(item, 1) for item in grads)


def slot_of(plan, count, base, step):
    return jnp.where(step < count, plan.half + base + step, base + step - count)


def pick(step, count, own, oth, rows):
    return jnp.where(step < count, oth[0, :rows], own[0, :rows])


def put(step, count, own, oth, value):
    @pl.when(step < count)
    def _():
        oth[0, : value.shape[0]] = value

    @pl.when(step >= count)
    def _():
        own[0, : value.shape[0]] = value


def encoder_attention(plan, meta, own, oth, gain, pieces, base, count):
    w3 = 3 * plan.width
    n = len(flat(pieces))

    def body(meta, own_ref, oth_ref, gain_ref, *rest):
        refs, (own_out, oth_out, kept, weight) = rest[:n], rest[n:]
        step = pl.program_id(0)

        @pl.when(step == 0)
        def _():
            plan.assemble(meta, pieces, refs, weight)

        value = pick(step, count, own_ref, oth_ref, ENC_LEN).astype(F32)
        normed = (value * rms_scale(value) * gain_ref[...]).astype(LOW)
        joined = mm(normed, weight[0, :, :w3]).astype(LOW)
        allowed = key_mask(meta, plan.pairs, slot_of(plan, count, base, step))
        width = plan.width
        mixed = attend_heads(
            plan, joined[:, :width], joined[:, width : 2 * width], joined[:, 2 * width :], allowed
        )
        kept[0, :, :w3] = joined
        kept[0, :, w3:] = mixed
        put(step, count, own_out, oth_out, mm_t(mixed, weight[0, :, w3:]).astype(LOW))

    rows = (LONG, D)
    return call(
        "encoder_attention",
        body,
        (2 * count,),
        meta,
        (own, oth, gain, *flat(pieces)),
        [own_spec(count, base, rows), oth_spec(count, base, rows), whole((1, D)), *plan.weight_specs(pieces)],
        [jax.ShapeDtypeStruct((count,) + rows, LOW)] * 2
        + [jax.ShapeDtypeStruct((2 * count, ENC_LEN, w3 + plan.width), LOW)],
        [own_spec(count, 0, rows), oth_spec(count, 0, rows), step_spec((ENC_LEN, w3 + plan.width))],
        plan.weight_scratch(pieces),
    )


def encoder_attention_back(plan, meta, own, oth, gain, pieces, kept, grad_own, grad_oth):
    count = plan.half
    width, w3 = plan.width, 3 * plan.width
    n = len(flat(pieces))

    def body(meta, own_ref, oth_ref, gain_ref, kept_ref, grad_own_ref, grad_oth_ref, *rest):
        refs, (own_out, oth_out), grad_refs = rest[:n], rest[n : n + 2], rest[n + 2 : -2]
        weight, acc = rest[-2:]
        step = pl.program_id(0)

        @pl.when(step == 0)
        def _():
            plan.assemble(meta, pieces, refs, weight)
            acc[...] = jnp.zeros_like(acc)

        value = pick(step, count, own_ref, oth_ref, ENC_LEN).astype(F32)
        normed = (value * rms_scale(value) * gain_ref[...]).astype(LOW)
        grad = pick(step, count, grad_own_ref, grad_oth_ref, ENC_LEN)
        allowed = key_mask(meta, plan.pairs, slot_of(plan, count, 0, step))
        grad_mixed = mm(grad, weight[0, :, w3:]).astype(LOW)
        acc[0, :, w3:] += t_mm(grad, kept_ref[0, :, w3:])
        joined = kept_ref[0, :, :w3]
        grads = attend_heads_back(
            plan, joined[:, :width], joined[:, width : 2 * width], joined[:, 2 * width :], allowed, grad_mixed
        )
        together = jnp.concatenate(grads, 1)
        acc[0, :, :w3] += t_mm(normed, together)
        put(step, count, own_out, oth_out, mm_t(together, weight[0, :, :w3]).astype(LOW))

        @pl.when(step == 2 * count - 1)
        def _():
            plan.emit(meta, acc, grad_refs)

    rows = (LONG, D)
    shapes = plan.grad_shapes(1)
    pair_specs = [own_spec(count, 0, rows), oth_spec(count, 0, rows)]
    return call(
        "encoder_attention_back",
        body,
        (2 * count,),
        meta,
        (own, oth, gain, kept, grad_own, grad_oth, *flat(pieces)),
        [*pair_specs, whole((1, D)), step_spec(kept.shape[1:]), *pair_specs, *plan.weight_specs(pieces)],
        [jax.ShapeDtypeStruct((count,) + rows, LOW)] * 2 + shapes,
        [*pair_specs, *[whole(item.shape) for item in shapes]],
        plan.weight_scratch(pieces) + [pltpu.VMEM((1, D, D), F32)],
    )


def encoder_feed(plan, meta, own, oth, pieces, base, count):
    n = len(flat(pieces))

    def body(meta, own_ref, oth_ref, *rest):
        refs, (own_out, oth_out, weight) = rest[:n], rest[n:]
        step = pl.program_id(0)

        @pl.when(step == 0)
        def _():
            plan.assemble(meta, pieces, refs, weight)

        normed = pick(step, count, own_ref, oth_ref, ENC_LEN)
        active = gelu_parts(mm(normed, weight[0]))[0].astype(LOW)
        put(step, count, own_out, oth_out, mm_t(active, weight[1]).astype(LOW))

    rows = (LONG, D)
    return call(
        "encoder_feed",
        body,
        (2 * count,),
        meta,
        (own, oth, *flat(pieces)),
        [own_spec(count, base, rows), oth_spec(count, base, rows), *plan.weight_specs(pieces)],
        [jax.ShapeDtypeStruct((count,) + rows, LOW)] * 2,
        [own_spec(count, 0, rows), oth_spec(count, 0, rows)],
        plan.weight_scratch(pieces),
    )


def encoder_feed_back(plan, meta, own, oth, grad_own, grad_oth, pieces):
    n = len(flat(pieces))
    count = plan.half

    def body(meta, own_ref, oth_ref, grad_own_ref, grad_oth_ref, *rest):
        refs, (own_out, oth_out), grad_refs = rest[:n], rest[n : n + 2], rest[n + 2 : -2]
        weight, acc = rest[-2:]
        step = pl.program_id(0)

        @pl.when(step == 0)
        def _():
            plan.assemble(meta, pieces, refs, weight)
            acc[...] = jnp.zeros_like(acc)

        normed = pick(step, count, own_ref, oth_ref, ENC_LEN)
        grad = pick(step, count, grad_own_ref, grad_oth_ref, ENC_LEN)
        active, slope = gelu_parts(mm(normed, weight[0]))
        grad_upper = (slope * mm(grad, weight[1])).astype(LOW)
        put(step, count, own_out, oth_out, mm_t(grad_upper, weight[0]).astype(LOW))
        acc[0] += t_mm(normed, grad_upper)
        acc[1] += t_mm(grad, active.astype(LOW))

        @pl.when(step == 2 * count - 1)
        def _():
            for index in range(2):
                size = len(grad_refs) // 2
                plan.emit(meta, acc.at[pl.ds(index, 1)], grad_refs[index * size : (index + 1) * size])

    rows = (LONG, D)
    shapes = plan.grad_shapes(1) * 2
    pair_specs = [own_spec(count, 0, rows), oth_spec(count, 0, rows)]
    return call(
        "encoder_feed_back",
        body,
        (2 * count,),
        meta,
        (own, oth, grad_own, grad_oth, *flat(pieces)),
        [*pair_specs, *pair_specs, *plan.weight_specs(pieces)],
        [jax.ShapeDtypeStruct((count,) + rows, LOW)] * 2 + shapes,
        [*pair_specs, *[whole(item.shape) for item in shapes]],
        plan.weight_scratch(pieces) + [pltpu.VMEM((2, D, D), F32)],
    )


def self_mask(plan, meta):
    rows = plan.pairs * SUFFIX
    query = lax.broadcasted_iota(jnp.int32, (rows, rows), 0)
    key = lax.broadcasted_iota(jnp.int32, (rows, rows), 1)
    pair = key // SUFFIX
    limit = jnp.zeros_like(key)
    for slot in range(plan.pairs):
        limit = jnp.where(pair == slot, meta[1 + 2 * plan.pairs + slot], limit)
    return (query // SUFFIX == pair) & (key <= query) & (key - pair * SUFFIX < limit)


def decoder_self(plan, meta, rows_in, gain, pieces):
    n = len(flat(pieces))
    width, w3 = plan.width, 3 * plan.width
    rows = plan.pairs * SUFFIX
    mid = rows // 2

    def body(meta, in_ref, gain_ref, *rest):
        refs, (own_out, oth_out, kept, weight) = rest[:n], rest[n:]
        plan.assemble(meta, pieces, refs, weight)
        value = in_ref[...].astype(F32)
        normed = (value * rms_scale(value) * gain_ref[...]).astype(LOW)
        joined = mm(normed, weight[0, :, :w3]).astype(LOW)
        mixed = attend_heads(
            plan, joined[:, :width], joined[:, width : 2 * width], joined[:, 2 * width :], self_mask(plan, meta)
        )
        kept[:, :w3] = joined
        kept[:, w3:] = mixed
        partial = mm_t(mixed, weight[0, :, w3:]).astype(LOW)
        own_out[...] = partial[:mid]
        oth_out[...] = partial[mid:]

    return call(
        "decoder_self",
        body,
        (1,),
        meta,
        (rows_in, gain, *flat(pieces)),
        [whole((rows, D)), whole((1, D)), *plan.weight_specs(pieces)],
        [jax.ShapeDtypeStruct((mid, D), LOW)] * 2 + [jax.ShapeDtypeStruct((rows, 4 * width), LOW)],
        [whole((mid, D))] * 2 + [whole((rows, 4 * width))],
        plan.weight_scratch(pieces),
    )


def decoder_self_back(plan, meta, rows_in, gain, pieces, kept, grad_own, grad_oth):
    n = len(flat(pieces))
    width, w3 = plan.width, 3 * plan.width
    rows = plan.pairs * SUFFIX
    mid = rows // 2

    def body(meta, in_ref, gain_ref, kept_ref, grad_own_ref, grad_oth_ref, *rest):
        refs, (own_out, oth_out), grad_refs = rest[:n], rest[n : n + 2], rest[n + 2 : -2]
        weight, acc = rest[-2:]
        plan.assemble(meta, pieces, refs, weight)
        value = in_ref[...].astype(F32)
        normed = (value * rms_scale(value) * gain_ref[...]).astype(LOW)
        grad = jnp.concatenate([grad_own_ref[...], grad_oth_ref[...]], 0)
        grad_mixed = mm(grad, weight[0, :, w3:]).astype(LOW)
        acc[0, :, w3:] = t_mm(grad, kept_ref[:, w3:])
        joined = kept_ref[:, :w3]
        grads = attend_heads_back(
            plan,
            joined[:, :width],
            joined[:, width : 2 * width],
            joined[:, 2 * width :],
            self_mask(plan, meta),
            grad_mixed,
        )
        together = jnp.concatenate(grads, 1)
        acc[0, :, :w3] = t_mm(normed, together)
        partial = mm_t(together, weight[0, :, :w3]).astype(LOW)
        own_out[...] = partial[:mid]
        oth_out[...] = partial[mid:]
        plan.emit(meta, acc, grad_refs)

    shapes = plan.grad_shapes(1)
    return call(
        "decoder_self_back",
        body,
        (1,),
        meta,
        (rows_in, gain, kept, grad_own, grad_oth, *flat(pieces)),
        [whole((rows, D)), whole((1, D)), whole(kept.shape), whole((mid, D)), whole((mid, D)), *plan.weight_specs(pieces)],
        [jax.ShapeDtypeStruct((mid, D), LOW)] * 2 + shapes,
        [whole((mid, D))] * 2 + [whole(item.shape) for item in shapes],
        plan.weight_scratch(pieces) + [pltpu.VMEM((1, D, D), F32)],
    )


def decoder_cross(plan, meta, own, oth, memory_own, memory_oth, pieces):
    n = len(flat(pieces))
    count = plan.half
    width, w3 = plan.width, 3 * plan.width

    def body(meta, own_ref, oth_ref, memory_own_ref, memory_oth_ref, *rest):
        refs, (own_out, oth_out, kept_query, kept_key, weight) = rest[:n], rest[n:]
        step = pl.program_id(0)

        @pl.when(step == 0)
        def _():
            plan.assemble(meta, pieces, refs, weight)

        normed = pick(step, count, own_ref, oth_ref, SUFFIX)
        memory = pick(step, count, memory_own_ref, memory_oth_ref, ENC_LEN)
        queries = mm(normed, weight[0, :, :width]).astype(LOW)
        both = mm(memory, weight[0, :, width:w3]).astype(LOW)
        allowed = key_mask(meta, plan.pairs, slot_of(plan, count, 0, step))
        mixed = attend_heads(plan, queries, both[:, :width], both[:, width:], allowed)
        kept_query[0, :, :width] = queries
        kept_query[0, :, width:] = mixed
        kept_key[0] = both
        put(step, count, own_out, oth_out, mm_t(mixed, weight[0, :, w3:]).astype(LOW))

    rows, long = (SUFFIX, D), (LONG, D)
    return call(
        "decoder_cross",
        body,
        (2 * count,),
        meta,
        (own, oth, memory_own, memory_oth, *flat(pieces)),
        [
            own_spec(count, 0, rows),
            oth_spec(count, 0, rows),
            own_spec(count, 0, long),
            oth_spec(count, 0, long),
            *plan.weight_specs(pieces),
        ],
        [jax.ShapeDtypeStruct((count,) + rows, LOW)] * 2
        + [
            jax.ShapeDtypeStruct((2 * count, SUFFIX, 2 * width), LOW),
            jax.ShapeDtypeStruct((2 * count, ENC_LEN, 2 * width), LOW),
        ],
        [
            own_spec(count, 0, rows),
            oth_spec(count, 0, rows),
            step_spec((SUFFIX, 2 * width)),
            step_spec((ENC_LEN, 2 * width)),
        ],
        plan.weight_scratch(pieces),
    )


def decoder_cross_back(
    plan, meta, own, oth, memory_own, memory_oth, pieces, kept_query, kept_key, grad_own, grad_oth
):
    n = len(flat(pieces))
    count = plan.half
    width, w3 = plan.width, 3 * plan.width
    rows = plan.pairs * SUFFIX
    mid = rows // 2

    def body(
        meta, own_ref, oth_ref, memory_own_ref, memory_oth_ref, query_ref, key_ref, grad_own_ref, grad_oth_ref, *rest
    ):
        refs, outs, grad_refs = rest[:n], rest[n : n + 4], rest[n + 4 : -4]
        weight, acc, grad_mixed, grad_query = rest[-4:]
        step = pl.program_id(0)

        @pl.when(step == 0)
        def _():
            plan.assemble(meta, pieces, refs, weight)
            grad = jnp.concatenate([grad_oth_ref[...], grad_own_ref[...]], 0).reshape(rows, D)
            grad_mixed[...] = mm(grad, weight[0, :, w3:]).astype(LOW)
            acc[0, :, w3:] = t_mm(grad, query_ref[:, :, width:].reshape(rows, width))
            acc[0, :, width:w3] = jnp.zeros((D, w3 - width), F32)

        memory = pick(step, count, memory_own_ref, memory_oth_ref, ENC_LEN)
        allowed = key_mask(meta, plan.pairs, slot_of(plan, count, 0, step))
        both = key_ref[0]
        here = pl.ds(pl.multiple_of(step * SUFFIX, SUFFIX), SUFFIX)
        query, grad_key, grad_value = attend_heads_back(
            plan, query_ref[step, :, :width], both[:, :width], both[:, width:], allowed, grad_mixed[here, :]
        )
        grad_query[here, :] = query
        together = jnp.concatenate([grad_key, grad_value], 1)
        acc[0, :, width:w3] += t_mm(memory, together)
        put(step, count, outs[2], outs[3], mm_t(together, weight[0, :, width:w3]).astype(LOW))

        @pl.when(step == 2 * count - 1)
        def _():
            normed = jnp.concatenate([oth_ref[...], own_ref[...]], 0).reshape(rows, D)
            queries = grad_query[...]
            acc[0, :, :width] = t_mm(normed, queries)
            back = mm_t(queries, weight[0, :, :width]).astype(LOW)
            outs[1][...] = back[:mid].reshape(count, SUFFIX, D)
            outs[0][...] = back[mid:].reshape(count, SUFFIX, D)
            plan.emit(meta, acc, grad_refs)

    part, long = (count, SUFFIX, D), (LONG, D)
    shapes = plan.grad_shapes(1)
    long_specs = [own_spec(count, 0, long), oth_spec(count, 0, long)]
    return call(
        "decoder_cross_back",
        body,
        (2 * count,),
        meta,
        (own, oth, memory_own, memory_oth, kept_query, kept_key, grad_own, grad_oth, *flat(pieces)),
        [
            whole(part),
            whole(part),
            *long_specs,
            whole(kept_query.shape),
            step_spec(kept_key.shape[1:]),
            whole(part),
            whole(part),
            *plan.weight_specs(pieces),
        ],
        [jax.ShapeDtypeStruct(part, LOW)] * 2
        + [jax.ShapeDtypeStruct((count,) + long, LOW)] * 2
        + shapes,
        [whole(part), whole(part), *long_specs, *[whole(item.shape) for item in shapes]],
        plan.weight_scratch(pieces)
        + [pltpu.VMEM((1, D, D), F32)]
        + [pltpu.VMEM((rows, width), LOW), pltpu.VMEM((rows, width), LOW)],
    )


def decoder_feed(plan, meta, own, oth, grad_in, pieces):
    n = len(flat(pieces))
    rows = plan.pairs * SUFFIX
    mid = rows // 2

    def body(meta, own_ref, oth_ref, grad_ref, *rest):
        refs, (own_out, oth_out), grad_refs = rest[:n], rest[n : n + 2], rest[n + 2 : -2]
        weight, acc = rest[-2:]
        plan.assemble(meta, pieces, refs, weight)
        normed = jnp.concatenate([own_ref[...], oth_ref[...]], 0)
        grad = grad_ref[...]
        active, slope = gelu_parts(mm(normed, weight[0]))
        active = active.astype(LOW)
        partial = mm_t(active, weight[1]).astype(LOW)
        grad_upper = (slope * mm(grad, weight[1])).astype(LOW)
        back = mm_t(grad_upper, weight[0]).astype(LOW)
        own_out[0] = partial[:mid]
        own_out[1] = back[:mid]
        oth_out[0] = partial[mid:]
        oth_out[1] = back[mid:]
        acc[0] = t_mm(normed, grad_upper)
        acc[1] = t_mm(grad, active)
        plan.emit(meta, acc, grad_refs)

    shapes = plan.grad_shapes(2)
    return call(
        "decoder_feed",
        body,
        (1,),
        meta,
        (own, oth, grad_in, *flat(pieces)),
        [whole((mid, D))] * 2 + [whole((rows, D)), *plan.weight_specs(pieces)],
        [jax.ShapeDtypeStruct((2, mid, D), LOW)] * 2 + shapes,
        [whole((2, mid, D))] * 2 + [whole(item.shape) for item in shapes],
        plan.weight_scratch(pieces) + [pltpu.VMEM((2, D, D), F32)],
    )


def add_norm(meta, name, base, first, second, gain):
    def body(meta, base_ref, first_ref, second_ref, gain_ref, sum_ref, norm_ref):
        value = base_ref[...].astype(F32) + (first_ref[...].astype(F32) + second_ref[...].astype(F32))
        sum_ref[...] = value
        norm_ref[...] = (value * rms_scale(value) * gain_ref[...]).astype(LOW)

    shape = base.shape
    part = (1,) + shape[1:] if len(shape) == 3 else shape
    spec = (
        pl.BlockSpec(part, lambda p, _: (p, 0, 0)) if len(shape) == 3 else whole(shape)
    )
    return call(
        name,
        body,
        (shape[0] if len(shape) == 3 else 1,),
        meta,
        (base, first, second, gain),
        [spec, spec, spec, whole((1, D))],
        [jax.ShapeDtypeStruct(shape, F32), jax.ShapeDtypeStruct(shape, LOW)],
        [spec, spec],
        [],
    )


def norm_back(meta, name, inputs, gain, grad, first, second, want_low):
    def body(meta, in_ref, gain_ref, grad_ref, first_ref, second_ref, *outs):
        value = in_ref[...].astype(F32)
        scale = rms_scale(value)
        unit = value * scale
        back = first_ref[...].astype(F32) + second_ref[...].astype(F32)
        product = back * unit
        real = product[0, :ENC_LEN] if value.ndim == 3 else product
        part = jnp.sum(real, 0, keepdims=True)
        weighted = product * gain_ref[...]
        total = grad_ref[...].astype(F32) + scale * (
            back * gain_ref[...] - unit * jnp.mean(weighted, -1, keepdims=True)
        )
        outs[0][...] = total
        if want_low:
            outs[1][...] = total.astype(LOW)
        step = pl.program_id(0)

        @pl.when(step == 0)
        def _():
            outs[-1][...] = part

        @pl.when(step > 0)
        def _():
            outs[-1][...] += part

    shape = inputs.shape
    part = (1,) + shape[1:] if len(shape) == 3 else shape
    spec = pl.BlockSpec(part, lambda p, _: (p, 0, 0)) if len(shape) == 3 else whole(shape)
    return call(
        name,
        body,
        (shape[0] if len(shape) == 3 else 1,),
        meta,
        (inputs, gain, grad, first, second),
        [spec, whole((1, D)), spec, spec, spec],
        [jax.ShapeDtypeStruct(shape, F32)]
        + [jax.ShapeDtypeStruct(shape, LOW)] * want_low
        + [jax.ShapeDtypeStruct((1, D), F32)],
        [spec] * (1 + want_low) + [whole((1, D))],
        [],
    )


def fold(plan, meta, keeps, mores, split):
    n = len(keeps)
    counts = [item.shape[1] for item in keeps]
    total = sum(counts)
    tail = keeps[0].shape[2:]
    blocks = keeps[0].shape[0]

    def body(meta, *rest):
        keep_refs, more_refs, outs = rest[:n], rest[n : 2 * n], rest[2 * n :]
        for index in range(blocks):
            start = 0
            out, at = split(index)
            for keep_ref, more_ref, count in zip(keep_refs, more_refs, counts):
                value = keep_ref[index] + more_ref[index].astype(F32)
                outs[out][at, start : start + count] = value.astype(outs[out].dtype)
                start += count

    places = [split(index) for index in range(blocks)]
    outs = [
        jax.ShapeDtypeStruct((sum(place[0] == out for place in places), total) + tail, LOW if out else F32)
        for out in range(1 + max(place[0] for place in places))
    ]
    return call(
        "fold",
        body,
        (1,),
        meta,
        (*keeps, *mores),
        [whole(item.shape) for item in (*keeps, *mores)],
        outs,
        [whole(item.shape) for item in outs],
        [],
    )


def halves(index):
    return index % 2, index // 2


def apart(index):
    return index, 0


def pack_first(plan, meta, project_in, project_out, gains):
    width, block = plan.width, plan.block

    def body(meta, in_ref, out_ref, gain_ref, packed):
        parts = [in_ref[0, index] for index in range(3)] + [jnp.transpose(out_ref[0])]
        packed[:block] = jnp.concatenate(parts, 1).astype(LOW)
        rows = jnp.concatenate([gain_ref[...], jnp.zeros((3, block), F32)], 0)
        wide = jnp.concatenate([rows, jnp.zeros((8, D - block), F32)], 1)
        packed[block:] = pltpu.roll(wide, meta[0] * block, 1).astype(LOW)

    shape = (block + 8, D)
    return call(
        "pack_first",
        body,
        (1,),
        meta,
        (project_in, project_out, gains),
        [
            pl.BlockSpec((1,) + project_in.shape[1:], lambda *_: (0, 0, 0, 0)),
            pl.BlockSpec((1,) + project_out.shape[1:], lambda *_: (0, 0, 0)),
            whole(gains.shape),
        ],
        [jax.ShapeDtypeStruct(shape, LOW)],
        [whole(shape)],
        [],
    )[0]


def one_hot(rows, offset):
    row = lax.broadcasted_iota(jnp.int32, (rows, D), 0)
    lane = lax.broadcasted_iota(jnp.int32, (rows, D), 1)
    return (lane == row + offset).astype(F32)


def collect(plan, meta, sets, attention):
    counts = [pieces[0].shape[-3] for pieces in sets]
    count = sum(counts)
    shape = (count,) + sets[0][0].shape[-2:]
    arrays = [item for pieces in sets for item in pieces]
    n = len(arrays)
    groups = D // plan.width

    def body(meta, *rest):
        refs, (out, tile_out) = rest[:n], rest[n:]
        dp_at, mp_at = meta[0], meta[1 + 3 * plan.pairs]
        group = lax.broadcasted_iota(jnp.int32, (8, D), 1) // plan.width
        row = lax.broadcasted_iota(jnp.int32, (8, D), 0)
        place = one_hot(plan.block, dp_at * plan.block)
        def one(first, refs, at, _):
            index = first + at
            heads = (jnp.zeros((8, D), jnp.int32) + index) < attention
            value = refs[0][0, at]
            for ref in refs[1:]:
                value = value + ref[0, at].astype(F32)
            out[index] = value
            square = value * value
            lanes = jnp.broadcast_to(jnp.sum(square, 0, keepdims=True), (8, D))
            mask = jnp.where(heads, (group == row).astype(F32), (row == 0).astype(F32))
            sums = lax.dot_general(
                mask, square, (((1,), (1,)), ((), ())), precision=EXACT, preferred_element_type=F32
            )
            tile = lax.dot_general(
                sums, place, (((1,), (0,)), ((), ())), precision=EXACT, preferred_element_type=F32
            )
            spread = jnp.zeros_like(tile)
            for part in range(groups):
                shift = lax.rem(mp_at * plan.width + (D - part * plan.width), D)
                moved = pltpu.roll(jnp.where(group == part, lanes, 0.0), shift, 1)
                spread = jnp.where(row == 4 + part, moved, spread)
            spread = jnp.where(heads, spread, jnp.where(row == 4 + mp_at, lanes, 0.0))
            tile_out[index] = jnp.where(row < 4, tile, spread)
            return 0

        first, start = 0, 0
        for pieces, size in zip(sets, counts):
            lax.fori_loop(0, size, functools.partial(one, first, refs[start : start + len(pieces)]), 0)
            first, start = first + size, start + len(pieces)

    return call(
        "collect",
        body,
        (1,),
        meta,
        tuple(arrays),
        [whole(item.shape) for item in arrays],
        [jax.ShapeDtypeStruct(shape, F32), jax.ShapeDtypeStruct((count, 8, D), F32)],
        [whole(shape), whole((count, 8, D))],
        [],
    )


def finish(plan, meta, sums, statistics, gain_state):
    counts = [item.shape for item in statistics]

    def body(meta, sum_ref, *rest):
        olds, gains = rest[:8], rest[8:12]
        norm_out, news, rates, gain_outs = rest[12], rest[13:21], rest[21], rest[22:]
        tiles = [sum_ref[6], sum_ref[1], sum_ref[0]]
        feeds = [(sum_ref[2], sum_ref[3]), (sum_ref[4], sum_ref[5])]
        gain_sum = 0.5 * sum_ref[7]
        total = jnp.sum(gain_sum * gain_sum)
        for tile in tiles:
            total = total + jnp.sum(tile[:4])
        for up, down in feeds:
            total = total + jnp.sum(up[:1]) + jnp.sum(down[:1])
        totals = jnp.full((8, D), total, F32)
        norm = jnp.sqrt(totals)
        factor = jnp.minimum(1.0, 1.0 / norm)
        squared = (factor * factor)[:1]
        norm_out[...] = norm[:, :128]
        rates[...] = factor[:, :128]

        def renew(old, sums, number):
            return DECAY * old + (1.0 - DECAY) * (sums * squared / number + EPS_STAT)

        for layer, tile in enumerate(tiles):
            for part in range(3):
                news[0][layer, part : part + 1] = renew(olds[0][layer, part : part + 1], tile[part : part + 1], D)
                news[1][layer, part : part + 1] = renew(
                    olds[1][layer, part : part + 1], tile[4 + part : 5 + part], D
                )
            news[2][layer : layer + 1] = renew(olds[2][layer : layer + 1], tile[7:8], D)
            news[3][layer : layer + 1] = renew(olds[3][layer : layer + 1], tile[3:4], D)
        for layer, (up, down) in enumerate(feeds):
            news[4][layer : layer + 1] = renew(olds[4][layer : layer + 1], up[:1], FF)
            news[7][layer : layer + 1] = renew(olds[7][layer : layer + 1], down[:1], FF)
            for part in range(FF // D):
                cut = slice(part * D, (part + 1) * D)
                news[5][layer : layer + 1, cut] = renew(
                    olds[5][layer : layer + 1, cut], up[4 + part : 5 + part], D
                )
                news[6][layer : layer + 1, cut] = renew(
                    olds[6][layer : layer + 1, cut], down[4 + part : 5 + part], D
                )
        shift = lax.rem(D - meta[0] * plan.block, D)
        grad = (pltpu.roll(gain_sum, shift, 1) * factor)[:5, : plan.block]
        master, square, moment, average = [item[...] for item in gains]
        square_new = DECAY * square + (1.0 - DECAY) * (grad * grad + EPS_STAT)
        stepped = grad * lax.rsqrt(square_new)
        moment_new = MOMENTUM * moment + stepped
        master_new = master - RATE_GAIN * (MOMENTUM * moment_new + stepped)
        values = (
            grad,
            square_new,
            moment_new,
            master_new,
            AVERAGE * average + (1.0 - AVERAGE) * master_new,
            master_new,
        )
        for out, value in zip(gain_outs, values):
            out[...] = value.astype(out.dtype)

    small = gain_state[0].shape
    outs = (
        [jax.ShapeDtypeStruct((8, 128), F32)]
        + [jax.ShapeDtypeStruct(shape, F32) for shape in counts]
        + [jax.ShapeDtypeStruct((8, 128), F32)]
        + [jax.ShapeDtypeStruct(small, F32)] * 5
        + [jax.ShapeDtypeStruct(small, LOW)]
    )
    inputs = (sums, *statistics, *gain_state)
    return call(
        "finish",
        body,
        (1,),
        meta,
        inputs,
        [whole(item.shape) for item in inputs],
        outs,
        [whole(item.shape) for item in outs],
        [],
    )


def part_spec(block, place):
    return pl.BlockSpec((2, block, D), lambda *_: (place, 0, 0))


def step_values(grad, scale, master, moment, average):
    stepped = grad * scale
    moment_new = MOMENTUM * moment + stepped
    master_new = master - RATE_MATRIX * (MOMENTUM * moment_new + stepped)
    return grad, moment_new, master_new, AVERAGE * average + (1.0 - AVERAGE) * master_new


def columns(rows, offset, size):
    filled = jnp.concatenate([rows] * (8 // rows.shape[0] + 1), 0)[:8]
    wide = (size + 127) // 128 * 128
    return jnp.transpose(pltpu.roll(filled, lax.rem(D - offset, D), 1)[:, :wide])[:size]


def update_attention(plan, meta, rates, grads, rows_in, cols_in, rows_out, cols_out, state_in, state_out):
    width, block = plan.width, plan.block

    def body(meta, rates_ref, grad_a, grad_b, rin, cin, rout, cout, *rest):
        ins, outs = rest[:6], rest[6:]
        layer = pl.program_id(0)
        dp_at, mp_at = meta[0], meta[1 + 3 * plan.pairs]
        grad = jnp.where(layer == 0, grad_a[0], jnp.where(layer == 1, grad_b[1], grad_b[0]))
        grad = grad * rates_ref[:1, :1]
        means = jnp.mean(rin[0], -1, keepdims=True)
        row_scale = lax.rsqrt(columns(rin[0] / means, dp_at * block, block))
        shift = lax.rem(D - mp_at * width, D)
        col_scale = lax.rsqrt(pltpu.roll(jnp.concatenate([cin[0]] * 3, 0)[:8], shift, 1)[:3, :width])
        for part in range(3):
            values = step_values(
                grad[:, part * width : (part + 1) * width],
                row_scale[:, part : part + 1] * col_scale[part : part + 1],
                ins[0][0, part],
                ins[1][0, part],
                ins[2][0, part],
            )
            for out, value in zip(outs[:4], values):
                out[0, part] = value
            outs[4][0, part] = values[2].astype(LOW)
        turned = jnp.transpose(grad[:, 3 * width :])
        row, col = rout[pl.ds(layer, 1), :], cout[pl.ds(layer, 1), :]
        mean = jnp.mean(row, -1, keepdims=True)
        row_scale = lax.rsqrt(columns(row / mean, mp_at * width, width))[:, :1]
        shift = lax.rem(D - dp_at * block, D)
        col_scale = lax.rsqrt(pltpu.roll(jnp.broadcast_to(col, (8, D)), shift, 1)[:1, :block])
        values = step_values(turned, row_scale * col_scale, ins[3][0], ins[4][0], ins[5][0])
        for out, value in zip(outs[5:9], values):
            out[0] = value
        outs[9][0] = values[2].astype(LOW)

    def spec(shape):
        return pl.BlockSpec((1,) + shape, lambda p, _: (p,) + (0,) * len(shape))

    shape_in, shape_out = (3, block, width), (width, block)
    outs = (
        [jax.ShapeDtypeStruct((3,) + shape_in, F32)] * 4
        + [jax.ShapeDtypeStruct((3,) + shape_in, LOW)]
        + [jax.ShapeDtypeStruct((3,) + shape_out, F32)] * 4
        + [jax.ShapeDtypeStruct((3,) + shape_out, LOW)]
    )
    return call(
        "update_attention",
        body,
        (3,),
        meta,
        (rates, *grads, rows_in, cols_in, rows_out, cols_out, *state_in, *state_out),
        [whole((8, 128)), whole((1, block, D)), part_spec(block, 0)]
        + [spec((3, D)), spec((3, D)), whole((3, D)), whole((3, D))]
        + [spec(shape_in)] * 3
        + [spec(shape_out)] * 3,
        outs,
        [spec(shape_in)] * 5 + [spec(shape_out)] * 5,
        [],
    )


def update_feed(plan, meta, rates, grads, rows_up, cols_up, rows_down, cols_down, state_up, state_down):
    hidden, block = plan.hidden, plan.block

    def body(meta, rates_ref, grad_a, grad_b, rup, cup, rdown, cdown, *rest):
        ins, outs = rest[:6], rest[6:]
        layer = pl.program_id(0)
        lanes = pl.ds(pl.multiple_of(meta[1 + 3 * plan.pairs] * hidden, 128), hidden)
        one = pl.ds(layer, 1)
        mean_up = jnp.mean(rup[one, :], -1, keepdims=True)
        mean_down = jnp.mean(rdown[one, :], -1, keepdims=True)
        along = (rup[one, :] / mean_up, cdown[one, :])
        across = (cup[one, lanes], rdown[one, lanes] / mean_down)
        for part in range(2):
            grad = jnp.where(layer == 0, grad_a[part], grad_b[part]) * rates_ref[:1, :1]
            row_scale = lax.rsqrt(columns(along[part], meta[0] * block, block))[:, :1]
            values = step_values(
                grad,
                row_scale * lax.rsqrt(across[part]),
                ins[3 * part][0],
                ins[3 * part + 1][0],
                ins[3 * part + 2][0],
            )
            for out, value in zip(outs[5 * part : 5 * part + 4], values):
                out[0] = value
            outs[5 * part + 4][0] = values[2].astype(LOW)

    state = pl.BlockSpec((1, block, hidden), lambda p, _: (p, 0, 0))
    outs = ([jax.ShapeDtypeStruct((2, block, hidden), F32)] * 4 + [jax.ShapeDtypeStruct((2, block, hidden), LOW)]) * 2
    values = call(
        "update_feed",
        body,
        (2,),
        meta,
        (
            rates,
            *grads,
            rows_up,
            cols_up,
            rows_down,
            cols_down,
            *state_up,
            *[item.transpose(0, 2, 1) for item in state_down],
        ),
        [whole((8, 128)), part_spec(block, 1), part_spec(block, 2)]
        + [whole((2, D)), whole((2, FF)), whole((2, FF)), whole((2, D))]
        + [state] * 6,
        outs,
        [state] * 10,
        [],
    )
    return [*values[:5], *[item.transpose(0, 2, 1) for item in values[5:]]]


def on_device(
    sizes,
    encoder_in,
    decoder_in,
    decoder_cotangent,
    counts,
    prefix_len,
    suffix_len,
    project_in,
    project_in_rows,
    project_in_cols,
    project_in_moment,
    project_in_average,
    project_out,
    project_out_rows,
    project_out_cols,
    project_out_moment,
    project_out_average,
    expand,
    expand_rows,
    expand_cols,
    expand_moment,
    expand_average,
    contract,
    contract_rows,
    contract_cols,
    contract_moment,
    contract_average,
    norm_gains,
    norm_gains_square,
    norm_gains_moment,
    norm_gains_average,
):
    dp_n, mp_n = sizes
    dp_index = lax.axis_index("dp")
    mp_index = lax.axis_index("mp")
    side = mp_index % 2
    pairs = prefix_len.shape[0]
    half = pairs // 2
    width = project_in.shape[-1]
    block = project_in.shape[-2]
    plan = Plan(dp_n, block, width, expand.shape[-1], pairs)
    low, f32 = LOW, F32

    def swap(value, axis, bit):
        count = dp_n if axis == "dp" else mp_n
        return lax.ppermute(value, axis, [(i, i ^ bit) for i in range(count)])

    def bits(count):
        return [1 << i for i in range(count.bit_length() - 1)]

    hold = lax.optimization_barrier

    class Gather:
        def __init__(self, blocks):
            self.items, self.sent, self.own = [{} for _ in blocks], [], list(blocks)

        def step(self, chain, *sends, later=()):
            names = [(item, name) for item, name in self.sent if (name, item) not in later]
            late = [(item, name) for item, name in self.sent if (name, item) in later]
            values = [self.items[item][name] for item, name in names]
            if names:
                chain, values, self.own = hold((list(chain), values, self.own))
            for (item, name), value in zip(names, values):
                self.items[item][name] = value
            self.sent = late
            for name, item in sends:
                if name == "fours":
                    four = swap(jnp.concatenate([self.own[at] for at in item]), "dp", 4)
                    for place, at in enumerate(item):
                        self.items[at]["four"] = four[place * block : (place + 1) * block]
                        self.sent.append((at, "four"))
                    continue
                parts = self.items[item]
                if name == "four":
                    parts[name] = swap(self.own[item], "dp", 4)
                    self.sent.append((item, name))
                    continue
                if "two" not in parts:
                    parts["two"] = jnp.concatenate([self.own[item], parts["four"]])
                if name == "far":
                    parts[name] = swap(parts["two"], "dp", 2)
                else:
                    parts[name] = swap(parts["two" if name == "near" else "far"], "dp", 1)
                self.sent.append((item, name))
            return chain

        def take(self, item, index=0):
            parts = self.items[item]
            height = self.own[item].shape[0]
            return [parts[name] for name in ("two", "far", "near", "last")], height, index * block

    class Plain:
        def __init__(self, blocks):
            self.own = list(blocks)

        def step(self, chain, *sends, later=()):
            return chain

        def take(self, item, index=0):
            own = self.own[item][index * block : (index + 1) * block]
            return [lax.all_gather(own, "dp", axis=0, tiled=True)], D, 0

    def total(value, axes):
        for axis, count in axes:
            for bit in bits(count):
                sent = value.astype(low)
                value = sent.astype(value.dtype) + swap(sent, axis, bit).astype(value.dtype)
        return value

    def total_dp(value):
        return total(value, [("dp", dp_n)])

    def total_all(value):
        return total(value, [("mp", mp_n), ("dp", dp_n)])

    def reduce_own(own, oth, first=()):
        sent = (own.astype(f32) + swap(oth, "mp", 1).astype(f32)).astype(low)
        for bit in bits(mp_n)[1:-1]:
            sent = (sent.astype(f32) + swap(sent, "mp", bit).astype(f32)).astype(low)
        sent, first = hold((sent, first))
        return sent, swap(sent, "mp", bits(mp_n)[-1])

    def relative(value):
        split = value.reshape((half, 2) + value.shape[1:])
        return (
            lax.dynamic_index_in_dim(split, side, 1, False),
            lax.dynamic_index_in_dim(split, 1 - side, 1, False),
        )

    def absolute(own):
        other = swap(own, "mp", 1)
        even = jnp.where(side == 0, own, other)
        odd = jnp.where(side == 0, other, own)
        return jnp.stack([even, odd], 1).reshape((pairs,) + own.shape[1:])

    def core(value):
        return swap(value, "mp", 1)

    def attention_block(layer):
        return jnp.concatenate(
            [project_in[layer, 0], project_in[layer, 1], project_in[layer, 2], project_out[layer].T], 1
        ).astype(low)

    def feed_block(layer):
        return [expand[layer].astype(low), contract[layer].T.astype(low)]

    direct = plan.direct
    place = dp_index[None].astype(jnp.int32)
    if direct:
        first = pack_first(plan, place, project_in, project_out, norm_gains)
    else:
        first = attention_block(0)
    blocks = [
        first,
        *feed_block(0),
        attention_block(1),
        attention_block(2),
        jnp.concatenate(feed_block(1)),
    ]
    gather = (Gather if direct else Plain)(blocks)
    gather.step((), ("four", 0))
    gather.step((), ("far", 0), ("near", 0), ("four", 1))
    gather.step((), ("last", 0), later=(("four", 1),))
    enc_att = [gather.take(0)]
    if direct:
        height = block + 8
        gain_rows = sum(
            item[at : at + 8].astype(f32) for item in enc_att[0][0] for at in (block, height + block)
        )
    else:
        gain_full = lax.dynamic_update_slice(
            jnp.zeros((8, D), low), norm_gains.astype(low), (0, dp_index * block)
        )
        gain_rows = total_dp(gain_full).astype(f32)
    gains = [gain_rows[i : i + 1] for i in range(5)]

    place_rel = jnp.concatenate([2 * jnp.arange(half) + side, 2 * jnp.arange(half) + 1 - side])
    prefix_rel = jnp.concatenate(relative(prefix_len))
    suffix_rel = jnp.concatenate(relative(suffix_len))
    images = place_rel < counts[0, 0]
    active = place_rel < counts[0, 0] + counts[0, 1]
    meta = jnp.concatenate(
        [
            dp_index[None].astype(jnp.int32),
            images.astype(jnp.int32),
            prefix_rel,
            suffix_rel,
            mp_index[None].astype(jnp.int32),
        ]
    )
    steps = jnp.arange(SUFFIX)
    live = active[:, None] & (steps[None, :] < suffix_rel[:, None])

    mid = half * SUFFIX
    enc_own, enc_oth = relative(
        jnp.pad(encoder_in.reshape(pairs, ENC_LEN, D), ((0, 0), (0, LONG - ENC_LEN), (0, 0)))
    )
    dec_rel = jnp.concatenate(relative(decoder_in.reshape(pairs, SUFFIX, D))).reshape(2 * mid, D)
    cot = jnp.concatenate(relative(decoder_cotangent.reshape(pairs, SUFFIX, D)))
    cot = jnp.where(live[:, :, None], cot, f32(0.0)).reshape(2 * mid, D)
    cot_low = cot.astype(low)

    def triple(value):
        return value.reshape(half, SUFFIX, D)

    (enc_oth,) = gather.step((enc_oth,), ("far", 1), ("near", 1), ("four", 2), later=(("last", 0),))
    own, oth, kept_enc = encoder_attention(plan, meta, enc_own, enc_oth, gains[0], enc_att, 0, half)
    own, oth, dec_rel, cot, cot_low = gather.step(
        (own, oth, dec_rel, cot, cot_low), ("last", 1), ("near", 2), ("far", 2), ("fours", (3, 4))
    )
    sums = gather.step(reduce_own(own, oth), ("last", 2))
    enc_feed = [gather.take(1), gather.take(2)]
    enc_mid, norm_mid = add_norm(meta, "add_norm_mid", enc_own, *sums, gains[1])
    (norm_mid,) = gather.step((norm_mid,))
    norm_mid_oth = core(norm_mid)

    (norm_mid_oth,) = gather.step(
        (norm_mid_oth,), ("far", 3), ("near", 3), ("four", 5)
    )
    own, oth = encoder_feed(plan, meta, norm_mid, norm_mid_oth, enc_feed, 0, half)
    own, oth = gather.step((own, oth), ("last", 3), ("far", 4), ("near", 4), later=(("four", 5),))
    sums = reduce_own(own, oth)
    (dec_rel,) = gather.step((dec_rel,), ("last", 4), later=(("last", 3),))

    self_att = [gather.take(3)]
    own, oth, kept_self = decoder_self(plan, meta, dec_rel, gains[2], self_att)
    sums = gather.step(sums)
    sums_self = reduce_own(own, oth, sums)
    gather.step((sums_self[0],), ("far", 5), ("near", 5))
    cross_att = [gather.take(4)]
    memory = (enc_mid + (sums[0].astype(f32) + sums[1].astype(f32))).astype(low)
    dec_one, norm_cross = add_norm(meta, "add_norm_cross", dec_rel[:mid], *sums_self, gains[3])
    memory, norm_cross = gather.step((memory, norm_cross), ("last", 5))
    memory_oth = core(memory)
    norm_cross_oth = core(norm_cross)

    cross_in = (triple(norm_cross), triple(norm_cross_oth), memory, memory_oth, cross_att)
    own, oth, *kept_cross = decoder_cross(plan, meta, *cross_in)
    sums = reduce_own(own, oth)
    dec_two, norm_last = add_norm(
        meta, "add_norm_last", dec_one, sums[0].reshape(mid, D), sums[1].reshape(mid, D), gains[4]
    )
    dec_feed = [gather.take(5), gather.take(5, 1)]

    own, oth, *grads_dec = decoder_feed(plan, meta, norm_last, core(norm_last), cot_low, dec_feed)
    if direct:
        more_dec = swap(grads_dec[0], "dp", 1)
    sums = reduce_own(own, oth)
    out_own = dec_two + (sums[0][0].astype(f32) + sums[1][0].astype(f32))
    grad, grad_low, gain_four = norm_back(
        meta, "norm_back_last", dec_two, gains[4], cot[:mid], sums[0][1], sums[1][1], True
    )

    own, oth, own_long, oth_long, *grads_cross = decoder_cross_back(
        plan, meta, *cross_in, *kept_cross, triple(grad_low), triple(core(grad_low))
    )
    if direct:
        own, oth, own_long, oth_long, more_dec = hold((own, oth, own_long, oth_long, more_dec))
        more_cross = swap(grads_cross[0], "dp", 1)
    sums = reduce_own(own, oth)
    sums_enc = reduce_own(own_long, oth_long, sums)
    if direct:
        keep, more_dec, _ = hold((grads_dec[1], more_dec, sums[0]))
        keep_dec, away_dec = fold(plan, meta, [keep], [more_dec], halves)
        *sums, away_dec = hold((*sums, away_dec))
        more_dec = swap(away_dec, "dp", 2)
    grad, grad_low, gain_three = norm_back(
        meta, "norm_back_cross", dec_one, gains[3], grad, sums[0].reshape(mid, D), sums[1].reshape(mid, D), True
    )
    grad_low_oth = core(grad_low)

    own_self, oth_self, *grads_self = decoder_self_back(
        plan, meta, dec_rel, gains[2], self_att, kept_self, grad_low, grad_low_oth
    )
    decoder_out = absolute(triple(out_own)).reshape(2 * mid, D)
    if direct:
        own_self, oth_self, decoder_out = hold((own_self, oth_self, decoder_out))
    sums_self = reduce_own(own_self, oth_self)
    if direct:
        *sums_enc, _, decoder_out, more_cross, more_dec = hold(
            (*sums_enc, sums_self[0], decoder_out, more_cross, more_dec)
        )
    grad_enc = sums_enc[0].astype(f32) + sums_enc[1].astype(f32)
    enc_low = grad_enc.astype(low)
    enc_low_oth = core(enc_low)

    if direct:
        keep_dec, away_dec = fold(plan, meta, [keep_dec], [more_dec], halves)
        enc_low_oth, away_self, away_dec = hold((enc_low_oth, grads_self[0], away_dec))
        more_self = swap(away_self, "dp", 1)
        more_dec = swap(away_dec, "dp", 4)
    own, oth, *grads_enc = encoder_feed_back(plan, meta, norm_mid, norm_mid_oth, enc_low, enc_low_oth, enc_feed)
    if direct:
        own, oth, more_self, more_dec, *sums_self = hold((own, oth, more_self, more_dec, *sums_self))
        more_up, more_down = [swap(item, "dp", 1) for item in grads_enc[::2]]
    sums = reduce_own(own, oth)
    if direct:
        keep_cross, keep_self, more_cross, more_self, _ = hold(
            (grads_cross[1], grads_self[1], more_cross, more_self, sums[0])
        )
        keep_mid, away_mid = fold(plan, meta, [keep_cross, keep_self], [more_cross, more_self], halves)
        more_mid = swap(away_mid, "dp", 2)
        sums_self, _, more_up = hold((sums_self, away_mid, more_up))
    grad, gain_two = norm_back(meta, "norm_back_self", dec_rel[:mid], gains[2], grad, *sums_self, False)
    decoder_in_grad = absolute(triple(grad)).reshape(2 * mid, D)
    if direct:
        *sums, decoder_in_grad, more_mid = hold((*sums, decoder_in_grad, more_mid))
    grad_enc, enc_low, gain_one = norm_back(
        meta, "norm_back_mid", enc_mid, gains[1], grad_enc, *sums, True
    )
    if direct:
        keep_mid, _ = hold((keep_mid, enc_low))
        keep_mid, away_mid = fold(plan, meta, [keep_mid], [more_mid], halves)
        enc_low, more_down, away_mid = hold((enc_low, more_down, away_mid))
    enc_low_oth = core(enc_low)

    if direct:
        keep_enc, away_enc = fold(plan, meta, grads_enc[1::2], [more_up, more_down], halves)
        enc_low_oth, away_enc, away_mid = hold((enc_low_oth, away_enc, away_mid))
        more_mid = swap(away_mid, "dp", 4)
        more_enc = swap(away_enc, "dp", 2)
    own, oth, *grads_att = encoder_attention_back(
        plan, meta, enc_own, enc_oth, gains[0], enc_att, kept_enc, enc_low, enc_low_oth
    )
    if direct:
        more_att = swap(grads_att[0], "dp", 1)
        own, oth, more_enc, more_mid = hold((own, oth, more_enc, more_mid))
        keep_enc, away_enc = fold(plan, meta, [keep_enc], [more_enc], halves)
        more_enc = swap(away_enc, "dp", 4)
        own, oth, _ = hold((own, oth, away_enc))
    sums = reduce_own(own, oth)
    if direct:
        keep_att, more_att, _ = hold((grads_att[1], more_att, sums[0]))
        mine, *others = fold(plan, meta, [keep_att], [more_att], apart)
        others, more_enc, keep_mid = hold((others, more_enc, keep_mid))
        pieces_att = [mine] + [swap(item, "dp", 2 * (i + 1)) for i, item in enumerate(others)]
        summed, tiles = collect(plan, meta, [[keep_mid, more_mid], [keep_enc, more_enc], [keep_dec, more_dec]], 2)
        *pieces_att, _ = hold((*pieces_att, tiles))
        *sums, _ = hold((*sums, pieces_att[1]))
        sum_att, tile_att = collect(plan, meta, [pieces_att], 1)
    else:
        parts = [grads_cross[0], grads_self[0], *grads_enc, grads_dec[0]]
        whole_sum = lax.psum_scatter(jnp.concatenate(parts), "dp", scatter_dimension=1, tiled=True)
        summed, tiles = collect(plan, meta, [[whole_sum[None]]], 2)
        whole_sum = lax.psum_scatter(grads_att[0], "dp", scatter_dimension=1, tiled=True)
        sum_att, tile_att = collect(plan, meta, [[whole_sum[None]]], 1)
    grad_enc, gain_zero = norm_back(meta, "norm_back_enc", enc_own, gains[0], grad_enc, *sums, False)
    encoder_in_grad = absolute(grad_enc)[:, :ENC_LEN].reshape(pairs * ENC_LEN, D)
    gain_tile = jnp.concatenate(
        [gain_zero, gain_one, gain_two, gain_three, gain_four, jnp.zeros((3, D), f32)]
    )[None]
    tiles = total_all(jnp.concatenate([tiles, tile_att, gain_tile]))
    done = finish(
        plan,
        meta,
        tiles,
        (
            project_in_rows,
            project_in_cols,
            project_out_rows,
            project_out_cols,
            expand_rows,
            expand_cols,
            contract_rows,
            contract_cols,
        ),
        (norm_gains, norm_gains_square, norm_gains_moment, norm_gains_average),
    )
    grad_norm, news, rates, pgain = done[0][0, 0], done[1:9], done[9], done[10:]
    att = update_attention(
        plan,
        meta,
        rates,
        (sum_att, summed),
        *news[:4],
        (project_in, project_in_moment, project_in_average),
        (project_out, project_out_moment, project_out_average),
    )
    feed = update_feed(
        plan,
        meta,
        rates,
        (summed, summed),
        *news[4:],
        (expand, expand_moment, expand_average),
        (contract, contract_moment, contract_average),
    )
    return (
        decoder_out,
        encoder_in_grad,
        decoder_in_grad,
        grad_norm,
        att[0],
        news[0],
        news[1],
        *att[1:5],
        att[5],
        news[2],
        news[3],
        *att[6:10],
        feed[0],
        news[4],
        news[5],
        *feed[1:5],
        feed[5],
        news[6],
        news[7],
        *feed[6:10],
        *pgain,
    )


def solution(mesh):
    placed = (
        P("dp", None),
        P("dp", None),
        P("dp", None),
        P("dp", None),
        P("dp"),
        P("dp"),
        P(None, None, "dp", "mp"),
        P(),
        P(),
        P(None, None, "dp", "mp"),
        P(None, None, "dp", "mp"),
        P(None, "mp", "dp"),
        P(),
        P(),
        P(None, "mp", "dp"),
        P(None, "mp", "dp"),
        P(None, "dp", "mp"),
        P(),
        P(),
        P(None, "dp", "mp"),
        P(None, "dp", "mp"),
        P(None, "mp", "dp"),
        P(),
        P(),
        P(None, "mp", "dp"),
        P(None, "mp", "dp"),
        P(None, "dp"),
        P(None, "dp"),
        P(None, "dp"),
        P(None, "dp"),
    )
    return jax.shard_map(
        functools.partial(on_device, (mesh.shape["dp"], mesh.shape["mp"])),
        mesh=mesh,
        in_specs=placed,
        out_specs=(
            P("dp", None),
            P("dp", None),
            P("dp", None),
            P(),
            P(None, None, "dp", "mp"),
            P(),
            P(),
            P(None, None, "dp", "mp"),
            P(None, None, "dp", "mp"),
            P(None, None, "dp", "mp"),
            P(None, None, "dp", "mp"),
            P(None, "mp", "dp"),
            P(),
            P(),
            P(None, "mp", "dp"),
            P(None, "mp", "dp"),
            P(None, "mp", "dp"),
            P(None, "mp", "dp"),
            P(None, "dp", "mp"),
            P(),
            P(),
            P(None, "dp", "mp"),
            P(None, "dp", "mp"),
            P(None, "dp", "mp"),
            P(None, "dp", "mp"),
            P(None, "mp", "dp"),
            P(),
            P(),
            P(None, "mp", "dp"),
            P(None, "mp", "dp"),
            P(None, "mp", "dp"),
            P(None, "mp", "dp"),
            P(None, "dp"),
            P(None, "dp"),
            P(None, "dp"),
            P(None, "dp"),
            P(None, "dp"),
            P(None, "dp"),
        ),
        check_vma=False,
    )
```

```python
import functools

import jax
import jax.numpy as jnp
from jax import lax
from jax.experimental import pallas as pl
from jax.experimental.pallas import tpu as pltpu
from jax.sharding import PartitionSpec as P

D = 768
HEAD_DIM = 64
FF = 3072
PATCHES = 196
SUFFIX = 32
ENC_LEN = 228


EPS_NORM = 1e-06
EPS_STAT = 1e-30
DECAY = 0.99
MOMENTUM = 0.9
AVERAGE = 0.6
RATE_MATRIX = 0.004
RATE_GAIN = 0.05
MASKED = -1000000000.0


LOW = jnp.bfloat16
F32 = jnp.float32
VMEM_LIMIT = 56 * 1024 * 1024
LONG = (ENC_LEN + 7) // 8 * 8
EXACT = lax.Precision.HIGHEST


def dot(left, right, contract):
    return lax.dot_general(left, right, (contract, ((), ())), preferred_element_type=F32)


def mm(left, right):
    return dot(left, right, ((1,), (0,)))


def mm_t(left, right):
    return dot(left, right, ((1,), (1,)))


def t_mm(left, right):
    return dot(left, right, ((0,), (0,)))


def rms_scale(value):
    return lax.rsqrt(jnp.mean(value * value, -1, keepdims=True) + EPS_NORM)


def softmax(scores):
    expons = jnp.exp(scores - jnp.max(scores, -1, keepdims=True))
    return expons / jnp.sum(expons, -1, keepdims=True)


def gelu_parts(upper):
    inner = 0.7978845608028654 * (upper + 0.044715 * upper * upper * upper)
    bent = jnp.tanh(inner)
    value = 0.5 * upper * (1.0 + bent)
    slope = 0.5 * (1.0 + bent) + 0.5 * upper * (1.0 - bent * bent) * 0.7978845608028654 * (
        1.0 + 3.0 * 0.044715 * upper * upper
    )
    return value, slope


class Plan:
    def __init__(self, dp_n, block, width, hidden, pairs):
        self.dp_n, self.block, self.width, self.hidden, self.pairs = dp_n, block, width, hidden, pairs
        self.half = pairs // 2
        self.heads = width // HEAD_DIM
        self.direct = dp_n == 8

    def weight_specs(self, pieces):
        return [whole(item.shape) for item in flat(pieces)]

    def weight_scratch(self, pieces):
        return [pltpu.VMEM((len(pieces), D, D), LOW)]

    def assemble(self, meta, pieces, refs, scratch):
        refs = iter(refs)
        for count in range(len(pieces)):
            if not self.direct:
                scratch[count] = next(refs)[...]
                continue
            _, height, start = pieces[count]
            for places in ((0, 4), (2, 6), (1, 5), (3, 7)):
                ref = next(refs)
                for index, place in enumerate(places):
                    row = pl.multiple_of(jnp.bitwise_xor(meta[0], place) * self.block, 32)
                    first = start + index * height
                    scratch[count, pl.ds(row, self.block), :] = ref[first : first + self.block]

    def grad_shapes(self, count):
        if not self.direct:
            return [jax.ShapeDtypeStruct((count, D, D), F32)]
        shape = (self.dp_n // 2, count, self.block, D)
        return [jax.ShapeDtypeStruct(shape, LOW), jax.ShapeDtypeStruct(shape, F32)]

    def emit(self, meta, acc, refs):
        if not self.direct:
            refs[0][...] = acc[...]
            return
        for index in range(self.dp_n // 2):
            here = pl.multiple_of(jnp.bitwise_xor(meta[0], 2 * index) * self.block, 32)
            away = pl.multiple_of(jnp.bitwise_xor(meta[0], 2 * index + 1) * self.block, 32)
            for count in range(acc.shape[0]):
                refs[0][index, count] = acc[count, pl.ds(away, self.block), :].astype(LOW)
                refs[1][index, count] = acc[count, pl.ds(here, self.block), :]


def flat(pieces):
    return [item for arrays, _, _ in pieces for item in arrays]


def whole(shape):
    return pl.BlockSpec(shape, lambda *_: (0,) * len(shape))


def own_spec(count, base, shape):
    return pl.BlockSpec(
        (1,) + shape, lambda p, _: (base + jnp.maximum(p - count, 0),) + (0,) * len(shape)
    )


def oth_spec(count, base, shape):
    return pl.BlockSpec(
        (1,) + shape, lambda p, _: (base + jnp.minimum(p, count - 1),) + (0,) * len(shape)
    )


def step_spec(shape):
    return pl.BlockSpec((1,) + shape, lambda p, _: (p,) + (0,) * len(shape))


def call(name, body, grid, meta, inputs, in_specs, outs, out_specs, scratch):
    return pl.pallas_call(
        body,
        name=name,
        out_shape=outs,
        grid_spec=pltpu.PrefetchScalarGridSpec(
            num_scalar_prefetch=1,
            grid=grid,
            in_specs=in_specs,
            out_specs=out_specs,
            scratch_shapes=scratch,
        ),
        cost_estimate=pl.CostEstimate(flops=1, transcendentals=0, bytes_accessed=1),
        compiler_params=pltpu.CompilerParams(
            dimension_semantics=("arbitrary",) * len(grid), vmem_limit_bytes=VMEM_LIMIT
        ),
    )(meta, *inputs)


def key_mask(meta, pairs, slot, turned=False):
    shape = (ENC_LEN, 1) if turned else (1, ENC_LEN)
    place = lax.broadcasted_iota(jnp.int32, shape, 1 - turned)
    image, prefix = meta[1 + slot], meta[1 + pairs + slot]
    return (place < image * PATCHES) | ((place >= PATCHES) & (place < PATCHES + prefix))


def attend_heads(plan, queries, keys, values, allowed):
    mixed = []
    for head in range(plan.heads):
        cut = slice(head * HEAD_DIM, (head + 1) * HEAD_DIM)
        scores = jnp.where(allowed, mm_t(queries[:, cut], keys[:, cut]) * 0.125, MASKED)
        mixed.append(mm(softmax(scores).astype(LOW), values[:, cut]).astype(LOW))
    return jnp.concatenate(mixed, 1)


def attend_heads_back(plan, queries, keys, values, allowed, grad_mixed):
    grads = ([], [], [])
    for head in range(plan.heads):
        cut = slice(head * HEAD_DIM, (head + 1) * HEAD_DIM)
        query, key, value, grad = queries[:, cut], keys[:, cut], values[:, cut], grad_mixed[:, cut]
        probs = softmax(jnp.where(allowed, mm_t(query, key) * 0.125, MASKED))
        grad_probs = mm_t(grad, value)
        inner = jnp.sum(grad_probs * probs, -1, keepdims=True)
        grad_scores = (probs * (grad_probs - inner)).astype(LOW)
        grads[0].append((mm(grad_scores, key) * 0.125).astype(LOW))
        grads[1].append((t_mm(grad_scores, query) * 0.125).astype(LOW))
        grads[2].append(t_mm(probs.astype(LOW), grad).astype(LOW))
    return tuple(jnp.concatenate(item, 1) for item in grads)


def attend_heads_turned(plan, queries, keys, values, allowed, grad_mixed):
    grads = ([], [], [])
    for head in range(plan.heads):
        cut = slice(head * HEAD_DIM, (head + 1) * HEAD_DIM)
        query, key, value, grad = queries[:, cut], keys[:, cut], values[:, cut], grad_mixed[:, cut]
        scores = jnp.where(allowed, mm_t(key, query) * 0.125, MASKED)
        expons = jnp.exp(scores - jnp.max(scores, 0, keepdims=True))
        probs = expons / jnp.sum(expons, 0, keepdims=True)
        grad_probs = mm_t(value, grad)
        inner = jnp.sum(grad_probs * probs, 0, keepdims=True)
        grad_scores = (probs * (grad_probs - inner)).astype(LOW)
        grads[0].append((t_mm(grad_scores, key) * 0.125).astype(LOW))
        grads[1].append((mm(grad_scores, query) * 0.125).astype(LOW))
        grads[2].append(mm(probs.astype(LOW), grad).astype(LOW))
    return tuple(jnp.concatenate(item, 1) for item in grads)


def slot_of(plan, count, base, step):
    return jnp.where(step < count, plan.half + base + step, base + step - count)


def pick(step, count, own, oth, rows):
    return jnp.where(step < count, oth[0, :rows], own[0, :rows])


def put(step, count, own, oth, value):
    @pl.when(step < count)
    def _():
        oth[0, : value.shape[0]] = value

    @pl.when(step >= count)
    def _():
        own[0, : value.shape[0]] = value


def encoder_attention(plan, meta, own, oth, gain, pieces, base, count):
    w3 = 3 * plan.width
    n = len(flat(pieces))

    def body(meta, own_ref, oth_ref, gain_ref, *rest):
        refs, (own_out, oth_out, kept, weight) = rest[:n], rest[n:]
        step = pl.program_id(0)

        @pl.when(step == 0)
        def _():
            plan.assemble(meta, pieces, refs, weight)

        value = pick(step, count, own_ref, oth_ref, ENC_LEN).astype(F32)
        normed = (value * rms_scale(value) * gain_ref[...]).astype(LOW)
        joined = mm(normed, weight[0, :, :w3]).astype(LOW)
        allowed = key_mask(meta, plan.pairs, slot_of(plan, count, base, step))
        width = plan.width
        mixed = attend_heads(
            plan, joined[:, :width], joined[:, width : 2 * width], joined[:, 2 * width :], allowed
        )
        kept[0, :, :w3] = joined
        kept[0, :, w3:] = mixed
        put(step, count, own_out, oth_out, mm_t(mixed, weight[0, :, w3:]).astype(LOW))

    rows = (LONG, D)
    return call(
        "encoder_attention",
        body,
        (2 * count,),
        meta,
        (own, oth, gain, *flat(pieces)),
        [own_spec(count, base, rows), oth_spec(count, base, rows), whole((1, D)), *plan.weight_specs(pieces)],
        [jax.ShapeDtypeStruct((count,) + rows, LOW)] * 2
        + [jax.ShapeDtypeStruct((2 * count, ENC_LEN, w3 + plan.width), LOW)],
        [own_spec(count, 0, rows), oth_spec(count, 0, rows), step_spec((ENC_LEN, w3 + plan.width))],
        plan.weight_scratch(pieces),
    )


def encoder_attention_back(plan, meta, own, oth, gain, pieces, kept, grad_own, grad_oth):
    count = plan.half
    width, w3 = plan.width, 3 * plan.width
    n = len(flat(pieces))

    def body(meta, own_ref, oth_ref, gain_ref, kept_ref, grad_own_ref, grad_oth_ref, *rest):
        refs, (own_out, oth_out), grad_refs = rest[:n], rest[n : n + 2], rest[n + 2 : -2]
        weight, acc = rest[-2:]
        step = pl.program_id(0)

        @pl.when(step == 0)
        def _():
            plan.assemble(meta, pieces, refs, weight)
            acc[...] = jnp.zeros_like(acc)

        value = pick(step, count, own_ref, oth_ref, ENC_LEN).astype(F32)
        normed = (value * rms_scale(value) * gain_ref[...]).astype(LOW)
        grad = pick(step, count, grad_own_ref, grad_oth_ref, ENC_LEN)
        allowed = key_mask(meta, plan.pairs, slot_of(plan, count, 0, step), True)
        grad_mixed = mm(grad, weight[0, :, w3:]).astype(LOW)
        acc[0, :, w3:] += t_mm(grad, kept_ref[0, :, w3:])
        joined = kept_ref[0, :, :w3]
        grads = attend_heads_turned(
            plan, joined[:, :width], joined[:, width : 2 * width], joined[:, 2 * width :], allowed, grad_mixed
        )
        together = jnp.concatenate(grads, 1)
        acc[0, :, :w3] += t_mm(normed, together)
        put(step, count, own_out, oth_out, mm_t(together, weight[0, :, :w3]).astype(LOW))

        @pl.when(step == 2 * count - 1)
        def _():
            plan.emit(meta, acc, grad_refs)

    rows = (LONG, D)
    shapes = plan.grad_shapes(1)
    pair_specs = [own_spec(count, 0, rows), oth_spec(count, 0, rows)]
    return call(
        "encoder_attention_back",
        body,
        (2 * count,),
        meta,
        (own, oth, gain, kept, grad_own, grad_oth, *flat(pieces)),
        [*pair_specs, whole((1, D)), step_spec(kept.shape[1:]), *pair_specs, *plan.weight_specs(pieces)],
        [jax.ShapeDtypeStruct((count,) + rows, LOW)] * 2 + shapes,
        [*pair_specs, *[whole(item.shape) for item in shapes]],
        plan.weight_scratch(pieces) + [pltpu.VMEM((1, D, D), F32)],
    )


def encoder_feed(plan, meta, own, oth, pieces, base, count):
    n = len(flat(pieces))

    def body(meta, own_ref, oth_ref, *rest):
        refs, (own_out, oth_out, weight) = rest[:n], rest[n:]
        step = pl.program_id(0)

        @pl.when(step == 0)
        def _():
            plan.assemble(meta, pieces, refs, weight)

        normed = pick(step, count, own_ref, oth_ref, ENC_LEN)
        active = gelu_parts(mm(normed, weight[0]))[0].astype(LOW)
        put(step, count, own_out, oth_out, mm_t(active, weight[1]).astype(LOW))

    rows = (LONG, D)
    return call(
        "encoder_feed",
        body,
        (2 * count,),
        meta,
        (own, oth, *flat(pieces)),
        [own_spec(count, base, rows), oth_spec(count, base, rows), *plan.weight_specs(pieces)],
        [jax.ShapeDtypeStruct((count,) + rows, LOW)] * 2,
        [own_spec(count, 0, rows), oth_spec(count, 0, rows)],
        plan.weight_scratch(pieces),
    )


def encoder_feed_back(plan, meta, own, oth, grad_own, grad_oth, pieces):
    n = len(flat(pieces))
    count = plan.half

    def body(meta, own_ref, oth_ref, grad_own_ref, grad_oth_ref, *rest):
        refs, (own_out, oth_out), grad_refs = rest[:n], rest[n : n + 2], rest[n + 2 : -2]
        weight, acc = rest[-2:]
        step = pl.program_id(0)

        @pl.when(step == 0)
        def _():
            plan.assemble(meta, pieces, refs, weight)
            acc[...] = jnp.zeros_like(acc)

        normed = pick(step, count, own_ref, oth_ref, ENC_LEN)
        grad = pick(step, count, grad_own_ref, grad_oth_ref, ENC_LEN)
        active, slope = gelu_parts(mm(normed, weight[0]))
        grad_upper = (slope * mm(grad, weight[1])).astype(LOW)
        put(step, count, own_out, oth_out, mm_t(grad_upper, weight[0]).astype(LOW))
        acc[0] += t_mm(normed, grad_upper)
        acc[1] += t_mm(grad, active.astype(LOW))

        @pl.when(step == 2 * count - 1)
        def _():
            for index in range(2):
                size = len(grad_refs) // 2
                plan.emit(meta, acc.at[pl.ds(index, 1)], grad_refs[index * size : (index + 1) * size])

    rows = (LONG, D)
    shapes = plan.grad_shapes(1) * 2
    pair_specs = [own_spec(count, 0, rows), oth_spec(count, 0, rows)]
    return call(
        "encoder_feed_back",
        body,
        (2 * count,),
        meta,
        (own, oth, grad_own, grad_oth, *flat(pieces)),
        [*pair_specs, *pair_specs, *plan.weight_specs(pieces)],
        [jax.ShapeDtypeStruct((count,) + rows, LOW)] * 2 + shapes,
        [*pair_specs, *[whole(item.shape) for item in shapes]],
        plan.weight_scratch(pieces) + [pltpu.VMEM((2, D, D), F32)],
    )


def self_mask(plan, meta, turned=False):
    rows = plan.pairs * SUFFIX
    query = lax.broadcasted_iota(jnp.int32, (rows, rows), int(turned))
    key = lax.broadcasted_iota(jnp.int32, (rows, rows), 1 - turned)
    pair = key // SUFFIX
    limit = jnp.zeros_like(key)
    for slot in range(plan.pairs):
        limit = jnp.where(pair == slot, meta[1 + 2 * plan.pairs + slot], limit)
    return (query // SUFFIX == pair) & (key <= query) & (key - pair * SUFFIX < limit)


def decoder_self(plan, meta, rows_in, gain, pieces):
    n = len(flat(pieces))
    width, w3 = plan.width, 3 * plan.width
    rows = plan.pairs * SUFFIX
    mid = rows // 2

    def body(meta, in_ref, gain_ref, *rest):
        refs, (own_out, oth_out, kept, weight) = rest[:n], rest[n:]
        plan.assemble(meta, pieces, refs, weight)
        value = in_ref[...].astype(F32)
        normed = (value * rms_scale(value) * gain_ref[...]).astype(LOW)
        joined = mm(normed, weight[0, :, :w3]).astype(LOW)
        mixed = attend_heads(
            plan, joined[:, :width], joined[:, width : 2 * width], joined[:, 2 * width :], self_mask(plan, meta)
        )
        kept[:, :w3] = joined
        kept[:, w3:] = mixed
        partial = mm_t(mixed, weight[0, :, w3:]).astype(LOW)
        own_out[...] = partial[:mid]
        oth_out[...] = partial[mid:]

    return call(
        "decoder_self",
        body,
        (1,),
        meta,
        (rows_in, gain, *flat(pieces)),
        [whole((rows, D)), whole((1, D)), *plan.weight_specs(pieces)],
        [jax.ShapeDtypeStruct((mid, D), LOW)] * 2 + [jax.ShapeDtypeStruct((rows, 4 * width), LOW)],
        [whole((mid, D))] * 2 + [whole((rows, 4 * width))],
        plan.weight_scratch(pieces),
    )


def decoder_self_back(plan, meta, rows_in, gain, pieces, kept, grad_own, grad_oth):
    n = len(flat(pieces))
    width, w3 = plan.width, 3 * plan.width
    rows = plan.pairs * SUFFIX
    mid = rows // 2

    def body(meta, in_ref, gain_ref, kept_ref, grad_own_ref, grad_oth_ref, *rest):
        refs, (own_out, oth_out), grad_refs = rest[:n], rest[n : n + 2], rest[n + 2 : -2]
        weight, acc = rest[-2:]
        plan.assemble(meta, pieces, refs, weight)
        value = in_ref[...].astype(F32)
        normed = (value * rms_scale(value) * gain_ref[...]).astype(LOW)
        grad = jnp.concatenate([grad_own_ref[...], grad_oth_ref[...]], 0)
        grad_mixed = mm(grad, weight[0, :, w3:]).astype(LOW)
        acc[0, :, w3:] = t_mm(grad, kept_ref[:, w3:])
        joined = kept_ref[:, :w3]
        grads = attend_heads_turned(
            plan,
            joined[:, :width],
            joined[:, width : 2 * width],
            joined[:, 2 * width :],
            self_mask(plan, meta, True),
            grad_mixed,
        )
        together = jnp.concatenate(grads, 1)
        acc[0, :, :w3] = t_mm(normed, together)
        partial = mm_t(together, weight[0, :, :w3]).astype(LOW)
        own_out[...] = partial[:mid]
        oth_out[...] = partial[mid:]
        plan.emit(meta, acc, grad_refs)

    shapes = plan.grad_shapes(1)
    return call(
        "decoder_self_back",
        body,
        (1,),
        meta,
        (rows_in, gain, kept, grad_own, grad_oth, *flat(pieces)),
        [whole((rows, D)), whole((1, D)), whole(kept.shape), whole((mid, D)), whole((mid, D)), *plan.weight_specs(pieces)],
        [jax.ShapeDtypeStruct((mid, D), LOW)] * 2 + shapes,
        [whole((mid, D))] * 2 + [whole(item.shape) for item in shapes],
        plan.weight_scratch(pieces) + [pltpu.VMEM((1, D, D), F32)],
    )


def decoder_cross(plan, meta, own, oth, memory_own, memory_oth, pieces):
    n = len(flat(pieces))
    count = plan.half
    width, w3 = plan.width, 3 * plan.width

    def body(meta, own_ref, oth_ref, memory_own_ref, memory_oth_ref, *rest):
        refs, (own_out, oth_out, kept_query, kept_key, weight) = rest[:n], rest[n:]
        step = pl.program_id(0)

        @pl.when(step == 0)
        def _():
            plan.assemble(meta, pieces, refs, weight)

        normed = pick(step, count, own_ref, oth_ref, SUFFIX)
        memory = pick(step, count, memory_own_ref, memory_oth_ref, ENC_LEN)
        queries = mm(normed, weight[0, :, :width]).astype(LOW)
        both = mm(memory, weight[0, :, width:w3]).astype(LOW)
        allowed = key_mask(meta, plan.pairs, slot_of(plan, count, 0, step))
        mixed = attend_heads(plan, queries, both[:, :width], both[:, width:], allowed)
        kept_query[0, :, :width] = queries
        kept_query[0, :, width:] = mixed
        kept_key[0] = both
        put(step, count, own_out, oth_out, mm_t(mixed, weight[0, :, w3:]).astype(LOW))

    rows, long = (SUFFIX, D), (LONG, D)
    return call(
        "decoder_cross",
        body,
        (2 * count,),
        meta,
        (own, oth, memory_own, memory_oth, *flat(pieces)),
        [
            own_spec(count, 0, rows),
            oth_spec(count, 0, rows),
            own_spec(count, 0, long),
            oth_spec(count, 0, long),
            *plan.weight_specs(pieces),
        ],
        [jax.ShapeDtypeStruct((count,) + rows, LOW)] * 2
        + [
            jax.ShapeDtypeStruct((2 * count, SUFFIX, 2 * width), LOW),
            jax.ShapeDtypeStruct((2 * count, ENC_LEN, 2 * width), LOW),
        ],
        [
            own_spec(count, 0, rows),
            oth_spec(count, 0, rows),
            step_spec((SUFFIX, 2 * width)),
            step_spec((ENC_LEN, 2 * width)),
        ],
        plan.weight_scratch(pieces),
    )


def decoder_cross_back(
    plan, meta, own, oth, memory_own, memory_oth, pieces, kept_query, kept_key, grad_own, grad_oth
):
    n = len(flat(pieces))
    count = plan.half
    width, w3 = plan.width, 3 * plan.width
    rows = plan.pairs * SUFFIX
    mid = rows // 2

    def body(
        meta, own_ref, oth_ref, memory_own_ref, memory_oth_ref, query_ref, key_ref, grad_own_ref, grad_oth_ref, *rest
    ):
        refs, outs, grad_refs = rest[:n], rest[n : n + 4], rest[n + 4 : -4]
        weight, acc, grad_mixed, grad_query = rest[-4:]
        step = pl.program_id(0)

        @pl.when(step == 0)
        def _():
            plan.assemble(meta, pieces, refs, weight)
            grad = jnp.concatenate([grad_oth_ref[...], grad_own_ref[...]], 0).reshape(rows, D)
            grad_mixed[...] = mm(grad, weight[0, :, w3:]).astype(LOW)
            acc[0, :, w3:] = t_mm(grad, query_ref[:, :, width:].reshape(rows, width))
            acc[0, :, width:w3] = jnp.zeros((D, w3 - width), F32)

        memory = pick(step, count, memory_own_ref, memory_oth_ref, ENC_LEN)
        allowed = key_mask(meta, plan.pairs, slot_of(plan, count, 0, step))
        both = key_ref[0]
        here = pl.ds(pl.multiple_of(step * SUFFIX, SUFFIX), SUFFIX)
        query, grad_key, grad_value = attend_heads_back(
            plan, query_ref[step, :, :width], both[:, :width], both[:, width:], allowed, grad_mixed[here, :]
        )
        grad_query[here, :] = query
        together = jnp.concatenate([grad_key, grad_value], 1)
        acc[0, :, width:w3] += t_mm(memory, together)
        put(step, count, outs[2], outs[3], mm_t(together, weight[0, :, width:w3]).astype(LOW))

        @pl.when(step == 2 * count - 1)
        def _():
            normed = jnp.concatenate([oth_ref[...], own_ref[...]], 0).reshape(rows, D)
            queries = grad_query[...]
            acc[0, :, :width] = t_mm(normed, queries)
            back = mm_t(queries, weight[0, :, :width]).astype(LOW)
            outs[1][...] = back[:mid].reshape(count, SUFFIX, D)
            outs[0][...] = back[mid:].reshape(count, SUFFIX, D)
            plan.emit(meta, acc, grad_refs)

    part, long = (count, SUFFIX, D), (LONG, D)
    shapes = plan.grad_shapes(1)
    long_specs = [own_spec(count, 0, long), oth_spec(count, 0, long)]
    return call(
        "decoder_cross_back",
        body,
        (2 * count,),
        meta,
        (own, oth, memory_own, memory_oth, kept_query, kept_key, grad_own, grad_oth, *flat(pieces)),
        [
            whole(part),
            whole(part),
            *long_specs,
            whole(kept_query.shape),
            step_spec(kept_key.shape[1:]),
            whole(part),
            whole(part),
            *plan.weight_specs(pieces),
        ],
        [jax.ShapeDtypeStruct(part, LOW)] * 2
        + [jax.ShapeDtypeStruct((count,) + long, LOW)] * 2
        + shapes,
        [whole(part), whole(part), *long_specs, *[whole(item.shape) for item in shapes]],
        plan.weight_scratch(pieces)
        + [pltpu.VMEM((1, D, D), F32)]
        + [pltpu.VMEM((rows, width), LOW), pltpu.VMEM((rows, width), LOW)],
    )


def decoder_feed(plan, meta, own, oth, grad_in, pieces):
    n = len(flat(pieces))
    rows = plan.pairs * SUFFIX
    mid = rows // 2

    def body(meta, own_ref, oth_ref, grad_ref, *rest):
        refs, (own_out, oth_out), grad_refs = rest[:n], rest[n : n + 2], rest[n + 2 : -2]
        weight, acc = rest[-2:]
        plan.assemble(meta, pieces, refs, weight)
        normed = jnp.concatenate([own_ref[...], oth_ref[...]], 0)
        grad = grad_ref[...]
        active, slope = gelu_parts(mm(normed, weight[0]))
        active = active.astype(LOW)
        partial = mm_t(active, weight[1]).astype(LOW)
        grad_upper = (slope * mm(grad, weight[1])).astype(LOW)
        back = mm_t(grad_upper, weight[0]).astype(LOW)
        own_out[0] = partial[:mid]
        own_out[1] = back[:mid]
        oth_out[0] = partial[mid:]
        oth_out[1] = back[mid:]
        acc[0] = t_mm(normed, grad_upper)
        acc[1] = t_mm(grad, active)
        plan.emit(meta, acc, grad_refs)

    shapes = plan.grad_shapes(2)
    return call(
        "decoder_feed",
        body,
        (1,),
        meta,
        (own, oth, grad_in, *flat(pieces)),
        [whole((mid, D))] * 2 + [whole((rows, D)), *plan.weight_specs(pieces)],
        [jax.ShapeDtypeStruct((2, mid, D), LOW)] * 2 + shapes,
        [whole((2, mid, D))] * 2 + [whole(item.shape) for item in shapes],
        plan.weight_scratch(pieces) + [pltpu.VMEM((2, D, D), F32)],
    )


def add_norm(meta, name, base, first, second, gain):
    def body(meta, base_ref, first_ref, second_ref, gain_ref, sum_ref, norm_ref):
        value = base_ref[...].astype(F32) + (first_ref[...].astype(F32) + second_ref[...].astype(F32))
        sum_ref[...] = value
        norm_ref[...] = (value * rms_scale(value) * gain_ref[...]).astype(LOW)

    shape = base.shape
    part = (1,) + shape[1:] if len(shape) == 3 else shape
    spec = (
        pl.BlockSpec(part, lambda p, _: (p, 0, 0)) if len(shape) == 3 else whole(shape)
    )
    return call(
        name,
        body,
        (shape[0] if len(shape) == 3 else 1,),
        meta,
        (base, first, second, gain),
        [spec, spec, spec, whole((1, D))],
        [jax.ShapeDtypeStruct(shape, F32), jax.ShapeDtypeStruct(shape, LOW)],
        [spec, spec],
        [],
    )


def norm_back(meta, name, inputs, gain, grad, first, second, want_low):
    def body(meta, in_ref, gain_ref, grad_ref, first_ref, second_ref, *outs):
        value = in_ref[...].astype(F32)
        scale = rms_scale(value)
        unit = value * scale
        back = first_ref[...].astype(F32) + second_ref[...].astype(F32)
        product = back * unit
        real = product[0, :ENC_LEN] if value.ndim == 3 else product
        part = jnp.sum(real, 0, keepdims=True)
        weighted = product * gain_ref[...]
        total = grad_ref[...].astype(F32) + scale * (
            back * gain_ref[...] - unit * jnp.mean(weighted, -1, keepdims=True)
        )
        outs[0][...] = total
        if want_low:
            outs[1][...] = total.astype(LOW)
        step = pl.program_id(0)

        @pl.when(step == 0)
        def _():
            outs[-1][...] = part

        @pl.when(step > 0)
        def _():
            outs[-1][...] += part

    shape = inputs.shape
    part = (1,) + shape[1:] if len(shape) == 3 else shape
    spec = pl.BlockSpec(part, lambda p, _: (p, 0, 0)) if len(shape) == 3 else whole(shape)
    return call(
        name,
        body,
        (shape[0] if len(shape) == 3 else 1,),
        meta,
        (inputs, gain, grad, first, second),
        [spec, whole((1, D)), spec, spec, spec],
        [jax.ShapeDtypeStruct(shape, F32)]
        + [jax.ShapeDtypeStruct(shape, LOW)] * want_low
        + [jax.ShapeDtypeStruct((1, D), F32)],
        [spec] * (1 + want_low) + [whole((1, D))],
        [],
    )


def fold(plan, meta, keeps, mores, split):
    n = len(keeps)
    counts = [item.shape[1] for item in keeps]
    total = sum(counts)
    tail = keeps[0].shape[2:]
    blocks = keeps[0].shape[0]

    def body(meta, *rest):
        keep_refs, more_refs, outs = rest[:n], rest[n : 2 * n], rest[2 * n :]
        for index in range(blocks):
            start = 0
            out, at = split(index)
            for keep_ref, more_ref, count in zip(keep_refs, more_refs, counts):
                value = keep_ref[index] + more_ref[index].astype(F32)
                outs[out][at, start : start + count] = value.astype(outs[out].dtype)
                start += count

    places = [split(index) for index in range(blocks)]
    outs = [
        jax.ShapeDtypeStruct((sum(place[0] == out for place in places), total) + tail, LOW if out else F32)
        for out in range(1 + max(place[0] for place in places))
    ]
    return call(
        "fold",
        body,
        (1,),
        meta,
        (*keeps, *mores),
        [whole(item.shape) for item in (*keeps, *mores)],
        outs,
        [whole(item.shape) for item in outs],
        [],
    )


def halves(index):
    return index % 2, index // 2


def apart(index):
    return index, 0


def pack_first(plan, meta, project_in, project_out, gains):
    width, block = plan.width, plan.block

    def body(meta, in_ref, out_ref, gain_ref, packed):
        parts = [in_ref[0, index] for index in range(3)] + [jnp.transpose(out_ref[0])]
        packed[:block] = jnp.concatenate(parts, 1).astype(LOW)
        rows = jnp.concatenate([gain_ref[...], jnp.zeros((3, block), F32)], 0)
        wide = jnp.concatenate([rows, jnp.zeros((8, D - block), F32)], 1)
        packed[block:] = pltpu.roll(wide, meta[0] * block, 1).astype(LOW)

    shape = (block + 8, D)
    return call(
        "pack_first",
        body,
        (1,),
        meta,
        (project_in, project_out, gains),
        [
            pl.BlockSpec((1,) + project_in.shape[1:], lambda *_: (0, 0, 0, 0)),
            pl.BlockSpec((1,) + project_out.shape[1:], lambda *_: (0, 0, 0)),
            whole(gains.shape),
        ],
        [jax.ShapeDtypeStruct(shape, LOW)],
        [whole(shape)],
        [],
    )[0]


def one_hot(rows, offset):
    row = lax.broadcasted_iota(jnp.int32, (rows, D), 0)
    lane = lax.broadcasted_iota(jnp.int32, (rows, D), 1)
    return (lane == row + offset).astype(F32)


def collect(plan, meta, sets, attention):
    counts = [pieces[0].shape[-3] for pieces in sets]
    count = sum(counts)
    shape = (count,) + sets[0][0].shape[-2:]
    arrays = [item for pieces in sets for item in pieces]
    n = len(arrays)
    groups = D // plan.width

    def body(meta, *rest):
        refs, (out, tile_out) = rest[:n], rest[n:]
        dp_at, mp_at = meta[0], meta[1 + 3 * plan.pairs]
        group = lax.broadcasted_iota(jnp.int32, (8, D), 1) // plan.width
        row = lax.broadcasted_iota(jnp.int32, (8, D), 0)
        place = one_hot(plan.block, dp_at * plan.block)
        def one(first, refs, at, _):
            index = first + at
            heads = (jnp.zeros((8, D), jnp.int32) + index) < attention
            value = refs[0][0, at]
            for ref in refs[1:]:
                value = value + ref[0, at].astype(F32)
            out[index] = value
            square = value * value
            lanes = jnp.broadcast_to(jnp.sum(square, 0, keepdims=True), (8, D))
            mask = jnp.where(heads, (group == row).astype(F32), (row == 0).astype(F32))
            sums = lax.dot_general(
                mask, square, (((1,), (1,)), ((), ())), precision=EXACT, preferred_element_type=F32
            )
            tile = lax.dot_general(
                sums, place, (((1,), (0,)), ((), ())), precision=EXACT, preferred_element_type=F32
            )
            spread = jnp.zeros_like(tile)
            for part in range(groups):
                shift = lax.rem(mp_at * plan.width + (D - part * plan.width), D)
                moved = pltpu.roll(jnp.where(group == part, lanes, 0.0), shift, 1)
                spread = jnp.where(row == 4 + part, moved, spread)
            spread = jnp.where(heads, spread, jnp.where(row == 4 + mp_at, lanes, 0.0))
            tile_out[index] = jnp.where(row < 4, tile, spread)
            return 0

        first, start = 0, 0
        for pieces, size in zip(sets, counts):
            lax.fori_loop(0, size, functools.partial(one, first, refs[start : start + len(pieces)]), 0)
            first, start = first + size, start + len(pieces)

    return call(
        "collect",
        body,
        (1,),
        meta,
        tuple(arrays),
        [whole(item.shape) for item in arrays],
        [jax.ShapeDtypeStruct(shape, F32), jax.ShapeDtypeStruct((count, 8, D), F32)],
        [whole(shape), whole((count, 8, D))],
        [],
    )


def finish(plan, meta, sums, statistics, gain_state):
    counts = [item.shape for item in statistics]

    def body(meta, sum_ref, *rest):
        olds, gains = rest[:8], rest[8:12]
        norm_out, news, rates, gain_outs = rest[12], rest[13:21], rest[21], rest[22:]
        tiles = [sum_ref[6], sum_ref[1], sum_ref[0]]
        feeds = [(sum_ref[2], sum_ref[3]), (sum_ref[4], sum_ref[5])]
        gain_sum = 0.5 * sum_ref[7]
        total = jnp.sum(gain_sum * gain_sum)
        for tile in tiles:
            total = total + jnp.sum(tile[:4])
        for up, down in feeds:
            total = total + jnp.sum(up[:1]) + jnp.sum(down[:1])
        totals = jnp.full((8, D), total, F32)
        norm = jnp.sqrt(totals)
        factor = jnp.minimum(1.0, 1.0 / norm)
        squared = (factor * factor)[:1]
        norm_out[...] = norm[:, :128]
        rates[...] = factor[:, :128]

        def renew(old, sums, number):
            return DECAY * old + (1.0 - DECAY) * (sums * squared / number + EPS_STAT)

        for layer, tile in enumerate(tiles):
            for part in range(3):
                news[0][layer, part : part + 1] = renew(olds[0][layer, part : part + 1], tile[part : part + 1], D)
                news[1][layer, part : part + 1] = renew(
                    olds[1][layer, part : part + 1], tile[4 + part : 5 + part], D
                )
            news[2][layer : layer + 1] = renew(olds[2][layer : layer + 1], tile[7:8], D)
            news[3][layer : layer + 1] = renew(olds[3][layer : layer + 1], tile[3:4], D)
        for layer, (up, down) in enumerate(feeds):
            news[4][layer : layer + 1] = renew(olds[4][layer : layer + 1], up[:1], FF)
            news[7][layer : layer + 1] = renew(olds[7][layer : layer + 1], down[:1], FF)
            for part in range(FF // D):
                cut = slice(part * D, (part + 1) * D)
                news[5][layer : layer + 1, cut] = renew(
                    olds[5][layer : layer + 1, cut], up[4 + part : 5 + part], D
                )
                news[6][layer : layer + 1, cut] = renew(
                    olds[6][layer : layer + 1, cut], down[4 + part : 5 + part], D
                )
        shift = lax.rem(D - meta[0] * plan.block, D)
        grad = (pltpu.roll(gain_sum, shift, 1) * factor)[:5, : plan.block]
        master, square, moment, average = [item[...] for item in gains]
        square_new = DECAY * square + (1.0 - DECAY) * (grad * grad + EPS_STAT)
        stepped = grad * lax.rsqrt(square_new)
        moment_new = MOMENTUM * moment + stepped
        master_new = master - RATE_GAIN * (MOMENTUM * moment_new + stepped)
        values = (
            grad,
            square_new,
            moment_new,
            master_new,
            AVERAGE * average + (1.0 - AVERAGE) * master_new,
            master_new,
        )
        for out, value in zip(gain_outs, values):
            out[...] = value.astype(out.dtype)

    small = gain_state[0].shape
    outs = (
        [jax.ShapeDtypeStruct((8, 128), F32)]
        + [jax.ShapeDtypeStruct(shape, F32) for shape in counts]
        + [jax.ShapeDtypeStruct((8, 128), F32)]
        + [jax.ShapeDtypeStruct(small, F32)] * 5
        + [jax.ShapeDtypeStruct(small, LOW)]
    )
    inputs = (sums, *statistics, *gain_state)
    return call(
        "finish",
        body,
        (1,),
        meta,
        inputs,
        [whole(item.shape) for item in inputs],
        outs,
        [whole(item.shape) for item in outs],
        [],
    )


def part_spec(block, place):
    return pl.BlockSpec((2, block, D), lambda *_: (place, 0, 0))


def step_values(grad, scale, master, moment, average):
    stepped = grad * scale
    moment_new = MOMENTUM * moment + stepped
    master_new = master - RATE_MATRIX * (MOMENTUM * moment_new + stepped)
    return grad, moment_new, master_new, AVERAGE * average + (1.0 - AVERAGE) * master_new


def columns(rows, offset, size):
    filled = jnp.concatenate([rows] * (8 // rows.shape[0] + 1), 0)[:8]
    wide = (size + 127) // 128 * 128
    return jnp.transpose(pltpu.roll(filled, lax.rem(D - offset, D), 1)[:, :wide])[:size]


def update_attention(plan, meta, rates, grads, rows_in, cols_in, rows_out, cols_out, state_in, state_out):
    width, block = plan.width, plan.block

    def body(meta, rates_ref, grad_a, grad_b, rin, cin, rout, cout, *rest):
        ins, outs = rest[:6], rest[6:]
        layer = pl.program_id(0)
        dp_at, mp_at = meta[0], meta[1 + 3 * plan.pairs]
        grad = jnp.where(layer == 0, grad_a[0], jnp.where(layer == 1, grad_b[1], grad_b[0]))
        grad = grad * rates_ref[:1, :1]
        means = jnp.mean(rin[0], -1, keepdims=True)
        row_scale = lax.rsqrt(columns(rin[0] / means, dp_at * block, block))
        shift = lax.rem(D - mp_at * width, D)
        col_scale = lax.rsqrt(pltpu.roll(jnp.concatenate([cin[0]] * 3, 0)[:8], shift, 1)[:3, :width])
        for part in range(3):
            values = step_values(
                grad[:, part * width : (part + 1) * width],
                row_scale[:, part : part + 1] * col_scale[part : part + 1],
                ins[0][0, part],
                ins[1][0, part],
                ins[2][0, part],
            )
            for out, value in zip(outs[:4], values):
                out[0, part] = value
            outs[4][0, part] = values[2].astype(LOW)
        turned = jnp.transpose(grad[:, 3 * width :])
        row, col = rout[pl.ds(layer, 1), :], cout[pl.ds(layer, 1), :]
        mean = jnp.mean(row, -1, keepdims=True)
        row_scale = lax.rsqrt(columns(row / mean, mp_at * width, width))[:, :1]
        shift = lax.rem(D - dp_at * block, D)
        col_scale = lax.rsqrt(pltpu.roll(jnp.broadcast_to(col, (8, D)), shift, 1)[:1, :block])
        values = step_values(turned, row_scale * col_scale, ins[3][0], ins[4][0], ins[5][0])
        for out, value in zip(outs[5:9], values):
            out[0] = value
        outs[9][0] = values[2].astype(LOW)

    def spec(shape):
        return pl.BlockSpec((1,) + shape, lambda p, _: (p,) + (0,) * len(shape))

    shape_in, shape_out = (3, block, width), (width, block)
    outs = (
        [jax.ShapeDtypeStruct((3,) + shape_in, F32)] * 4
        + [jax.ShapeDtypeStruct((3,) + shape_in, LOW)]
        + [jax.ShapeDtypeStruct((3,) + shape_out, F32)] * 4
        + [jax.ShapeDtypeStruct((3,) + shape_out, LOW)]
    )
    return call(
        "update_attention",
        body,
        (3,),
        meta,
        (rates, *grads, rows_in, cols_in, rows_out, cols_out, *state_in, *state_out),
        [whole((8, 128)), whole((1, block, D)), part_spec(block, 0)]
        + [spec((3, D)), spec((3, D)), whole((3, D)), whole((3, D))]
        + [spec(shape_in)] * 3
        + [spec(shape_out)] * 3,
        outs,
        [spec(shape_in)] * 5 + [spec(shape_out)] * 5,
        [],
    )


def update_feed(plan, meta, rates, grads, rows_up, cols_up, rows_down, cols_down, state_up, state_down):
    hidden, block = plan.hidden, plan.block

    def body(meta, rates_ref, grad_a, grad_b, rup, cup, rdown, cdown, *rest):
        ins, outs = rest[:6], rest[6:]
        layer = pl.program_id(0)
        lanes = pl.ds(pl.multiple_of(meta[1 + 3 * plan.pairs] * hidden, 128), hidden)
        one = pl.ds(layer, 1)
        mean_up = jnp.mean(rup[one, :], -1, keepdims=True)
        mean_down = jnp.mean(rdown[one, :], -1, keepdims=True)
        along = (rup[one, :] / mean_up, cdown[one, :])
        across = (cup[one, lanes], rdown[one, lanes] / mean_down)
        for part in range(2):
            grad = jnp.where(layer == 0, grad_a[part], grad_b[part]) * rates_ref[:1, :1]
            row_scale = lax.rsqrt(columns(along[part], meta[0] * block, block))[:, :1]
            values = step_values(
                grad,
                row_scale * lax.rsqrt(across[part]),
                ins[3 * part][0],
                ins[3 * part + 1][0],
                ins[3 * part + 2][0],
            )
            for out, value in zip(outs[5 * part : 5 * part + 4], values):
                out[0] = value
            outs[5 * part + 4][0] = values[2].astype(LOW)

    state = pl.BlockSpec((1, block, hidden), lambda p, _: (p, 0, 0))
    outs = ([jax.ShapeDtypeStruct((2, block, hidden), F32)] * 4 + [jax.ShapeDtypeStruct((2, block, hidden), LOW)]) * 2
    values = call(
        "update_feed",
        body,
        (2,),
        meta,
        (
            rates,
            *grads,
            rows_up,
            cols_up,
            rows_down,
            cols_down,
            *state_up,
            *[item.transpose(0, 2, 1) for item in state_down],
        ),
        [whole((8, 128)), part_spec(block, 1), part_spec(block, 2)]
        + [whole((2, D)), whole((2, FF)), whole((2, FF)), whole((2, D))]
        + [state] * 6,
        outs,
        [state] * 10,
        [],
    )
    return [*values[:5], *[item.transpose(0, 2, 1) for item in values[5:]]]


def on_device(
    sizes,
    encoder_in,
    decoder_in,
    decoder_cotangent,
    counts,
    prefix_len,
    suffix_len,
    project_in,
    project_in_rows,
    project_in_cols,
    project_in_moment,
    project_in_average,
    project_out,
    project_out_rows,
    project_out_cols,
    project_out_moment,
    project_out_average,
    expand,
    expand_rows,
    expand_cols,
    expand_moment,
    expand_average,
    contract,
    contract_rows,
    contract_cols,
    contract_moment,
    contract_average,
    norm_gains,
    norm_gains_square,
    norm_gains_moment,
    norm_gains_average,
):
    dp_n, mp_n = sizes
    dp_index = lax.axis_index("dp")
    mp_index = lax.axis_index("mp")
    side = mp_index % 2
    pairs = prefix_len.shape[0]
    half = pairs // 2
    width = project_in.shape[-1]
    block = project_in.shape[-2]
    plan = Plan(dp_n, block, width, expand.shape[-1], pairs)
    low, f32 = LOW, F32

    def swap(value, axis, bit):
        count = dp_n if axis == "dp" else mp_n
        return lax.ppermute(value, axis, [(i, i ^ bit) for i in range(count)])

    def bits(count):
        return [1 << i for i in range(count.bit_length() - 1)]

    hold = lax.optimization_barrier

    class Gather:
        def __init__(self, blocks):
            self.items, self.sent, self.own = [{} for _ in blocks], [], list(blocks)

        def step(self, chain, *sends, later=()):
            names = [(item, name) for item, name in self.sent if (name, item) not in later]
            late = [(item, name) for item, name in self.sent if (name, item) in later]
            values = [self.items[item][name] for item, name in names]
            if names:
                chain, values, self.own = hold((list(chain), values, self.own))
            for (item, name), value in zip(names, values):
                self.items[item][name] = value
            self.sent = late
            for name, item in sends:
                if name == "fours":
                    four = swap(jnp.concatenate([self.own[at] for at in item]), "dp", 4)
                    for place, at in enumerate(item):
                        self.items[at]["four"] = four[place * block : (place + 1) * block]
                        self.sent.append((at, "four"))
                    continue
                parts = self.items[item]
                if name == "four":
                    parts[name] = swap(self.own[item], "dp", 4)
                    self.sent.append((item, name))
                    continue
                if "two" not in parts:
                    parts["two"] = jnp.concatenate([self.own[item], parts["four"]])
                if name == "far":
                    parts[name] = swap(parts["two"], "dp", 2)
                else:
                    parts[name] = swap(parts["two" if name == "near" else "far"], "dp", 1)
                self.sent.append((item, name))
            return chain

        def take(self, item, index=0):
            parts = self.items[item]
            height = self.own[item].shape[0]
            return [parts[name] for name in ("two", "far", "near", "last")], height, index * block

    class Plain:
        def __init__(self, blocks):
            self.own = list(blocks)

        def step(self, chain, *sends, later=()):
            return chain

        def take(self, item, index=0):
            own = self.own[item][index * block : (index + 1) * block]
            return [lax.all_gather(own, "dp", axis=0, tiled=True)], D, 0

    def total(value, axes):
        for axis, count in axes:
            for bit in bits(count):
                sent = value.astype(low)
                value = sent.astype(value.dtype) + swap(sent, axis, bit).astype(value.dtype)
        return value

    def total_dp(value):
        return total(value, [("dp", dp_n)])

    def total_all(value):
        return total(value, [("mp", mp_n), ("dp", dp_n)])

    def reduce_own(own, oth, first=()):
        sent = (own.astype(f32) + swap(oth, "mp", 1).astype(f32)).astype(low)
        for bit in bits(mp_n)[1:-1]:
            sent = (sent.astype(f32) + swap(sent, "mp", bit).astype(f32)).astype(low)
        sent, first = hold((sent, first))
        return sent, swap(sent, "mp", bits(mp_n)[-1])

    def relative(value):
        split = value.reshape((half, 2) + value.shape[1:])
        return (
            lax.dynamic_index_in_dim(split, side, 1, False),
            lax.dynamic_index_in_dim(split, 1 - side, 1, False),
        )

    def absolute(own):
        other = swap(own, "mp", 1)
        even = jnp.where(side == 0, own, other)
        odd = jnp.where(side == 0, other, own)
        return jnp.stack([even, odd], 1).reshape((pairs,) + own.shape[1:])

    def core(value):
        return swap(value, "mp", 1)

    def attention_block(layer):
        return jnp.concatenate(
            [project_in[layer, 0], project_in[layer, 1], project_in[layer, 2], project_out[layer].T], 1
        ).astype(low)

    def feed_block(layer):
        return [expand[layer].astype(low), contract[layer].T.astype(low)]

    direct = plan.direct
    place = dp_index[None].astype(jnp.int32)
    if direct:
        first = pack_first(plan, place, project_in, project_out, norm_gains)
    else:
        first = attention_block(0)
    blocks = [
        first,
        *feed_block(0),
        attention_block(1),
        attention_block(2),
        jnp.concatenate(feed_block(1)),
    ]
    gather = (Gather if direct else Plain)(blocks)
    gather.step((), ("four", 0))
    gather.step((), ("far", 0), ("near", 0), ("four", 1))
    gather.step((), ("last", 0), later=(("four", 1),))
    enc_att = [gather.take(0)]
    if direct:
        height = block + 8
        gain_rows = sum(
            item[at : at + 8].astype(f32) for item in enc_att[0][0] for at in (block, height + block)
        )
    else:
        gain_full = lax.dynamic_update_slice(
            jnp.zeros((8, D), low), norm_gains.astype(low), (0, dp_index * block)
        )
        gain_rows = total_dp(gain_full).astype(f32)
    gains = [gain_rows[i : i + 1] for i in range(5)]

    place_rel = jnp.concatenate([2 * jnp.arange(half) + side, 2 * jnp.arange(half) + 1 - side])
    prefix_rel = jnp.concatenate(relative(prefix_len))
    suffix_rel = jnp.concatenate(relative(suffix_len))
    images = place_rel < counts[0, 0]
    active = place_rel < counts[0, 0] + counts[0, 1]
    meta = jnp.concatenate(
        [
            dp_index[None].astype(jnp.int32),
            images.astype(jnp.int32),
            prefix_rel,
            suffix_rel,
            mp_index[None].astype(jnp.int32),
        ]
    )
    steps = jnp.arange(SUFFIX)
    live = active[:, None] & (steps[None, :] < suffix_rel[:, None])

    mid = half * SUFFIX
    enc_own, enc_oth = relative(
        jnp.pad(encoder_in.reshape(pairs, ENC_LEN, D), ((0, 0), (0, LONG - ENC_LEN), (0, 0)))
    )
    dec_rel = jnp.concatenate(relative(decoder_in.reshape(pairs, SUFFIX, D))).reshape(2 * mid, D)
    cot = jnp.concatenate(relative(decoder_cotangent.reshape(pairs, SUFFIX, D)))
    cot = jnp.where(live[:, :, None], cot, f32(0.0)).reshape(2 * mid, D)
    cot_low = cot.astype(low)

    def triple(value):
        return value.reshape(half, SUFFIX, D)

    (enc_oth,) = gather.step((enc_oth,), ("far", 1), ("near", 1), ("four", 2), later=(("last", 0),))
    own, oth, kept_enc = encoder_attention(plan, meta, enc_own, enc_oth, gains[0], enc_att, 0, half)
    own, oth, dec_rel, cot, cot_low = gather.step(
        (own, oth, dec_rel, cot, cot_low), ("last", 1), ("near", 2), ("far", 2), ("fours", (3, 4))
    )
    sums = gather.step(reduce_own(own, oth), ("last", 2))
    enc_feed = [gather.take(1), gather.take(2)]
    enc_mid, norm_mid = add_norm(meta, "add_norm_mid", enc_own, *sums, gains[1])
    (norm_mid,) = gather.step((norm_mid,))
    norm_mid_oth = core(norm_mid)

    (norm_mid_oth,) = gather.step(
        (norm_mid_oth,), ("far", 3), ("near", 3), ("four", 5)
    )
    own, oth = encoder_feed(plan, meta, norm_mid, norm_mid_oth, enc_feed, 0, half)
    own, oth = gather.step((own, oth), ("last", 3), ("far", 4), ("near", 4), later=(("four", 5),))
    sums = reduce_own(own, oth)
    (dec_rel,) = gather.step((dec_rel,), ("last", 4), ("far", 5), ("near", 5), later=(("last", 3),))

    self_att = [gather.take(3)]
    own, oth, kept_self = decoder_self(plan, meta, dec_rel, gains[2], self_att)
    sums = gather.step(sums, later=(("far", 5), ("near", 5)))
    sums_self = reduce_own(own, oth, sums)
    cross_att = [gather.take(4)]
    memory = (enc_mid + (sums[0].astype(f32) + sums[1].astype(f32))).astype(low)
    dec_one, norm_cross = add_norm(meta, "add_norm_cross", dec_rel[:mid], *sums_self, gains[3])
    memory, norm_cross = gather.step((memory, norm_cross), ("last", 5))
    memory_oth = core(memory)
    norm_cross_oth = core(norm_cross)

    cross_in = (triple(norm_cross), triple(norm_cross_oth), memory, memory_oth, cross_att)
    own, oth, *kept_cross = decoder_cross(plan, meta, *cross_in)
    sums = reduce_own(own, oth)
    dec_two, norm_last = add_norm(
        meta, "add_norm_last", dec_one, sums[0].reshape(mid, D), sums[1].reshape(mid, D), gains[4]
    )
    dec_feed = [gather.take(5), gather.take(5, 1)]

    own, oth, *grads_dec = decoder_feed(plan, meta, norm_last, core(norm_last), cot_low, dec_feed)
    if direct:
        more_dec = swap(grads_dec[0], "dp", 1)
    sums = reduce_own(own, oth)
    out_own = dec_two + (sums[0][0].astype(f32) + sums[1][0].astype(f32))
    grad, grad_low, gain_four = norm_back(
        meta, "norm_back_last", dec_two, gains[4], cot[:mid], sums[0][1], sums[1][1], True
    )

    own, oth, own_long, oth_long, *grads_cross = decoder_cross_back(
        plan, meta, *cross_in, *kept_cross, triple(grad_low), triple(core(grad_low))
    )
    if direct:
        own, oth, own_long, oth_long, more_dec = hold((own, oth, own_long, oth_long, more_dec))
        more_cross = swap(grads_cross[0], "dp", 1)
    sums = reduce_own(own, oth)
    sums_enc = reduce_own(own_long, oth_long, sums[0])
    if direct:
        keep, more_dec, _ = hold((grads_dec[1], more_dec, sums[0]))
        keep_dec, away_dec = fold(plan, meta, [keep], [more_dec], halves)
        *sums, away_dec = hold((*sums, away_dec))
        more_dec = swap(away_dec, "dp", 2)
    grad, grad_low, gain_three = norm_back(
        meta, "norm_back_cross", dec_one, gains[3], grad, sums[0].reshape(mid, D), sums[1].reshape(mid, D), True
    )
    grad_low_oth = core(grad_low)

    own_self, oth_self, *grads_self = decoder_self_back(
        plan, meta, dec_rel, gains[2], self_att, kept_self, grad_low, grad_low_oth
    )
    decoder_out = absolute(triple(out_own)).reshape(2 * mid, D)
    if direct:
        own_self, oth_self, decoder_out = hold((own_self, oth_self, decoder_out))
    sums_self = reduce_own(own_self, oth_self)
    if direct:
        *sums_enc, _, decoder_out, more_cross, more_dec = hold(
            (*sums_enc, sums_self[0], decoder_out, more_cross, more_dec)
        )
    grad_enc = sums_enc[0].astype(f32) + sums_enc[1].astype(f32)
    enc_low = grad_enc.astype(low)
    enc_low_oth = core(enc_low)

    if direct:
        keep_dec, away_dec = fold(plan, meta, [keep_dec], [more_dec], halves)
        enc_low_oth, away_self, away_dec = hold((enc_low_oth, grads_self[0], away_dec))
        more_self = swap(away_self, "dp", 1)
        more_dec = swap(away_dec, "dp", 4)
    own, oth, *grads_enc = encoder_feed_back(plan, meta, norm_mid, norm_mid_oth, enc_low, enc_low_oth, enc_feed)
    if direct:
        own, oth, more_self, more_dec, *sums_self = hold((own, oth, more_self, more_dec, *sums_self))
        more_up, more_down = [swap(item, "dp", 1) for item in grads_enc[::2]]
    sums = reduce_own(own, oth)
    if direct:
        keep_cross, keep_self, more_cross, more_self, _ = hold(
            (grads_cross[1], grads_self[1], more_cross, more_self, sums[0])
        )
        keep_mid, away_mid = fold(plan, meta, [keep_cross, keep_self], [more_cross, more_self], halves)
        more_mid = swap(away_mid, "dp", 2)
        sums_self, _, more_up = hold((sums_self, away_mid, more_up))
    grad, gain_two = norm_back(meta, "norm_back_self", dec_rel[:mid], gains[2], grad, *sums_self, False)
    decoder_in_grad = absolute(triple(grad)).reshape(2 * mid, D)
    if direct:
        *sums, decoder_in_grad, more_mid = hold((*sums, decoder_in_grad, more_mid))
    grad_enc, enc_low, gain_one = norm_back(
        meta, "norm_back_mid", enc_mid, gains[1], grad_enc, *sums, True
    )
    if direct:
        keep_mid, _ = hold((keep_mid, enc_low))
        keep_mid, away_mid = fold(plan, meta, [keep_mid], [more_mid], halves)
        enc_low, more_down, away_mid = hold((enc_low, more_down, away_mid))
    enc_low_oth = core(enc_low)

    if direct:
        keep_enc, away_enc = fold(plan, meta, grads_enc[1::2], [more_up, more_down], halves)
        enc_low_oth, away_enc, away_mid = hold((enc_low_oth, away_enc, away_mid))
        more_mid = swap(away_mid, "dp", 4)
        more_enc = swap(away_enc, "dp", 2)
    own, oth, *grads_att = encoder_attention_back(
        plan, meta, enc_own, enc_oth, gains[0], enc_att, kept_enc, enc_low, enc_low_oth
    )
    if direct:
        more_att = swap(grads_att[0], "dp", 1)
        own, oth, more_enc, more_mid = hold((own, oth, more_enc, more_mid))
        keep_enc, away_enc = fold(plan, meta, [keep_enc], [more_enc], halves)
        more_enc = swap(away_enc, "dp", 4)
        own, oth, _ = hold((own, oth, away_enc))
    sums = reduce_own(own, oth)
    if direct:
        keep_att, more_att, _ = hold((grads_att[1], more_att, sums[0]))
        mine, *others = fold(plan, meta, [keep_att], [more_att], apart)
        others, more_enc, keep_mid = hold((others, more_enc, keep_mid))
        pieces_att = [mine] + [swap(item, "dp", 2 * (i + 1)) for i, item in enumerate(others)]
        summed, tiles = collect(plan, meta, [[keep_mid, more_mid], [keep_enc, more_enc], [keep_dec, more_dec]], 2)
        *pieces_att, _ = hold((*pieces_att, tiles))
        *sums, _ = hold((*sums, pieces_att[1]))
        sum_att, tile_att = collect(plan, meta, [pieces_att], 1)
    else:
        parts = [grads_cross[0], grads_self[0], *grads_enc, grads_dec[0]]
        whole_sum = lax.psum_scatter(jnp.concatenate(parts), "dp", scatter_dimension=1, tiled=True)
        summed, tiles = collect(plan, meta, [[whole_sum[None]]], 2)
        whole_sum = lax.psum_scatter(grads_att[0], "dp", scatter_dimension=1, tiled=True)
        sum_att, tile_att = collect(plan, meta, [[whole_sum[None]]], 1)
    grad_enc, gain_zero = norm_back(meta, "norm_back_enc", enc_own, gains[0], grad_enc, *sums, False)
    encoder_in_grad = absolute(grad_enc)[:, :ENC_LEN].reshape(pairs * ENC_LEN, D)
    gain_tile = jnp.concatenate(
        [gain_zero, gain_one, gain_two, gain_three, gain_four, jnp.zeros((3, D), f32)]
    )[None]
    tiles = total_all(jnp.concatenate([tiles, tile_att, gain_tile]))
    done = finish(
        plan,
        meta,
        tiles,
        (
            project_in_rows,
            project_in_cols,
            project_out_rows,
            project_out_cols,
            expand_rows,
            expand_cols,
            contract_rows,
            contract_cols,
        ),
        (norm_gains, norm_gains_square, norm_gains_moment, norm_gains_average),
    )
    grad_norm, news, rates, pgain = done[0][0, 0], done[1:9], done[9], done[10:]
    att = update_attention(
        plan,
        meta,
        rates,
        (sum_att, summed),
        *news[:4],
        (project_in, project_in_moment, project_in_average),
        (project_out, project_out_moment, project_out_average),
    )
    feed = update_feed(
        plan,
        meta,
        rates,
        (summed, summed),
        *news[4:],
        (expand, expand_moment, expand_average),
        (contract, contract_moment, contract_average),
    )
    return (
        decoder_out,
        encoder_in_grad,
        decoder_in_grad,
        grad_norm,
        att[0],
        news[0],
        news[1],
        *att[1:5],
        att[5],
        news[2],
        news[3],
        *att[6:10],
        feed[0],
        news[4],
        news[5],
        *feed[1:5],
        feed[5],
        news[6],
        news[7],
        *feed[6:10],
        *pgain,
    )


def solution(mesh):
    placed = (
        P("dp", None),
        P("dp", None),
        P("dp", None),
        P("dp", None),
        P("dp"),
        P("dp"),
        P(None, None, "dp", "mp"),
        P(),
        P(),
        P(None, None, "dp", "mp"),
        P(None, None, "dp", "mp"),
        P(None, "mp", "dp"),
        P(),
        P(),
        P(None, "mp", "dp"),
        P(None, "mp", "dp"),
        P(None, "dp", "mp"),
        P(),
        P(),
        P(None, "dp", "mp"),
        P(None, "dp", "mp"),
        P(None, "mp", "dp"),
        P(),
        P(),
        P(None, "mp", "dp"),
        P(None, "mp", "dp"),
        P(None, "dp"),
        P(None, "dp"),
        P(None, "dp"),
        P(None, "dp"),
    )
    return jax.shard_map(
        functools.partial(on_device, (mesh.shape["dp"], mesh.shape["mp"])),
        mesh=mesh,
        in_specs=placed,
        out_specs=(
            P("dp", None),
            P("dp", None),
            P("dp", None),
            P(),
            P(None, None, "dp", "mp"),
            P(),
            P(),
            P(None, None, "dp", "mp"),
            P(None, None, "dp", "mp"),
            P(None, None, "dp", "mp"),
            P(None, None, "dp", "mp"),
            P(None, "mp", "dp"),
            P(),
            P(),
            P(None, "mp", "dp"),
            P(None, "mp", "dp"),
            P(None, "mp", "dp"),
            P(None, "mp", "dp"),
            P(None, "dp", "mp"),
            P(),
            P(),
            P(None, "dp", "mp"),
            P(None, "dp", "mp"),
            P(None, "dp", "mp"),
            P(None, "dp", "mp"),
            P(None, "mp", "dp"),
            P(),
            P(),
            P(None, "mp", "dp"),
            P(None, "mp", "dp"),
            P(None, "mp", "dp"),
            P(None, "mp", "dp"),
            P(None, "dp"),
            P(None, "dp"),
            P(None, "dp"),
            P(None, "dp"),
            P(None, "dp"),
            P(None, "dp"),
        ),
        check_vma=False,
    )
```

```python
import functools

import jax
import jax.numpy as jnp
from jax import lax
from jax.experimental import pallas as pl
from jax.experimental.pallas import tpu as pltpu
from jax.sharding import PartitionSpec as P

D = 768
HEAD_DIM = 64
FF = 3072
PATCHES = 196
SUFFIX = 32
ENC_LEN = 228


EPS_NORM = 1e-06
EPS_STAT = 1e-30
DECAY = 0.99
MOMENTUM = 0.9
AVERAGE = 0.6
RATE_MATRIX = 0.004
RATE_GAIN = 0.05
MASKED = -1000000000.0


LOW = jnp.bfloat16
F32 = jnp.float32
VMEM_LIMIT = 56 * 1024 * 1024
LONG = (ENC_LEN + 7) // 8 * 8
EXACT = lax.Precision.HIGHEST


def dot(left, right, contract):
    return lax.dot_general(left, right, (contract, ((), ())), preferred_element_type=F32)


def mm(left, right):
    return dot(left, right, ((1,), (0,)))


def mm_t(left, right):
    return dot(left, right, ((1,), (1,)))


def t_mm(left, right):
    return dot(left, right, ((0,), (0,)))


def rms_scale(value):
    return lax.rsqrt(jnp.mean(value * value, -1, keepdims=True) + EPS_NORM)


def softmax(scores):
    expons = jnp.exp(scores - jnp.max(scores, -1, keepdims=True))
    return expons / jnp.sum(expons, -1, keepdims=True)


def gelu_parts(upper):
    inner = 0.7978845608028654 * (upper + 0.044715 * upper * upper * upper)
    bent = jnp.tanh(inner)
    value = 0.5 * upper * (1.0 + bent)
    slope = 0.5 * (1.0 + bent) + 0.5 * upper * (1.0 - bent * bent) * 0.7978845608028654 * (
        1.0 + 3.0 * 0.044715 * upper * upper
    )
    return value, slope


class Plan:
    def __init__(self, dp_n, block, width, hidden, pairs):
        self.dp_n, self.block, self.width, self.hidden, self.pairs = dp_n, block, width, hidden, pairs
        self.half = pairs // 2
        self.heads = width // HEAD_DIM
        self.direct = dp_n == 8

    def weight_specs(self, pieces):
        return [whole(item.shape) for item in flat(pieces)]

    def weight_scratch(self, pieces):
        return [pltpu.VMEM((len(pieces), D, D), LOW)]

    def assemble(self, meta, pieces, refs, scratch):
        refs = iter(refs)
        for count in range(len(pieces)):
            if not self.direct:
                scratch[count] = next(refs)[...]
                continue
            _, height, start = pieces[count]
            for places in ((0, 4), (2, 6), (1, 5), (3, 7)):
                ref = next(refs)
                for index, place in enumerate(places):
                    row = pl.multiple_of(jnp.bitwise_xor(meta[0], place) * self.block, 32)
                    first = start + index * height
                    scratch[count, pl.ds(row, self.block), :] = ref[first : first + self.block]

    def grad_shapes(self, count):
        if not self.direct:
            return [jax.ShapeDtypeStruct((count, D, D), F32)]
        shape = (self.dp_n // 2, count, self.block, D)
        return [jax.ShapeDtypeStruct(shape, LOW), jax.ShapeDtypeStruct(shape, F32)]

    def emit(self, meta, acc, refs):
        if not self.direct:
            refs[0][...] = acc[...]
            return
        for index in range(self.dp_n // 2):
            here = pl.multiple_of(jnp.bitwise_xor(meta[0], 2 * index) * self.block, 32)
            away = pl.multiple_of(jnp.bitwise_xor(meta[0], 2 * index + 1) * self.block, 32)
            for count in range(acc.shape[0]):
                refs[0][index, count] = acc[count, pl.ds(away, self.block), :].astype(LOW)
                refs[1][index, count] = acc[count, pl.ds(here, self.block), :]


def flat(pieces):
    return [item for arrays, _, _ in pieces for item in arrays]


def whole(shape):
    return pl.BlockSpec(shape, lambda *_: (0,) * len(shape))


def own_spec(count, base, shape):
    return pl.BlockSpec(
        (1,) + shape, lambda p, _: (base + jnp.maximum(p - count, 0),) + (0,) * len(shape)
    )


def oth_spec(count, base, shape):
    return pl.BlockSpec(
        (1,) + shape, lambda p, _: (base + jnp.minimum(p, count - 1),) + (0,) * len(shape)
    )


def step_spec(shape):
    return pl.BlockSpec((1,) + shape, lambda p, _: (p,) + (0,) * len(shape))


def call(name, body, grid, meta, inputs, in_specs, outs, out_specs, scratch):
    return pl.pallas_call(
        body,
        name=name,
        out_shape=outs,
        grid_spec=pltpu.PrefetchScalarGridSpec(
            num_scalar_prefetch=1,
            grid=grid,
            in_specs=in_specs,
            out_specs=out_specs,
            scratch_shapes=scratch,
        ),
        cost_estimate=pl.CostEstimate(flops=1, transcendentals=0, bytes_accessed=1),
        compiler_params=pltpu.CompilerParams(
            dimension_semantics=("arbitrary",) * len(grid), vmem_limit_bytes=VMEM_LIMIT
        ),
    )(meta, *inputs)


def key_mask(meta, pairs, slot, turned=False):
    shape = (ENC_LEN, 1) if turned else (1, ENC_LEN)
    place = lax.broadcasted_iota(jnp.int32, shape, 1 - turned)
    image, prefix = meta[1 + slot], meta[1 + pairs + slot]
    return (place < image * PATCHES) | ((place >= PATCHES) & (place < PATCHES + prefix))


def attend_heads(plan, queries, keys, values, allowed):
    mixed = []
    for head in range(plan.heads):
        cut = slice(head * HEAD_DIM, (head + 1) * HEAD_DIM)
        scores = jnp.where(allowed, mm_t(queries[:, cut], keys[:, cut]) * 0.125, MASKED)
        mixed.append(mm(softmax(scores).astype(LOW), values[:, cut]).astype(LOW))
    return jnp.concatenate(mixed, 1)


def attend_heads_back(plan, queries, keys, values, allowed, grad_mixed):
    grads = ([], [], [])
    for head in range(plan.heads):
        cut = slice(head * HEAD_DIM, (head + 1) * HEAD_DIM)
        query, key, value, grad = queries[:, cut], keys[:, cut], values[:, cut], grad_mixed[:, cut]
        probs = softmax(jnp.where(allowed, mm_t(query, key) * 0.125, MASKED))
        grad_probs = mm_t(grad, value)
        inner = jnp.sum(grad_probs * probs, -1, keepdims=True)
        grad_scores = (probs * (grad_probs - inner)).astype(LOW)
        grads[0].append((mm(grad_scores, key) * 0.125).astype(LOW))
        grads[1].append((t_mm(grad_scores, query) * 0.125).astype(LOW))
        grads[2].append(t_mm(probs.astype(LOW), grad).astype(LOW))
    return tuple(jnp.concatenate(item, 1) for item in grads)


def attend_heads_turned(plan, queries, keys, values, allowed, grad_mixed):
    grads = ([], [], [])
    for head in range(plan.heads):
        cut = slice(head * HEAD_DIM, (head + 1) * HEAD_DIM)
        query, key, value, grad = queries[:, cut], keys[:, cut], values[:, cut], grad_mixed[:, cut]
        scores = jnp.where(allowed, mm_t(key, query) * 0.125, MASKED)
        expons = jnp.exp(scores - jnp.max(scores, 0, keepdims=True))
        probs = expons / jnp.sum(expons, 0, keepdims=True)
        grad_probs = mm_t(value, grad)
        inner = jnp.sum(grad_probs * probs, 0, keepdims=True)
        grad_scores = (probs * (grad_probs - inner)).astype(LOW)
        grads[0].append((t_mm(grad_scores, key) * 0.125).astype(LOW))
        grads[1].append((mm(grad_scores, query) * 0.125).astype(LOW))
        grads[2].append(mm(probs.astype(LOW), grad).astype(LOW))
    return tuple(jnp.concatenate(item, 1) for item in grads)


def slot_of(plan, count, base, step):
    return jnp.where(step < count, plan.half + base + step, base + step - count)


def pick(step, count, own, oth, rows):
    return jnp.where(step < count, oth[0, :rows], own[0, :rows])


def put(step, count, own, oth, value):
    @pl.when(step < count)
    def _():
        oth[0, : value.shape[0]] = value

    @pl.when(step >= count)
    def _():
        own[0, : value.shape[0]] = value


def encoder_attention(plan, meta, own, oth, gain, pieces, base, count):
    w3 = 3 * plan.width
    n = len(flat(pieces))

    def body(meta, own_ref, oth_ref, gain_ref, *rest):
        refs, (own_out, oth_out, kept, weight) = rest[:n], rest[n:]
        step = pl.program_id(0)

        @pl.when(step == 0)
        def _():
            plan.assemble(meta, pieces, refs, weight)

        value = pick(step, count, own_ref, oth_ref, ENC_LEN).astype(F32)
        normed = (value * rms_scale(value) * gain_ref[...]).astype(LOW)
        joined = mm(normed, weight[0, :, :w3]).astype(LOW)
        allowed = key_mask(meta, plan.pairs, slot_of(plan, count, base, step))
        width = plan.width
        mixed = attend_heads(
            plan, joined[:, :width], joined[:, width : 2 * width], joined[:, 2 * width :], allowed
        )
        kept[0, :, :w3] = joined
        kept[0, :, w3:] = mixed
        put(step, count, own_out, oth_out, mm_t(mixed, weight[0, :, w3:]).astype(LOW))

    rows = (LONG, D)
    return call(
        "encoder_attention",
        body,
        (2 * count,),
        meta,
        (own, oth, gain, *flat(pieces)),
        [own_spec(count, base, rows), oth_spec(count, base, rows), whole((1, D)), *plan.weight_specs(pieces)],
        [jax.ShapeDtypeStruct((count,) + rows, LOW)] * 2
        + [jax.ShapeDtypeStruct((2 * count, ENC_LEN, w3 + plan.width), LOW)],
        [own_spec(count, 0, rows), oth_spec(count, 0, rows), step_spec((ENC_LEN, w3 + plan.width))],
        plan.weight_scratch(pieces),
    )


def encoder_attention_back(plan, meta, own, oth, gain, pieces, kept, grad_own, grad_oth):
    count = plan.half
    width, w3 = plan.width, 3 * plan.width
    n = len(flat(pieces))

    def body(meta, own_ref, oth_ref, gain_ref, kept_ref, grad_own_ref, grad_oth_ref, *rest):
        refs, (own_out, oth_out), grad_refs = rest[:n], rest[n : n + 2], rest[n + 2 : -2]
        weight, acc = rest[-2:]
        step = pl.program_id(0)

        @pl.when(step == 0)
        def _():
            plan.assemble(meta, pieces, refs, weight)
            acc[...] = jnp.zeros_like(acc)

        value = pick(step, count, own_ref, oth_ref, ENC_LEN).astype(F32)
        normed = (value * rms_scale(value) * gain_ref[...]).astype(LOW)
        grad = pick(step, count, grad_own_ref, grad_oth_ref, ENC_LEN)
        allowed = key_mask(meta, plan.pairs, slot_of(plan, count, 0, step), True)
        grad_mixed = mm(grad, weight[0, :, w3:]).astype(LOW)
        acc[0, :, w3:] += t_mm(grad, kept_ref[0, :, w3:])
        joined = kept_ref[0, :, :w3]
        grads = attend_heads_turned(
            plan, joined[:, :width], joined[:, width : 2 * width], joined[:, 2 * width :], allowed, grad_mixed
        )
        together = jnp.concatenate(grads, 1)
        acc[0, :, :w3] += t_mm(normed, together)
        put(step, count, own_out, oth_out, mm_t(together, weight[0, :, :w3]).astype(LOW))

        @pl.when(step == 2 * count - 1)
        def _():
            plan.emit(meta, acc, grad_refs)

    rows = (LONG, D)
    shapes = plan.grad_shapes(1)
    pair_specs = [own_spec(count, 0, rows), oth_spec(count, 0, rows)]
    return call(
        "encoder_attention_back",
        body,
        (2 * count,),
        meta,
        (own, oth, gain, kept, grad_own, grad_oth, *flat(pieces)),
        [*pair_specs, whole((1, D)), step_spec(kept.shape[1:]), *pair_specs, *plan.weight_specs(pieces)],
        [jax.ShapeDtypeStruct((count,) + rows, LOW)] * 2 + shapes,
        [*pair_specs, *[whole(item.shape) for item in shapes]],
        plan.weight_scratch(pieces) + [pltpu.VMEM((1, D, D), F32)],
    )


def encoder_feed(plan, meta, own, oth, pieces, base, count):
    n = len(flat(pieces))

    def body(meta, own_ref, oth_ref, *rest):
        refs, (own_out, oth_out, weight) = rest[:n], rest[n:]
        step = pl.program_id(0)

        @pl.when(step == 0)
        def _():
            plan.assemble(meta, pieces, refs, weight)

        normed = pick(step, count, own_ref, oth_ref, ENC_LEN)
        active = gelu_parts(mm(normed, weight[0]))[0].astype(LOW)
        put(step, count, own_out, oth_out, mm_t(active, weight[1]).astype(LOW))

    rows = (LONG, D)
    return call(
        "encoder_feed",
        body,
        (2 * count,),
        meta,
        (own, oth, *flat(pieces)),
        [own_spec(count, base, rows), oth_spec(count, base, rows), *plan.weight_specs(pieces)],
        [jax.ShapeDtypeStruct((count,) + rows, LOW)] * 2,
        [own_spec(count, 0, rows), oth_spec(count, 0, rows)],
        plan.weight_scratch(pieces),
    )


def encoder_feed_back(plan, meta, own, oth, grad_own, grad_oth, pieces):
    n = len(flat(pieces))
    count = plan.half

    def body(meta, own_ref, oth_ref, grad_own_ref, grad_oth_ref, *rest):
        refs, (own_out, oth_out), grad_refs = rest[:n], rest[n : n + 2], rest[n + 2 : -2]
        weight, acc = rest[-2:]
        step = pl.program_id(0)

        @pl.when(step == 0)
        def _():
            plan.assemble(meta, pieces, refs, weight)
            acc[...] = jnp.zeros_like(acc)

        normed = pick(step, count, own_ref, oth_ref, ENC_LEN)
        grad = pick(step, count, grad_own_ref, grad_oth_ref, ENC_LEN)
        active, slope = gelu_parts(mm(normed, weight[0]))
        grad_upper = (slope * mm(grad, weight[1])).astype(LOW)
        put(step, count, own_out, oth_out, mm_t(grad_upper, weight[0]).astype(LOW))
        acc[0] += t_mm(normed, grad_upper)
        acc[1] += t_mm(grad, active.astype(LOW))

        @pl.when(step == 2 * count - 1)
        def _():
            for index in range(2):
                size = len(grad_refs) // 2
                plan.emit(meta, acc.at[pl.ds(index, 1)], grad_refs[index * size : (index + 1) * size])

    rows = (LONG, D)
    shapes = plan.grad_shapes(1) * 2
    pair_specs = [own_spec(count, 0, rows), oth_spec(count, 0, rows)]
    return call(
        "encoder_feed_back",
        body,
        (2 * count,),
        meta,
        (own, oth, grad_own, grad_oth, *flat(pieces)),
        [*pair_specs, *pair_specs, *plan.weight_specs(pieces)],
        [jax.ShapeDtypeStruct((count,) + rows, LOW)] * 2 + shapes,
        [*pair_specs, *[whole(item.shape) for item in shapes]],
        plan.weight_scratch(pieces) + [pltpu.VMEM((2, D, D), F32)],
    )


def self_mask(plan, meta, turned=False):
    rows = plan.pairs * SUFFIX
    query = lax.broadcasted_iota(jnp.int32, (rows, rows), int(turned))
    key = lax.broadcasted_iota(jnp.int32, (rows, rows), 1 - turned)
    pair = key // SUFFIX
    limit = jnp.zeros_like(key)
    for slot in range(plan.pairs):
        limit = jnp.where(pair == slot, meta[1 + 2 * plan.pairs + slot], limit)
    return (query // SUFFIX == pair) & (key <= query) & (key - pair * SUFFIX < limit)


def decoder_self(plan, meta, rows_in, gain, pieces):
    n = len(flat(pieces))
    width, w3 = plan.width, 3 * plan.width
    rows = plan.pairs * SUFFIX
    mid = rows // 2

    def body(meta, in_ref, gain_ref, *rest):
        refs, (own_out, oth_out, kept, weight) = rest[:n], rest[n:]
        plan.assemble(meta, pieces, refs, weight)
        value = in_ref[...].astype(F32)
        normed = (value * rms_scale(value) * gain_ref[...]).astype(LOW)
        joined = mm(normed, weight[0, :, :w3]).astype(LOW)
        mixed = attend_heads(
            plan, joined[:, :width], joined[:, width : 2 * width], joined[:, 2 * width :], self_mask(plan, meta)
        )
        kept[:, :w3] = joined
        kept[:, w3:] = mixed
        partial = mm_t(mixed, weight[0, :, w3:]).astype(LOW)
        own_out[...] = partial[:mid]
        oth_out[...] = partial[mid:]

    return call(
        "decoder_self",
        body,
        (1,),
        meta,
        (rows_in, gain, *flat(pieces)),
        [whole((rows, D)), whole((1, D)), *plan.weight_specs(pieces)],
        [jax.ShapeDtypeStruct((mid, D), LOW)] * 2 + [jax.ShapeDtypeStruct((rows, 4 * width), LOW)],
        [whole((mid, D))] * 2 + [whole((rows, 4 * width))],
        plan.weight_scratch(pieces),
    )


def decoder_self_back(plan, meta, rows_in, gain, pieces, kept, grad_own, grad_oth):
    n = len(flat(pieces))
    width, w3 = plan.width, 3 * plan.width
    rows = plan.pairs * SUFFIX
    mid = rows // 2

    def body(meta, in_ref, gain_ref, kept_ref, grad_own_ref, grad_oth_ref, *rest):
        refs, (own_out, oth_out), grad_refs = rest[:n], rest[n : n + 2], rest[n + 2 : -2]
        weight, acc = rest[-2:]
        plan.assemble(meta, pieces, refs, weight)
        value = in_ref[...].astype(F32)
        normed = (value * rms_scale(value) * gain_ref[...]).astype(LOW)
        grad = jnp.concatenate([grad_own_ref[...], grad_oth_ref[...]], 0)
        grad_mixed = mm(grad, weight[0, :, w3:]).astype(LOW)
        acc[0, :, w3:] = t_mm(grad, kept_ref[:, w3:])
        joined = kept_ref[:, :w3]
        grads = attend_heads_turned(
            plan,
            joined[:, :width],
            joined[:, width : 2 * width],
            joined[:, 2 * width :],
            self_mask(plan, meta, True),
            grad_mixed,
        )
        together = jnp.concatenate(grads, 1)
        acc[0, :, :w3] = t_mm(normed, together)
        partial = mm_t(together, weight[0, :, :w3]).astype(LOW)
        own_out[...] = partial[:mid]
        oth_out[...] = partial[mid:]
        plan.emit(meta, acc, grad_refs)

    shapes = plan.grad_shapes(1)
    return call(
        "decoder_self_back",
        body,
        (1,),
        meta,
        (rows_in, gain, kept, grad_own, grad_oth, *flat(pieces)),
        [whole((rows, D)), whole((1, D)), whole(kept.shape), whole((mid, D)), whole((mid, D)), *plan.weight_specs(pieces)],
        [jax.ShapeDtypeStruct((mid, D), LOW)] * 2 + shapes,
        [whole((mid, D))] * 2 + [whole(item.shape) for item in shapes],
        plan.weight_scratch(pieces) + [pltpu.VMEM((1, D, D), F32)],
    )


def decoder_cross(plan, meta, own, oth, memory_own, memory_oth, pieces):
    n = len(flat(pieces))
    count = plan.half
    width, w3 = plan.width, 3 * plan.width

    def body(meta, own_ref, oth_ref, memory_own_ref, memory_oth_ref, *rest):
        refs, (own_out, oth_out, kept_query, kept_key, weight) = rest[:n], rest[n:]
        step = pl.program_id(0)

        @pl.when(step == 0)
        def _():
            plan.assemble(meta, pieces, refs, weight)

        normed = pick(step, count, own_ref, oth_ref, SUFFIX)
        memory = pick(step, count, memory_own_ref, memory_oth_ref, ENC_LEN)
        queries = mm(normed, weight[0, :, :width]).astype(LOW)
        both = mm(memory, weight[0, :, width:w3]).astype(LOW)
        allowed = key_mask(meta, plan.pairs, slot_of(plan, count, 0, step))
        mixed = attend_heads(plan, queries, both[:, :width], both[:, width:], allowed)
        kept_query[0, :, :width] = queries
        kept_query[0, :, width:] = mixed
        kept_key[0] = both
        put(step, count, own_out, oth_out, mm_t(mixed, weight[0, :, w3:]).astype(LOW))

    rows, long = (SUFFIX, D), (LONG, D)
    return call(
        "decoder_cross",
        body,
        (2 * count,),
        meta,
        (own, oth, memory_own, memory_oth, *flat(pieces)),
        [
            own_spec(count, 0, rows),
            oth_spec(count, 0, rows),
            own_spec(count, 0, long),
            oth_spec(count, 0, long),
            *plan.weight_specs(pieces),
        ],
        [jax.ShapeDtypeStruct((count,) + rows, LOW)] * 2
        + [
            jax.ShapeDtypeStruct((2 * count, SUFFIX, 2 * width), LOW),
            jax.ShapeDtypeStruct((2 * count, ENC_LEN, 2 * width), LOW),
        ],
        [
            own_spec(count, 0, rows),
            oth_spec(count, 0, rows),
            step_spec((SUFFIX, 2 * width)),
            step_spec((ENC_LEN, 2 * width)),
        ],
        plan.weight_scratch(pieces),
    )


def pair_spec(shape):
    return pl.BlockSpec((1,) + shape, lambda p, _: (p,) + (0,) * len(shape))


def sides_spec(shape):
    return pl.BlockSpec((2, 1) + shape, lambda p, _: (0, p) + (0,) * len(shape))


def decoder_cross_back(
    plan, meta, own, oth, memory_own, memory_oth, pieces, kept_query, kept_key, grad_own, grad_oth
):
    n = len(flat(pieces))
    count = plan.half
    width, w3 = plan.width, 3 * plan.width
    rows = plan.pairs * SUFFIX
    mid = rows // 2

    def body(
        meta, own_ref, oth_ref, memory_own_ref, memory_oth_ref, query_ref, key_ref, grad_own_ref, grad_oth_ref, *rest
    ):
        refs, outs, grad_refs = rest[:n], rest[n : n + 4], rest[n + 4 : -4]
        weight, acc, grad_mixed, grad_query = rest[-4:]
        step = pl.program_id(0)

        @pl.when(step == 0)
        def _():
            plan.assemble(meta, pieces, refs, weight)
            grad = jnp.concatenate([grad_oth_ref[...], grad_own_ref[...]], 0).reshape(rows, D)
            grad_mixed[...] = mm(grad, weight[0, :, w3:]).astype(LOW)
            acc[0, :, w3:] = t_mm(grad, query_ref[:, :, :, width:].reshape(rows, width))
            acc[0, :, width:w3] = jnp.zeros((D, w3 - width), F32)

        total = None
        for side, (memory_ref, out) in enumerate(((memory_oth_ref, outs[3]), (memory_own_ref, outs[2]))):
            allowed = key_mask(meta, plan.pairs, (1 - side) * plan.half + step)
            both = key_ref[side, 0]
            here = pl.ds(pl.multiple_of((side * count + step) * SUFFIX, SUFFIX), SUFFIX)
            query, grad_key, grad_value = attend_heads_back(
                plan, query_ref[side, step, :, :width], both[:, :width], both[:, width:], allowed, grad_mixed[here, :]
            )
            grad_query[here, :] = query
            together = jnp.concatenate([grad_key, grad_value], 1)
            product = t_mm(memory_ref[0, :ENC_LEN], together)
            total = product if total is None else total + product
            out[0, :ENC_LEN] = mm_t(together, weight[0, :, width:w3]).astype(LOW)
        acc[0, :, width:w3] += total

        @pl.when(step == count - 1)
        def _():
            normed = jnp.concatenate([oth_ref[...], own_ref[...]], 0).reshape(rows, D)
            queries = grad_query[...]
            acc[0, :, :width] = t_mm(normed, queries)
            back = mm_t(queries, weight[0, :, :width]).astype(LOW)
            outs[1][...] = back[:mid].reshape(count, SUFFIX, D)
            outs[0][...] = back[mid:].reshape(count, SUFFIX, D)
            plan.emit(meta, acc, grad_refs)

    part, long = (count, SUFFIX, D), (LONG, D)
    shapes = plan.grad_shapes(1)
    return call(
        "decoder_cross_back",
        body,
        (count,),
        meta,
        (own, oth, memory_own, memory_oth, kept_query, kept_key, grad_own, grad_oth, *flat(pieces)),
        [
            whole(part),
            whole(part),
            pair_spec(long),
            pair_spec(long),
            whole(kept_query.shape),
            sides_spec(kept_key.shape[2:]),
            whole(part),
            whole(part),
            *plan.weight_specs(pieces),
        ],
        [jax.ShapeDtypeStruct(part, LOW)] * 2
        + [jax.ShapeDtypeStruct((count,) + long, LOW)] * 2
        + shapes,
        [whole(part), whole(part), pair_spec(long), pair_spec(long), *[whole(item.shape) for item in shapes]],
        plan.weight_scratch(pieces)
        + [pltpu.VMEM((1, D, D), F32), pltpu.VMEM((rows, width), LOW), pltpu.VMEM((rows, width), LOW)],
    )


def decoder_feed(plan, meta, own, oth, grad_in, pieces):
    n = len(flat(pieces))
    rows = plan.pairs * SUFFIX
    mid = rows // 2

    def body(meta, own_ref, oth_ref, grad_ref, *rest):
        refs, (own_out, oth_out), grad_refs = rest[:n], rest[n : n + 2], rest[n + 2 : -2]
        weight, acc = rest[-2:]
        plan.assemble(meta, pieces, refs, weight)
        normed = jnp.concatenate([own_ref[...], oth_ref[...]], 0)
        grad = grad_ref[...]
        active, slope = gelu_parts(mm(normed, weight[0]))
        active = active.astype(LOW)
        partial = mm_t(active, weight[1]).astype(LOW)
        grad_upper = (slope * mm(grad, weight[1])).astype(LOW)
        back = mm_t(grad_upper, weight[0]).astype(LOW)
        own_out[0] = partial[:mid]
        own_out[1] = back[:mid]
        oth_out[0] = partial[mid:]
        oth_out[1] = back[mid:]
        acc[0] = t_mm(normed, grad_upper)
        acc[1] = t_mm(grad, active)
        plan.emit(meta, acc, grad_refs)

    shapes = plan.grad_shapes(2)
    return call(
        "decoder_feed",
        body,
        (1,),
        meta,
        (own, oth, grad_in, *flat(pieces)),
        [whole((mid, D))] * 2 + [whole((rows, D)), *plan.weight_specs(pieces)],
        [jax.ShapeDtypeStruct((2, mid, D), LOW)] * 2 + shapes,
        [whole((2, mid, D))] * 2 + [whole(item.shape) for item in shapes],
        plan.weight_scratch(pieces) + [pltpu.VMEM((2, D, D), F32)],
    )


def add_norm(meta, name, base, first, second, gain):
    def body(meta, base_ref, first_ref, second_ref, gain_ref, sum_ref, norm_ref):
        value = base_ref[...].astype(F32) + (first_ref[...].astype(F32) + second_ref[...].astype(F32))
        sum_ref[...] = value
        norm_ref[...] = (value * rms_scale(value) * gain_ref[...]).astype(LOW)

    shape = base.shape
    part = (1,) + shape[1:] if len(shape) == 3 else shape
    spec = (
        pl.BlockSpec(part, lambda p, _: (p, 0, 0)) if len(shape) == 3 else whole(shape)
    )
    return call(
        name,
        body,
        (shape[0] if len(shape) == 3 else 1,),
        meta,
        (base, first, second, gain),
        [spec, spec, spec, whole((1, D))],
        [jax.ShapeDtypeStruct(shape, F32), jax.ShapeDtypeStruct(shape, LOW)],
        [spec, spec],
        [],
    )


def norm_back(meta, name, inputs, gain, grad, first, second, want_low):
    def body(meta, in_ref, gain_ref, grad_ref, first_ref, second_ref, *outs):
        value = in_ref[...].astype(F32)
        scale = rms_scale(value)
        unit = value * scale
        back = first_ref[...].astype(F32) + second_ref[...].astype(F32)
        product = back * unit
        real = product[0, :ENC_LEN] if value.ndim == 3 else product
        part = jnp.sum(real, 0, keepdims=True)
        weighted = product * gain_ref[...]
        total = grad_ref[...].astype(F32) + scale * (
            back * gain_ref[...] - unit * jnp.mean(weighted, -1, keepdims=True)
        )
        outs[0][...] = total
        if want_low:
            outs[1][...] = total.astype(LOW)
        step = pl.program_id(0)

        @pl.when(step == 0)
        def _():
            outs[-1][...] = part

        @pl.when(step > 0)
        def _():
            outs[-1][...] += part

    shape = inputs.shape
    part = (1,) + shape[1:] if len(shape) == 3 else shape
    spec = pl.BlockSpec(part, lambda p, _: (p, 0, 0)) if len(shape) == 3 else whole(shape)
    return call(
        name,
        body,
        (shape[0] if len(shape) == 3 else 1,),
        meta,
        (inputs, gain, grad, first, second),
        [spec, whole((1, D)), spec, spec, spec],
        [jax.ShapeDtypeStruct(shape, F32)]
        + [jax.ShapeDtypeStruct(shape, LOW)] * want_low
        + [jax.ShapeDtypeStruct((1, D), F32)],
        [spec] * (1 + want_low) + [whole((1, D))],
        [],
    )


def fold(plan, meta, keeps, mores, split):
    n = len(keeps)
    counts = [item.shape[1] for item in keeps]
    total = sum(counts)
    tail = keeps[0].shape[2:]
    blocks = keeps[0].shape[0]

    def body(meta, *rest):
        keep_refs, more_refs, outs = rest[:n], rest[n : 2 * n], rest[2 * n :]
        for index in range(blocks):
            start = 0
            out, at = split(index)
            for keep_ref, more_ref, count in zip(keep_refs, more_refs, counts):
                value = keep_ref[index] + more_ref[index].astype(F32)
                outs[out][at, start : start + count] = value.astype(outs[out].dtype)
                start += count

    places = [split(index) for index in range(blocks)]
    outs = [
        jax.ShapeDtypeStruct((sum(place[0] == out for place in places), total) + tail, LOW if out else F32)
        for out in range(1 + max(place[0] for place in places))
    ]
    return call(
        "fold",
        body,
        (1,),
        meta,
        (*keeps, *mores),
        [whole(item.shape) for item in (*keeps, *mores)],
        outs,
        [whole(item.shape) for item in outs],
        [],
    )


def halves(index):
    return index % 2, index // 2


def apart(index):
    return index, 0


def pack_first(plan, meta, project_in, project_out, gains):
    width, block = plan.width, plan.block

    def body(meta, in_ref, out_ref, gain_ref, packed):
        parts = [in_ref[0, index] for index in range(3)] + [jnp.transpose(out_ref[0])]
        packed[:block] = jnp.concatenate(parts, 1).astype(LOW)
        rows = jnp.concatenate([gain_ref[...], jnp.zeros((3, block), F32)], 0)
        wide = jnp.concatenate([rows, jnp.zeros((8, D - block), F32)], 1)
        packed[block:] = pltpu.roll(wide, meta[0] * block, 1).astype(LOW)

    shape = (block + 8, D)
    return call(
        "pack_first",
        body,
        (1,),
        meta,
        (project_in, project_out, gains),
        [
            pl.BlockSpec((1,) + project_in.shape[1:], lambda *_: (0, 0, 0, 0)),
            pl.BlockSpec((1,) + project_out.shape[1:], lambda *_: (0, 0, 0)),
            whole(gains.shape),
        ],
        [jax.ShapeDtypeStruct(shape, LOW)],
        [whole(shape)],
        [],
    )[0]


def one_hot(rows, offset):
    row = lax.broadcasted_iota(jnp.int32, (rows, D), 0)
    lane = lax.broadcasted_iota(jnp.int32, (rows, D), 1)
    return (lane == row + offset).astype(F32)


def collect(plan, meta, sets, attention):
    counts = [pieces[0].shape[-3] for pieces in sets]
    count = sum(counts)
    shape = (count,) + sets[0][0].shape[-2:]
    arrays = [item for pieces in sets for item in pieces]
    n = len(arrays)
    groups = D // plan.width

    def body(meta, *rest):
        refs, (out, tile_out) = rest[:n], rest[n:]
        dp_at, mp_at = meta[0], meta[1 + 3 * plan.pairs]
        group = lax.broadcasted_iota(jnp.int32, (8, D), 1) // plan.width
        row = lax.broadcasted_iota(jnp.int32, (8, D), 0)
        place = one_hot(plan.block, dp_at * plan.block)
        def one(first, refs, at, _):
            index = first + at
            heads = (jnp.zeros((8, D), jnp.int32) + index) < attention
            value = refs[0][0, at]
            for ref in refs[1:]:
                value = value + ref[0, at].astype(F32)
            out[index] = value
            square = value * value
            lanes = jnp.broadcast_to(jnp.sum(square, 0, keepdims=True), (8, D))
            mask = jnp.where(heads, (group == row).astype(F32), (row == 0).astype(F32))
            sums = lax.dot_general(
                mask, square, (((1,), (1,)), ((), ())), precision=EXACT, preferred_element_type=F32
            )
            tile = lax.dot_general(
                sums, place, (((1,), (0,)), ((), ())), precision=EXACT, preferred_element_type=F32
            )
            spread = jnp.zeros_like(tile)
            for part in range(groups):
                shift = lax.rem(mp_at * plan.width + (D - part * plan.width), D)
                moved = pltpu.roll(jnp.where(group == part, lanes, 0.0), shift, 1)
                spread = jnp.where(row == 4 + part, moved, spread)
            spread = jnp.where(heads, spread, jnp.where(row == 4 + mp_at, lanes, 0.0))
            tile_out[index] = jnp.where(row < 4, tile, spread)
            return 0

        first, start = 0, 0
        for pieces, size in zip(sets, counts):
            lax.fori_loop(0, size, functools.partial(one, first, refs[start : start + len(pieces)]), 0)
            first, start = first + size, start + len(pieces)

    return call(
        "collect",
        body,
        (1,),
        meta,
        tuple(arrays),
        [whole(item.shape) for item in arrays],
        [jax.ShapeDtypeStruct(shape, F32), jax.ShapeDtypeStruct((count, 8, D), F32)],
        [whole(shape), whole((count, 8, D))],
        [],
    )


def finish(plan, meta, sums, statistics, gain_state):
    counts = [item.shape for item in statistics]

    def body(meta, sum_ref, *rest):
        olds, gains = rest[:8], rest[8:12]
        norm_out, news, rates, gain_outs = rest[12], rest[13:21], rest[21], rest[22:]
        tiles = [sum_ref[6], sum_ref[1], sum_ref[0]]
        feeds = [(sum_ref[2], sum_ref[3]), (sum_ref[4], sum_ref[5])]
        gain_sum = 0.5 * sum_ref[7]
        total = jnp.sum(gain_sum * gain_sum)
        for tile in tiles:
            total = total + jnp.sum(tile[:4])
        for up, down in feeds:
            total = total + jnp.sum(up[:1]) + jnp.sum(down[:1])
        totals = jnp.full((8, D), total, F32)
        norm = jnp.sqrt(totals)
        factor = jnp.minimum(1.0, 1.0 / norm)
        squared = (factor * factor)[:1]
        norm_out[...] = norm[:, :128]
        rates[...] = factor[:, :128]

        def renew(old, sums, number):
            return DECAY * old + (1.0 - DECAY) * (sums * squared / number + EPS_STAT)

        for layer, tile in enumerate(tiles):
            for part in range(3):
                news[0][layer, part : part + 1] = renew(olds[0][layer, part : part + 1], tile[part : part + 1], D)
                news[1][layer, part : part + 1] = renew(
                    olds[1][layer, part : part + 1], tile[4 + part : 5 + part], D
                )
            news[2][layer : layer + 1] = renew(olds[2][layer : layer + 1], tile[7:8], D)
            news[3][layer : layer + 1] = renew(olds[3][layer : layer + 1], tile[3:4], D)
        for layer, (up, down) in enumerate(feeds):
            news[4][layer : layer + 1] = renew(olds[4][layer : layer + 1], up[:1], FF)
            news[7][layer : layer + 1] = renew(olds[7][layer : layer + 1], down[:1], FF)
            for part in range(FF // D):
                cut = slice(part * D, (part + 1) * D)
                news[5][layer : layer + 1, cut] = renew(
                    olds[5][layer : layer + 1, cut], up[4 + part : 5 + part], D
                )
                news[6][layer : layer + 1, cut] = renew(
                    olds[6][layer : layer + 1, cut], down[4 + part : 5 + part], D
                )
        shift = lax.rem(D - meta[0] * plan.block, D)
        grad = (pltpu.roll(gain_sum, shift, 1) * factor)[:5, : plan.block]
        master, square, moment, average = [item[...] for item in gains]
        square_new = DECAY * square + (1.0 - DECAY) * (grad * grad + EPS_STAT)
        stepped = grad * lax.rsqrt(square_new)
        moment_new = MOMENTUM * moment + stepped
        master_new = master - RATE_GAIN * (MOMENTUM * moment_new + stepped)
        values = (
            grad,
            square_new,
            moment_new,
            master_new,
            AVERAGE * average + (1.0 - AVERAGE) * master_new,
            master_new,
        )
        for out, value in zip(gain_outs, values):
            out[...] = value.astype(out.dtype)

    small = gain_state[0].shape
    outs = (
        [jax.ShapeDtypeStruct((8, 128), F32)]
        + [jax.ShapeDtypeStruct(shape, F32) for shape in counts]
        + [jax.ShapeDtypeStruct((8, 128), F32)]
        + [jax.ShapeDtypeStruct(small, F32)] * 5
        + [jax.ShapeDtypeStruct(small, LOW)]
    )
    inputs = (sums, *statistics, *gain_state)
    return call(
        "finish",
        body,
        (1,),
        meta,
        inputs,
        [whole(item.shape) for item in inputs],
        outs,
        [whole(item.shape) for item in outs],
        [],
    )


def part_spec(block, place):
    return pl.BlockSpec((2, block, D), lambda *_: (place, 0, 0))


def step_values(grad, scale, master, moment, average):
    stepped = grad * scale
    moment_new = MOMENTUM * moment + stepped
    master_new = master - RATE_MATRIX * (MOMENTUM * moment_new + stepped)
    return grad, moment_new, master_new, AVERAGE * average + (1.0 - AVERAGE) * master_new


def columns(rows, offset, size):
    filled = jnp.concatenate([rows] * (8 // rows.shape[0] + 1), 0)[:8]
    wide = (size + 127) // 128 * 128
    return jnp.transpose(pltpu.roll(filled, lax.rem(D - offset, D), 1)[:, :wide])[:size]


def update_attention(plan, meta, rates, grads, rows_in, cols_in, rows_out, cols_out, state_in, state_out):
    width, block = plan.width, plan.block

    def body(meta, rates_ref, grad_a, grad_b, rin, cin, rout, cout, *rest):
        ins, outs = rest[:6], rest[6:]
        layer = pl.program_id(0)
        dp_at, mp_at = meta[0], meta[1 + 3 * plan.pairs]
        grad = jnp.where(layer == 0, grad_a[0], jnp.where(layer == 1, grad_b[1], grad_b[0]))
        grad = grad * rates_ref[:1, :1]
        means = jnp.mean(rin[0], -1, keepdims=True)
        row_scale = lax.rsqrt(columns(rin[0] / means, dp_at * block, block))
        shift = lax.rem(D - mp_at * width, D)
        col_scale = lax.rsqrt(pltpu.roll(jnp.concatenate([cin[0]] * 3, 0)[:8], shift, 1)[:3, :width])
        for part in range(3):
            values = step_values(
                grad[:, part * width : (part + 1) * width],
                row_scale[:, part : part + 1] * col_scale[part : part + 1],
                ins[0][0, part],
                ins[1][0, part],
                ins[2][0, part],
            )
            for out, value in zip(outs[:4], values):
                out[0, part] = value
            outs[4][0, part] = values[2].astype(LOW)
        turned = jnp.transpose(grad[:, 3 * width :])
        row, col = rout[pl.ds(layer, 1), :], cout[pl.ds(layer, 1), :]
        mean = jnp.mean(row, -1, keepdims=True)
        row_scale = lax.rsqrt(columns(row / mean, mp_at * width, width))[:, :1]
        shift = lax.rem(D - dp_at * block, D)
        col_scale = lax.rsqrt(pltpu.roll(jnp.broadcast_to(col, (8, D)), shift, 1)[:1, :block])
        values = step_values(turned, row_scale * col_scale, ins[3][0], ins[4][0], ins[5][0])
        for out, value in zip(outs[5:9], values):
            out[0] = value
        outs[9][0] = values[2].astype(LOW)

    def spec(shape):
        return pl.BlockSpec((1,) + shape, lambda p, _: (p,) + (0,) * len(shape))

    shape_in, shape_out = (3, block, width), (width, block)
    outs = (
        [jax.ShapeDtypeStruct((3,) + shape_in, F32)] * 4
        + [jax.ShapeDtypeStruct((3,) + shape_in, LOW)]
        + [jax.ShapeDtypeStruct((3,) + shape_out, F32)] * 4
        + [jax.ShapeDtypeStruct((3,) + shape_out, LOW)]
    )
    return call(
        "update_attention",
        body,
        (3,),
        meta,
        (rates, *grads, rows_in, cols_in, rows_out, cols_out, *state_in, *state_out),
        [whole((8, 128)), whole((1, block, D)), part_spec(block, 0)]
        + [spec((3, D)), spec((3, D)), whole((3, D)), whole((3, D))]
        + [spec(shape_in)] * 3
        + [spec(shape_out)] * 3,
        outs,
        [spec(shape_in)] * 5 + [spec(shape_out)] * 5,
        [],
    )


def update_feed(plan, meta, rates, grads, rows_up, cols_up, rows_down, cols_down, state_up, state_down):
    hidden, block = plan.hidden, plan.block

    def body(meta, rates_ref, grad_a, grad_b, rup, cup, rdown, cdown, *rest):
        ins, outs = rest[:6], rest[6:]
        layer = pl.program_id(0)
        lanes = pl.ds(pl.multiple_of(meta[1 + 3 * plan.pairs] * hidden, 128), hidden)
        one = pl.ds(layer, 1)
        mean_up = jnp.mean(rup[one, :], -1, keepdims=True)
        mean_down = jnp.mean(rdown[one, :], -1, keepdims=True)
        along = (rup[one, :] / mean_up, cdown[one, :])
        across = (cup[one, lanes], rdown[one, lanes] / mean_down)
        for part in range(2):
            grad = jnp.where(layer == 0, grad_a[part], grad_b[part]) * rates_ref[:1, :1]
            row_scale = lax.rsqrt(columns(along[part], meta[0] * block, block))[:, :1]
            values = step_values(
                grad,
                row_scale * lax.rsqrt(across[part]),
                ins[3 * part][0],
                ins[3 * part + 1][0],
                ins[3 * part + 2][0],
            )
            for out, value in zip(outs[5 * part : 5 * part + 4], values):
                out[0] = value
            outs[5 * part + 4][0] = values[2].astype(LOW)

    state = pl.BlockSpec((1, block, hidden), lambda p, _: (p, 0, 0))
    outs = ([jax.ShapeDtypeStruct((2, block, hidden), F32)] * 4 + [jax.ShapeDtypeStruct((2, block, hidden), LOW)]) * 2
    values = call(
        "update_feed",
        body,
        (2,),
        meta,
        (
            rates,
            *grads,
            rows_up,
            cols_up,
            rows_down,
            cols_down,
            *state_up,
            *[item.transpose(0, 2, 1) for item in state_down],
        ),
        [whole((8, 128)), part_spec(block, 1), part_spec(block, 2)]
        + [whole((2, D)), whole((2, FF)), whole((2, FF)), whole((2, D))]
        + [state] * 6,
        outs,
        [state] * 10,
        [],
    )
    return [*values[:5], *[item.transpose(0, 2, 1) for item in values[5:]]]


def on_device(
    sizes,
    encoder_in,
    decoder_in,
    decoder_cotangent,
    counts,
    prefix_len,
    suffix_len,
    project_in,
    project_in_rows,
    project_in_cols,
    project_in_moment,
    project_in_average,
    project_out,
    project_out_rows,
    project_out_cols,
    project_out_moment,
    project_out_average,
    expand,
    expand_rows,
    expand_cols,
    expand_moment,
    expand_average,
    contract,
    contract_rows,
    contract_cols,
    contract_moment,
    contract_average,
    norm_gains,
    norm_gains_square,
    norm_gains_moment,
    norm_gains_average,
):
    dp_n, mp_n = sizes
    dp_index = lax.axis_index("dp")
    mp_index = lax.axis_index("mp")
    side = mp_index % 2
    pairs = prefix_len.shape[0]
    half = pairs // 2
    width = project_in.shape[-1]
    block = project_in.shape[-2]
    plan = Plan(dp_n, block, width, expand.shape[-1], pairs)
    low, f32 = LOW, F32

    def swap(value, axis, bit):
        count = dp_n if axis == "dp" else mp_n
        return lax.ppermute(value, axis, [(i, i ^ bit) for i in range(count)])

    def bits(count):
        return [1 << i for i in range(count.bit_length() - 1)]

    hold = lax.optimization_barrier

    class Gather:
        def __init__(self, blocks):
            self.items, self.sent, self.own = [{} for _ in blocks], [], list(blocks)

        def step(self, chain, *sends, later=()):
            names = [(item, name) for item, name in self.sent if (name, item) not in later]
            late = [(item, name) for item, name in self.sent if (name, item) in later]
            values = [self.items[item][name] for item, name in names]
            if names:
                chain, values, self.own = hold((list(chain), values, self.own))
            for (item, name), value in zip(names, values):
                self.items[item][name] = value
            self.sent = late
            for name, item in sends:
                if name == "fours":
                    four = swap(jnp.concatenate([self.own[at] for at in item]), "dp", 4)
                    for place, at in enumerate(item):
                        self.items[at]["four"] = four[place * block : (place + 1) * block]
                        self.sent.append((at, "four"))
                    continue
                parts = self.items[item]
                if name == "four":
                    parts[name] = swap(self.own[item], "dp", 4)
                    self.sent.append((item, name))
                    continue
                if "two" not in parts:
                    parts["two"] = jnp.concatenate([self.own[item], parts["four"]])
                if name == "far":
                    parts[name] = swap(parts["two"], "dp", 2)
                else:
                    parts[name] = swap(parts["two" if name == "near" else "far"], "dp", 1)
                self.sent.append((item, name))
            return chain

        def take(self, item, index=0):
            parts = self.items[item]
            height = self.own[item].shape[0]
            return [parts[name] for name in ("two", "far", "near", "last")], height, index * block

    class Plain:
        def __init__(self, blocks):
            self.own = list(blocks)

        def step(self, chain, *sends, later=()):
            return chain

        def take(self, item, index=0):
            own = self.own[item][index * block : (index + 1) * block]
            return [lax.all_gather(own, "dp", axis=0, tiled=True)], D, 0

    def total(value, axes):
        for axis, count in axes:
            for bit in bits(count):
                sent = value.astype(low)
                value = sent.astype(value.dtype) + swap(sent, axis, bit).astype(value.dtype)
        return value

    def total_dp(value):
        return total(value, [("dp", dp_n)])

    def total_all(value):
        return total(value, [("mp", mp_n), ("dp", dp_n)])

    def reduce_own(own, oth, first=()):
        sent = (own.astype(f32) + swap(oth, "mp", 1).astype(f32)).astype(low)
        for bit in bits(mp_n)[1:-1]:
            sent = (sent.astype(f32) + swap(sent, "mp", bit).astype(f32)).astype(low)
        sent, first = hold((sent, first))
        return sent, swap(sent, "mp", bits(mp_n)[-1])

    def relative(value):
        split = value.reshape((half, 2) + value.shape[1:])
        return (
            lax.dynamic_index_in_dim(split, side, 1, False),
            lax.dynamic_index_in_dim(split, 1 - side, 1, False),
        )

    def absolute(own):
        other = swap(own, "mp", 1)
        even = jnp.where(side == 0, own, other)
        odd = jnp.where(side == 0, other, own)
        return jnp.stack([even, odd], 1).reshape((pairs,) + own.shape[1:])

    def core(value):
        return swap(value, "mp", 1)

    def attention_block(layer):
        return jnp.concatenate(
            [project_in[layer, 0], project_in[layer, 1], project_in[layer, 2], project_out[layer].T], 1
        ).astype(low)

    def feed_block(layer):
        return [expand[layer].astype(low), contract[layer].T.astype(low)]

    direct = plan.direct
    place = dp_index[None].astype(jnp.int32)
    if direct:
        first = pack_first(plan, place, project_in, project_out, norm_gains)
    else:
        first = attention_block(0)
    blocks = [
        first,
        *feed_block(0),
        attention_block(1),
        attention_block(2),
        jnp.concatenate(feed_block(1)),
    ]
    gather = (Gather if direct else Plain)(blocks)
    gather.step((), ("four", 0))
    gather.step((), ("far", 0), ("near", 0), ("four", 1))
    gather.step((), ("last", 0), later=(("four", 1),))
    enc_att = [gather.take(0)]
    if direct:
        height = block + 8
        gain_rows = sum(
            item[at : at + 8].astype(f32) for item in enc_att[0][0] for at in (block, height + block)
        )
    else:
        gain_full = lax.dynamic_update_slice(
            jnp.zeros((8, D), low), norm_gains.astype(low), (0, dp_index * block)
        )
        gain_rows = total_dp(gain_full).astype(f32)
    gains = [gain_rows[i : i + 1] for i in range(5)]

    place_rel = jnp.concatenate([2 * jnp.arange(half) + side, 2 * jnp.arange(half) + 1 - side])
    prefix_rel = jnp.concatenate(relative(prefix_len))
    suffix_rel = jnp.concatenate(relative(suffix_len))
    images = place_rel < counts[0, 0]
    active = place_rel < counts[0, 0] + counts[0, 1]
    meta = jnp.concatenate(
        [
            dp_index[None].astype(jnp.int32),
            images.astype(jnp.int32),
            prefix_rel,
            suffix_rel,
            mp_index[None].astype(jnp.int32),
        ]
    )
    steps = jnp.arange(SUFFIX)
    live = active[:, None] & (steps[None, :] < suffix_rel[:, None])

    mid = half * SUFFIX
    enc_own, enc_oth = relative(
        jnp.pad(encoder_in.reshape(pairs, ENC_LEN, D), ((0, 0), (0, LONG - ENC_LEN), (0, 0)))
    )
    dec_rel = jnp.concatenate(relative(decoder_in.reshape(pairs, SUFFIX, D))).reshape(2 * mid, D)
    cot = jnp.concatenate(relative(decoder_cotangent.reshape(pairs, SUFFIX, D)))
    cot = jnp.where(live[:, :, None], cot, f32(0.0)).reshape(2 * mid, D)
    cot_low = cot.astype(low)

    def triple(value):
        return value.reshape(half, SUFFIX, D)

    (enc_oth,) = gather.step((enc_oth,), ("far", 1), ("near", 1), ("four", 2), later=(("last", 0),))
    own, oth, kept_enc = encoder_attention(plan, meta, enc_own, enc_oth, gains[0], enc_att, 0, half)
    own, oth, dec_rel, cot, cot_low = gather.step(
        (own, oth, dec_rel, cot, cot_low), ("last", 1), ("near", 2), ("far", 2), ("fours", (3, 4))
    )
    sums = gather.step(reduce_own(own, oth), ("last", 2))
    enc_feed = [gather.take(1), gather.take(2)]
    enc_mid, norm_mid = add_norm(meta, "add_norm_mid", enc_own, *sums, gains[1])
    (norm_mid,) = gather.step((norm_mid,))
    norm_mid_oth = core(norm_mid)

    (norm_mid_oth,) = gather.step(
        (norm_mid_oth,), ("far", 3), ("near", 3), ("four", 5)
    )
    own, oth = encoder_feed(plan, meta, norm_mid, norm_mid_oth, enc_feed, 0, half)
    own, oth = gather.step((own, oth), ("last", 3), ("far", 4), ("near", 4), later=(("four", 5),))
    sums = reduce_own(own, oth)
    (dec_rel,) = gather.step((dec_rel,), ("last", 4), ("far", 5), ("near", 5), later=(("last", 3),))

    self_att = [gather.take(3)]
    own, oth, kept_self = decoder_self(plan, meta, dec_rel, gains[2], self_att)
    sums = gather.step(sums, later=(("far", 5), ("near", 5)))
    sums_self = reduce_own(own, oth, sums)
    cross_att = [gather.take(4)]
    memory = (enc_mid + (sums[0].astype(f32) + sums[1].astype(f32))).astype(low)
    dec_one, norm_cross = add_norm(meta, "add_norm_cross", dec_rel[:mid], *sums_self, gains[3])
    memory, norm_cross = gather.step((memory, norm_cross), ("last", 5))
    memory_oth = core(memory)
    norm_cross_oth = core(norm_cross)

    cross_in = (triple(norm_cross), triple(norm_cross_oth), memory, memory_oth, cross_att)
    own, oth, *kept_cross = decoder_cross(plan, meta, *cross_in)
    kept_cross = [item.reshape((2, half) + item.shape[1:]) for item in kept_cross]
    sums = reduce_own(own, oth)
    dec_two, norm_last = add_norm(
        meta, "add_norm_last", dec_one, sums[0].reshape(mid, D), sums[1].reshape(mid, D), gains[4]
    )
    dec_feed = [gather.take(5), gather.take(5, 1)]

    own, oth, *grads_dec = decoder_feed(plan, meta, norm_last, core(norm_last), cot_low, dec_feed)
    if direct:
        more_dec = swap(grads_dec[0], "dp", 1)
    sums = reduce_own(own, oth)
    out_own = dec_two + (sums[0][0].astype(f32) + sums[1][0].astype(f32))
    grad, grad_low, gain_four = norm_back(
        meta, "norm_back_last", dec_two, gains[4], cot[:mid], sums[0][1], sums[1][1], True
    )

    own, oth, own_long, oth_long, *grads_cross = decoder_cross_back(
        plan, meta, *cross_in, *kept_cross, triple(grad_low), triple(core(grad_low))
    )
    if direct:
        own, oth, own_long, oth_long, more_dec = hold((own, oth, own_long, oth_long, more_dec))
        more_cross = swap(grads_cross[0], "dp", 1)
    sums = reduce_own(own, oth)
    sums_enc = reduce_own(own_long, oth_long, sums[0])
    if direct:
        keep, more_dec, _ = hold((grads_dec[1], more_dec, sums[0]))
        keep_dec, away_dec = fold(plan, meta, [keep], [more_dec], halves)
        *sums, away_dec = hold((*sums, away_dec))
        more_dec = swap(away_dec, "dp", 2)
    grad, grad_low, gain_three = norm_back(
        meta, "norm_back_cross", dec_one, gains[3], grad, sums[0].reshape(mid, D), sums[1].reshape(mid, D), True
    )
    grad_low_oth = core(grad_low)

    own_self, oth_self, *grads_self = decoder_self_back(
        plan, meta, dec_rel, gains[2], self_att, kept_self, grad_low, grad_low_oth
    )
    decoder_out = absolute(triple(out_own)).reshape(2 * mid, D)
    if direct:
        own_self, oth_self, decoder_out = hold((own_self, oth_self, decoder_out))
    sums_self = reduce_own(own_self, oth_self)
    if direct:
        *sums_enc, _, decoder_out, more_cross, more_dec = hold(
            (*sums_enc, sums_self[0], decoder_out, more_cross, more_dec)
        )
    grad_enc = sums_enc[0].astype(f32) + sums_enc[1].astype(f32)
    enc_low = grad_enc.astype(low)
    enc_low_oth = core(enc_low)

    if direct:
        enc_low_oth, away_self = hold((enc_low_oth, grads_self[0]))
        more_self = swap(away_self, "dp", 1)
    own, oth, *grads_enc = encoder_feed_back(plan, meta, norm_mid, norm_mid_oth, enc_low, enc_low_oth, enc_feed)
    if direct:
        own, oth, more_self, *sums_self = hold((own, oth, more_self, *sums_self))
        more_up, more_down = [swap(item, "dp", 1) for item in grads_enc[::2]]
    sums = reduce_own(own, oth)
    if direct:
        keep_cross, keep_self, more_cross, more_self, _ = hold(
            (grads_cross[1], grads_self[1], more_cross, more_self, sums[0])
        )
        keep_mid, away_mid = fold(plan, meta, [keep_cross, keep_self], [more_cross, more_self], halves)
        more_mid = swap(away_mid, "dp", 2)
        keep_dec, more_dec, _ = hold((keep_dec, more_dec, away_mid))
        keep_dec, away_dec = fold(plan, meta, [keep_dec], [more_dec], halves)
        more_dec = swap(away_dec, "dp", 4)
        sums_self, _, more_up = hold((sums_self, away_dec, more_up))
    grad, gain_two = norm_back(meta, "norm_back_self", dec_rel[:mid], gains[2], grad, *sums_self, False)
    decoder_in_grad = absolute(triple(grad)).reshape(2 * mid, D)
    if direct:
        *sums, decoder_in_grad, more_mid = hold((*sums, decoder_in_grad, more_mid))
    grad_enc, enc_low, gain_one = norm_back(
        meta, "norm_back_mid", enc_mid, gains[1], grad_enc, *sums, True
    )
    if direct:
        keep_mid, _ = hold((keep_mid, enc_low))
        keep_mid, away_mid = fold(plan, meta, [keep_mid], [more_mid], halves)
        enc_low, more_down, away_mid, more_dec = hold((enc_low, more_down, away_mid, more_dec))
    enc_low_oth = core(enc_low)

    if direct:
        keep_enc, away_enc = fold(plan, meta, grads_enc[1::2], [more_up, more_down], halves)
        enc_low_oth, away_enc, away_mid = hold((enc_low_oth, away_enc, away_mid))
        more_mid = swap(away_mid, "dp", 4)
        more_enc = swap(away_enc, "dp", 2)
    own, oth, *grads_att = encoder_attention_back(
        plan, meta, enc_own, enc_oth, gains[0], enc_att, kept_enc, enc_low, enc_low_oth
    )
    if direct:
        more_att = swap(grads_att[0], "dp", 1)
        own, oth, more_enc, more_mid = hold((own, oth, more_enc, more_mid))
        keep_enc, away_enc = fold(plan, meta, [keep_enc], [more_enc], halves)
        more_enc = swap(away_enc, "dp", 4)
        own, oth, _ = hold((own, oth, away_enc))
    sums = reduce_own(own, oth)
    if direct:
        keep_att, more_att, _ = hold((grads_att[1], more_att, sums[0]))
        mine, *others = fold(plan, meta, [keep_att], [more_att], apart)
        others, more_enc, keep_mid = hold((others, more_enc, keep_mid))
        pieces_att = [mine] + [swap(item, "dp", 2 * (i + 1)) for i, item in enumerate(others)]
        summed, tiles = collect(plan, meta, [[keep_mid, more_mid], [keep_enc, more_enc], [keep_dec, more_dec]], 2)
        *pieces_att, _ = hold((*pieces_att, tiles))
        *sums, _ = hold((*sums, pieces_att[1]))
        sum_att, tile_att = collect(plan, meta, [pieces_att], 1)
    else:
        parts = [grads_cross[0], grads_self[0], *grads_enc, grads_dec[0]]
        whole_sum = lax.psum_scatter(jnp.concatenate(parts), "dp", scatter_dimension=1, tiled=True)
        summed, tiles = collect(plan, meta, [[whole_sum[None]]], 2)
        whole_sum = lax.psum_scatter(grads_att[0], "dp", scatter_dimension=1, tiled=True)
        sum_att, tile_att = collect(plan, meta, [[whole_sum[None]]], 1)
    grad_enc, gain_zero = norm_back(meta, "norm_back_enc", enc_own, gains[0], grad_enc, *sums, False)
    encoder_in_grad = absolute(grad_enc)[:, :ENC_LEN].reshape(pairs * ENC_LEN, D)
    gain_tile = jnp.concatenate(
        [gain_zero, gain_one, gain_two, gain_three, gain_four, jnp.zeros((3, D), f32)]
    )[None]
    tiles = total_all(jnp.concatenate([tiles, tile_att, gain_tile]))
    done = finish(
        plan,
        meta,
        tiles,
        (
            project_in_rows,
            project_in_cols,
            project_out_rows,
            project_out_cols,
            expand_rows,
            expand_cols,
            contract_rows,
            contract_cols,
        ),
        (norm_gains, norm_gains_square, norm_gains_moment, norm_gains_average),
    )
    grad_norm, news, rates, pgain = done[0][0, 0], done[1:9], done[9], done[10:]
    att = update_attention(
        plan,
        meta,
        rates,
        (sum_att, summed),
        *news[:4],
        (project_in, project_in_moment, project_in_average),
        (project_out, project_out_moment, project_out_average),
    )
    feed = update_feed(
        plan,
        meta,
        rates,
        (summed, summed),
        *news[4:],
        (expand, expand_moment, expand_average),
        (contract, contract_moment, contract_average),
    )
    return (
        decoder_out,
        encoder_in_grad,
        decoder_in_grad,
        grad_norm,
        att[0],
        news[0],
        news[1],
        *att[1:5],
        att[5],
        news[2],
        news[3],
        *att[6:10],
        feed[0],
        news[4],
        news[5],
        *feed[1:5],
        feed[5],
        news[6],
        news[7],
        *feed[6:10],
        *pgain,
    )


def solution(mesh):
    placed = (
        P("dp", None),
        P("dp", None),
        P("dp", None),
        P("dp", None),
        P("dp"),
        P("dp"),
        P(None, None, "dp", "mp"),
        P(),
        P(),
        P(None, None, "dp", "mp"),
        P(None, None, "dp", "mp"),
        P(None, "mp", "dp"),
        P(),
        P(),
        P(None, "mp", "dp"),
        P(None, "mp", "dp"),
        P(None, "dp", "mp"),
        P(),
        P(),
        P(None, "dp", "mp"),
        P(None, "dp", "mp"),
        P(None, "mp", "dp"),
        P(),
        P(),
        P(None, "mp", "dp"),
        P(None, "mp", "dp"),
        P(None, "dp"),
        P(None, "dp"),
        P(None, "dp"),
        P(None, "dp"),
    )
    return jax.shard_map(
        functools.partial(on_device, (mesh.shape["dp"], mesh.shape["mp"])),
        mesh=mesh,
        in_specs=placed,
        out_specs=(
            P("dp", None),
            P("dp", None),
            P("dp", None),
            P(),
            P(None, None, "dp", "mp"),
            P(),
            P(),
            P(None, None, "dp", "mp"),
            P(None, None, "dp", "mp"),
            P(None, None, "dp", "mp"),
            P(None, None, "dp", "mp"),
            P(None, "mp", "dp"),
            P(),
            P(),
            P(None, "mp", "dp"),
            P(None, "mp", "dp"),
            P(None, "mp", "dp"),
            P(None, "mp", "dp"),
            P(None, "dp", "mp"),
            P(),
            P(),
            P(None, "dp", "mp"),
            P(None, "dp", "mp"),
            P(None, "dp", "mp"),
            P(None, "dp", "mp"),
            P(None, "mp", "dp"),
            P(),
            P(),
            P(None, "mp", "dp"),
            P(None, "mp", "dp"),
            P(None, "mp", "dp"),
            P(None, "mp", "dp"),
            P(None, "dp"),
            P(None, "dp"),
            P(None, "dp"),
            P(None, "dp"),
            P(None, "dp"),
            P(None, "dp"),
        ),
        check_vma=False,
    )
```

```python
import functools

import jax
import jax.numpy as jnp
from jax import lax
from jax.experimental import pallas as pl
from jax.experimental.pallas import tpu as pltpu
from jax.sharding import PartitionSpec as P

D = 768
HEAD_DIM = 64
FF = 3072
PATCHES = 196
SUFFIX = 32
ENC_LEN = 228


EPS_NORM = 1e-06
EPS_STAT = 1e-30
DECAY = 0.99
MOMENTUM = 0.9
AVERAGE = 0.6
RATE_MATRIX = 0.004
RATE_GAIN = 0.05
MASKED = -1000000000.0


LOW = jnp.bfloat16
F32 = jnp.float32
VMEM_LIMIT = 56 * 1024 * 1024
LONG = (ENC_LEN + 7) // 8 * 8
EXACT = lax.Precision.HIGHEST


def dot(left, right, contract):
    return lax.dot_general(left, right, (contract, ((), ())), preferred_element_type=F32)


def mm(left, right):
    return dot(left, right, ((1,), (0,)))


def mm_t(left, right):
    return dot(left, right, ((1,), (1,)))


def t_mm(left, right):
    return dot(left, right, ((0,), (0,)))


def rms_scale(value):
    return lax.rsqrt(jnp.mean(value * value, -1, keepdims=True) + EPS_NORM)


def softmax(scores):
    expons = jnp.exp(scores - jnp.max(scores, -1, keepdims=True))
    return expons / jnp.sum(expons, -1, keepdims=True)


def gelu_parts(upper):
    inner = 0.7978845608028654 * (upper + 0.044715 * upper * upper * upper)
    bent = jnp.tanh(inner)
    value = 0.5 * upper * (1.0 + bent)
    slope = 0.5 * (1.0 + bent) + 0.5 * upper * (1.0 - bent * bent) * 0.7978845608028654 * (
        1.0 + 3.0 * 0.044715 * upper * upper
    )
    return value, slope


class Plan:
    def __init__(self, dp_n, block, width, hidden, pairs):
        self.dp_n, self.block, self.width, self.hidden, self.pairs = dp_n, block, width, hidden, pairs
        self.half = pairs // 2
        self.heads = width // HEAD_DIM
        self.direct = dp_n == 8

    def weight_specs(self, pieces):
        return [whole(item.shape) for item in flat(pieces)]

    def weight_scratch(self, pieces):
        return [pltpu.VMEM((len(pieces), D, D), LOW)]

    def assemble(self, meta, pieces, refs, scratch):
        refs = iter(refs)
        for count in range(len(pieces)):
            if not self.direct:
                scratch[count] = next(refs)[...]
                continue
            _, height, start = pieces[count]
            for places in ((0, 4), (2, 6), (1, 5), (3, 7)):
                ref = next(refs)
                for index, place in enumerate(places):
                    row = pl.multiple_of(jnp.bitwise_xor(meta[0], place) * self.block, 32)
                    first = start + index * height
                    scratch[count, pl.ds(row, self.block), :] = ref[first : first + self.block]

    def grad_shapes(self, count):
        if not self.direct:
            return [jax.ShapeDtypeStruct((count, D, D), F32)]
        shape = (self.dp_n // 2, count, self.block, D)
        return [jax.ShapeDtypeStruct(shape, LOW), jax.ShapeDtypeStruct(shape, F32)]

    def emit(self, meta, acc, refs):
        if not self.direct:
            refs[0][...] = acc[...]
            return
        for index in range(self.dp_n // 2):
            here = pl.multiple_of(jnp.bitwise_xor(meta[0], 2 * index) * self.block, 32)
            away = pl.multiple_of(jnp.bitwise_xor(meta[0], 2 * index + 1) * self.block, 32)
            for count in range(acc.shape[0]):
                refs[0][index, count] = acc[count, pl.ds(away, self.block), :].astype(LOW)
                refs[1][index, count] = acc[count, pl.ds(here, self.block), :]


def flat(pieces):
    return [item for arrays, _, _ in pieces for item in arrays]


def whole(shape):
    return pl.BlockSpec(shape, lambda *_: (0,) * len(shape))


def own_spec(count, base, shape):
    return pl.BlockSpec(
        (1,) + shape, lambda p, _: (base + jnp.maximum(p - count, 0),) + (0,) * len(shape)
    )


def oth_spec(count, base, shape):
    return pl.BlockSpec(
        (1,) + shape, lambda p, _: (base + jnp.minimum(p, count - 1),) + (0,) * len(shape)
    )


def step_spec(shape):
    return pl.BlockSpec((1,) + shape, lambda p, _: (p,) + (0,) * len(shape))


def call(name, body, grid, meta, inputs, in_specs, outs, out_specs, scratch):
    return pl.pallas_call(
        body,
        name=name,
        out_shape=outs,
        grid_spec=pltpu.PrefetchScalarGridSpec(
            num_scalar_prefetch=1,
            grid=grid,
            in_specs=in_specs,
            out_specs=out_specs,
            scratch_shapes=scratch,
        ),
        cost_estimate=pl.CostEstimate(flops=1, transcendentals=0, bytes_accessed=1),
        compiler_params=pltpu.CompilerParams(
            dimension_semantics=("arbitrary",) * len(grid), vmem_limit_bytes=VMEM_LIMIT
        ),
    )(meta, *inputs)


def key_mask(meta, pairs, slot, turned=False):
    shape = (ENC_LEN, 1) if turned else (1, ENC_LEN)
    place = lax.broadcasted_iota(jnp.int32, shape, 1 - turned)
    image, prefix = meta[1 + slot], meta[1 + pairs + slot]
    return (place < image * PATCHES) | ((place >= PATCHES) & (place < PATCHES + prefix))


def attend_heads(plan, queries, keys, values, allowed):
    mixed = []
    for head in range(plan.heads):
        cut = slice(head * HEAD_DIM, (head + 1) * HEAD_DIM)
        scores = jnp.where(allowed, mm_t(queries[:, cut], keys[:, cut]) * 0.125, MASKED)
        mixed.append(mm(softmax(scores).astype(LOW), values[:, cut]).astype(LOW))
    return jnp.concatenate(mixed, 1)


def attend_heads_back(plan, queries, keys, values, allowed, grad_mixed):
    grads = ([], [], [])
    for head in range(plan.heads):
        cut = slice(head * HEAD_DIM, (head + 1) * HEAD_DIM)
        query, key, value, grad = queries[:, cut], keys[:, cut], values[:, cut], grad_mixed[:, cut]
        probs = softmax(jnp.where(allowed, mm_t(query, key) * 0.125, MASKED))
        grad_probs = mm_t(grad, value)
        inner = jnp.sum(grad_probs * probs, -1, keepdims=True)
        grad_scores = (probs * (grad_probs - inner)).astype(LOW)
        grads[0].append((mm(grad_scores, key) * 0.125).astype(LOW))
        grads[1].append((t_mm(grad_scores, query) * 0.125).astype(LOW))
        grads[2].append(t_mm(probs.astype(LOW), grad).astype(LOW))
    return tuple(jnp.concatenate(item, 1) for item in grads)


def attend_heads_turned(plan, queries, keys, values, allowed, grad_mixed):
    grads = ([], [], [])
    for head in range(plan.heads):
        cut = slice(head * HEAD_DIM, (head + 1) * HEAD_DIM)
        query, key, value, grad = queries[:, cut], keys[:, cut], values[:, cut], grad_mixed[:, cut]
        scores = jnp.where(allowed, mm_t(key, query) * 0.125, MASKED)
        expons = jnp.exp(scores - jnp.max(scores, 0, keepdims=True))
        probs = expons / jnp.sum(expons, 0, keepdims=True)
        grad_probs = mm_t(value, grad)
        inner = jnp.sum(grad_probs * probs, 0, keepdims=True)
        grad_scores = (probs * (grad_probs - inner)).astype(LOW)
        grads[0].append((t_mm(grad_scores, key) * 0.125).astype(LOW))
        grads[1].append((mm(grad_scores, query) * 0.125).astype(LOW))
        grads[2].append(mm(probs.astype(LOW), grad).astype(LOW))
    return tuple(jnp.concatenate(item, 1) for item in grads)


def slot_of(plan, count, base, step):
    return jnp.where(step < count, plan.half + base + step, base + step - count)


def pick(step, count, own, oth, rows):
    return jnp.where(step < count, oth[0, :rows], own[0, :rows])


def put(step, count, own, oth, value):
    @pl.when(step < count)
    def _():
        oth[0, : value.shape[0]] = value

    @pl.when(step >= count)
    def _():
        own[0, : value.shape[0]] = value


def encoder_attention(plan, meta, own, oth, gain, pieces, base, count):
    w3 = 3 * plan.width
    n = len(flat(pieces))

    def body(meta, own_ref, oth_ref, gain_ref, *rest):
        refs, (own_out, oth_out, kept, weight) = rest[:n], rest[n:]
        step = pl.program_id(0)

        @pl.when(step == 0)
        def _():
            plan.assemble(meta, pieces, refs, weight)

        value = pick(step, count, own_ref, oth_ref, ENC_LEN).astype(F32)
        normed = (value * rms_scale(value) * gain_ref[...]).astype(LOW)
        joined = mm(normed, weight[0, :, :w3]).astype(LOW)
        allowed = key_mask(meta, plan.pairs, slot_of(plan, count, base, step))
        width = plan.width
        mixed = attend_heads(
            plan, joined[:, :width], joined[:, width : 2 * width], joined[:, 2 * width :], allowed
        )
        kept[0, :, :w3] = joined
        kept[0, :, w3:] = mixed
        put(step, count, own_out, oth_out, mm_t(mixed, weight[0, :, w3:]).astype(LOW))

    rows = (LONG, D)
    return call(
        "encoder_attention",
        body,
        (2 * count,),
        meta,
        (own, oth, gain, *flat(pieces)),
        [own_spec(count, base, rows), oth_spec(count, base, rows), whole((1, D)), *plan.weight_specs(pieces)],
        [jax.ShapeDtypeStruct((count,) + rows, LOW)] * 2
        + [jax.ShapeDtypeStruct((2 * count, ENC_LEN, w3 + plan.width), LOW)],
        [own_spec(count, 0, rows), oth_spec(count, 0, rows), step_spec((ENC_LEN, w3 + plan.width))],
        plan.weight_scratch(pieces),
    )


def encoder_attention_back(plan, meta, own, oth, gain, pieces, kept, grad_own, grad_oth):
    count = plan.half
    width, w3 = plan.width, 3 * plan.width
    n = len(flat(pieces))

    def body(meta, own_ref, oth_ref, gain_ref, kept_ref, grad_own_ref, grad_oth_ref, *rest):
        refs, (own_out, oth_out), grad_refs = rest[:n], rest[n : n + 2], rest[n + 2 : -2]
        weight, acc = rest[-2:]
        step = pl.program_id(0)

        @pl.when(step == 0)
        def _():
            plan.assemble(meta, pieces, refs, weight)
            acc[...] = jnp.zeros_like(acc)

        value = pick(step, count, own_ref, oth_ref, ENC_LEN).astype(F32)
        normed = (value * rms_scale(value) * gain_ref[...]).astype(LOW)
        grad = pick(step, count, grad_own_ref, grad_oth_ref, ENC_LEN)
        allowed = key_mask(meta, plan.pairs, slot_of(plan, count, 0, step), True)
        grad_mixed = mm(grad, weight[0, :, w3:]).astype(LOW)
        acc[0, :, w3:] += t_mm(grad, kept_ref[0, :, w3:])
        joined = kept_ref[0, :, :w3]
        grads = attend_heads_turned(
            plan, joined[:, :width], joined[:, width : 2 * width], joined[:, 2 * width :], allowed, grad_mixed
        )
        together = jnp.concatenate(grads, 1)
        acc[0, :, :w3] += t_mm(normed, together)
        put(step, count, own_out, oth_out, mm_t(together, weight[0, :, :w3]).astype(LOW))

        @pl.when(step == 2 * count - 1)
        def _():
            plan.emit(meta, acc, grad_refs)

    rows = (LONG, D)
    shapes = plan.grad_shapes(1)
    pair_specs = [own_spec(count, 0, rows), oth_spec(count, 0, rows)]
    return call(
        "encoder_attention_back",
        body,
        (2 * count,),
        meta,
        (own, oth, gain, kept, grad_own, grad_oth, *flat(pieces)),
        [*pair_specs, whole((1, D)), step_spec(kept.shape[1:]), *pair_specs, *plan.weight_specs(pieces)],
        [jax.ShapeDtypeStruct((count,) + rows, LOW)] * 2 + shapes,
        [*pair_specs, *[whole(item.shape) for item in shapes]],
        plan.weight_scratch(pieces) + [pltpu.VMEM((1, D, D), F32)],
    )


def encoder_feed(plan, meta, own, oth, pieces, base, count):
    n = len(flat(pieces))

    def body(meta, own_ref, oth_ref, *rest):
        refs, (own_out, oth_out, weight) = rest[:n], rest[n:]
        step = pl.program_id(0)

        @pl.when(step == 0)
        def _():
            plan.assemble(meta, pieces, refs, weight)

        normed = pick(step, count, own_ref, oth_ref, ENC_LEN)
        active = gelu_parts(mm(normed, weight[0]))[0].astype(LOW)
        put(step, count, own_out, oth_out, mm_t(active, weight[1]).astype(LOW))

    rows = (LONG, D)
    return call(
        "encoder_feed",
        body,
        (2 * count,),
        meta,
        (own, oth, *flat(pieces)),
        [own_spec(count, base, rows), oth_spec(count, base, rows), *plan.weight_specs(pieces)],
        [jax.ShapeDtypeStruct((count,) + rows, LOW)] * 2,
        [own_spec(count, 0, rows), oth_spec(count, 0, rows)],
        plan.weight_scratch(pieces),
    )


def encoder_feed_back(plan, meta, own, oth, grad_own, grad_oth, pieces):
    n = len(flat(pieces))
    count = plan.half

    def body(meta, own_ref, oth_ref, grad_own_ref, grad_oth_ref, *rest):
        refs, (own_out, oth_out), grad_refs = rest[:n], rest[n : n + 2], rest[n + 2 : -2]
        weight, acc = rest[-2:]
        step = pl.program_id(0)

        @pl.when(step == 0)
        def _():
            plan.assemble(meta, pieces, refs, weight)
            acc[...] = jnp.zeros_like(acc)

        normed = pick(step, count, own_ref, oth_ref, ENC_LEN)
        grad = pick(step, count, grad_own_ref, grad_oth_ref, ENC_LEN)
        active, slope = gelu_parts(mm(normed, weight[0]))
        grad_upper = (slope * mm(grad, weight[1])).astype(LOW)
        put(step, count, own_out, oth_out, mm_t(grad_upper, weight[0]).astype(LOW))
        acc[0] += t_mm(normed, grad_upper)
        acc[1] += t_mm(grad, active.astype(LOW))

        @pl.when(step == 2 * count - 1)
        def _():
            for index in range(2):
                size = len(grad_refs) // 2
                plan.emit(meta, acc.at[pl.ds(index, 1)], grad_refs[index * size : (index + 1) * size])

    rows = (LONG, D)
    shapes = plan.grad_shapes(1) * 2
    pair_specs = [own_spec(count, 0, rows), oth_spec(count, 0, rows)]
    return call(
        "encoder_feed_back",
        body,
        (2 * count,),
        meta,
        (own, oth, grad_own, grad_oth, *flat(pieces)),
        [*pair_specs, *pair_specs, *plan.weight_specs(pieces)],
        [jax.ShapeDtypeStruct((count,) + rows, LOW)] * 2 + shapes,
        [*pair_specs, *[whole(item.shape) for item in shapes]],
        plan.weight_scratch(pieces) + [pltpu.VMEM((2, D, D), F32)],
    )


def self_mask(plan, meta, turned=False):
    rows = plan.pairs * SUFFIX
    query = lax.broadcasted_iota(jnp.int32, (rows, rows), int(turned))
    key = lax.broadcasted_iota(jnp.int32, (rows, rows), 1 - turned)
    pair = key // SUFFIX
    limit = jnp.zeros_like(key)
    for slot in range(plan.pairs):
        limit = jnp.where(pair == slot, meta[1 + 2 * plan.pairs + slot], limit)
    return (query // SUFFIX == pair) & (key <= query) & (key - pair * SUFFIX < limit)


def decoder_self(plan, meta, rows_in, gain, pieces):
    n = len(flat(pieces))
    width, w3 = plan.width, 3 * plan.width
    rows = plan.pairs * SUFFIX
    mid = rows // 2

    def body(meta, in_ref, gain_ref, *rest):
        refs, (own_out, oth_out, kept, weight) = rest[:n], rest[n:]
        plan.assemble(meta, pieces, refs, weight)
        value = in_ref[...].astype(F32)
        normed = (value * rms_scale(value) * gain_ref[...]).astype(LOW)
        joined = mm(normed, weight[0, :, :w3]).astype(LOW)
        mixed = attend_heads(
            plan, joined[:, :width], joined[:, width : 2 * width], joined[:, 2 * width :], self_mask(plan, meta)
        )
        kept[:, :w3] = joined
        kept[:, w3:] = mixed
        partial = mm_t(mixed, weight[0, :, w3:]).astype(LOW)
        own_out[...] = partial[:mid]
        oth_out[...] = partial[mid:]

    return call(
        "decoder_self",
        body,
        (1,),
        meta,
        (rows_in, gain, *flat(pieces)),
        [whole((rows, D)), whole((1, D)), *plan.weight_specs(pieces)],
        [jax.ShapeDtypeStruct((mid, D), LOW)] * 2 + [jax.ShapeDtypeStruct((rows, 4 * width), LOW)],
        [whole((mid, D))] * 2 + [whole((rows, 4 * width))],
        plan.weight_scratch(pieces),
    )


def decoder_self_back(plan, meta, rows_in, gain, pieces, kept, grad_own, grad_oth):
    n = len(flat(pieces))
    width, w3 = plan.width, 3 * plan.width
    rows = plan.pairs * SUFFIX
    mid = rows // 2

    def body(meta, in_ref, gain_ref, kept_ref, grad_own_ref, grad_oth_ref, *rest):
        refs, (own_out, oth_out), grad_refs = rest[:n], rest[n : n + 2], rest[n + 2 : -2]
        weight, acc = rest[-2:]
        plan.assemble(meta, pieces, refs, weight)
        value = in_ref[...].astype(F32)
        normed = (value * rms_scale(value) * gain_ref[...]).astype(LOW)
        grad = jnp.concatenate([grad_own_ref[...], grad_oth_ref[...]], 0)
        grad_mixed = mm(grad, weight[0, :, w3:]).astype(LOW)
        acc[0, :, w3:] = t_mm(grad, kept_ref[:, w3:])
        joined = kept_ref[:, :w3]
        grads = attend_heads_turned(
            plan,
            joined[:, :width],
            joined[:, width : 2 * width],
            joined[:, 2 * width :],
            self_mask(plan, meta, True),
            grad_mixed,
        )
        together = jnp.concatenate(grads, 1)
        acc[0, :, :w3] = t_mm(normed, together)
        partial = mm_t(together, weight[0, :, :w3]).astype(LOW)
        own_out[...] = partial[:mid]
        oth_out[...] = partial[mid:]
        plan.emit(meta, acc, grad_refs)

    shapes = plan.grad_shapes(1)
    return call(
        "decoder_self_back",
        body,
        (1,),
        meta,
        (rows_in, gain, kept, grad_own, grad_oth, *flat(pieces)),
        [whole((rows, D)), whole((1, D)), whole(kept.shape), whole((mid, D)), whole((mid, D)), *plan.weight_specs(pieces)],
        [jax.ShapeDtypeStruct((mid, D), LOW)] * 2 + shapes,
        [whole((mid, D))] * 2 + [whole(item.shape) for item in shapes],
        plan.weight_scratch(pieces) + [pltpu.VMEM((1, D, D), F32)],
    )


def decoder_cross(plan, meta, own, oth, memory_own, memory_oth, pieces):
    n = len(flat(pieces))
    count = plan.half
    width, w3 = plan.width, 3 * plan.width

    def body(meta, own_ref, oth_ref, memory_own_ref, memory_oth_ref, *rest):
        refs, (own_out, oth_out, kept_query, kept_key, weight) = rest[:n], rest[n:]
        step = pl.program_id(0)

        @pl.when(step == 0)
        def _():
            plan.assemble(meta, pieces, refs, weight)

        normed = pick(step, count, own_ref, oth_ref, SUFFIX)
        memory = pick(step, count, memory_own_ref, memory_oth_ref, ENC_LEN)
        queries = mm(normed, weight[0, :, :width]).astype(LOW)
        both = mm(memory, weight[0, :, width:w3]).astype(LOW)
        allowed = key_mask(meta, plan.pairs, slot_of(plan, count, 0, step))
        mixed = attend_heads(plan, queries, both[:, :width], both[:, width:], allowed)
        kept_query[0, :, :width] = queries
        kept_query[0, :, width:] = mixed
        kept_key[0] = both
        put(step, count, own_out, oth_out, mm_t(mixed, weight[0, :, w3:]).astype(LOW))

    rows, long = (SUFFIX, D), (LONG, D)
    return call(
        "decoder_cross",
        body,
        (2 * count,),
        meta,
        (own, oth, memory_own, memory_oth, *flat(pieces)),
        [
            own_spec(count, 0, rows),
            oth_spec(count, 0, rows),
            own_spec(count, 0, long),
            oth_spec(count, 0, long),
            *plan.weight_specs(pieces),
        ],
        [jax.ShapeDtypeStruct((count,) + rows, LOW)] * 2
        + [
            jax.ShapeDtypeStruct((2 * count, SUFFIX, 2 * width), LOW),
            jax.ShapeDtypeStruct((2 * count, ENC_LEN, 2 * width), LOW),
        ],
        [
            own_spec(count, 0, rows),
            oth_spec(count, 0, rows),
            step_spec((SUFFIX, 2 * width)),
            step_spec((ENC_LEN, 2 * width)),
        ],
        plan.weight_scratch(pieces),
    )


def pair_spec(shape):
    return pl.BlockSpec((1,) + shape, lambda p, _: (p,) + (0,) * len(shape))


def sides_spec(shape):
    return pl.BlockSpec((2, 1) + shape, lambda p, _: (0, p) + (0,) * len(shape))


def decoder_cross_back(
    plan, meta, own, oth, memory_own, memory_oth, pieces, kept_query, kept_key, grad_own, grad_oth
):
    n = len(flat(pieces))
    count = plan.half
    width, w3 = plan.width, 3 * plan.width
    rows = plan.pairs * SUFFIX
    mid = rows // 2

    def body(
        meta, own_ref, oth_ref, memory_own_ref, memory_oth_ref, query_ref, key_ref, grad_own_ref, grad_oth_ref, *rest
    ):
        refs, outs, grad_refs = rest[:n], rest[n : n + 4], rest[n + 4 : -4]
        weight, acc, grad_mixed, grad_query = rest[-4:]
        step = pl.program_id(0)

        @pl.when(step == 0)
        def _():
            plan.assemble(meta, pieces, refs, weight)
            grad = jnp.concatenate([grad_oth_ref[...], grad_own_ref[...]], 0).reshape(rows, D)
            grad_mixed[...] = mm(grad, weight[0, :, w3:]).astype(LOW)
            acc[0, :, w3:] = t_mm(grad, query_ref[:, :, :, width:].reshape(rows, width))
            acc[0, :, width:w3] = jnp.zeros((D, w3 - width), F32)

        total = None
        for side, (memory_ref, out) in enumerate(((memory_oth_ref, outs[3]), (memory_own_ref, outs[2]))):
            allowed = key_mask(meta, plan.pairs, (1 - side) * plan.half + step)
            both = key_ref[side, 0]
            here = pl.ds(pl.multiple_of((side * count + step) * SUFFIX, SUFFIX), SUFFIX)
            query, grad_key, grad_value = attend_heads_back(
                plan, query_ref[side, step, :, :width], both[:, :width], both[:, width:], allowed, grad_mixed[here, :]
            )
            grad_query[here, :] = query
            together = jnp.concatenate([grad_key, grad_value], 1)
            product = t_mm(memory_ref[0, :ENC_LEN], together)
            total = product if total is None else total + product
            out[0, :ENC_LEN] = mm_t(together, weight[0, :, width:w3]).astype(LOW)
        acc[0, :, width:w3] += total

        @pl.when(step == count - 1)
        def _():
            normed = jnp.concatenate([oth_ref[...], own_ref[...]], 0).reshape(rows, D)
            queries = grad_query[...]
            acc[0, :, :width] = t_mm(normed, queries)
            back = mm_t(queries, weight[0, :, :width]).astype(LOW)
            outs[1][...] = back[:mid].reshape(count, SUFFIX, D)
            outs[0][...] = back[mid:].reshape(count, SUFFIX, D)
            plan.emit(meta, acc, grad_refs)

    part, long = (count, SUFFIX, D), (LONG, D)
    shapes = plan.grad_shapes(1)
    return call(
        "decoder_cross_back",
        body,
        (count,),
        meta,
        (own, oth, memory_own, memory_oth, kept_query, kept_key, grad_own, grad_oth, *flat(pieces)),
        [
            whole(part),
            whole(part),
            pair_spec(long),
            pair_spec(long),
            whole(kept_query.shape),
            sides_spec(kept_key.shape[2:]),
            whole(part),
            whole(part),
            *plan.weight_specs(pieces),
        ],
        [jax.ShapeDtypeStruct(part, LOW)] * 2
        + [jax.ShapeDtypeStruct((count,) + long, LOW)] * 2
        + shapes,
        [whole(part), whole(part), pair_spec(long), pair_spec(long), *[whole(item.shape) for item in shapes]],
        plan.weight_scratch(pieces)
        + [pltpu.VMEM((1, D, D), F32), pltpu.VMEM((rows, width), LOW), pltpu.VMEM((rows, width), LOW)],
    )


def decoder_feed(plan, meta, own, oth, grad_in, pieces):
    n = len(flat(pieces))
    rows = plan.pairs * SUFFIX
    mid = rows // 2

    def body(meta, own_ref, oth_ref, grad_ref, *rest):
        refs, (own_out, oth_out), grad_refs = rest[:n], rest[n : n + 2], rest[n + 2 : -2]
        weight, acc = rest[-2:]
        plan.assemble(meta, pieces, refs, weight)
        normed = jnp.concatenate([own_ref[...], oth_ref[...]], 0)
        grad = grad_ref[...]
        active, slope = gelu_parts(mm(normed, weight[0]))
        active = active.astype(LOW)
        partial = mm_t(active, weight[1]).astype(LOW)
        grad_upper = (slope * mm(grad, weight[1])).astype(LOW)
        back = mm_t(grad_upper, weight[0]).astype(LOW)
        own_out[0] = partial[:mid]
        own_out[1] = back[:mid]
        oth_out[0] = partial[mid:]
        oth_out[1] = back[mid:]
        acc[0] = t_mm(normed, grad_upper)
        acc[1] = t_mm(grad, active)
        plan.emit(meta, acc, grad_refs)

    shapes = plan.grad_shapes(2)
    return call(
        "decoder_feed",
        body,
        (1,),
        meta,
        (own, oth, grad_in, *flat(pieces)),
        [whole((mid, D))] * 2 + [whole((rows, D)), *plan.weight_specs(pieces)],
        [jax.ShapeDtypeStruct((2, mid, D), LOW)] * 2 + shapes,
        [whole((2, mid, D))] * 2 + [whole(item.shape) for item in shapes],
        plan.weight_scratch(pieces) + [pltpu.VMEM((2, D, D), F32)],
    )


def add_norm(meta, name, base, first, second, gain):
    def body(meta, base_ref, first_ref, second_ref, gain_ref, sum_ref, norm_ref):
        value = base_ref[...].astype(F32) + (first_ref[...].astype(F32) + second_ref[...].astype(F32))
        sum_ref[...] = value
        norm_ref[...] = (value * rms_scale(value) * gain_ref[...]).astype(LOW)

    shape = base.shape
    part = (1,) + shape[1:] if len(shape) == 3 else shape
    spec = (
        pl.BlockSpec(part, lambda p, _: (p, 0, 0)) if len(shape) == 3 else whole(shape)
    )
    return call(
        name,
        body,
        (shape[0] if len(shape) == 3 else 1,),
        meta,
        (base, first, second, gain),
        [spec, spec, spec, whole((1, D))],
        [jax.ShapeDtypeStruct(shape, F32), jax.ShapeDtypeStruct(shape, LOW)],
        [spec, spec],
        [],
    )


def norm_back(meta, name, inputs, gain, grad, first, second, want_low):
    def body(meta, in_ref, gain_ref, grad_ref, first_ref, second_ref, *outs):
        value = in_ref[...].astype(F32)
        scale = rms_scale(value)
        unit = value * scale
        back = first_ref[...].astype(F32) + second_ref[...].astype(F32)
        product = back * unit
        real = product[0, :ENC_LEN] if value.ndim == 3 else product
        part = jnp.sum(real, 0, keepdims=True)
        weighted = product * gain_ref[...]
        total = grad_ref[...].astype(F32) + scale * (
            back * gain_ref[...] - unit * jnp.mean(weighted, -1, keepdims=True)
        )
        outs[0][...] = total
        if want_low:
            outs[1][...] = total.astype(LOW)
        step = pl.program_id(0)

        @pl.when(step == 0)
        def _():
            outs[-1][...] = part

        @pl.when(step > 0)
        def _():
            outs[-1][...] += part

    shape = inputs.shape
    part = (1,) + shape[1:] if len(shape) == 3 else shape
    spec = pl.BlockSpec(part, lambda p, _: (p, 0, 0)) if len(shape) == 3 else whole(shape)
    return call(
        name,
        body,
        (shape[0] if len(shape) == 3 else 1,),
        meta,
        (inputs, gain, grad, first, second),
        [spec, whole((1, D)), spec, spec, spec],
        [jax.ShapeDtypeStruct(shape, F32)]
        + [jax.ShapeDtypeStruct(shape, LOW)] * want_low
        + [jax.ShapeDtypeStruct((1, D), F32)],
        [spec] * (1 + want_low) + [whole((1, D))],
        [],
    )


def fold(plan, meta, keeps, mores, split):
    n = len(keeps)
    counts = [item.shape[1] for item in keeps]
    total = sum(counts)
    tail = keeps[0].shape[2:]
    blocks = keeps[0].shape[0]

    def body(meta, *rest):
        keep_refs, more_refs, outs = rest[:n], rest[n : 2 * n], rest[2 * n :]
        for index in range(blocks):
            start = 0
            out, at = split(index)
            for keep_ref, more_ref, count in zip(keep_refs, more_refs, counts):
                value = keep_ref[index] + more_ref[index].astype(F32)
                outs[out][at, start : start + count] = value.astype(outs[out].dtype)
                start += count

    places = [split(index) for index in range(blocks)]
    outs = [
        jax.ShapeDtypeStruct((sum(place[0] == out for place in places), total) + tail, LOW if out else F32)
        for out in range(1 + max(place[0] for place in places))
    ]
    return call(
        "fold",
        body,
        (1,),
        meta,
        (*keeps, *mores),
        [whole(item.shape) for item in (*keeps, *mores)],
        outs,
        [whole(item.shape) for item in outs],
        [],
    )


def halves(index):
    return index % 2, index // 2


def apart(index):
    return index, 0


def pack_first(plan, meta, project_in, project_out, gains):
    width, block = plan.width, plan.block

    def body(meta, in_ref, out_ref, gain_ref, packed):
        parts = [in_ref[0, index] for index in range(3)] + [jnp.transpose(out_ref[0])]
        packed[:block] = jnp.concatenate(parts, 1).astype(LOW)
        rows = jnp.concatenate([gain_ref[...], jnp.zeros((3, block), F32)], 0)
        wide = jnp.concatenate([rows, jnp.zeros((8, D - block), F32)], 1)
        packed[block:] = pltpu.roll(wide, meta[0] * block, 1).astype(LOW)

    shape = (block + 8, D)
    return call(
        "pack_first",
        body,
        (1,),
        meta,
        (project_in, project_out, gains),
        [
            pl.BlockSpec((1,) + project_in.shape[1:], lambda *_: (0, 0, 0, 0)),
            pl.BlockSpec((1,) + project_out.shape[1:], lambda *_: (0, 0, 0)),
            whole(gains.shape),
        ],
        [jax.ShapeDtypeStruct(shape, LOW)],
        [whole(shape)],
        [],
    )[0]


def one_hot(rows, offset):
    row = lax.broadcasted_iota(jnp.int32, (rows, D), 0)
    lane = lax.broadcasted_iota(jnp.int32, (rows, D), 1)
    return (lane == row + offset).astype(F32)


def collect(plan, meta, sets, attention):
    counts = [pieces[0].shape[-3] for pieces in sets]
    count = sum(counts)
    shape = (count,) + sets[0][0].shape[-2:]
    arrays = [item for pieces in sets for item in pieces]
    n = len(arrays)
    groups = D // plan.width

    def body(meta, *rest):
        refs, (out, tile_out) = rest[:n], rest[n:]
        dp_at, mp_at = meta[0], meta[1 + 3 * plan.pairs]
        group = lax.broadcasted_iota(jnp.int32, (8, D), 1) // plan.width
        row = lax.broadcasted_iota(jnp.int32, (8, D), 0)
        place = one_hot(plan.block, dp_at * plan.block)
        def one(first, refs, at, _):
            index = first + at
            heads = (jnp.zeros((8, D), jnp.int32) + index) < attention
            value = refs[0][0, at]
            for ref in refs[1:]:
                value = value + ref[0, at].astype(F32)
            out[index] = value
            square = value * value
            lanes = jnp.broadcast_to(jnp.sum(square, 0, keepdims=True), (8, D))
            mask = jnp.where(heads, (group == row).astype(F32), (row == 0).astype(F32))
            sums = lax.dot_general(
                mask, square, (((1,), (1,)), ((), ())), precision=EXACT, preferred_element_type=F32
            )
            tile = lax.dot_general(
                sums, place, (((1,), (0,)), ((), ())), precision=EXACT, preferred_element_type=F32
            )
            spread = jnp.zeros_like(tile)
            for part in range(groups):
                shift = lax.rem(mp_at * plan.width + (D - part * plan.width), D)
                moved = pltpu.roll(jnp.where(group == part, lanes, 0.0), shift, 1)
                spread = jnp.where(row == 4 + part, moved, spread)
            spread = jnp.where(heads, spread, jnp.where(row == 4 + mp_at, lanes, 0.0))
            tile_out[index] = jnp.where(row < 4, tile, spread)
            return 0

        first, start = 0, 0
        for pieces, size in zip(sets, counts):
            lax.fori_loop(0, size, functools.partial(one, first, refs[start : start + len(pieces)]), 0)
            first, start = first + size, start + len(pieces)

    return call(
        "collect",
        body,
        (1,),
        meta,
        tuple(arrays),
        [whole(item.shape) for item in arrays],
        [jax.ShapeDtypeStruct(shape, F32), jax.ShapeDtypeStruct((count, 8, D), F32)],
        [whole(shape), whole((count, 8, D))],
        [],
    )


def finish(plan, meta, sums, statistics, gain_state):
    counts = [item.shape for item in statistics]

    def body(meta, sum_ref, *rest):
        olds, gains = rest[:8], rest[8:12]
        norm_out, news, rates, gain_outs = rest[12], rest[13:21], rest[21], rest[22:]
        tiles = [sum_ref[6], sum_ref[1], sum_ref[0]]
        feeds = [(sum_ref[2], sum_ref[3]), (sum_ref[4], sum_ref[5])]
        gain_sum = 0.5 * sum_ref[7]
        total = jnp.sum(gain_sum * gain_sum)
        for tile in tiles:
            total = total + jnp.sum(tile[:4])
        for up, down in feeds:
            total = total + jnp.sum(up[:1]) + jnp.sum(down[:1])
        totals = jnp.full((8, D), total, F32)
        norm = jnp.sqrt(totals)
        factor = jnp.minimum(1.0, 1.0 / norm)
        squared = (factor * factor)[:1]
        norm_out[...] = norm[:, :128]
        rates[...] = factor[:, :128]

        def renew(old, sums, number):
            return DECAY * old + (1.0 - DECAY) * (sums * squared / number + EPS_STAT)

        for layer, tile in enumerate(tiles):
            for part in range(3):
                news[0][layer, part : part + 1] = renew(olds[0][layer, part : part + 1], tile[part : part + 1], D)
                news[1][layer, part : part + 1] = renew(
                    olds[1][layer, part : part + 1], tile[4 + part : 5 + part], D
                )
            news[2][layer : layer + 1] = renew(olds[2][layer : layer + 1], tile[7:8], D)
            news[3][layer : layer + 1] = renew(olds[3][layer : layer + 1], tile[3:4], D)
        for layer, (up, down) in enumerate(feeds):
            news[4][layer : layer + 1] = renew(olds[4][layer : layer + 1], up[:1], FF)
            news[7][layer : layer + 1] = renew(olds[7][layer : layer + 1], down[:1], FF)
            for part in range(FF // D):
                cut = slice(part * D, (part + 1) * D)
                news[5][layer : layer + 1, cut] = renew(
                    olds[5][layer : layer + 1, cut], up[4 + part : 5 + part], D
                )
                news[6][layer : layer + 1, cut] = renew(
                    olds[6][layer : layer + 1, cut], down[4 + part : 5 + part], D
                )
        shift = lax.rem(D - meta[0] * plan.block, D)
        grad = (pltpu.roll(gain_sum, shift, 1) * factor)[:5, : plan.block]
        master, square, moment, average = [item[...] for item in gains]
        square_new = DECAY * square + (1.0 - DECAY) * (grad * grad + EPS_STAT)
        stepped = grad * lax.rsqrt(square_new)
        moment_new = MOMENTUM * moment + stepped
        master_new = master - RATE_GAIN * (MOMENTUM * moment_new + stepped)
        values = (
            grad,
            square_new,
            moment_new,
            master_new,
            AVERAGE * average + (1.0 - AVERAGE) * master_new,
            master_new,
        )
        for out, value in zip(gain_outs, values):
            out[...] = value.astype(out.dtype)

    small = gain_state[0].shape
    outs = (
        [jax.ShapeDtypeStruct((8, 128), F32)]
        + [jax.ShapeDtypeStruct(shape, F32) for shape in counts]
        + [jax.ShapeDtypeStruct((8, 128), F32)]
        + [jax.ShapeDtypeStruct(small, F32)] * 5
        + [jax.ShapeDtypeStruct(small, LOW)]
    )
    inputs = (sums, *statistics, *gain_state)
    return call(
        "finish",
        body,
        (1,),
        meta,
        inputs,
        [whole(item.shape) for item in inputs],
        outs,
        [whole(item.shape) for item in outs],
        [],
    )


def part_spec(block, place):
    return pl.BlockSpec((2, block, D), lambda *_: (place, 0, 0))


def step_values(grad, scale, master, moment, average):
    stepped = grad * scale
    moment_new = MOMENTUM * moment + stepped
    master_new = master - RATE_MATRIX * (MOMENTUM * moment_new + stepped)
    return grad, moment_new, master_new, AVERAGE * average + (1.0 - AVERAGE) * master_new


def columns(rows, offset, size):
    filled = jnp.concatenate([rows] * (8 // rows.shape[0] + 1), 0)[:8]
    wide = (size + 127) // 128 * 128
    return jnp.transpose(pltpu.roll(filled, lax.rem(D - offset, D), 1)[:, :wide])[:size]


def update_attention(plan, meta, rates, grads, rows_in, cols_in, rows_out, cols_out, state_in, state_out):
    width, block = plan.width, plan.block

    def body(meta, rates_ref, grad_a, grad_b, rin, cin, rout, cout, *rest):
        ins, outs = rest[:6], rest[6:]
        layer = pl.program_id(0)
        dp_at, mp_at = meta[0], meta[1 + 3 * plan.pairs]
        grad = jnp.where(layer == 0, grad_a[0], jnp.where(layer == 1, grad_b[1], grad_b[0]))
        grad = grad * rates_ref[:1, :1]
        means = jnp.mean(rin[0], -1, keepdims=True)
        row_scale = lax.rsqrt(columns(rin[0] / means, dp_at * block, block))
        shift = lax.rem(D - mp_at * width, D)
        col_scale = lax.rsqrt(pltpu.roll(jnp.concatenate([cin[0]] * 3, 0)[:8], shift, 1)[:3, :width])
        for part in range(3):
            values = step_values(
                grad[:, part * width : (part + 1) * width],
                row_scale[:, part : part + 1] * col_scale[part : part + 1],
                ins[0][0, part],
                ins[1][0, part],
                ins[2][0, part],
            )
            for out, value in zip(outs[:4], values):
                out[0, part] = value
            outs[4][0, part] = values[2].astype(LOW)
        turned = jnp.transpose(grad[:, 3 * width :])
        row, col = rout[pl.ds(layer, 1), :], cout[pl.ds(layer, 1), :]
        mean = jnp.mean(row, -1, keepdims=True)
        row_scale = lax.rsqrt(columns(row / mean, mp_at * width, width))[:, :1]
        shift = lax.rem(D - dp_at * block, D)
        col_scale = lax.rsqrt(pltpu.roll(jnp.broadcast_to(col, (8, D)), shift, 1)[:1, :block])
        values = step_values(turned, row_scale * col_scale, ins[3][0], ins[4][0], ins[5][0])
        for out, value in zip(outs[5:9], values):
            out[0] = value
        outs[9][0] = values[2].astype(LOW)

    def spec(shape):
        return pl.BlockSpec((1,) + shape, lambda p, _: (p,) + (0,) * len(shape))

    shape_in, shape_out = (3, block, width), (width, block)
    outs = (
        [jax.ShapeDtypeStruct((3,) + shape_in, F32)] * 4
        + [jax.ShapeDtypeStruct((3,) + shape_in, LOW)]
        + [jax.ShapeDtypeStruct((3,) + shape_out, F32)] * 4
        + [jax.ShapeDtypeStruct((3,) + shape_out, LOW)]
    )
    return call(
        "update_attention",
        body,
        (3,),
        meta,
        (rates, *grads, rows_in, cols_in, rows_out, cols_out, *state_in, *state_out),
        [whole((8, 128)), whole((1, block, D)), part_spec(block, 0)]
        + [spec((3, D)), spec((3, D)), whole((3, D)), whole((3, D))]
        + [spec(shape_in)] * 3
        + [spec(shape_out)] * 3,
        outs,
        [spec(shape_in)] * 5 + [spec(shape_out)] * 5,
        [],
    )


def update_feed(plan, meta, rates, grads, rows_up, cols_up, rows_down, cols_down, state_up, state_down):
    hidden, block = plan.hidden, plan.block

    def body(meta, rates_ref, grad_a, grad_b, rup, cup, rdown, cdown, *rest):
        ins, outs = rest[:6], rest[6:]
        layer = pl.program_id(0)
        lanes = pl.ds(pl.multiple_of(meta[1 + 3 * plan.pairs] * hidden, 128), hidden)
        one = pl.ds(layer, 1)
        mean_up = jnp.mean(rup[one, :], -1, keepdims=True)
        mean_down = jnp.mean(rdown[one, :], -1, keepdims=True)
        along = (rup[one, :] / mean_up, cdown[one, :])
        across = (cup[one, lanes], rdown[one, lanes] / mean_down)
        for part in range(2):
            grad = jnp.where(layer == 0, grad_a[part], grad_b[part]) * rates_ref[:1, :1]
            row_scale = lax.rsqrt(columns(along[part], meta[0] * block, block))[:, :1]
            values = step_values(
                grad,
                row_scale * lax.rsqrt(across[part]),
                ins[3 * part][0],
                ins[3 * part + 1][0],
                ins[3 * part + 2][0],
            )
            for out, value in zip(outs[5 * part : 5 * part + 4], values):
                out[0] = value
            outs[5 * part + 4][0] = values[2].astype(LOW)

    state = pl.BlockSpec((1, block, hidden), lambda p, _: (p, 0, 0))
    outs = ([jax.ShapeDtypeStruct((2, block, hidden), F32)] * 4 + [jax.ShapeDtypeStruct((2, block, hidden), LOW)]) * 2
    values = call(
        "update_feed",
        body,
        (2,),
        meta,
        (
            rates,
            *grads,
            rows_up,
            cols_up,
            rows_down,
            cols_down,
            *state_up,
            *[item.transpose(0, 2, 1) for item in state_down],
        ),
        [whole((8, 128)), part_spec(block, 1), part_spec(block, 2)]
        + [whole((2, D)), whole((2, FF)), whole((2, FF)), whole((2, D))]
        + [state] * 6,
        outs,
        [state] * 10,
        [],
    )
    return [*values[:5], *[item.transpose(0, 2, 1) for item in values[5:]]]


def on_device(
    sizes,
    encoder_in,
    decoder_in,
    decoder_cotangent,
    counts,
    prefix_len,
    suffix_len,
    project_in,
    project_in_rows,
    project_in_cols,
    project_in_moment,
    project_in_average,
    project_out,
    project_out_rows,
    project_out_cols,
    project_out_moment,
    project_out_average,
    expand,
    expand_rows,
    expand_cols,
    expand_moment,
    expand_average,
    contract,
    contract_rows,
    contract_cols,
    contract_moment,
    contract_average,
    norm_gains,
    norm_gains_square,
    norm_gains_moment,
    norm_gains_average,
):
    dp_n, mp_n = sizes
    dp_index = lax.axis_index("dp")
    mp_index = lax.axis_index("mp")
    side = mp_index % 2
    pairs = prefix_len.shape[0]
    half = pairs // 2
    width = project_in.shape[-1]
    block = project_in.shape[-2]
    plan = Plan(dp_n, block, width, expand.shape[-1], pairs)
    low, f32 = LOW, F32

    def swap(value, axis, bit):
        count = dp_n if axis == "dp" else mp_n
        return lax.ppermute(value, axis, [(i, i ^ bit) for i in range(count)])

    def bits(count):
        return [1 << i for i in range(count.bit_length() - 1)]

    hold = lax.optimization_barrier

    class Gather:
        def __init__(self, blocks):
            self.items, self.sent, self.own = [{} for _ in blocks], [], list(blocks)

        def step(self, chain, *sends, later=()):
            names = [(item, name) for item, name in self.sent if (name, item) not in later]
            late = [(item, name) for item, name in self.sent if (name, item) in later]
            values = [self.items[item][name] for item, name in names]
            if names:
                chain, values, self.own = hold((list(chain), values, self.own))
            for (item, name), value in zip(names, values):
                self.items[item][name] = value
            self.sent = late
            for name, item in sends:
                if name == "fours":
                    four = swap(jnp.concatenate([self.own[at] for at in item]), "dp", 4)
                    for place, at in enumerate(item):
                        self.items[at]["four"] = four[place * block : (place + 1) * block]
                        self.sent.append((at, "four"))
                    continue
                parts = self.items[item]
                if name == "four":
                    parts[name] = swap(self.own[item], "dp", 4)
                    self.sent.append((item, name))
                    continue
                if "two" not in parts:
                    parts["two"] = jnp.concatenate([self.own[item], parts["four"]])
                if name == "far":
                    parts[name] = swap(parts["two"], "dp", 2)
                else:
                    parts[name] = swap(parts["two" if name == "near" else "far"], "dp", 1)
                self.sent.append((item, name))
            return chain

        def take(self, item, index=0):
            parts = self.items[item]
            height = self.own[item].shape[0]
            return [parts[name] for name in ("two", "far", "near", "last")], height, index * block

    class Plain:
        def __init__(self, blocks):
            self.own = list(blocks)

        def step(self, chain, *sends, later=()):
            return chain

        def take(self, item, index=0):
            own = self.own[item][index * block : (index + 1) * block]
            return [lax.all_gather(own, "dp", axis=0, tiled=True)], D, 0

    def total(value, axes):
        for axis, count in axes:
            for bit in bits(count):
                sent = value.astype(low)
                value = sent.astype(value.dtype) + swap(sent, axis, bit).astype(value.dtype)
        return value

    def total_dp(value):
        return total(value, [("dp", dp_n)])

    def total_all(value):
        return total(value, [("mp", mp_n), ("dp", dp_n)])

    def reduce_own(own, oth, first=()):
        sent = (own.astype(f32) + swap(oth, "mp", 1).astype(f32)).astype(low)
        for bit in bits(mp_n)[1:-1]:
            sent = (sent.astype(f32) + swap(sent, "mp", bit).astype(f32)).astype(low)
        sent, first = hold((sent, first))
        return sent, swap(sent, "mp", bits(mp_n)[-1])

    def relative(value):
        split = value.reshape((half, 2) + value.shape[1:])
        return (
            lax.dynamic_index_in_dim(split, side, 1, False),
            lax.dynamic_index_in_dim(split, 1 - side, 1, False),
        )

    def absolute(own):
        other = swap(own, "mp", 1)
        even = jnp.where(side == 0, own, other)
        odd = jnp.where(side == 0, other, own)
        return jnp.stack([even, odd], 1).reshape((pairs,) + own.shape[1:])

    def core(value):
        return swap(value, "mp", 1)

    def attention_block(layer):
        return jnp.concatenate(
            [project_in[layer, 0], project_in[layer, 1], project_in[layer, 2], project_out[layer].T], 1
        ).astype(low)

    def feed_block(layer):
        return [expand[layer].astype(low), contract[layer].T.astype(low)]

    direct = plan.direct
    place = dp_index[None].astype(jnp.int32)
    if direct:
        first = pack_first(plan, place, project_in, project_out, norm_gains)
    else:
        first = attention_block(0)
    blocks = [
        first,
        *feed_block(0),
        attention_block(1),
        attention_block(2),
        jnp.concatenate(feed_block(1)),
    ]
    gather = (Gather if direct else Plain)(blocks)
    gather.step((), ("four", 0))
    gather.step((), ("far", 0), ("near", 0), ("four", 1))
    gather.step((), ("last", 0), later=(("four", 1),))
    enc_att = [gather.take(0)]
    if direct:
        height = block + 8
        gain_rows = sum(
            item[at : at + 8].astype(f32) for item in enc_att[0][0] for at in (block, height + block)
        )
    else:
        gain_full = lax.dynamic_update_slice(
            jnp.zeros((8, D), low), norm_gains.astype(low), (0, dp_index * block)
        )
        gain_rows = total_dp(gain_full).astype(f32)
    gains = [gain_rows[i : i + 1] for i in range(5)]

    place_rel = jnp.concatenate([2 * jnp.arange(half) + side, 2 * jnp.arange(half) + 1 - side])
    prefix_rel = jnp.concatenate(relative(prefix_len))
    suffix_rel = jnp.concatenate(relative(suffix_len))
    images = place_rel < counts[0, 0]
    active = place_rel < counts[0, 0] + counts[0, 1]
    meta = jnp.concatenate(
        [
            dp_index[None].astype(jnp.int32),
            images.astype(jnp.int32),
            prefix_rel,
            suffix_rel,
            mp_index[None].astype(jnp.int32),
        ]
    )
    steps = jnp.arange(SUFFIX)
    live = active[:, None] & (steps[None, :] < suffix_rel[:, None])

    mid = half * SUFFIX
    enc_own, enc_oth = relative(
        jnp.pad(encoder_in.reshape(pairs, ENC_LEN, D), ((0, 0), (0, LONG - ENC_LEN), (0, 0)))
    )
    dec_rel = jnp.concatenate(relative(decoder_in.reshape(pairs, SUFFIX, D))).reshape(2 * mid, D)
    cot = jnp.concatenate(relative(decoder_cotangent.reshape(pairs, SUFFIX, D)))
    cot = jnp.where(live[:, :, None], cot, f32(0.0)).reshape(2 * mid, D)
    cot_low = cot.astype(low)

    def triple(value):
        return value.reshape(half, SUFFIX, D)

    (enc_oth,) = gather.step((enc_oth,), ("far", 1), ("near", 1), ("four", 2), later=(("last", 0),))
    own, oth, kept_enc = encoder_attention(plan, meta, enc_own, enc_oth, gains[0], enc_att, 0, half)
    own, oth, dec_rel, cot, cot_low = gather.step(
        (own, oth, dec_rel, cot, cot_low), ("last", 1), ("near", 2), ("far", 2), ("fours", (3, 4))
    )
    sums = gather.step(reduce_own(own, oth), ("last", 2))
    enc_feed = [gather.take(1), gather.take(2)]
    enc_mid, norm_mid = add_norm(meta, "add_norm_mid", enc_own, *sums, gains[1])
    (norm_mid,) = gather.step((norm_mid,))
    norm_mid_oth = core(norm_mid)

    (norm_mid_oth,) = gather.step(
        (norm_mid_oth,), ("far", 3), ("near", 3), ("four", 5)
    )
    own, oth = encoder_feed(plan, meta, norm_mid, norm_mid_oth, enc_feed, 0, half)
    own, oth = gather.step((own, oth), ("last", 3), ("far", 4), ("near", 4), later=(("four", 5),))
    sums = reduce_own(own, oth)
    (dec_rel,) = gather.step((dec_rel,), ("last", 4), ("far", 5), ("near", 5), later=(("last", 3),))

    self_att = [gather.take(3)]
    own, oth, kept_self = decoder_self(plan, meta, dec_rel, gains[2], self_att)
    sums = gather.step(sums, later=(("far", 5), ("near", 5)))
    sums_self = reduce_own(own, oth, sums)
    cross_att = [gather.take(4)]
    memory = (enc_mid + (sums[0].astype(f32) + sums[1].astype(f32))).astype(low)
    dec_one, norm_cross = add_norm(meta, "add_norm_cross", dec_rel[:mid], *sums_self, gains[3])
    memory, norm_cross = gather.step((memory, norm_cross), ("last", 5))
    memory_oth = core(memory)
    norm_cross_oth = core(norm_cross)

    cross_in = (triple(norm_cross), triple(norm_cross_oth), memory, memory_oth, cross_att)
    own, oth, *kept_cross = decoder_cross(plan, meta, *cross_in)
    kept_cross = [item.reshape((2, half) + item.shape[1:]) for item in kept_cross]
    sums = reduce_own(own, oth)
    dec_two, norm_last = add_norm(
        meta, "add_norm_last", dec_one, sums[0].reshape(mid, D), sums[1].reshape(mid, D), gains[4]
    )
    dec_feed = [gather.take(5), gather.take(5, 1)]

    own, oth, *grads_dec = decoder_feed(plan, meta, norm_last, core(norm_last), cot_low, dec_feed)
    if direct:
        more_dec = swap(grads_dec[0], "dp", 1)
    sums = reduce_own(own, oth)
    out_own = dec_two + (sums[0][0].astype(f32) + sums[1][0].astype(f32))
    grad, grad_low, gain_four = norm_back(
        meta, "norm_back_last", dec_two, gains[4], cot[:mid], sums[0][1], sums[1][1], True
    )

    own, oth, own_long, oth_long, *grads_cross = decoder_cross_back(
        plan, meta, *cross_in, *kept_cross, triple(grad_low), triple(core(grad_low))
    )
    if direct:
        own, oth, own_long, oth_long, more_dec = hold((own, oth, own_long, oth_long, more_dec))
        more_cross = swap(grads_cross[0], "dp", 1)
    sums = reduce_own(own, oth)
    sums_enc = reduce_own(own_long, oth_long, sums[0])
    if direct:
        keep, more_dec, _ = hold((grads_dec[1], more_dec, sums[0]))
        keep_dec, away_dec = fold(plan, meta, [keep], [more_dec], halves)
        *sums, away_dec = hold((*sums, away_dec))
        more_dec = swap(away_dec, "dp", 2)
    grad, grad_low, gain_three = norm_back(
        meta, "norm_back_cross", dec_one, gains[3], grad, sums[0].reshape(mid, D), sums[1].reshape(mid, D), True
    )
    grad_low_oth = core(grad_low)

    own_self, oth_self, *grads_self = decoder_self_back(
        plan, meta, dec_rel, gains[2], self_att, kept_self, grad_low, grad_low_oth
    )
    decoder_out = absolute(triple(out_own)).reshape(2 * mid, D)
    if direct:
        own_self, oth_self, decoder_out = hold((own_self, oth_self, decoder_out))
    sums_self = reduce_own(own_self, oth_self)
    if direct:
        *sums_enc, _, decoder_out, more_cross, more_dec = hold(
            (*sums_enc, sums_self[0], decoder_out, more_cross, more_dec)
        )
    grad_enc = sums_enc[0].astype(f32) + sums_enc[1].astype(f32)
    enc_low = grad_enc.astype(low)
    enc_low_oth = core(enc_low)

    if direct:
        enc_low_oth, away_self = hold((enc_low_oth, grads_self[0]))
        more_self = swap(away_self, "dp", 1)
    own, oth, *grads_enc = encoder_feed_back(plan, meta, norm_mid, norm_mid_oth, enc_low, enc_low_oth, enc_feed)
    if direct:
        own, oth, more_self, *sums_self = hold((own, oth, more_self, *sums_self))
        more_up, more_down = [swap(item, "dp", 1) for item in grads_enc[::2]]
    sums = reduce_own(own, oth)
    if direct:
        keep_cross, keep_self, more_cross, more_self, _ = hold(
            (grads_cross[1], grads_self[1], more_cross, more_self, sums[0])
        )
        keep_mid, away_mid = fold(plan, meta, [keep_cross, keep_self], [more_cross, more_self], halves)
        more_mid = swap(away_mid, "dp", 2)
        keep_dec, more_dec, _ = hold((keep_dec, more_dec, away_mid))
        keep_dec, away_dec = fold(plan, meta, [keep_dec], [more_dec], halves)
        more_dec = swap(away_dec, "dp", 4)
        sums_self, _, more_up = hold((sums_self, away_dec, more_up))
    grad, gain_two = norm_back(meta, "norm_back_self", dec_rel[:mid], gains[2], grad, *sums_self, False)
    decoder_in_grad = absolute(triple(grad)).reshape(2 * mid, D)
    if direct:
        *sums, decoder_in_grad, more_mid = hold((*sums, decoder_in_grad, more_mid))
    grad_enc, enc_low, gain_one = norm_back(
        meta, "norm_back_mid", enc_mid, gains[1], grad_enc, *sums, True
    )
    if direct:
        keep_mid, _ = hold((keep_mid, enc_low))
        keep_mid, away_mid = fold(plan, meta, [keep_mid], [more_mid], halves)
        enc_low, more_down, away_mid, more_dec = hold((enc_low, more_down, away_mid, more_dec))
    enc_low_oth = core(enc_low)

    if direct:
        keep_enc, away_enc = fold(plan, meta, grads_enc[1::2], [more_up, more_down], halves)
        enc_low_oth, away_enc, away_mid = hold((enc_low_oth, away_enc, away_mid))
        more_mid = swap(away_mid, "dp", 4)
        more_enc = swap(away_enc, "dp", 2)
    own, oth, *grads_att = encoder_attention_back(
        plan, meta, enc_own, enc_oth, gains[0], enc_att, kept_enc, enc_low, enc_low_oth
    )
    if direct:
        more_att = swap(grads_att[0], "dp", 1)
        own, oth, more_enc, more_mid = hold((own, oth, more_enc, more_mid))
        keep_enc, away_enc = fold(plan, meta, [keep_enc], [more_enc], halves)
        more_enc = swap(away_enc, "dp", 4)
        own, oth, _ = hold((own, oth, away_enc))
    sums = reduce_own(own, oth)
    if direct:
        keep_att, more_att, _ = hold((grads_att[1], more_att, sums[0]))
        mine, *others = fold(plan, meta, [keep_att], [more_att], apart)
        others, more_enc, keep_mid = hold((others, more_enc, keep_mid))
        pieces_att = [mine] + [swap(item, "dp", 2 * (i + 1)) for i, item in enumerate(others)]
        summed, tiles = collect(plan, meta, [[keep_mid, more_mid], [keep_enc, more_enc], [keep_dec, more_dec]], 2)
        *pieces_att, _ = hold((*pieces_att, tiles))
        *sums, _ = hold((*sums, pieces_att[1]))
        sum_att, tile_att = collect(plan, meta, [pieces_att], 1)
    else:
        parts = [grads_cross[0], grads_self[0], *grads_enc, grads_dec[0]]
        whole_sum = lax.psum_scatter(jnp.concatenate(parts), "dp", scatter_dimension=1, tiled=True)
        summed, tiles = collect(plan, meta, [[whole_sum[None]]], 2)
        whole_sum = lax.psum_scatter(grads_att[0], "dp", scatter_dimension=1, tiled=True)
        sum_att, tile_att = collect(plan, meta, [[whole_sum[None]]], 1)
    grad_enc, gain_zero = norm_back(meta, "norm_back_enc", enc_own, gains[0], grad_enc, *sums, False)
    encoder_in_grad = absolute(grad_enc)[:, :ENC_LEN].reshape(pairs * ENC_LEN, D)
    gain_tile = jnp.concatenate(
        [gain_zero, gain_one, gain_two, gain_three, gain_four, jnp.zeros((3, D), f32)]
    )[None]
    tiles = total(jnp.concatenate([tiles, tile_att, gain_tile]), [("mp", mp_n)])
    if direct:
        sent = tiles.astype(low)
        other = swap(sent, "dp", 1)
        sent, encoder_in_grad = hold((sent, encoder_in_grad))
        tiles = sent.astype(f32) + other.astype(f32)
        for bit in bits(dp_n)[1:]:
            sent = tiles.astype(low)
            tiles = sent.astype(f32) + swap(sent, "dp", bit).astype(f32)
    else:
        tiles = total_dp(tiles)
    done = finish(
        plan,
        meta,
        tiles,
        (
            project_in_rows,
            project_in_cols,
            project_out_rows,
            project_out_cols,
            expand_rows,
            expand_cols,
            contract_rows,
            contract_cols,
        ),
        (norm_gains, norm_gains_square, norm_gains_moment, norm_gains_average),
    )
    grad_norm, news, rates, pgain = done[0][0, 0], done[1:9], done[9], done[10:]
    att = update_attention(
        plan,
        meta,
        rates,
        (sum_att, summed),
        *news[:4],
        (project_in, project_in_moment, project_in_average),
        (project_out, project_out_moment, project_out_average),
    )
    feed = update_feed(
        plan,
        meta,
        rates,
        (summed, summed),
        *news[4:],
        (expand, expand_moment, expand_average),
        (contract, contract_moment, contract_average),
    )
    return (
        decoder_out,
        encoder_in_grad,
        decoder_in_grad,
        grad_norm,
        att[0],
        news[0],
        news[1],
        *att[1:5],
        att[5],
        news[2],
        news[3],
        *att[6:10],
        feed[0],
        news[4],
        news[5],
        *feed[1:5],
        feed[5],
        news[6],
        news[7],
        *feed[6:10],
        *pgain,
    )


def solution(mesh):
    placed = (
        P("dp", None),
        P("dp", None),
        P("dp", None),
        P("dp", None),
        P("dp"),
        P("dp"),
        P(None, None, "dp", "mp"),
        P(),
        P(),
        P(None, None, "dp", "mp"),
        P(None, None, "dp", "mp"),
        P(None, "mp", "dp"),
        P(),
        P(),
        P(None, "mp", "dp"),
        P(None, "mp", "dp"),
        P(None, "dp", "mp"),
        P(),
        P(),
        P(None, "dp", "mp"),
        P(None, "dp", "mp"),
        P(None, "mp", "dp"),
        P(),
        P(),
        P(None, "mp", "dp"),
        P(None, "mp", "dp"),
        P(None, "dp"),
        P(None, "dp"),
        P(None, "dp"),
        P(None, "dp"),
    )
    return jax.shard_map(
        functools.partial(on_device, (mesh.shape["dp"], mesh.shape["mp"])),
        mesh=mesh,
        in_specs=placed,
        out_specs=(
            P("dp", None),
            P("dp", None),
            P("dp", None),
            P(),
            P(None, None, "dp", "mp"),
            P(),
            P(),
            P(None, None, "dp", "mp"),
            P(None, None, "dp", "mp"),
            P(None, None, "dp", "mp"),
            P(None, None, "dp", "mp"),
            P(None, "mp", "dp"),
            P(),
            P(),
            P(None, "mp", "dp"),
            P(None, "mp", "dp"),
            P(None, "mp", "dp"),
            P(None, "mp", "dp"),
            P(None, "dp", "mp"),
            P(),
            P(),
            P(None, "dp", "mp"),
            P(None, "dp", "mp"),
            P(None, "dp", "mp"),
            P(None, "dp", "mp"),
            P(None, "mp", "dp"),
            P(),
            P(),
            P(None, "mp", "dp"),
            P(None, "mp", "dp"),
            P(None, "mp", "dp"),
            P(None, "mp", "dp"),
            P(None, "dp"),
            P(None, "dp"),
            P(None, "dp"),
            P(None, "dp"),
            P(None, "dp"),
            P(None, "dp"),
        ),
        check_vma=False,
    )
```
